32 devices in a mesh: fsdp: 32 (over z, y, x, core).
Axes of the slice: x: 2, y: 2, z: 4, core: 2. Of those that a mesh axis runs over, the one named last changes fastest.
Arguments:
- tok_ids: int32 [32, 128], P('fsdp')
- tok_labels: int32 [32, 128], P('fsdp')
- embed: bfloat16 [32128, 768], P('fsdp')
- w_gate: bfloat16 [768, 3072], P('fsdp')
- w_up: bfloat16 [768, 3072], P('fsdp')
- w_down: bfloat16 [3072, 768], P('fsdp')
- gain_mlp: float32 [768], replicated
- gain_final: float32 [768], replicated
Outputs:
- output 1: float32 [], replicated
- output 2: float32 [32128, 768], P('fsdp')
- output 3: float32 [768, 3072], P('fsdp')
- output 4: float32 [768, 3072], P('fsdp')
- output 5: float32 [3072, 768], P('fsdp')
All inputs are finite; a program needn't handle non-finite values.
Results may differ from the reference program's by a relative error of at most 0.0122675.
Values are sent between devices in bfloat16 or wider.
A program may use at most 1 GiB of HBM per device.

```python
import math
import jax
import jax.numpy as jnp
from jax import lax

VOCAB_SIZE = 32128
MODEL_DIM = 768
FFN_DIM = 3072
GLOBAL_BATCH = 32
SEQ_LEN = 128
NUM_CHUNKS = 32
TOKEN_GROUPS = 32
NORM_EPS = 1e-6
CHUNK_ROWS = VOCAB_SIZE // NUM_CHUNKS
NUM_TOKENS = GLOBAL_BATCH * SEQ_LEN
GROUP_TOKENS = NUM_TOKENS // TOKEN_GROUPS
INV_TOKENS = 1.0 / NUM_TOKENS
EMB_SCALE = math.sqrt(MODEL_DIM)


def setup_inputs(seed: int = 0) -> dict:
    base_key = jax.random.key(seed)
    sub_keys = jax.random.split(base_key, 8)
    tok_ids = jax.random.randint(sub_keys[0], (GLOBAL_BATCH, SEQ_LEN), 0, VOCAB_SIZE, dtype=jnp.int32)
    tok_ids = tok_ids.at[0, 0].set(0).at[GLOBAL_BATCH - 1, SEQ_LEN - 1].set(VOCAB_SIZE - 1)
    tok_labels = jax.random.randint(sub_keys[1], (GLOBAL_BATCH, SEQ_LEN), 0, VOCAB_SIZE, dtype=jnp.int32)
    tok_labels = tok_labels.at[0, 0].set(VOCAB_SIZE - 1).at[GLOBAL_BATCH - 1, SEQ_LEN - 1].set(0)
    embed = (jax.random.normal(sub_keys[2], (VOCAB_SIZE, MODEL_DIM), jnp.float32) * MODEL_DIM ** -0.5).astype(jnp.bfloat16)
    w_gate = (jax.random.normal(sub_keys[3], (MODEL_DIM, FFN_DIM), jnp.float32) * MODEL_DIM ** -0.5).astype(jnp.bfloat16)
    w_up = (jax.random.normal(sub_keys[4], (MODEL_DIM, FFN_DIM), jnp.float32) * MODEL_DIM ** -0.5).astype(jnp.bfloat16)
    w_down = (jax.random.normal(sub_keys[5], (FFN_DIM, MODEL_DIM), jnp.float32) * (2.0 * FFN_DIM ** -0.5)).astype(jnp.bfloat16)
    gain_mlp = jax.random.uniform(sub_keys[6], (MODEL_DIM,), jnp.float32, 0.5, 1.5)
    gain_final = jax.random.uniform(sub_keys[7], (MODEL_DIM,), jnp.float32, 1.0, 2.5)
    return dict(tok_ids=tok_ids, tok_labels=tok_labels, embed=embed, w_gate=w_gate, w_up=w_up, w_down=w_down, gain_mlp=gain_mlp, gain_final=gain_final)


def rms_apply(values, gain_vec):
    inv_rms = lax.rsqrt(jnp.mean(values * values, axis=-1, keepdims=True) + NORM_EPS)
    return (values * inv_rms * gain_vec).astype(jnp.bfloat16), inv_rms


def rms_backward(values, inv_rms, gain_vec, grad_out):
    scaled = grad_out * gain_vec
    return inv_rms * scaled - values * (inv_rms ** 3) * jnp.mean(scaled * values, axis=-1, keepdims=True)


def group_grads(ids_grp, lab_grp, d_emb_acc, embed, w_gate, w_up, w_down, gain_mlp, gain_final):
    x_emb = embed[ids_grp].astype(jnp.float32) * EMB_SCALE
    normed, inv_first = rms_apply(x_emb, gain_mlp)
    gate = jnp.dot(normed, w_gate, preferred_element_type=jnp.float32).astype(jnp.bfloat16)
    up_val = jnp.dot(normed, w_up, preferred_element_type=jnp.float32).astype(jnp.bfloat16)
    gate32 = gate.astype(jnp.float32)
    up32 = up_val.astype(jnp.float32)
    hidden_act = (jax.nn.silu(gate32) * up32).astype(jnp.bfloat16)
    mlp_out = jnp.dot(hidden_act, w_down, preferred_element_type=jnp.float32).astype(jnp.bfloat16)
    hid32 = (x_emb + mlp_out.astype(jnp.float32)).astype(jnp.bfloat16).astype(jnp.float32)
    hid_norm, inv_final = rms_apply(hid32, gain_final)
    emb_chunks = embed.reshape(NUM_CHUNKS, CHUNK_ROWS, MODEL_DIM)
    chunk_index = jnp.arange(NUM_CHUNKS, dtype=jnp.int32)
    col_ids = jnp.arange(CHUNK_ROWS, dtype=jnp.int32)

    def chunk_logits(chunk_emb, chunk_idx):
        logits = jnp.dot(hid_norm, chunk_emb.T, preferred_element_type=jnp.float32)
        label_hit = (lab_grp - chunk_idx * CHUNK_ROWS)[:, None] == col_ids[None, :]
        return logits, label_hit

    def fwd_step(carry, chunk_in):
        run_max, run_sum, lab_logit = carry
        logits, label_hit = chunk_logits(chunk_in[0], chunk_in[1])
        new_max = jnp.maximum(run_max, jnp.max(logits, axis=1))
        run_sum = run_sum * jnp.exp(run_max - new_max) + jnp.sum(jnp.exp(logits - new_max[:, None]), axis=1)
        lab_logit = lab_logit + jnp.sum(jnp.where(label_hit, logits, 0.0), axis=1)
        return (new_max, run_sum, lab_logit), None

    zero_tok = jnp.zeros((GROUP_TOKENS,), jnp.float32)
    start_fwd = (jnp.full((GROUP_TOKENS,), -jnp.inf, jnp.float32), zero_tok, zero_tok)
    (run_max, run_sum, lab_logit), unused_fwd = lax.scan(fwd_step, start_fwd, (emb_chunks, chunk_index))
    log_norm = run_max + jnp.log(run_sum)
    loss_part = jnp.sum(log_norm - lab_logit)

    def bwd_step(carry, chunk_in):
        d_hid, d_rows = carry
        logits, label_hit = chunk_logits(chunk_in[0], chunk_in[1])
        prob_mat = jnp.exp(logits - log_norm[:, None])
        grad_logits = ((prob_mat - label_hit.astype(jnp.float32)) * INV_TOKENS).astype(jnp.bfloat16)
        d_rows = d_rows.at[chunk_in[1]].add(jnp.dot(grad_logits.T, hid_norm, preferred_element_type=jnp.float32))
        d_hid = d_hid + jnp.dot(grad_logits, chunk_in[0], preferred_element_type=jnp.float32)
        return (d_hid, d_rows), None

    start_bwd = (jnp.zeros((GROUP_TOKENS, MODEL_DIM), jnp.float32), d_emb_acc.reshape(NUM_CHUNKS, CHUNK_ROWS, MODEL_DIM))
    (d_hid, d_rows), unused_bwd = lax.scan(bwd_step, start_bwd, (emb_chunks, chunk_index))
    d_hidden = rms_backward(hid32, inv_final, gain_final, d_hid)
    d_mlp = d_hidden.astype(jnp.bfloat16)
    d_down = jnp.dot(hidden_act.T, d_mlp, preferred_element_type=jnp.float32)
    d_act = jnp.dot(d_mlp, w_down.T, preferred_element_type=jnp.float32)
    gate_sig = jax.nn.sigmoid(gate32)
    d_gate_pre = (d_act * up32 * gate_sig * (1.0 + gate32 * (1.0 - gate_sig))).astype(jnp.bfloat16)
    d_up_pre = (d_act * gate32 * gate_sig).astype(jnp.bfloat16)
    d_gate = jnp.dot(normed.T, d_gate_pre, preferred_element_type=jnp.float32)
    d_up = jnp.dot(normed.T, d_up_pre, preferred_element_type=jnp.float32)
    d_normed = jnp.dot(d_gate_pre, w_gate.T, preferred_element_type=jnp.float32) + jnp.dot(d_up_pre, w_up.T, preferred_element_type=jnp.float32)
    d_x = (d_hidden + rms_backward(x_emb, inv_first, gain_mlp, d_normed)).astype(jnp.bfloat16)
    d_emb_new = d_rows.reshape(VOCAB_SIZE, MODEL_DIM).at[ids_grp].add(d_x.astype(jnp.float32) * EMB_SCALE)
    return loss_part, d_emb_new, d_gate, d_up, d_down


def reference(tok_ids, tok_labels, embed, w_gate, w_up, w_down, gain_mlp, gain_final):
    ids_groups = tok_ids.reshape(TOKEN_GROUPS, GROUP_TOKENS)
    lab_groups = tok_labels.reshape(TOKEN_GROUPS, GROUP_TOKENS)

    def group_step(carry, group_in):
        loss_acc, d_emb_acc, gate_acc, up_acc, down_acc = carry
        loss_part, d_emb_acc, d_gate, d_up, d_down = group_grads(group_in[0], group_in[1], d_emb_acc, embed, w_gate, w_up, w_down, gain_mlp, gain_final)
        return (loss_acc + loss_part, d_emb_acc, gate_acc + d_gate, up_acc + d_up, down_acc + d_down), None

    start = (jnp.zeros((), jnp.float32), jnp.zeros((VOCAB_SIZE, MODEL_DIM), jnp.float32), jnp.zeros((MODEL_DIM, FFN_DIM), jnp.float32), jnp.zeros((MODEL_DIM, FFN_DIM), jnp.float32), jnp.zeros((FFN_DIM, MODEL_DIM), jnp.float32))
    totals, unused = lax.scan(group_step, start, (ids_groups, lab_groups))
    return (totals[0] * INV_TOKENS, totals[1], totals[2], totals[3], totals[4])
```

```python
import math
import jax
import jax.numpy as jnp
from jax import lax
from jax.experimental import pallas as pl
from jax.experimental.pallas import tpu as pltpu
from jax.sharding import PartitionSpec as P

NORM_EPS = 1e-6
MESH = pl.DeviceIdType.MESH
F32 = jnp.float32
BF16 = jnp.bfloat16
VMEM_CAP = 63 * 1024 * 1024
LANE = 128
DIM = 768
WIDE = 1536
PIECE = 288
GUROWS = 192
TWICE = 256
PAIR = 48
NDEV = 32
VPAD = 1024
VROWS = 1004
VSPEC = pl.BlockSpec(memory_space=pltpu.VMEM)


def my_place():
    me = lax.axis_index('fsdp')
    core = lax.rem(me, 2)
    x = lax.rem(lax.div(me, 2), 2)
    y = lax.rem(lax.div(me, 4), 2)
    z = lax.div(me, 8)
    p = x * (1 - core) + y * core
    q = y * (1 - core) + x * core
    return me, z, p, q, core


def chip_of(z, p, q, core):
    x = p * (1 - core) + q * core
    y = q * (1 - core) + p * core
    return (z * 2 + y) * 2 + x


def device_of(z, p, q, core):
    return chip_of(z, p, q, core) * 2 + core


def barrier_neighbours(place):
    me, z, p, q, core = place
    sem = pltpu.get_barrier_semaphore()
    for dev in (device_of(z, 1 - p, q, core), device_of(z, p, 1 - q, core), device_of(z, p, q, core) + 1 - 2 * core):
        pl.semaphore_signal(sem, inc=1, device_id=(dev,), device_id_type=MESH)

    @pl.when(z > 0)
    def _():
        pl.semaphore_signal(sem, inc=1, device_id=(me - 8,), device_id_type=MESH)

    @pl.when(z < 3)
    def _():
        pl.semaphore_signal(sem, inc=1, device_id=(me + 8,), device_id_type=MESH)

    at_end = jnp.logical_or(z == 0, z == 3)

    @pl.when(at_end)
    def _():
        pl.semaphore_wait(sem, 4)

    @pl.when(jnp.logical_not(at_end))
    def _():
        pl.semaphore_wait(sem, 5)


def when_level(z, step, body):
    if step == 0:
        body()
    elif step > 0:
        pl.when(z + step < 4)(body)
    else:
        pl.when(z + step >= 0)(body)


def gather_blocks(in_ref, out_ref, send_sem, recv_sem, place, on_block=None):
    me, z, p, q, core = place
    peers = (me + 8, me - 8, device_of(z, 1 - p, q, core), device_of(z, p, 1 - q, core), me + 1 - 2 * core)

    def desc(block, way):
        src = out_ref.at[block]
        return pltpu.make_async_remote_copy(
            src_ref=src, dst_ref=out_ref.at[block], send_sem=send_sem.at[way, block], recv_sem=recv_sem.at[block],
            device_id=(peers[way],), device_id_type=MESH)

    def desc_own(way):
        return pltpu.make_async_remote_copy(
            src_ref=in_ref, dst_ref=out_ref.at[me], send_sem=send_sem.at[way, me], recv_sem=recv_sem.at[me],
            device_id=(peers[way],), device_id_type=MESH)

    pl.when(z < 3)(lambda: desc_own(0).start())
    pl.when(z > 0)(lambda: desc_own(1).start())
    for way in (3, 2, 4):
        desc_own(way).start()
    out_ref[me] = in_ref[...]
    if on_block is not None:
        on_block(me)

    def got(block):
        desc(block, 4).wait_recv()

    def take_z(step):
        def body():
            block = me + 8 * step
            got(block)
            if step < 0:
                pl.when(z < 3)(lambda: desc(block, 0).start())
            else:
                pl.when(z > 0)(lambda: desc(block, 1).start())
            for way in (3, 2, 4):
                desc(block, way).start()
            if on_block is not None:
                on_block(block)
        when_level(z, step, body)

    def take_p(step):
        def body():
            block = device_of(z + step, 1 - p, q, core)
            got(block)
            for way in (3, 4):
                desc(block, way).start()
            if on_block is not None:
                on_block(block)
        when_level(z, step, body)

    def take_q(step, mid):
        def body():
            block = device_of(z + step, mid, 1 - q, core)
            got(block)
            desc(block, 4).start()
            if on_block is not None:
                on_block(block)
        when_level(z, step, body)

    for far in range(6):
        for step in ((far + 1, -far - 1) if far < 3 else ()):
            take_z(step)
        for step in ((far, -far) if far else (0,)) if far < 4 else ():
            take_p(step)
        for step in ((far, -far) if far else (0,)) if far < 4 else ():
            take_q(step, p)
        if far >= 1:
            near = far - 1
            for step in ((near, -near) if near else (0,)) if near < 4 else ():
                take_q(step, 1 - p)

    for chip in range(16):
        block = chip * 2 + 1 - core
        got(block)
        if on_block is not None:
            on_block(block)
    for level in range(4):
        desc(device_of(level, p, q, core), 2).wait_send()
        for mid in range(2):
            desc(device_of(level, mid, q, core), 3).wait_send()
        pl.when(jnp.logical_and(z < 3, level <= z))(lambda: desc(device_of(level, p, q, core), 0).wait_send())
        pl.when(jnp.logical_and(z > 0, level >= z))(lambda: desc(device_of(level, p, q, core), 1).wait_send())
    for chip in range(16):
        desc(chip * 2 + core, 4).wait_send()


def gather_call(block, cid):
    rows, cols = block.shape

    def kernel(in_ref, out_ref, send_sem, recv_sem):
        place = my_place()
        barrier_neighbours(place)
        gather_blocks(in_ref, out_ref, send_sem, recv_sem, place)

    return pl.pallas_call(
        kernel,
        out_shape=jax.ShapeDtypeStruct((NDEV, rows, cols), block.dtype),
        in_specs=[VSPEC], out_specs=VSPEC,
        scratch_shapes=[pltpu.SemaphoreType.DMA((5, NDEV)), pltpu.SemaphoreType.DMA((NDEV,))],
        compiler_params=pltpu.CompilerParams(collective_id=cid, has_side_effects=True, vmem_limit_bytes=VMEM_CAP),
        name='gather%d' % cid,
    )(block)


def add_into(dst, srcs, rows):
    step = 32

    def body(i, carry):
        sl = pl.ds(pl.multiple_of(i * step, step), step)
        total = srcs[0][sl, :].astype(F32)
        for src in srcs[1:]:
            total = total + src[sl, :].astype(F32)
        dst[sl, :] = total.astype(dst.dtype)
        return carry

    lax.fori_loop(0, rows // step, body, 0)


def scatter_scratch(rows, cols):
    return [
        pltpu.VMEM((16, rows, cols), BF16), pltpu.VMEM((8, rows, cols), BF16), pltpu.VMEM((4, rows, cols), BF16),
        pltpu.VMEM((4, rows, cols), BF16), pltpu.VMEM((4, rows, cols), BF16), pltpu.VMEM((16, rows, cols), BF16),
        pltpu.VMEM((rows, cols), F32),
        pltpu.SemaphoreType.DMA((2, 16)), pltpu.SemaphoreType.DMA((2, 8)), pltpu.SemaphoreType.DMA((2, 4)),
        pltpu.SemaphoreType.DMA((2, 4)), pltpu.SemaphoreType.DMA((2, 4)),
    ]


def scatter_blocks(in_ref, out_ref, scratch, place):
    from_core, from_q, from_p, from_low, from_high, outgo, acc, sem_c, sem_q, sem_p, sem_up, sem_dn = scratch
    me, z, p, q, core = place
    rows = out_ref.shape[0]

    def copy(src, dst, sems, slot, dev):
        return pltpu.make_async_remote_copy(
            src_ref=src, dst_ref=dst, send_sem=sems.at[0, slot], recv_sem=sems.at[1, slot],
            device_id=(dev,), device_id_type=MESH)

    def core_copy(chip):
        return copy(in_ref.at[chip * 2 + 1 - core], from_core.at[chip], sem_c, chip, me + 1 - 2 * core)

    def local(level, mid, last):
        return level * 4 + mid * 2 + last

    def q_copy(level, mid):
        return copy(outgo.at[local(level, mid, 1 - q)], from_q.at[level * 2 + mid], sem_q, level * 2 + mid,
                    device_of(z, p, 1 - q, core))

    def p_copy(level):
        return copy(outgo.at[local(level, 1 - p, q)], from_p.at[level], sem_p, level, device_of(z, 1 - p, q, core))

    def up_copy(level):
        return copy(outgo.at[local(level, p, q)], from_low.at[level], sem_up, level, me + 8)

    def dn_copy(level):
        return copy(outgo.at[local(level, p, q)], from_high.at[level], sem_dn, level, me - 8)

    levels = [lax.rem(z + k, 4) for k in (2, 3, 1, 0)]
    for last in (0, 1):
        for mid in (0, 1):
            for level in levels:
                other = 1 - core
                their_p, their_q = q, p
                mid_d = 1 - their_p if mid == 0 else their_p
                last_d = 1 - their_q if last == 0 else their_q
                core_copy(chip_of(level, mid_d, last_d, other)).start()

    def own(level, mid, last):
        chip = chip_of(level, mid, last, core)
        return [in_ref.at[chip * 2 + core], from_core.at[chip]]

    def wait_core(level, mid, last):
        core_copy(chip_of(level, mid, last, core)).wait_recv()

    for mid in (1 - p, p):
        for level in levels:
            wait_core(level, mid, 1 - q)
            add_into(outgo.at[local(level, mid, 1 - q)], own(level, mid, 1 - q), rows)
            q_copy(level, mid).start()
    for level in levels:
        wait_core(level, 1 - p, q)
        q_copy(level, 1 - p).wait_recv()
        add_into(outgo.at[local(level, 1 - p, q)], own(level, 1 - p, q) + [from_q.at[level * 2 + 1 - p]], rows)
        p_copy(level).start()

    def gather_here(level):
        wait_core(level, p, q)
        q_copy(level, p).wait_recv()
        p_copy(level).wait_recv()
        return own(level, p, q) + [from_q.at[level * 2 + p], from_p.at[level]]

    def send_up(step):
        level = z + step

        @pl.when(level < 4)
        def _():
            add_into(acc, gather_here(level), rows)

            @pl.when(z > 0)
            def _():
                up_copy(level).wait_recv()
                add_into(acc, [acc, from_low.at[level]], rows)
            add_into(outgo.at[local(level, p, q)], [acc], rows)
            up_copy(level).start()

    def send_down(step):
        level = z - step

        @pl.when(level >= 0)
        def _():
            add_into(acc, gather_here(level), rows)

            @pl.when(z < 3)
            def _():
                dn_copy(level).wait_recv()
                add_into(acc, [acc, from_high.at[level]], rows)
            add_into(outgo.at[local(level, p, q)], [acc], rows)
            dn_copy(level).start()

    for step in (3, 2, 1):
        send_up(step)
        send_down(step)
    add_into(out_ref, gather_here(z), rows)

    @pl.when(z > 0)
    def _():
        up_copy(z).wait_recv()
        add_into(out_ref, [out_ref, from_low.at[z]], rows)

    @pl.when(z < 3)
    def _():
        dn_copy(z).wait_recv()
        add_into(out_ref, [out_ref, from_high.at[z]], rows)

    for chip in range(16):
        core_copy(chip).wait_send()
    for level in range(4):
        for mid in range(2):
            q_copy(level, mid).wait_send()
        p_copy(level).wait_send()
        pl.when(level > z)(lambda: up_copy(level).wait_send())
        pl.when(level < z)(lambda: dn_copy(level).wait_send())


def scatter_call(parts, cid):
    _, rows, cols = parts.shape

    def kernel(in_ref, out_ref, *scratch):
        place = my_place()
        barrier_neighbours(place)
        scatter_blocks(in_ref, out_ref, scratch, place)

    return pl.pallas_call(
        kernel,
        out_shape=jax.ShapeDtypeStruct((rows, cols), F32),
        in_specs=[VSPEC], out_specs=VSPEC,
        scratch_shapes=scatter_scratch(rows, cols),
        compiler_params=pltpu.CompilerParams(collective_id=cid, has_side_effects=True, vmem_limit_bytes=VMEM_CAP),
        name='scatter%d' % cid,
    )(parts)


def dot(left, right, ld, rd):
    return lax.dot_general(left, right, (((ld,), (rd,)), ((), ())), preferred_element_type=F32)


TILE = 4
TOKS = TILE * LANE


def id_rows(tok_ref, row, start):
    ids = jnp.concatenate([tok_ref[t, row:row + 1, :] for t in range(TILE)], axis=1) - start
    return jnp.where(jnp.logical_and(ids >= 0, ids < VROWS), ids, -1)


def hits_of(ids):
    return lax.broadcasted_iota(jnp.int32, (VPAD, TOKS), 0) == ids


def shard_start():
    return lax.axis_index('fsdp') * VROWS


TOK_SPEC = pl.BlockSpec((TILE, 8, LANE), lambda i: (i, 0, 0))
ACT_SPEC = pl.BlockSpec((TILE, LANE, DIM), lambda i: (i, 0, 0))
EMB_SPEC = pl.BlockSpec((VPAD, DIM), lambda i: (0, 0))


def lookup_call(toks, emb_pad):
    def kernel(tok_ref, emb_ref, out_ref):
        hit = hits_of(id_rows(tok_ref, 0, shard_start())).astype(F32).astype(BF16)
        out_ref[...] = dot(hit, emb_ref[...], 0, 0).astype(BF16).reshape(TILE, LANE, DIM)

    return pl.pallas_call(
        kernel, grid=(NDEV // TILE,),
        out_shape=jax.ShapeDtypeStruct((NDEV, LANE, DIM), BF16),
        in_specs=[TOK_SPEC, EMB_SPEC], out_specs=ACT_SPEC,
        compiler_params=pltpu.CompilerParams(vmem_limit_bytes=VMEM_CAP),
        cost_estimate=pl.CostEstimate(flops=6400000000, bytes_accessed=8000000, transcendentals=0),
        name='lookup',
    )(toks, emb_pad)


def head_forward_call(toks, emb_pad, hid_all):
    def kernel(tok_ref, emb_ref, hid_ref, out_ref, lab_ref):
        i = pl.program_id(0)
        hid = hid_ref[...].reshape(TOKS, DIM)
        logits = dot(emb_ref[...], hid, 1, 1)
        row = lax.broadcasted_iota(jnp.int32, (VPAD, TOKS), 0)
        real = row < VROWS
        hit = row == id_rows(tok_ref, 1, shard_start())
        lab = jnp.sum(jnp.where(hit, logits, 0.0), axis=0, keepdims=True)
        logits = jnp.where(real, logits, -1e30)
        top = jnp.max(logits, axis=0, keepdims=True)
        total = jnp.sum(jnp.exp(logits - top), axis=0, keepdims=True)
        local = top + jnp.log(total)
        for t in range(TILE):
            out_ref[pl.ds(i * TILE + t, 1), :] = local[:, t * LANE:(t + 1) * LANE]

        @pl.when(i == 0)
        def _():
            lab_ref[...] = jnp.zeros_like(lab_ref)
        part = lab[:, 0:LANE]
        for t in range(1, TILE):
            part = part + lab[:, t * LANE:(t + 1) * LANE]
        lab_ref[0:1, :] = lab_ref[0:1, :] + part

    return pl.pallas_call(
        kernel, grid=(NDEV // TILE,),
        out_shape=(jax.ShapeDtypeStruct((NDEV, LANE), F32), jax.ShapeDtypeStruct((8, LANE), F32)),
        in_specs=[TOK_SPEC, EMB_SPEC, ACT_SPEC],
        out_specs=(pl.BlockSpec((NDEV, LANE), lambda i: (0, 0)), pl.BlockSpec((8, LANE), lambda i: (0, 0))),
        compiler_params=pltpu.CompilerParams(vmem_limit_bytes=VMEM_CAP),
        cost_estimate=pl.CostEstimate(flops=6400000000, bytes_accessed=8000000, transcendentals=4200000),
        name='head_forward',
    )(toks, emb_pad, hid_all)


def head_backward_call(toks, emb_pad, hid_all, stats, inv_count):
    def kernel(tok_ref, emb_ref, hid_ref, stat_ref, dhid_ref, demb_ref, loss_ref, lse_ref):
        i = pl.program_id(0)

        @pl.when(i == 0)
        def _():
            local = stat_ref[:, 0:NDEV, :]
            top = jnp.max(local, axis=0)
            lse = top + jnp.log(jnp.sum(jnp.exp(local - top[None]), axis=0))
            lse_ref[...] = lse
            labs = jnp.sum(jnp.sum(stat_ref[:, NDEV:40, :], axis=0))
            loss_ref[...] = jnp.full((8, LANE), (jnp.sum(lse) - labs) * inv_count, F32)
            demb_ref[...] = jnp.zeros_like(demb_ref)

        hid = hid_ref[...].reshape(TOKS, DIM)
        emb = emb_ref[...]
        logits = dot(emb, hid, 1, 1)
        lse_row = jnp.concatenate([lse_ref[pl.ds(i * TILE + t, 1), :] for t in range(TILE)], axis=1)
        row = lax.broadcasted_iota(jnp.int32, (VPAD, TOKS), 0)
        hit = row == id_rows(tok_ref, 1, shard_start())
        prob = jnp.exp(jnp.where(row < VROWS, logits, -1e30) - lse_row)
        grad = ((prob - jnp.where(hit, 1.0, 0.0)) * inv_count).astype(BF16)
        dhid_ref[...] = dot(grad, emb, 0, 0).astype(BF16).reshape(TILE, LANE, DIM)
        demb_ref[...] += dot(grad, hid, 1, 0)

    return pl.pallas_call(
        kernel, grid=(NDEV // TILE,),
        out_shape=(jax.ShapeDtypeStruct((NDEV, LANE, DIM), BF16), jax.ShapeDtypeStruct((VPAD, DIM), F32),
                   jax.ShapeDtypeStruct((8, LANE), F32)),
        in_specs=[TOK_SPEC, EMB_SPEC, ACT_SPEC, pl.BlockSpec((NDEV, 40, LANE), lambda i: (0, 0, 0))],
        out_specs=(ACT_SPEC, EMB_SPEC, pl.BlockSpec((8, LANE), lambda i: (0, 0))),
        scratch_shapes=[pltpu.VMEM((NDEV, LANE), F32)],
        compiler_params=pltpu.CompilerParams(vmem_limit_bytes=VMEM_CAP),
        cost_estimate=pl.CostEstimate(flops=19300000000, bytes_accessed=17000000, transcendentals=4200000),
        name='head_backward',
    )(toks, emb_pad, hid_all, stats)


def scatter_rows_call(toks, d_head, dx_all, emb_scale):
    steps = NDEV // TILE

    def kernel(tok_ref, head_ref, dx_ref, out_ref, acc_ref):
        i = pl.program_id(0)

        @pl.when(i == 0)
        def _():
            acc_ref[...] = jnp.zeros_like(acc_ref)
        hit = hits_of(id_rows(tok_ref, 0, shard_start())).astype(F32).astype(BF16)
        acc_ref[...] += dot(hit, dx_ref[...].reshape(TOKS, DIM), 1, 0)

        @pl.when(i == steps - 1)
        def _():
            out_ref[...] = head_ref[0:VROWS, :] + acc_ref[0:VROWS, :] * emb_scale

    return pl.pallas_call(
        kernel, grid=(steps,),
        out_shape=jax.ShapeDtypeStruct((VROWS, DIM), F32),
        in_specs=[TOK_SPEC, EMB_SPEC, ACT_SPEC],
        out_specs=pl.BlockSpec((VROWS, DIM), lambda i: (0, 0)),
        scratch_shapes=[pltpu.VMEM((VPAD, DIM), F32)],
        compiler_params=pltpu.CompilerParams(vmem_limit_bytes=VMEM_CAP),
        cost_estimate=pl.CostEstimate(flops=6400000000, bytes_accessed=13000000, transcendentals=0),
        name='scatter_rows',
    )(toks, d_head, dx_all)


def wide_split():
    col = lax.broadcasted_iota(jnp.int32, (1, WIDE), 1)
    dev = lax.shift_right_logical(col * 1366, 16)
    off = col - dev * PAIR
    is_up = off >= 24
    return is_up, dev * 24 + jnp.where(is_up, off - 24, off)


def place_matrix():
    is_up, home = wide_split()
    row = lax.broadcasted_iota(jnp.int32, (DIM, WIDE), 0)
    return is_up, jnp.where(row == home, 1.0, 0.0).astype(BF16)


def rms_inv(values):
    return lax.rsqrt(jnp.mean(values * values, axis=-1, keepdims=True) + NORM_EPS)


def rms_backward(values, inv_rms, gain_vec, grad_out):
    scaled = grad_out * gain_vec
    return inv_rms * scaled - values * (inv_rms ** 3) * jnp.mean(scaled * values, axis=-1, keepdims=True)


def gate_up(wall_ref, j):
    return wall_ref[:, j * PAIR:(j + 1) * PAIR, :].reshape(WIDE, DIM)


def down(wall_ref, j):
    return wall_ref[8 * j:8 * j + 8, GUROWS:PIECE, :].reshape(DIM, DIM)


def both_wide(normed, place, is_up):
    wide = dot(normed, place, 1, 0).astype(BF16)
    zero = jnp.zeros_like(wide)
    return jnp.concatenate([jnp.where(is_up, zero, wide), jnp.where(is_up, wide, zero)], axis=0)


def mlp_forward_call(x_raw, wall, gain_mlp, gain_final, emb_scale):
    def kernel(x_ref, wall_ref, gm_ref, gf_ref, hn_ref, h_ref, gu_ref):
        x = x_ref[...] * emb_scale
        normed = (x * rms_inv(x) * gm_ref[...]).astype(BF16)
        is_up, place = place_matrix()
        wide = both_wide(normed, place, is_up)
        mlp = jnp.zeros((LANE, DIM), F32)
        for j in range(4):
            gu = dot(wide, gate_up(wall_ref, j), 1, 0).astype(BF16)
            gu_ref[j] = gu
            g = gu[0:LANE].astype(F32)
            act = (jax.nn.silu(g) * gu[LANE:TWICE].astype(F32)).astype(BF16)
            mlp = mlp + dot(act, down(wall_ref, j), 1, 0)
        h = (x + mlp.astype(BF16).astype(F32)).astype(BF16)
        h_ref[...] = h
        h32 = h.astype(F32)
        hn_ref[...] = (h32 * rms_inv(h32) * gf_ref[...]).astype(BF16)

    return pl.pallas_call(
        kernel,
        out_shape=(jax.ShapeDtypeStruct((LANE, DIM), BF16), jax.ShapeDtypeStruct((LANE, DIM), BF16),
                   jax.ShapeDtypeStruct((4, TWICE, DIM), BF16)),
        in_specs=[VSPEC] * 4, out_specs=(VSPEC,) * 3,
        compiler_params=pltpu.CompilerParams(vmem_limit_bytes=VMEM_CAP),
        cost_estimate=pl.CostEstimate(flops=3000000000, bytes_accessed=15000000, transcendentals=400000),
        name='mlp_forward',
    )(x_raw, wall, gain_mlp, gain_final)


def mlp_backward_call(dhn, x_raw, h, gu_all, wall, gain_mlp, gain_final, emb_scale):
    def kernel(dhn_ref, x_ref, h_ref, gu_ref, wall_ref, gm_ref, gf_ref, dx_ref, grad_ref):
        x = x_ref[...] * emb_scale
        inv_x = rms_inv(x)
        normed = (x * inv_x * gm_ref[...]).astype(BF16)
        is_up, place = place_matrix()
        wide = both_wide(normed, place, is_up)
        h32 = h_ref[...].astype(F32)
        dh = rms_backward(h32, rms_inv(h32), gf_ref[...], dhn_ref[...])
        dm = dh.astype(BF16)
        dwide = jnp.zeros((TWICE, WIDE), F32)
        for j in range(4):
            gu = gu_ref[j]
            g = gu[0:LANE].astype(F32)
            u = gu[LANE:TWICE].astype(F32)
            act = (jax.nn.silu(g) * u).astype(BF16)
            wd = down(wall_ref, j)
            grad_ref[8 * j:8 * j + 8, GUROWS:PIECE, :] = dot(act, dm, 0, 0).astype(BF16).reshape(8, 96, DIM)
            dq = dot(dm, wd, 1, 1)
            sig = jax.nn.sigmoid(g)
            dg = (dq * u * sig * (1.0 + g * (1.0 - sig))).astype(BF16)
            du = (dq * g * sig).astype(BF16)
            dgu = jnp.concatenate([dg, du], axis=0)
            grad_ref[:, j * PAIR:(j + 1) * PAIR, :] = dot(wide, dgu, 0, 0).astype(BF16).reshape(NDEV, PAIR, DIM)
            dwide = dwide + dot(dgu, gate_up(wall_ref, j), 1, 1)
        dsel = jnp.where(is_up, dwide[LANE:TWICE], dwide[0:LANE])
        hi = dsel.astype(BF16)
        rest = dsel - hi.astype(F32)
        mid = rest.astype(BF16)
        low = (rest - mid.astype(F32)).astype(BF16)
        back = dot(jnp.concatenate([hi, mid, low], axis=0), place, 1, 1)
        da = back[0:LANE] + back[LANE:TWICE] + back[TWICE:384]
        dx_ref[...] = (dh + rms_backward(x, inv_x, gm_ref[...], da)).astype(BF16)

    return pl.pallas_call(
        kernel,
        out_shape=(jax.ShapeDtypeStruct((LANE, DIM), BF16), jax.ShapeDtypeStruct((NDEV, PIECE, DIM), BF16)),
        in_specs=[VSPEC] * 7, out_specs=(VSPEC,) * 2,
        compiler_params=pltpu.CompilerParams(vmem_limit_bytes=VMEM_CAP),
        cost_estimate=pl.CostEstimate(flops=9000000000, bytes_accessed=30000000, transcendentals=800000),
        name='mlp_backward',
    )(dhn, x_raw, h, gu_all, wall, gain_mlp, gain_final)


def solution(mesh):
    group = mesh.shape['fsdp']

    def local_step(ids_blk, lab_blk, emb_shard, gate_shard, up_shard, down_shard, gain_mlp, gain_final):
        model_dim = emb_shard.shape[1]
        emb_scale = math.sqrt(model_dim)
        inv_count = 1.0 / (ids_blk.size * group)
        gm, gf = gain_mlp.reshape(1, -1), gain_final.reshape(1, -1)
        emb_pad = jnp.pad(emb_shard, ((0, VPAD - VROWS), (0, 0)))
        tok_blk = jnp.concatenate([ids_blk, lab_blk, jnp.zeros((6, LANE), jnp.int32)], axis=0)
        gu = jnp.concatenate([gate_shard, up_shard], axis=0).reshape(PAIR, 4, DIM).transpose(1, 0, 2).reshape(GUROWS, DIM)
        wall = gather_call(jnp.concatenate([gu, down_shard], axis=0), 0)
        toks = gather_call(tok_blk, 1)
        x_raw = scatter_call(lookup_call(toks, emb_pad), 2)
        hid_norm, h, gu_all = mlp_forward_call(x_raw, wall, gm, gf, emb_scale)
        hid_all = gather_call(hid_norm, 3)
        local_lse, lab_part = head_forward_call(toks, emb_pad, hid_all)
        stats = gather_call(jnp.concatenate([local_lse, lab_part], axis=0), 4)
        d_hid, d_head, loss = head_backward_call(toks, emb_pad, hid_all, stats, inv_count)
        dhn = scatter_call(d_hid, 5)
        d_x, w_grads = mlp_backward_call(dhn, x_raw, h, gu_all, wall, gm, gf, emb_scale)
        mine = scatter_call(w_grads, 6)
        dx_all = gather_call(d_x, 7)
        d_embed = scatter_rows_call(toks, d_head, dx_all, emb_scale)
        dgu = mine[0:GUROWS].reshape(4, PAIR, DIM).transpose(1, 0, 2).reshape(PAIR, 3072)
        return loss[0, 0], d_embed, dgu[0:24], dgu[24:PAIR], mine[GUROWS:PIECE]

    shard_spec = P('fsdp', None)
    return jax.shard_map(local_step, mesh=mesh, in_specs=(shard_spec, shard_spec, shard_spec, shard_spec, shard_spec, shard_spec, P(), P()), out_specs=(P(), shard_spec, shard_spec, shard_spec, shard_spec), check_vma=False)
```

```python
import math
import jax
import jax.numpy as jnp
from jax import lax
from jax.experimental import pallas as pl
from jax.experimental.pallas import tpu as pltpu
from jax.sharding import PartitionSpec as P

NORM_EPS = 1e-6
MESH = pl.DeviceIdType.MESH
F32 = jnp.float32
BF16 = jnp.bfloat16
VMEM_CAP = 63 * 1024 * 1024
LANE = 128
DIM = 768
PAIR = 48
UNITS = 384
NDEV = 32
VPAD = 1024
VROWS = 1004
LEVEL = 8
HEIGHT = 4
DROWS = 96
CHIPS = 16
GROWS = 24
TWO = 2
TOP = 3
VSPEC = pl.BlockSpec(memory_space=pltpu.VMEM)


def my_place():
    me = lax.axis_index('fsdp')
    core = lax.rem(me, TWO)
    x = lax.rem(lax.div(me, TWO), TWO)
    y = lax.rem(lax.div(me, HEIGHT), TWO)
    z = lax.div(me, LEVEL)
    p = x * (1 - core) + y * core
    q = y * (1 - core) + x * core
    return me, z, p, q, core


def chip_of(z, p, q, core):
    x = p * (1 - core) + q * core
    y = q * (1 - core) + p * core
    return (z * TWO + y) * TWO + x


def device_of(z, p, q, core):
    return chip_of(z, p, q, core) * TWO + core


def barrier_neighbours(place):
    me, z, p, q, core = place
    sem = pltpu.get_barrier_semaphore()
    for step in range(1, LEVEL):
        dev = z * LEVEL + lax.rem(me + step, LEVEL)
        pl.semaphore_signal(sem, inc=1, device_id=(dev,), device_id_type=MESH)

    @pl.when(z > 0)
    def _():
        pl.semaphore_signal(sem, inc=1, device_id=(me - LEVEL,), device_id_type=MESH)

    @pl.when(z < TOP)
    def _():
        pl.semaphore_signal(sem, inc=1, device_id=(me + LEVEL,), device_id_type=MESH)

    at_end = jnp.logical_or(z == 0, z == TOP)

    @pl.when(at_end)
    def _():
        pl.semaphore_wait(sem, LEVEL)

    @pl.when(jnp.logical_not(at_end))
    def _():
        pl.semaphore_wait(sem, 9)


def when_level(z, step, body):
    if step == 0:
        body()
    elif step > 0:
        pl.when(z + step < HEIGHT)(body)
    else:
        pl.when(z + step >= 0)(body)


def gather_blocks(in_ref, out_ref, send_sem, recv_sem, place, on_block=None):
    me, z, p, q, core = place
    peers = (me + LEVEL, me - LEVEL, device_of(z, 1 - p, q, core), device_of(z, p, 1 - q, core), me + 1 - TWO * core)

    def desc(block, way):
        src = out_ref.at[block]
        return pltpu.make_async_remote_copy(
            src_ref=src, dst_ref=out_ref.at[block], send_sem=send_sem.at[way, block], recv_sem=recv_sem.at[block],
            device_id=(peers[way],), device_id_type=MESH)

    def desc_own(way):
        return pltpu.make_async_remote_copy(
            src_ref=in_ref, dst_ref=out_ref.at[me], send_sem=send_sem.at[way, me], recv_sem=recv_sem.at[me],
            device_id=(peers[way],), device_id_type=MESH)

    pl.when(z < TOP)(lambda: desc_own(0).start())
    pl.when(z > 0)(lambda: desc_own(1).start())
    for way in (TOP, TWO, HEIGHT):
        desc_own(way).start()
    out_ref[me] = in_ref[...]
    if on_block is not None:
        on_block(me)

    def got(block):
        desc(block, HEIGHT).wait_recv()

    def take_z(step):
        def body():
            block = me + LEVEL * step
            got(block)
            if step < 0:
                pl.when(z < TOP)(lambda: desc(block, 0).start())
            else:
                pl.when(z > 0)(lambda: desc(block, 1).start())
            for way in (TOP, TWO, HEIGHT):
                desc(block, way).start()
            if on_block is not None:
                on_block(block)
        when_level(z, step, body)

    def take_p(step):
        def body():
            block = device_of(z + step, 1 - p, q, core)
            got(block)
            for way in (TOP, HEIGHT):
                desc(block, way).start()
            if on_block is not None:
                on_block(block)
        when_level(z, step, body)

    def take_q(step, mid):
        def body():
            block = device_of(z + step, mid, 1 - q, core)
            got(block)
            desc(block, HEIGHT).start()
            if on_block is not None:
                on_block(block)
        when_level(z, step, body)

    for far in range(6):
        for step in ((far + 1, -far - 1) if far < TOP else ()):
            take_z(step)
        for step in ((far, -far) if far else (0,)) if far < HEIGHT else ():
            take_p(step)
        for step in ((far, -far) if far else (0,)) if far < HEIGHT else ():
            take_q(step, p)
        if far >= 1:
            near = far - 1
            for step in ((near, -near) if near else (0,)) if near < HEIGHT else ():
                take_q(step, 1 - p)

    for chip in range(CHIPS):
        block = chip * TWO + 1 - core
        got(block)
        if on_block is not None:
            on_block(block)
    for level in range(HEIGHT):
        desc(device_of(level, p, q, core), TWO).wait_send()
        for mid in range(TWO):
            desc(device_of(level, mid, q, core), TOP).wait_send()
        pl.when(jnp.logical_and(z < TOP, level <= z))(lambda: desc(device_of(level, p, q, core), 0).wait_send())
        pl.when(jnp.logical_and(z > 0, level >= z))(lambda: desc(device_of(level, p, q, core), 1).wait_send())
    for chip in range(CHIPS):
        desc(chip * TWO + core, HEIGHT).wait_send()


def gather_call(block, cid):
    rows, cols = block.shape

    def kernel(in_ref, out_ref, send_sem, recv_sem):
        place = my_place()
        barrier_neighbours(place)
        gather_blocks(in_ref, out_ref, send_sem, recv_sem, place)

    return pl.pallas_call(
        kernel,
        out_shape=jax.ShapeDtypeStruct((NDEV, rows, cols), block.dtype),
        in_specs=[VSPEC], out_specs=VSPEC,
        scratch_shapes=[pltpu.SemaphoreType.DMA((5, NDEV)), pltpu.SemaphoreType.DMA((NDEV,))],
        compiler_params=pltpu.CompilerParams(collective_id=cid, has_side_effects=True, vmem_limit_bytes=VMEM_CAP),
        name='gather%d' % cid,
    )(block)


def add_into(dst, srcs, rows):
    step = 32

    def body(i, carry):
        sl = pl.ds(pl.multiple_of(i * step, step), step)
        total = srcs[0][sl, :].astype(F32)
        for src in srcs[1:]:
            total = total + src[sl, :].astype(F32)
        dst[sl, :] = total.astype(dst.dtype)
        return carry

    lax.fori_loop(0, rows // step, body, 0)


def scatter_scratch(rows, cols):
    return [
        pltpu.VMEM((CHIPS, rows, cols), BF16), pltpu.VMEM((LEVEL, rows, cols), BF16), pltpu.VMEM((HEIGHT, rows, cols), BF16),
        pltpu.VMEM((HEIGHT, rows, cols), BF16), pltpu.VMEM((HEIGHT, rows, cols), BF16), pltpu.VMEM((CHIPS, rows, cols), BF16),
        pltpu.VMEM((rows, cols), F32),
        pltpu.SemaphoreType.DMA((TWO, CHIPS)), pltpu.SemaphoreType.DMA((TWO, LEVEL)), pltpu.SemaphoreType.DMA((TWO, HEIGHT)),
        pltpu.SemaphoreType.DMA((TWO, HEIGHT)), pltpu.SemaphoreType.DMA((TWO, HEIGHT)),
    ]


def far_first(z):
    half = lax.div(z, TWO)
    inner = lax.rem(z + half, TWO)
    return (TOP - TOP * half, (1 - inner) * (TWO - half) + inner * TOP * half, 1 + lax.rem(z, TWO), z)


def scatter_blocks(in_ref, out_ref, scratch, place):
    from_core, from_q, from_p, from_low, from_high, outgo, acc, sem_c, sem_q, sem_p, sem_up, sem_dn = scratch
    me, z, p, q, core = place
    rows = out_ref.shape[0]

    def copy(src, dst, sems, slot, dev):
        return pltpu.make_async_remote_copy(
            src_ref=src, dst_ref=dst, send_sem=sems.at[0, slot], recv_sem=sems.at[1, slot],
            device_id=(dev,), device_id_type=MESH)

    def core_copy(chip):
        return copy(in_ref.at[chip * TWO + 1 - core], from_core.at[chip], sem_c, chip, me + 1 - TWO * core)

    def local(level, mid, last):
        return level * HEIGHT + mid * TWO + last

    def q_copy(level, mid):
        return copy(outgo.at[local(level, mid, 1 - q)], from_q.at[level * TWO + mid], sem_q, level * TWO + mid,
                    device_of(z, p, 1 - q, core))

    def p_copy(level):
        return copy(outgo.at[local(level, 1 - p, q)], from_p.at[level], sem_p, level, device_of(z, 1 - p, q, core))

    def up_copy(level):
        return copy(outgo.at[local(level, p, q)], from_low.at[level], sem_up, level, me + LEVEL)

    def dn_copy(level):
        return copy(outgo.at[local(level, p, q)], from_high.at[level], sem_dn, level, me - LEVEL)

    levels = far_first(z)
    other = 1 - core
    for level in levels:
        for last in (1 - p, p):
            for mid in (1 - q, q):
                core_copy(chip_of(level, mid, last, other)).start()

    def own(level, mid, last):
        chip = chip_of(level, mid, last, core)
        return [in_ref.at[chip * TWO + core], from_core.at[chip]]

    def wait_core(level, mid, last):
        core_copy(chip_of(level, mid, last, core)).wait_recv()

    for level in levels:
        for mid in (1 - p, p):
            wait_core(level, mid, 1 - q)
            add_into(outgo.at[local(level, mid, 1 - q)], own(level, mid, 1 - q), rows)
            q_copy(level, mid).start()

    def send_p(level):
        wait_core(level, 1 - p, q)
        q_copy(level, 1 - p).wait_recv()
        add_into(outgo.at[local(level, 1 - p, q)], own(level, 1 - p, q) + [from_q.at[level * TWO + 1 - p]], rows)
        p_copy(level).start()

    def gather_here(level):
        wait_core(level, p, q)
        q_copy(level, p).wait_recv()
        p_copy(level).wait_recv()
        return own(level, p, q) + [from_q.at[level * TWO + p], from_p.at[level]]

    def send_z(level):
        add_into(acc, gather_here(level), rows)

        @pl.when(level > z)
        def _():
            @pl.when(z > 0)
            def _():
                up_copy(level).wait_recv()
                add_into(acc, [acc, from_low.at[level]], rows)
            add_into(outgo.at[local(level, p, q)], [acc], rows)
            up_copy(level).start()

        @pl.when(level < z)
        def _():
            @pl.when(z < TOP)
            def _():
                dn_copy(level).wait_recv()
                add_into(acc, [acc, from_high.at[level]], rows)
            add_into(outgo.at[local(level, p, q)], [acc], rows)
            dn_copy(level).start()

    send_p(levels[0])
    for at in range(TOP):
        send_p(levels[at + 1])
        send_z(levels[at])
    add_into(out_ref, gather_here(z), rows)

    @pl.when(z > 0)
    def _():
        up_copy(z).wait_recv()
        add_into(out_ref, [out_ref, from_low.at[z]], rows)

    @pl.when(z < TOP)
    def _():
        dn_copy(z).wait_recv()
        add_into(out_ref, [out_ref, from_high.at[z]], rows)

    for chip in range(CHIPS):
        core_copy(chip).wait_send()
    for level in range(HEIGHT):
        for mid in range(TWO):
            q_copy(level, mid).wait_send()
        p_copy(level).wait_send()
        pl.when(level > z)(lambda: up_copy(level).wait_send())
        pl.when(level < z)(lambda: dn_copy(level).wait_send())


def scatter_call(parts, cid):
    _, rows, cols = parts.shape

    def kernel(in_ref, out_ref, *scratch):
        place = my_place()
        barrier_neighbours(place)
        scatter_blocks(in_ref, out_ref, scratch, place)

    return pl.pallas_call(
        kernel,
        out_shape=jax.ShapeDtypeStruct((rows, cols), F32),
        in_specs=[VSPEC], out_specs=VSPEC,
        scratch_shapes=scatter_scratch(rows, cols),
        compiler_params=pltpu.CompilerParams(collective_id=cid, has_side_effects=True, vmem_limit_bytes=VMEM_CAP),
        name='scatter%d' % cid,
    )(parts)


def dot(left, right, ld, rd):
    return lax.dot_general(left, right, (((ld,), (rd,)), ((), ())), preferred_element_type=F32)


TILE = HEIGHT
TOKS = TILE * LANE


def id_rows(tok_ref, row, start):
    ids = jnp.concatenate([tok_ref[t, row:row + 1, :] for t in range(TILE)], axis=1) - start
    return jnp.where(jnp.logical_and(ids >= 0, ids < VROWS), ids, -1)


def hits_of(ids):
    return lax.broadcasted_iota(jnp.int32, (VPAD, TOKS), 0) == ids


def shard_start():
    return lax.axis_index('fsdp') * VROWS


TOK_SPEC = pl.BlockSpec((TILE, LEVEL, LANE), lambda i: (i, 0, 0))
ACT_SPEC = pl.BlockSpec((TILE, LANE, DIM), lambda i: (i, 0, 0))
EMB_SPEC = pl.BlockSpec((VPAD, DIM), lambda i: (0, 0))


def lookup_call(toks, emb_pad):
    def kernel(tok_ref, emb_ref, out_ref):
        hit = hits_of(id_rows(tok_ref, 0, shard_start())).astype(F32).astype(BF16)
        out_ref[...] = dot(hit, emb_ref[...], 0, 0).astype(BF16).reshape(TILE, LANE, DIM)

    return pl.pallas_call(
        kernel, grid=(NDEV // TILE,),
        out_shape=jax.ShapeDtypeStruct((NDEV, LANE, DIM), BF16),
        in_specs=[TOK_SPEC, EMB_SPEC], out_specs=ACT_SPEC,
        compiler_params=pltpu.CompilerParams(vmem_limit_bytes=VMEM_CAP),
        cost_estimate=pl.CostEstimate(flops=6400000000, bytes_accessed=8000000, transcendentals=0),
        name='lookup',
    )(toks, emb_pad)


def head_forward_call(toks, emb_pad, hid_all):
    def kernel(tok_ref, emb_ref, hid_ref, out_ref, lab_ref):
        i = pl.program_id(0)
        hid = hid_ref[...].reshape(TOKS, DIM)
        logits = dot(emb_ref[...], hid, 1, 1)
        row = lax.broadcasted_iota(jnp.int32, (VPAD, TOKS), 0)
        real = row < VROWS
        hit = row == id_rows(tok_ref, 1, shard_start())
        lab = jnp.sum(jnp.where(hit, logits, 0.0), axis=0, keepdims=True)
        logits = jnp.where(real, logits, -1e30)
        top = jnp.max(logits, axis=0, keepdims=True)
        total = jnp.sum(jnp.exp(logits - top), axis=0, keepdims=True)
        local = top + jnp.log(total)
        for t in range(TILE):
            out_ref[pl.ds(i * TILE + t, 1), :] = local[:, t * LANE:(t + 1) * LANE]

        @pl.when(i == 0)
        def _():
            lab_ref[...] = jnp.zeros_like(lab_ref)
        part = lab[:, 0:LANE]
        for t in range(1, TILE):
            part = part + lab[:, t * LANE:(t + 1) * LANE]
        lab_ref[0:1, :] = lab_ref[0:1, :] + part

    return pl.pallas_call(
        kernel, grid=(NDEV // TILE,),
        out_shape=(jax.ShapeDtypeStruct((NDEV, LANE), F32), jax.ShapeDtypeStruct((LEVEL, LANE), F32)),
        in_specs=[TOK_SPEC, EMB_SPEC, ACT_SPEC],
        out_specs=(pl.BlockSpec((NDEV, LANE), lambda i: (0, 0)), pl.BlockSpec((LEVEL, LANE), lambda i: (0, 0))),
        compiler_params=pltpu.CompilerParams(vmem_limit_bytes=VMEM_CAP),
        cost_estimate=pl.CostEstimate(flops=6400000000, bytes_accessed=8000000, transcendentals=4200000),
        name='head_forward',
    )(toks, emb_pad, hid_all)


def head_backward_call(toks, emb_pad, hid_all, stats, inv_count):
    def kernel(tok_ref, emb_ref, hid_ref, stat_ref, dhid_ref, demb_ref, loss_ref, lse_ref):
        i = pl.program_id(0)

        @pl.when(i == 0)
        def _():
            local = stat_ref[:, 0:NDEV, :]
            top = jnp.max(local, axis=0)
            lse = top + jnp.log(jnp.sum(jnp.exp(local - top[None]), axis=0))
            lse_ref[...] = lse
            labs = jnp.sum(jnp.sum(stat_ref[:, NDEV:40, :], axis=0))
            loss_ref[...] = jnp.full((LEVEL, LANE), (jnp.sum(lse) - labs) * inv_count, F32)
            demb_ref[...] = jnp.zeros_like(demb_ref)

        hid = hid_ref[...].reshape(TOKS, DIM)
        emb = emb_ref[...]
        logits = dot(emb, hid, 1, 1)
        lse_row = jnp.concatenate([lse_ref[pl.ds(i * TILE + t, 1), :] for t in range(TILE)], axis=1)
        row = lax.broadcasted_iota(jnp.int32, (VPAD, TOKS), 0)
        hit = row == id_rows(tok_ref, 1, shard_start())
        prob = jnp.exp(jnp.where(row < VROWS, logits, -1e30) - lse_row)
        grad = ((prob - jnp.where(hit, 1.0, 0.0)) * inv_count).astype(BF16)
        dhid_ref[...] = dot(grad, emb, 0, 0).astype(BF16).reshape(TILE, LANE, DIM)
        demb_ref[...] += dot(grad, hid, 1, 0)

    return pl.pallas_call(
        kernel, grid=(NDEV // TILE,),
        out_shape=(jax.ShapeDtypeStruct((NDEV, LANE, DIM), BF16), jax.ShapeDtypeStruct((VPAD, DIM), F32),
                   jax.ShapeDtypeStruct((LEVEL, LANE), F32)),
        in_specs=[TOK_SPEC, EMB_SPEC, ACT_SPEC, pl.BlockSpec((NDEV, 40, LANE), lambda i: (0, 0, 0))],
        out_specs=(ACT_SPEC, EMB_SPEC, pl.BlockSpec((LEVEL, LANE), lambda i: (0, 0))),
        scratch_shapes=[pltpu.VMEM((NDEV, LANE), F32)],
        compiler_params=pltpu.CompilerParams(vmem_limit_bytes=VMEM_CAP),
        cost_estimate=pl.CostEstimate(flops=19300000000, bytes_accessed=17000000, transcendentals=4200000),
        name='head_backward',
    )(toks, emb_pad, hid_all, stats)


def scatter_rows_call(toks, d_head, dx_all, emb_scale):
    steps = NDEV // TILE

    def kernel(tok_ref, head_ref, dx_ref, out_ref, acc_ref):
        i = pl.program_id(0)

        @pl.when(i == 0)
        def _():
            acc_ref[...] = jnp.zeros_like(acc_ref)
        hit = hits_of(id_rows(tok_ref, 0, shard_start())).astype(F32).astype(BF16)
        acc_ref[...] += dot(hit, dx_ref[...].reshape(TOKS, DIM), 1, 0)

        @pl.when(i == steps - 1)
        def _():
            out_ref[...] = head_ref[0:VROWS, :] + acc_ref[0:VROWS, :] * emb_scale

    return pl.pallas_call(
        kernel, grid=(steps,),
        out_shape=jax.ShapeDtypeStruct((VROWS, DIM), F32),
        in_specs=[TOK_SPEC, EMB_SPEC, ACT_SPEC],
        out_specs=pl.BlockSpec((VROWS, DIM), lambda i: (0, 0)),
        scratch_shapes=[pltpu.VMEM((VPAD, DIM), F32)],
        compiler_params=pltpu.CompilerParams(vmem_limit_bytes=VMEM_CAP),
        cost_estimate=pl.CostEstimate(flops=6400000000, bytes_accessed=13000000, transcendentals=0),
        name='scatter_rows',
    )(toks, d_head, dx_all)


def rms_inv(values):
    return lax.rsqrt(jnp.mean(values * values, axis=-1, keepdims=True) + NORM_EPS)


def rms_backward(values, inv_rms, gain_vec, grad_out):
    scaled = grad_out * gain_vec
    return inv_rms * scaled - values * (inv_rms ** TOP) * jnp.mean(scaled * values, axis=-1, keepdims=True)


def side_specs(n):
    return [pltpu.SemaphoreType.DMA((n,)), pltpu.SemaphoreType.DMA((n,))]


def weights_call(pieces, down_shard, cid):
    def kernel(piece_ref, down_ref, gu_ref, wd_ref, a_send, a_recv, z_send, z_recv, d_send, d_recv):
        place = my_place()
        me, z, p, q, core = place
        rank = lax.rem(me, LEVEL)
        barrier_neighbours(place)

        def exchange(step):
            peer = lax.rem(rank + step, LEVEL)
            return pltpu.make_async_remote_copy(
                src_ref=piece_ref.at[peer], dst_ref=gu_ref.at[me], send_sem=a_send.at[step], recv_sem=a_recv.at[step],
                device_id=(z * LEVEL + peer,), device_id_type=MESH)

        def slab(level, way):
            part = gu_ref.at[pl.ds(level * LEVEL, LEVEL)]
            return pltpu.make_async_remote_copy(
                src_ref=part, dst_ref=part, send_sem=z_send.at[way * HEIGHT + level], recv_sem=z_recv.at[level],
                device_id=(me + LEVEL - CHIPS * way,), device_id_type=MESH)

        def slab_down(level, way, src):
            return pltpu.make_async_remote_copy(
                src_ref=src, dst_ref=wd_ref.at[level], send_sem=d_send.at[way * HEIGHT + level], recv_sem=d_recv.at[level],
                device_id=(me + LEVEL - CHIPS * way,), device_id_type=MESH)

        for step in range(1, LEVEL):
            exchange(step).start()
        pl.when(z < TOP)(lambda: slab_down(z, 0, down_ref).start())
        pl.when(z > 0)(lambda: slab_down(z, 1, down_ref).start())
        wd_ref[z] = down_ref[...]
        gu_ref[me] = piece_ref[rank]
        for step in range(1, LEVEL):
            exchange(step).wait_recv()
        pl.when(z < TOP)(lambda: slab(z, 0).start())
        pl.when(z > 0)(lambda: slab(z, 1).start())

        def take(level, way, more):
            slab_down(level, 0, wd_ref.at[level]).wait_recv()
            pl.when(more)(lambda: slab_down(level, way, wd_ref.at[level]).start())
            slab(level, 0).wait_recv()
            pl.when(more)(lambda: slab(level, way).start())

        for far in (1, TWO, TOP):
            pl.when(z - far >= 0)(lambda: take(z - far, 0, z < TOP))
            pl.when(z + far < HEIGHT)(lambda: take(z + far, 1, z > 0))
        for step in range(1, LEVEL):
            exchange(step).wait_send()

        def sent(level, way):
            slab(level, way).wait_send()
            slab_down(level, way, wd_ref.at[level]).wait_send()

        for level in range(HEIGHT):
            pl.when(jnp.logical_and(z < TOP, level <= z))(lambda: sent(level, 0))
            pl.when(jnp.logical_and(z > 0, level >= z))(lambda: sent(level, 1))

    return pl.pallas_call(
        kernel,
        out_shape=(jax.ShapeDtypeStruct((NDEV, PAIR, UNITS), BF16), jax.ShapeDtypeStruct((HEIGHT, DROWS, DIM), BF16)),
        in_specs=[VSPEC] * TWO, out_specs=(VSPEC,) * TWO,
        scratch_shapes=side_specs(LEVEL) + [pltpu.SemaphoreType.DMA((LEVEL,)), pltpu.SemaphoreType.DMA((HEIGHT,))] * TWO,
        compiler_params=pltpu.CompilerParams(collective_id=cid, has_side_effects=True, vmem_limit_bytes=VMEM_CAP),
        name='weights',
    )(pieces, down_shard)


def grads_call(gu_parts, down_parts, cid):
    def kernel(gu_ref, gd_ref, out_ref, dn_ref, from_low, from_high, low_d, high_d, outgo, outgo_d, acc, acc_d,
               a_send, a_recv, z_send, z_recv, d_send, d_recv):
        place = my_place()
        me, z, p, q, core = place
        rank = lax.rem(me, LEVEL)
        barrier_neighbours(place)

        def rows_of(ref, level):
            return ref.at[pl.ds(level * LEVEL, LEVEL)]

        def add_slab(dst, srcs):
            def body(i, carry):
                total = srcs[0][i].astype(F32)
                for src in srcs[1:]:
                    total = total + src[i].astype(F32)
                dst[i] = total.astype(dst.dtype)
                return carry
            lax.fori_loop(0, LEVEL, body, 0)

        def hop(level, way):
            land = (from_low, from_high)[way]
            return pltpu.make_async_remote_copy(
                src_ref=rows_of(outgo, level), dst_ref=rows_of(land, level), send_sem=z_send.at[way * HEIGHT + level],
                recv_sem=z_recv.at[way * HEIGHT + level], device_id=(me + LEVEL - CHIPS * way,), device_id_type=MESH)

        def hop_d(level, way):
            land = (low_d, high_d)[way]
            return pltpu.make_async_remote_copy(
                src_ref=outgo_d.at[level], dst_ref=land.at[level], send_sem=d_send.at[way * HEIGHT + level],
                recv_sem=d_recv.at[way * HEIGHT + level], device_id=(me + LEVEL - CHIPS * way,), device_id_type=MESH)

        def send(level, way, more):
            @pl.when(more)
            def _():
                hop(level, way).wait_recv()
                add_slab(rows_of(outgo, level), [rows_of(gu_ref, level), rows_of((from_low, from_high)[way], level)])

            @pl.when(jnp.logical_not(more))
            def _():
                add_slab(rows_of(outgo, level), [rows_of(gu_ref, level)])
            hop(level, way).start()

            @pl.when(more)
            def _():
                hop_d(level, way).wait_recv()
                add_into(outgo_d.at[level], [gd_ref.at[level], (low_d, high_d)[way].at[level]], DROWS)

            @pl.when(jnp.logical_not(more))
            def _():
                add_into(outgo_d.at[level], [gd_ref.at[level]], DROWS)
            hop_d(level, way).start()

        for far in (TOP, TWO, 1):
            pl.when(z + far < HEIGHT)(lambda: send(z + far, 0, z > 0))
            pl.when(z - far >= 0)(lambda: send(z - far, 1, z < TOP))
        add_slab(acc, [rows_of(gu_ref, z)])
        add_into(dn_ref, [gd_ref.at[z]], DROWS)

        def last(way):
            hop(z, way).wait_recv()
            add_slab(acc, [acc, rows_of((from_low, from_high)[way], z)])
            hop_d(z, way).wait_recv()
            add_into(dn_ref, [dn_ref, (low_d, high_d)[way].at[z]], DROWS)

        pl.when(z > 0)(lambda: last(0))
        pl.when(z < TOP)(lambda: last(1))

        def exchange(step):
            peer = lax.rem(rank + step, LEVEL)
            return pltpu.make_async_remote_copy(
                src_ref=acc.at[peer], dst_ref=out_ref.at[rank], send_sem=a_send.at[step], recv_sem=a_recv.at[step],
                device_id=(z * LEVEL + peer,), device_id_type=MESH)

        for step in range(1, LEVEL):
            exchange(step).start()
        out_ref[rank] = acc[rank]
        for step in range(1, LEVEL):
            exchange(step).wait_recv()
        for step in range(1, LEVEL):
            exchange(step).wait_send()

        def sent(level, way):
            hop(level, way).wait_send()
            hop_d(level, way).wait_send()

        for level in range(HEIGHT):
            pl.when(level > z)(lambda: sent(level, 0))
            pl.when(level < z)(lambda: sent(level, 1))

    slab = pltpu.VMEM((NDEV, PAIR, UNITS), BF16)
    slab_d = pltpu.VMEM((HEIGHT, DROWS, DIM), BF16)
    return pl.pallas_call(
        kernel,
        out_shape=(jax.ShapeDtypeStruct((LEVEL, PAIR, UNITS), F32), jax.ShapeDtypeStruct((DROWS, DIM), F32)),
        in_specs=[VSPEC] * TWO, out_specs=(VSPEC,) * TWO,
        scratch_shapes=[slab, slab, slab_d, slab_d, slab, slab_d, pltpu.VMEM((LEVEL, PAIR, UNITS), F32),
                        pltpu.VMEM((DROWS, DIM), F32)] + side_specs(LEVEL) * TOP,
        compiler_params=pltpu.CompilerParams(collective_id=cid, has_side_effects=True, vmem_limit_bytes=VMEM_CAP),
        name='grads',
    )(gu_parts, down_parts)


def rank_of(p, q, core):
    return device_of(0, p, q, core)


def level_gather(in_ref, out_ref, send_sem, recv_sem, place):
    me, z, p, q, core = place
    rank = lax.rem(me, LEVEL)
    peers = (device_of(z, 1 - p, q, core), device_of(z, p, 1 - q, core), me + 1 - TWO * core)

    def desc(block, way, src=None):
        return pltpu.make_async_remote_copy(
            src_ref=out_ref.at[block] if src is None else src, dst_ref=out_ref.at[block],
            send_sem=send_sem.at[way * LEVEL + block], recv_sem=recv_sem.at[block],
            device_id=(peers[way],), device_id_type=MESH)

    for way in (1, 0, TWO):
        desc(rank, way, in_ref).start()
    out_ref[rank] = in_ref[...]
    side = rank_of(1 - p, q, core)
    desc(side, 0).wait_recv()
    for way in (1, TWO):
        desc(side, way).start()
    for mid in (p, 1 - p):
        block = rank_of(mid, 1 - q, core)
        desc(block, 1).wait_recv()
        desc(block, TWO).start()
    for chip in range(HEIGHT):
        desc(chip * TWO + 1 - core, TWO).wait_recv()
    desc(rank, 0, in_ref).wait_send()
    desc(rank, 1, in_ref).wait_send()
    desc(side, 1).wait_send()
    for chip in range(HEIGHT):
        desc(chip * TWO + core, TWO).wait_send()


def level_scatter(in_ref, out_ref, from_core, from_q, from_p, outgo, sem_s, sem_r, place):
    me, z, p, q, core = place
    rows = out_ref.shape[0]

    def copy(src, dst, slot, dev):
        return pltpu.make_async_remote_copy(
            src_ref=src, dst_ref=dst, send_sem=sem_s.at[slot], recv_sem=sem_r.at[slot],
            device_id=(dev,), device_id_type=MESH)

    def core_copy(chip):
        return copy(in_ref.at[chip * TWO + 1 - core], from_core.at[chip], chip, me + 1 - TWO * core)

    def q_copy(mid):
        return copy(outgo.at[mid], from_q.at[mid], HEIGHT + mid, device_of(z, p, 1 - q, core))

    def p_copy():
        return copy(outgo.at[TWO], from_p, 6, device_of(z, 1 - p, q, core))

    def own(mid, last):
        chip = chip_of(0, mid, last, core)
        core_copy(chip).wait_recv()
        return [in_ref.at[chip * TWO + core], from_core.at[chip]]

    for last in (1 - p, p):
        for mid in (1 - q, q):
            core_copy(chip_of(0, mid, last, 1 - core)).start()
    for mid in (1 - p, p):
        add_into(outgo.at[mid], own(mid, 1 - q), rows)
        q_copy(mid).start()
    side = own(1 - p, q)
    q_copy(1 - p).wait_recv()
    add_into(outgo.at[TWO], side + [from_q.at[1 - p]], rows)
    p_copy().start()
    mine = own(p, q)
    q_copy(p).wait_recv()
    p_copy().wait_recv()
    add_into(out_ref, mine + [from_q.at[p], from_p], rows)
    for chip in range(HEIGHT):
        core_copy(chip).wait_send()
    for mid in range(TWO):
        q_copy(mid).wait_send()
    p_copy().wait_send()


LEVEL_SCRATCH = [
    pltpu.VMEM((LANE, DIM), BF16), pltpu.VMEM((LEVEL, LANE, DIM), BF16), pltpu.VMEM((LANE, DIM), F32),
    pltpu.VMEM((HEIGHT, LANE, DIM), BF16), pltpu.VMEM((TWO, LANE, DIM), BF16), pltpu.VMEM((LANE, DIM), BF16),
    pltpu.VMEM((TOP, LANE, DIM), BF16),
    pltpu.SemaphoreType.DMA((GROWS,)), pltpu.SemaphoreType.DMA((LEVEL,)),
    pltpu.SemaphoreType.DMA((7,)), pltpu.SemaphoreType.DMA((7,)),
]


def split_weights(gu_ref):
    wide = gu_ref[...].astype(F32)
    return (wide[:, 0:GROWS, :].reshape(DIM, UNITS).astype(BF16), wide[:, GROWS:PAIR, :].reshape(DIM, UNITS).astype(BF16))


def mlp_forward_call(x_raw, w_gu, w_dn, gain_mlp, gain_final, emb_scale, cid):
    def kernel(x_ref, wgu_ref, wd_ref, gm_ref, gf_ref, hn_ref, h_ref, a_ref, g_ref, u_ref, mine, parts, total, *scratch):
        place = my_place()
        barrier_neighbours(place)
        x = x_ref[...] * emb_scale
        mine[...] = (x * rms_inv(x) * gm_ref[...]).astype(BF16)
        level_gather(mine, a_ref, scratch[HEIGHT], scratch[5], place)
        wg, wu = split_weights(wgu_ref)
        wd = wd_ref[...].reshape(UNITS, DIM)
        for half in range(TWO):
            four = slice(HEIGHT * half, HEIGHT * half + HEIGHT)
            act_in = a_ref[four].reshape(TOKS, DIM)
            g = dot(act_in, wg, 1, 0).astype(BF16)
            u = dot(act_in, wu, 1, 0).astype(BF16)
            g_ref[four] = g.reshape(HEIGHT, LANE, UNITS)
            u_ref[four] = u.reshape(HEIGHT, LANE, UNITS)
            act = (jax.nn.silu(g.astype(F32)) * u.astype(F32)).astype(BF16)
            parts[four] = dot(act, wd, 1, 0).astype(BF16).reshape(HEIGHT, LANE, DIM)
        level_scatter(parts, total, *scratch[:HEIGHT], *scratch[6:], place)
        h = (x + total[...].astype(BF16).astype(F32)).astype(BF16)
        h_ref[...] = h
        h32 = h.astype(F32)
        hn_ref[...] = (h32 * rms_inv(h32) * gf_ref[...]).astype(BF16)

    act = jax.ShapeDtypeStruct((LANE, DIM), BF16)
    unit = jax.ShapeDtypeStruct((LEVEL, LANE, UNITS), BF16)
    return pl.pallas_call(
        kernel,
        out_shape=(act, act, jax.ShapeDtypeStruct((LEVEL, LANE, DIM), BF16), unit, unit),
        in_specs=[VSPEC] * 5, out_specs=(VSPEC,) * 5,
        scratch_shapes=LEVEL_SCRATCH,
        compiler_params=pltpu.CompilerParams(collective_id=cid, has_side_effects=True, vmem_limit_bytes=VMEM_CAP),
        name='mlp_forward',
    )(x_raw, w_gu, w_dn, gain_mlp, gain_final)


def mlp_backward_call(dhn, x_raw, h, a_all, g_all, u_all, w_gu, w_dn, gain_mlp, gain_final, emb_scale, cid):
    def kernel(dhn_ref, x_ref, h_ref, a_ref, g_ref, u_ref, wgu_ref, wd_ref, gm_ref, gf_ref, dx_ref, ggu_ref, gd_ref,
               dm_ref, grad_gate, grad_up, grad_down, mine, parts, total, *scratch):
        place = my_place()
        barrier_neighbours(place)
        h32 = h_ref[...].astype(F32)
        dh = rms_backward(h32, rms_inv(h32), gf_ref[...], dhn_ref[...])
        mine[...] = dh.astype(BF16)
        level_gather(mine, dm_ref, scratch[HEIGHT], scratch[5], place)
        wg, wu = split_weights(wgu_ref)
        wd = wd_ref[...].reshape(UNITS, DIM)
        for half in range(TWO):
            four = slice(HEIGHT * half, HEIGHT * half + HEIGHT)
            act_in = a_ref[four].reshape(TOKS, DIM)
            dm = dm_ref[four].reshape(TOKS, DIM)
            g = g_ref[four].reshape(TOKS, UNITS).astype(F32)
            u = u_ref[four].reshape(TOKS, UNITS).astype(F32)
            act = (jax.nn.silu(g) * u).astype(BF16)
            dq = dot(dm, wd, 1, 1)
            sig = jax.nn.sigmoid(g)
            dg = (dq * u * sig * (1.0 + g * (1.0 - sig))).astype(BF16)
            du = (dq * g * sig).astype(BF16)
            parts[four] = (dot(dg, wg, 1, 1) + dot(du, wu, 1, 1)).astype(BF16).reshape(HEIGHT, LANE, DIM)
            news = (dot(act_in, dg, 0, 0), dot(act_in, du, 0, 0), dot(act, dm, 0, 0))
            for ref, new in zip((grad_gate, grad_up, grad_down), news):
                ref[...] = new if half == 0 else ref[...] + new
        level_scatter(parts, total, *scratch[:HEIGHT], *scratch[6:], place)
        both = jnp.concatenate([grad_gate[...].reshape(NDEV, GROWS, UNITS), grad_up[...].reshape(NDEV, GROWS, UNITS)], axis=1)
        ggu_ref[...] = both.astype(BF16)
        gd_ref[...] = grad_down[...].astype(BF16).reshape(HEIGHT, DROWS, DIM)
        x = x_ref[...] * emb_scale
        dx_ref[...] = (dh + rms_backward(x, rms_inv(x), gm_ref[...], total[...])).astype(BF16)

    return pl.pallas_call(
        kernel,
        out_shape=(jax.ShapeDtypeStruct((LANE, DIM), BF16), jax.ShapeDtypeStruct((NDEV, PAIR, UNITS), BF16),
                   jax.ShapeDtypeStruct((HEIGHT, DROWS, DIM), BF16)),
        in_specs=[VSPEC] * 10, out_specs=(VSPEC,) * TOP,
        scratch_shapes=[pltpu.VMEM((LEVEL, LANE, DIM), BF16), pltpu.VMEM((DIM, UNITS), F32), pltpu.VMEM((DIM, UNITS), F32),
                        pltpu.VMEM((UNITS, DIM), F32)] + LEVEL_SCRATCH,
        compiler_params=pltpu.CompilerParams(collective_id=cid, has_side_effects=True, vmem_limit_bytes=VMEM_CAP),
        name='mlp_backward',
    )(dhn, x_raw, h, a_all, g_all, u_all, w_gu, w_dn, gain_mlp, gain_final)


def solution(mesh):
    group = mesh.shape['fsdp']

    def local_step(ids_blk, lab_blk, emb_shard, gate_shard, up_shard, down_shard, gain_mlp, gain_final):
        model_dim = emb_shard.shape[1]
        emb_scale = math.sqrt(model_dim)
        inv_count = 1.0 / (ids_blk.size * group)
        gm, gf = gain_mlp.reshape(1, -1), gain_final.reshape(1, -1)
        emb_pad = jnp.pad(emb_shard, ((0, VPAD - VROWS), (0, 0)))
        tok_blk = jnp.concatenate([ids_blk, lab_blk, jnp.zeros((6, LANE), jnp.int32)], axis=0)
        pieces = jnp.concatenate([gate_shard, up_shard], axis=0).reshape(PAIR, HEIGHT, LEVEL, DROWS)
        pieces = pieces.transpose(TWO, 0, 1, TOP).reshape(LEVEL, PAIR, UNITS)
        w_gu, w_dn = weights_call(pieces, down_shard, 0)
        toks = gather_call(tok_blk, 1)
        x_raw = scatter_call(lookup_call(toks, emb_pad), TWO)
        hid_norm, h, a_all, g_all, u_all = mlp_forward_call(x_raw, w_gu, w_dn, gm, gf, emb_scale, LEVEL)
        hid_all = gather_call(hid_norm, TOP)
        local_lse, lab_part = head_forward_call(toks, emb_pad, hid_all)
        stats = gather_call(jnp.concatenate([local_lse, lab_part], axis=0), HEIGHT)
        d_hid, d_head, loss = head_backward_call(toks, emb_pad, hid_all, stats, inv_count)
        dhn = scatter_call(d_hid, 5)
        d_x, g_gu, g_dn = mlp_backward_call(dhn, x_raw, h, a_all, g_all, u_all, w_gu, w_dn, gm, gf, emb_scale, 9)
        d_gu, d_down = grads_call(g_gu, g_dn, 6)
        dx_all = gather_call(d_x, 7)
        d_embed = scatter_rows_call(toks, d_head, dx_all, emb_scale)
        d_gu = d_gu.reshape(LEVEL, PAIR, HEIGHT, DROWS).transpose(1, TWO, 0, TOP).reshape(PAIR, 3072)
        return loss[0, 0], d_embed, d_gu[0:GROWS], d_gu[GROWS:PAIR], d_down

    shard_spec = P('fsdp', None)
    return jax.shard_map(local_step, mesh=mesh, in_specs=(shard_spec, shard_spec, shard_spec, shard_spec, shard_spec, shard_spec, P(), P()), out_specs=(P(), shard_spec, shard_spec, shard_spec, shard_spec), check_vma=False)
```

```python
import math
import jax
import jax.numpy as jnp
from jax import lax
from jax.experimental import pallas as pl
from jax.experimental.pallas import tpu as pltpu
from jax.sharding import PartitionSpec as P

NORM_EPS = 1e-6
MESH = pl.DeviceIdType.MESH
F32 = jnp.float32
BF16 = jnp.bfloat16
VMEM_CAP = 63 * 1024 * 1024
LANE = 128
DIM = 768
PAIR = 48
UNITS = 384
NDEV = 32
LEVEL = 8
HEIGHT = 4
DROWS = 96
CHIPS = 16
GROWS = 24
TWO = 2
TOP = 3
VSPEC = pl.BlockSpec(memory_space=pltpu.VMEM)


def my_place():
    me = lax.axis_index('fsdp')
    core = lax.rem(me, TWO)
    x = lax.rem(lax.div(me, TWO), TWO)
    y = lax.rem(lax.div(me, HEIGHT), TWO)
    z = lax.div(me, LEVEL)
    p = x * (1 - core) + y * core
    q = y * (1 - core) + x * core
    return me, z, p, q, core


def chip_of(z, p, q, core):
    x = p * (1 - core) + q * core
    y = q * (1 - core) + p * core
    return (z * TWO + y) * TWO + x


def device_of(z, p, q, core):
    return chip_of(z, p, q, core) * TWO + core


def barrier_peers(place):
    me, z = place[0], place[1]
    sem = pltpu.get_barrier_semaphore()
    for step in range(1, LEVEL):
        dev = z * LEVEL + lax.rem(me + step, LEVEL)
        pl.semaphore_signal(sem, inc=1, device_id=(dev,), device_id_type=MESH)
    for step in range(1, HEIGHT):
        dev = lax.rem(me + LEVEL * step, NDEV)
        pl.semaphore_signal(sem, inc=1, device_id=(dev,), device_id_type=MESH)
    pl.semaphore_wait(sem, 10)


def far_level(z, at):
    half = lax.div(z, TWO)
    inner = lax.rem(z + half, TWO)
    order = (TOP - TOP * half, (1 - inner) * (TWO - half) + inner * TOP * half, 1 + lax.rem(z, TWO), z)
    if isinstance(at, int):
        return order[at]
    low, high = lax.rem(at, TWO), lax.div(at, TWO)
    return ((1 - low) * (1 - high) * order[0] + low * (1 - high) * order[1]
            + (1 - low) * high * order[TWO] + low * high * order[TOP])


def remote(src, dst, sems, slot, dev):
    return pltpu.make_async_remote_copy(
        src_ref=src, dst_ref=dst, send_sem=sems.at[0, slot], recv_sem=sems.at[1, slot],
        device_id=(dev,), device_id_type=MESH)


def sem_pair(n):
    return pltpu.SemaphoreType.DMA((TWO, n))


def gather_levels(in_ref, out_ref, send_sem, recv_sem, place, work):
    me, z, p, q, core = place
    peers = (me + LEVEL, me - LEVEL, device_of(z, 1 - p, q, core), device_of(z, p, 1 - q, core), me + 1 - TWO * core)

    def desc(block, way, src=None):
        return pltpu.make_async_remote_copy(
            src_ref=out_ref.at[block] if src is None else src, dst_ref=out_ref.at[block],
            send_sem=send_sem.at[way, block], recv_sem=recv_sem.at[block],
            device_id=(peers[way],), device_id_type=MESH)

    def got(block):
        desc(block, HEIGHT).wait_recv()

    pl.when(z < TOP)(lambda: desc(me, 0, in_ref).start())
    pl.when(z > 0)(lambda: desc(me, 1, in_ref).start())
    for way in (TOP, TWO, HEIGHT):
        desc(me, way, in_ref).start()
    out_ref[me] = in_ref[...]

    def take_z(level):
        block = device_of(level, p, q, core)
        got(block)
        pl.when(jnp.logical_and(level < z, z < TOP))(lambda: desc(block, 0).start())
        pl.when(jnp.logical_and(level > z, z > 0))(lambda: desc(block, 1).start())
        for way in (TOP, TWO, HEIGHT):
            desc(block, way).start()

    def take_p(level):
        block = device_of(level, 1 - p, q, core)
        got(block)
        for way in (TOP, HEIGHT):
            desc(block, way).start()

    def take_q(level):
        for mid in (p, 1 - p):
            block = device_of(level, mid, 1 - q, core)
            got(block)
            desc(block, HEIGHT).start()
        for chip in range(HEIGHT):
            got(level * LEVEL + chip * TWO + 1 - core)

    def step(t, carry):
        pl.when(t < TOP)(lambda: take_z(far_level(z, TWO - lax.rem(t, TOP))))
        pl.when(t < HEIGHT)(lambda: take_p(far_level(z, TOP - lax.rem(t, HEIGHT))))

        @pl.when(t > 0)
        def _():
            level = far_level(z, HEIGHT - (t + lax.div(HEIGHT - t, HEIGHT)))
            take_q(level)
            work(t, level)
        return carry

    lax.fori_loop(0, 5, step, 0)
    for level in range(HEIGHT):
        desc(device_of(level, p, q, core), TWO).wait_send()
        for mid in range(TWO):
            desc(device_of(level, mid, q, core), TOP).wait_send()
        pl.when(jnp.logical_and(z < TOP, level <= z))(lambda: desc(device_of(level, p, q, core), 0).wait_send())
        pl.when(jnp.logical_and(z > 0, level >= z))(lambda: desc(device_of(level, p, q, core), 1).wait_send())
    for chip in range(CHIPS):
        desc(chip * TWO + core, HEIGHT).wait_send()


def add_into(dst, srcs, rows):
    step = 32

    def body(i, carry):
        sl = pl.ds(pl.multiple_of(i * step, step), step)
        total = srcs[0][sl, :].astype(F32)
        for src in srcs[1:]:
            total = total + src[sl, :].astype(F32)
        dst[sl, :] = total.astype(dst.dtype)
        return carry

    lax.fori_loop(0, rows // step, body, 0)


def scatter_scratch(rows, cols):
    return [
        pltpu.VMEM((CHIPS, rows, cols), BF16), pltpu.VMEM((LEVEL, rows, cols), BF16), pltpu.VMEM((HEIGHT, rows, cols), BF16),
        pltpu.VMEM((HEIGHT, rows, cols), BF16), pltpu.VMEM((HEIGHT, rows, cols), BF16), pltpu.VMEM((CHIPS, rows, cols), BF16),
        pltpu.VMEM((rows, cols), F32),
        pltpu.SemaphoreType.DMA((TWO, CHIPS)), pltpu.SemaphoreType.DMA((TWO, LEVEL)), pltpu.SemaphoreType.DMA((TWO, HEIGHT)),
        pltpu.SemaphoreType.DMA((TWO, HEIGHT)), pltpu.SemaphoreType.DMA((TWO, HEIGHT)),
    ]


def scatter_levels(in_ref, out_ref, scratch, place, work):
    from_core, from_q, from_p, from_low, from_high, outgo, acc, sem_c, sem_q, sem_p, sem_up, sem_dn = scratch
    me, z, p, q, core = place
    rows = out_ref.shape[0]
    other = 1 - core

    def core_copy(chip):
        return remote(in_ref.at[chip * TWO + other], from_core.at[chip], sem_c, chip, me + 1 - TWO * core)

    def local(level, mid, last):
        return level * HEIGHT + mid * TWO + last

    def q_copy(level, mid):
        return remote(outgo.at[local(level, mid, 1 - q)], from_q.at[level * TWO + mid], sem_q, level * TWO + mid,
                      device_of(z, p, 1 - q, core))

    def p_copy(level):
        return remote(outgo.at[local(level, 1 - p, q)], from_p.at[level], sem_p, level, device_of(z, 1 - p, q, core))

    def up_copy(level):
        return remote(outgo.at[local(level, p, q)], from_low.at[level], sem_up, level, me + LEVEL)

    def dn_copy(level):
        return remote(outgo.at[local(level, p, q)], from_high.at[level], sem_dn, level, me - LEVEL)

    def own(level, mid, last):
        chip = chip_of(level, mid, last, core)
        core_copy(chip).wait_recv()
        return [in_ref.at[chip * TWO + core], from_core.at[chip]]

    def make(level):
        work(level)
        for last in (1 - p, p):
            for mid in (1 - q, q):
                core_copy(chip_of(level, mid, last, other)).start()

    def send_q(level):
        for mid in (1 - p, p):
            add_into(outgo.at[local(level, mid, 1 - q)], own(level, mid, 1 - q), rows)
            q_copy(level, mid).start()

    def send_p(level):
        side = own(level, 1 - p, q)
        q_copy(level, 1 - p).wait_recv()
        add_into(outgo.at[local(level, 1 - p, q)], side + [from_q.at[level * TWO + 1 - p]], rows)
        p_copy(level).start()

    def gather_here(level):
        mine = own(level, p, q)
        q_copy(level, p).wait_recv()
        p_copy(level).wait_recv()
        return mine + [from_q.at[level * TWO + p], from_p.at[level]]

    def send_z(level):
        add_into(acc, gather_here(level), rows)

        @pl.when(level > z)
        def _():
            @pl.when(z > 0)
            def _():
                up_copy(level).wait_recv()
                add_into(acc, [acc, from_low.at[level]], rows)
            add_into(outgo.at[local(level, p, q)], [acc], rows)
            up_copy(level).start()

        @pl.when(level < z)
        def _():
            @pl.when(z < TOP)
            def _():
                dn_copy(level).wait_recv()
                add_into(acc, [acc, from_high.at[level]], rows)
            add_into(outgo.at[local(level, p, q)], [acc], rows)
            dn_copy(level).start()

    def level_at(t):
        return far_level(z, lax.rem(t, HEIGHT))

    def step(t, carry):
        pl.when(t < HEIGHT)(lambda: make(level_at(t)))
        pl.when(jnp.logical_and(t > 0, t < 5))(lambda: send_q(level_at(t + TOP)))
        pl.when(jnp.logical_and(t > 1, t < 6))(lambda: send_p(level_at(t + TWO)))
        pl.when(t > TWO)(lambda: send_z(level_at(t + 1)))
        return carry

    lax.fori_loop(0, 6, step, 0)
    add_into(out_ref, gather_here(z), rows)

    @pl.when(z > 0)
    def _():
        up_copy(z).wait_recv()
        add_into(out_ref, [out_ref, from_low.at[z]], rows)

    @pl.when(z < TOP)
    def _():
        dn_copy(z).wait_recv()
        add_into(out_ref, [out_ref, from_high.at[z]], rows)

    for chip in range(CHIPS):
        core_copy(chip).wait_send()
    for level in range(HEIGHT):
        for mid in range(TWO):
            q_copy(level, mid).wait_send()
        p_copy(level).wait_send()
        pl.when(level > z)(lambda: up_copy(level).wait_send())
        pl.when(level < z)(lambda: dn_copy(level).wait_send())


def rank_of(p, q, core):
    return device_of(0, p, q, core)


def level_gather(in_ref, out_ref, send_sem, recv_sem, place):
    me, z, p, q, core = place
    rank = lax.rem(me, LEVEL)
    peers = (device_of(z, 1 - p, q, core), device_of(z, p, 1 - q, core), me + 1 - TWO * core)

    def desc(block, way, src=None):
        return pltpu.make_async_remote_copy(
            src_ref=out_ref.at[block] if src is None else src, dst_ref=out_ref.at[block],
            send_sem=send_sem.at[way * LEVEL + block], recv_sem=recv_sem.at[block],
            device_id=(peers[way],), device_id_type=MESH)

    for way in (1, 0, TWO):
        desc(rank, way, in_ref).start()
    out_ref[rank] = in_ref[...]
    side = rank_of(1 - p, q, core)
    desc(side, 0).wait_recv()
    for way in (1, TWO):
        desc(side, way).start()
    for mid in (p, 1 - p):
        block = rank_of(mid, 1 - q, core)
        desc(block, 1).wait_recv()
        desc(block, TWO).start()
    for chip in range(HEIGHT):
        desc(chip * TWO + 1 - core, TWO).wait_recv()
    desc(rank, 0, in_ref).wait_send()
    desc(rank, 1, in_ref).wait_send()
    desc(side, 1).wait_send()
    for chip in range(HEIGHT):
        desc(chip * TWO + core, TWO).wait_send()


def level_scatter(in_ref, out_ref, from_core, from_q, from_p, outgo, sem_s, sem_r, place):
    me, z, p, q, core = place
    rows = out_ref.shape[0]

    def copy(src, dst, slot, dev):
        return pltpu.make_async_remote_copy(
            src_ref=src, dst_ref=dst, send_sem=sem_s.at[slot], recv_sem=sem_r.at[slot],
            device_id=(dev,), device_id_type=MESH)

    def core_copy(chip):
        return copy(in_ref.at[chip * TWO + 1 - core], from_core.at[chip], chip, me + 1 - TWO * core)

    def q_copy(mid):
        return copy(outgo.at[mid], from_q.at[mid], HEIGHT + mid, device_of(z, p, 1 - q, core))

    def p_copy():
        return copy(outgo.at[TWO], from_p, 6, device_of(z, 1 - p, q, core))

    def own(mid, last):
        chip = chip_of(0, mid, last, core)
        core_copy(chip).wait_recv()
        return [in_ref.at[chip * TWO + core], from_core.at[chip]]

    for last in (1 - p, p):
        for mid in (1 - q, q):
            core_copy(chip_of(0, mid, last, 1 - core)).start()
    for mid in (1 - p, p):
        add_into(outgo.at[mid], own(mid, 1 - q), rows)
        q_copy(mid).start()
    side = own(1 - p, q)
    q_copy(1 - p).wait_recv()
    add_into(outgo.at[TWO], side + [from_q.at[1 - p]], rows)
    p_copy().start()
    mine = own(p, q)
    q_copy(p).wait_recv()
    p_copy().wait_recv()
    add_into(out_ref, mine + [from_q.at[p], from_p], rows)
    for chip in range(HEIGHT):
        core_copy(chip).wait_send()
    for mid in range(TWO):
        q_copy(mid).wait_send()
    p_copy().wait_send()


def dot(left, right, ld, rd):
    return lax.dot_general(left, right, (((ld,), (rd,)), ((), ())), preferred_element_type=F32)


TOKS = 512
VPAD = 1024
VROWS = 1004


def id_rows(tok_ref, row, first):
    ids = jnp.concatenate([tok_ref[first + t, row:row + 1, :] for t in range(HEIGHT)], axis=1) - shard_start()
    return jnp.where(jnp.logical_and(ids >= 0, ids < VROWS), ids, -1)


def vocab_iota():
    return lax.broadcasted_iota(jnp.int32, (VPAD, TOKS), 0)


def shard_start():
    return lax.axis_index('fsdp') * VROWS


def fill_table(table, emb_ref):
    table[VPAD - 32:VPAD, :] = jnp.zeros((32, DIM), BF16)
    table[0:VROWS, :] = emb_ref[...]


def halves(level, body):
    def one(i, carry):
        body(level * LEVEL + i * HEIGHT)
        return carry
    lax.fori_loop(0, TWO, one, 0)


def rms_inv(values):
    return lax.rsqrt(jnp.mean(values * values, axis=-1, keepdims=True) + NORM_EPS)


def rms_backward(values, inv_rms, gain_vec, grad_out):
    scaled = grad_out * gain_vec
    return inv_rms * scaled - values * (inv_rms ** TOP) * jnp.mean(scaled * values, axis=-1, keepdims=True)


LEVEL_SCRATCH = [
    pltpu.VMEM((LANE, DIM), BF16), pltpu.VMEM((LEVEL, LANE, DIM), BF16), pltpu.VMEM((LANE, DIM), F32),
    pltpu.VMEM((HEIGHT, LANE, DIM), BF16), pltpu.VMEM((TWO, LANE, DIM), BF16), pltpu.VMEM((LANE, DIM), BF16),
    pltpu.VMEM((TOP, LANE, DIM), BF16),
    pltpu.SemaphoreType.DMA((GROWS,)), pltpu.SemaphoreType.DMA((LEVEL,)),
    pltpu.SemaphoreType.DMA((7,)), pltpu.SemaphoreType.DMA((7,)),
]


def split_weights(gu_ref):
    wide = gu_ref[...].astype(F32)
    return (wide[:, 0:GROWS, :].reshape(DIM, UNITS).astype(BF16), wide[:, GROWS:PAIR, :].reshape(DIM, UNITS).astype(BF16))


GU_SHAPE = (NDEV, PAIR, UNITS)
WD_SHAPE = (HEIGHT, DROWS, DIM)


def call(kernel, name, cid, outs, ins, scratch):
    return pl.pallas_call(
        kernel, out_shape=outs, in_specs=[VSPEC] * len(ins), out_specs=(VSPEC,) * len(outs), scratch_shapes=scratch,
        compiler_params=pltpu.CompilerParams(collective_id=cid, has_side_effects=True, vmem_limit_bytes=VMEM_CAP),
        name=name)(*ins)


def start_call(ids, labs, emb, pieces, down_shard, gain_mlp, gain_final, emb_scale):
    def kernel(ids_ref, lab_ref, emb_ref, piece_ref, down_ref, gm_ref, gf_ref,
               tok_ref, x_ref, gu_ref, wd_ref, hn_ref, h_ref, a_ref, g_ref, u_ref,
               tok_mine, table, rows, sem_t, sem_a, z_send, z_recv, d_send, d_recv, *scratch):
        ring, (mine, parts, total, *level) = scratch[:12], scratch[12:]
        place = my_place()
        me, z, p, q, core = place
        rank = lax.rem(me, LEVEL)
        tok_mine[...] = jnp.zeros((LEVEL, LANE), jnp.int32)
        tok_mine[0:1, :] = ids_ref[...]
        tok_mine[1:TWO, :] = lab_ref[...]
        barrier_peers(place)

        def exchange(step):
            peer = lax.rem(rank + step, LEVEL)
            return remote(piece_ref.at[peer], gu_ref.at[me], sem_a, step, z * LEVEL + peer)

        def slab(lv, way):
            part = gu_ref.at[pl.ds(lv * LEVEL, LEVEL)]
            return pltpu.make_async_remote_copy(
                src_ref=part, dst_ref=part, send_sem=z_send.at[way * HEIGHT + lv], recv_sem=z_recv.at[lv],
                device_id=(me + LEVEL - CHIPS * way,), device_id_type=MESH)

        def slab_down(lv, way, src):
            return pltpu.make_async_remote_copy(
                src_ref=src, dst_ref=wd_ref.at[lv], send_sem=d_send.at[way * HEIGHT + lv], recv_sem=d_recv.at[lv],
                device_id=(me + LEVEL - CHIPS * way,), device_id_type=MESH)

        pair = remote(tok_mine, tok_ref.at[me], sem_t, 0, me + 1 - TWO * core)
        pair.start()
        for step in range(1, LEVEL):
            exchange(step).start()
        pl.when(z < TOP)(lambda: slab_down(z, 0, down_ref).start())
        pl.when(z > 0)(lambda: slab_down(z, 1, down_ref).start())
        tok_ref[me] = tok_mine[...]
        wd_ref[z] = down_ref[...]
        gu_ref[me] = piece_ref[rank]
        fill_table(table, emb_ref)
        pair.wait()
        for stage, (size, dev) in enumerate(((TWO, device_of(z, *flip_x(p, q, core))), (HEIGHT, device_of(z, *flip_y(p, q, core))))):
            part = tok_ref.at[pl.ds(lax.div(me, size) * size, size)]
            ship = remote(part, part, sem_t, stage + 1, dev)
            ship.start()
            ship.wait()
        part = tok_ref.at[pl.ds(z * LEVEL, LEVEL)]
        ships = [remote(part, part, sem_t, TWO + step, lax.rem(me + LEVEL * step, NDEV)) for step in range(1, HEIGHT)]
        for ship in ships:
            ship.start()
        for ship in ships:
            ship.wait()
        for step in range(1, LEVEL):
            exchange(step).wait_recv()
        pl.when(z < TOP)(lambda: slab(z, 0).start())
        pl.when(z > 0)(lambda: slab(z, 1).start())

        def take(lv, way, more):
            slab_down(lv, 0, wd_ref.at[lv]).wait_recv()
            pl.when(more)(lambda: slab_down(lv, way, wd_ref.at[lv]).start())
            slab(lv, 0).wait_recv()
            pl.when(more)(lambda: slab(lv, way).start())

        def take_far(far):
            pl.when(z - far >= 0)(lambda: take(z - far, 0, z < TOP))
            pl.when(z + far < HEIGHT)(lambda: take(z + far, 1, z > 0))

        def find(lv):
            def body(first):
                hit = (vocab_iota() == id_rows(tok_ref, 0, first)).astype(F32).astype(BF16)
                rows[pl.ds(first, HEIGHT)] = dot(hit, table[...], 0, 0).astype(BF16).reshape(HEIGHT, LANE, DIM)
            halves(lv, body)

        scatter_levels(rows, x_ref, ring, place, find)
        take_far(1)
        x = x_ref[...] * emb_scale
        mine[...] = (x * rms_inv(x) * gm_ref[...]).astype(BF16)
        level_gather(mine, a_ref, level[HEIGHT], level[5], place)
        take_far(TWO)
        take_far(TOP)
        wg, wu = split_weights(gu_ref)
        wd = wd_ref[...].reshape(UNITS, DIM)
        for half in range(TWO):
            four = slice(HEIGHT * half, HEIGHT * half + HEIGHT)
            act_in = a_ref[four].reshape(TOKS, DIM)
            g = dot(act_in, wg, 1, 0).astype(BF16)
            u = dot(act_in, wu, 1, 0).astype(BF16)
            g_ref[four] = g.reshape(HEIGHT, LANE, UNITS)
            u_ref[four] = u.reshape(HEIGHT, LANE, UNITS)
            act = (jax.nn.silu(g.astype(F32)) * u.astype(F32)).astype(BF16)
            parts[four] = dot(act, wd, 1, 0).astype(BF16).reshape(HEIGHT, LANE, DIM)
        level_scatter(parts, total, *level[:HEIGHT], *level[6:], place)
        h = (x + total[...].astype(BF16).astype(F32)).astype(BF16)
        h_ref[...] = h
        h32 = h.astype(F32)
        hn_ref[...] = (h32 * rms_inv(h32) * gf_ref[...]).astype(BF16)
        for step in range(1, LEVEL):
            exchange(step).wait_send()

        def sent(lv, way):
            slab(lv, way).wait_send()
            slab_down(lv, way, wd_ref.at[lv]).wait_send()

        for lv in range(HEIGHT):
            pl.when(jnp.logical_and(z < TOP, lv <= z))(lambda: sent(lv, 0))
            pl.when(jnp.logical_and(z > 0, lv >= z))(lambda: sent(lv, 1))

    act = jax.ShapeDtypeStruct((LANE, DIM), BF16)
    unit = jax.ShapeDtypeStruct((LEVEL, LANE, UNITS), BF16)
    return call(
        kernel, 'start', 0,
        (jax.ShapeDtypeStruct((NDEV, LEVEL, LANE), jnp.int32), jax.ShapeDtypeStruct((LANE, DIM), F32),
         jax.ShapeDtypeStruct(GU_SHAPE, BF16), jax.ShapeDtypeStruct(WD_SHAPE, BF16), act, act,
         jax.ShapeDtypeStruct((LEVEL, LANE, DIM), BF16), unit, unit),
        (ids, labs, emb, pieces, down_shard, gain_mlp, gain_final),
        [pltpu.VMEM((LEVEL, LANE), jnp.int32), pltpu.VMEM((VPAD, DIM), BF16), pltpu.VMEM((NDEV, LANE, DIM), BF16),
         sem_pair(6), sem_pair(LEVEL), pltpu.SemaphoreType.DMA((LEVEL,)), pltpu.SemaphoreType.DMA((HEIGHT,)),
         pltpu.SemaphoreType.DMA((LEVEL,)), pltpu.SemaphoreType.DMA((HEIGHT,))] + scatter_scratch(LANE, DIM) + LEVEL_SCRATCH)


def flip_x(p, q, core):
    return p * core + (1 - p) * (1 - core), q * (1 - core) + (1 - q) * core, core


def flip_y(p, q, core):
    return p * (1 - core) + (1 - p) * core, q * core + (1 - q) * (1 - core), core


STAT = 40


def merge_stats(blocks):
    logs = [b[0:32, :] for b in blocks]
    top = logs[0]
    for one in logs[1:]:
        top = jnp.maximum(top, one)
    total = jnp.exp(logs[0] - top)
    labs = blocks[0][32:STAT, :]
    for one, b in zip(logs[1:], blocks[1:]):
        total = total + jnp.exp(one - top)
        labs = labs + b[32:STAT, :]
    return jnp.concatenate([top + jnp.log(total), labs], axis=0)


def head_call(toks, emb, hid_norm, inv_count):
    def kernel(tok_ref, emb_ref, hn_ref, dhn_ref, demb_ref, loss_ref,
               table, hid_all, parts, stat, land, land_z, lse_ref, g_send, g_recv, sem_s, *ring):
        place = my_place()
        me, z, p, q, core = place
        barrier_peers(place)
        fill_table(table, emb_ref)
        stat[...] = jnp.zeros_like(stat)
        demb_ref[...] = jnp.zeros_like(demb_ref)

        def forward(t, lv):
            def body(first):
                logits = dot(table[...], hid_all[pl.ds(first, HEIGHT)].reshape(TOKS, DIM), 1, 1)
                row = vocab_iota()
                lab = jnp.sum(jnp.where(row == id_rows(tok_ref, 1, first), logits, 0.0), axis=0, keepdims=True)
                logits = jnp.where(row < VROWS, logits, -1e30)
                top = jnp.max(logits, axis=0, keepdims=True)
                local = top + jnp.log(jnp.sum(jnp.exp(logits - top), axis=0, keepdims=True))
                for t in range(HEIGHT):
                    stat[0, pl.ds(first + t, 1), :] = local[:, t * LANE:(t + 1) * LANE]
                    stat[0, 32:33, :] = stat[0, 32:33, :] + lab[:, t * LANE:(t + 1) * LANE]
            halves(lv, body)

        gather_levels(hn_ref, hid_all, g_send, g_recv, place, forward)

        devs = (me + 1 - TWO * core, device_of(z, *flip_x(p, q, core)), device_of(z, *flip_y(p, q, core)))
        for stage, dev in enumerate(devs):
            ship = remote(stat.at[stage], land.at[stage], sem_s, stage, dev)
            ship.start()
            ship.wait()
            stat[stage + 1] = merge_stats([stat[stage], land[stage]])
        ships = [remote(stat.at[TOP], land_z.at[z], sem_s, TWO + step, lax.rem(me + LEVEL * step, NDEV)) for step in range(1, HEIGHT)]
        for ship in ships:
            ship.start()
        land_z[z] = stat[TOP]
        for ship in ships:
            ship.wait()
        final = merge_stats([land_z[lv] for lv in range(HEIGHT)])
        lse_ref[...] = final[0:32, :]
        loss_ref[...] = jnp.full((LEVEL, LANE), (jnp.sum(final[0:32, :]) - jnp.sum(final[32:STAT, :])) * inv_count, F32)

        def backward(lv):
            def body(first):
                hid = hid_all[pl.ds(first, HEIGHT)].reshape(TOKS, DIM)
                logits = dot(table[...], hid, 1, 1)
                lse_row = jnp.concatenate([lse_ref[pl.ds(first + t, 1), :] for t in range(HEIGHT)], axis=1)
                row = vocab_iota()
                prob = jnp.exp(jnp.where(row < VROWS, logits, -1e30) - lse_row)
                hit = jnp.where(row == id_rows(tok_ref, 1, first), 1.0, 0.0)
                grad = ((prob - hit) * inv_count).astype(BF16)
                parts[pl.ds(first, HEIGHT)] = dot(grad, table[...], 0, 0).astype(BF16).reshape(HEIGHT, LANE, DIM)
                demb_ref[...] += dot(grad, hid, 1, 0)
            halves(lv, body)

        scatter_levels(parts, dhn_ref, ring, place, backward)

    whole = pltpu.VMEM((NDEV, LANE, DIM), BF16)
    return call(
        kernel, 'head', 1,
        (jax.ShapeDtypeStruct((LANE, DIM), F32), jax.ShapeDtypeStruct((VPAD, DIM), F32), jax.ShapeDtypeStruct((LEVEL, LANE), F32)),
        (toks, emb, hid_norm),
        [pltpu.VMEM((VPAD, DIM), BF16), whole, whole, pltpu.VMEM((HEIGHT, STAT, LANE), F32), pltpu.VMEM((TOP, STAT, LANE), F32),
         pltpu.VMEM((HEIGHT, STAT, LANE), F32), pltpu.VMEM((32, LANE), F32), pltpu.SemaphoreType.DMA((5, NDEV)),
         pltpu.SemaphoreType.DMA((NDEV,)), sem_pair(6)] + scatter_scratch(LANE, DIM))


def end_call(dhn, x_raw, h, a_all, g_all, u_all, w_gu, w_dn, gain_mlp, gain_final, toks, d_head, emb_scale):
    def kernel(dhn_ref, x_ref, h_ref, a_ref, g_ref, u_ref, wgu_ref, wd_ref, gm_ref, gf_ref, tok_ref, head_ref,
               out_ref, own_ref, dn_ref,
               dm_ref, grad_gate, grad_up, grad_down, ggu, gd, d_gate, d_up, acts, dx_ref, dx_all, acc_rows,
               from_low, from_high, low_d, high_d, outgo, outgo_d, acc, g_send, g_recv, sem_a, sem_z, sem_d,
               mine, parts, total, *scratch):
        place = my_place()
        me, z, p, q, core = place
        rank = lax.rem(me, LEVEL)
        barrier_peers(place)
        h32 = h_ref[...].astype(F32)
        dh = rms_backward(h32, rms_inv(h32), gf_ref[...], dhn_ref[...])
        mine[...] = dh.astype(BF16)
        level_gather(mine, dm_ref, scratch[HEIGHT], scratch[5], place)
        wg, wu = split_weights(wgu_ref)
        wd = wd_ref[...].reshape(UNITS, DIM)
        for half in range(TWO):
            four = slice(HEIGHT * half, HEIGHT * half + HEIGHT)
            g = g_ref[four].reshape(TOKS, UNITS).astype(F32)
            u = u_ref[four].reshape(TOKS, UNITS).astype(F32)
            dq = dot(dm_ref[four].reshape(TOKS, DIM), wd, 1, 1)
            sig = jax.nn.sigmoid(g)
            dg = (dq * u * sig * (1.0 + g * (1.0 - sig))).astype(BF16)
            du = (dq * g * sig).astype(BF16)
            d_gate[half] = dg
            d_up[half] = du
            acts[half] = (jax.nn.silu(g) * u).astype(BF16)
            parts[four] = (dot(dg, wg, 1, 1) + dot(du, wu, 1, 1)).astype(BF16).reshape(HEIGHT, LANE, DIM)
        level_scatter(parts, total, *scratch[:HEIGHT], *scratch[6:], place)
        x = x_ref[...] * emb_scale
        dx_ref[...] = (dh + rms_backward(x, rms_inv(x), gm_ref[...], total[...])).astype(BF16)
        acc_rows[...] = jnp.zeros_like(acc_rows)

        def rows_of(ref, lv):
            return ref.at[pl.ds(lv * LEVEL, LEVEL)]

        def add_slab(dst, srcs):
            def body(i, carry):
                value = srcs[0][i].astype(F32)
                for src in srcs[1:]:
                    value = value + src[i].astype(F32)
                dst[i] = value.astype(dst.dtype)
                return carry
            lax.fori_loop(0, LEVEL, body, 0)

        def hop(lv, way):
            land = (from_low, from_high)[way]
            return remote(rows_of(outgo, lv), rows_of(land, lv), sem_z, way * HEIGHT + lv, me + LEVEL - CHIPS * way)

        def hop_d(lv, way):
            land = (low_d, high_d)[way]
            return remote(outgo_d.at[lv], land.at[lv], sem_d, way * HEIGHT + lv, me + LEVEL - CHIPS * way)

        def send(lv, way, more):
            low = rows_of((from_low, from_high)[way], lv)
            low_down = (low_d, high_d)[way].at[lv]

            @pl.when(more)
            def _():
                hop(lv, way).wait_recv()
                add_slab(rows_of(outgo, lv), [rows_of(ggu, lv), low])
                hop_d(lv, way).wait_recv()
                add_into(outgo_d.at[lv], [gd.at[lv], low_down], DROWS)

            @pl.when(jnp.logical_not(more))
            def _():
                add_slab(rows_of(outgo, lv), [rows_of(ggu, lv)])
                add_into(outgo_d.at[lv], [gd.at[lv]], DROWS)
            hop(lv, way).start()
            hop_d(lv, way).start()

        def send_far(far):
            pl.when(z + far < HEIGHT)(lambda: send(z + far, 0, z > 0))
            pl.when(z - far >= 0)(lambda: send(z - far, 1, z < TOP))

        def weight_grads():
            for half in range(TWO):
                four = slice(HEIGHT * half, HEIGHT * half + HEIGHT)
                act_in = a_ref[four].reshape(TOKS, DIM)
                news = (dot(act_in, d_gate[half], 0, 0), dot(act_in, d_up[half], 0, 0),
                        dot(acts[half], dm_ref[four].reshape(TOKS, DIM), 0, 0))
                for ref, new in zip((grad_gate, grad_up, grad_down), news):
                    ref[...] = new if half == 0 else ref[...] + new
            both = jnp.concatenate([grad_gate[...].reshape(NDEV, GROWS, UNITS), grad_up[...].reshape(NDEV, GROWS, UNITS)], axis=1)
            ggu[...] = both.astype(BF16)
            gd[...] = grad_down[...].astype(BF16).reshape(WD_SHAPE)

        def add_rows(t, lv):
            def body(first):
                hit = (vocab_iota() == id_rows(tok_ref, 0, first)).astype(F32).astype(BF16)
                acc_rows[...] += dot(hit, dx_all[pl.ds(first, HEIGHT)].reshape(TOKS, DIM), 1, 0)
            halves(lv, body)

            @pl.when(t == 1)
            def _():
                weight_grads()
                send_far(TOP)
            pl.when(t == TWO)(lambda: send_far(TWO))
            pl.when(t == TOP)(lambda: send_far(1))

        gather_levels(dx_ref, dx_all, g_send, g_recv, place, add_rows)
        out_ref[...] = head_ref[0:VROWS, :] + acc_rows[0:VROWS, :] * emb_scale

        add_slab(acc, [rows_of(ggu, z)])
        add_into(dn_ref, [gd.at[z]], DROWS)

        def last(way):
            hop(z, way).wait_recv()
            add_slab(acc, [acc, rows_of((from_low, from_high)[way], z)])
            hop_d(z, way).wait_recv()
            add_into(dn_ref, [dn_ref, (low_d, high_d)[way].at[z]], DROWS)

        pl.when(z > 0)(lambda: last(0))
        pl.when(z < TOP)(lambda: last(1))

        def exchange(step):
            peer = lax.rem(rank + step, LEVEL)
            return remote(acc.at[peer], own_ref.at[rank], sem_a, step, z * LEVEL + peer)

        for step in range(1, LEVEL):
            exchange(step).start()
        own_ref[rank] = acc[rank]
        for step in range(1, LEVEL):
            exchange(step).wait_recv()
        for step in range(1, LEVEL):
            exchange(step).wait_send()

        def sent(lv, way):
            hop(lv, way).wait_send()
            hop_d(lv, way).wait_send()

        for lv in range(HEIGHT):
            pl.when(lv > z)(lambda: sent(lv, 0))
            pl.when(lv < z)(lambda: sent(lv, 1))

    slab, slab_d = pltpu.VMEM(GU_SHAPE, BF16), pltpu.VMEM(WD_SHAPE, BF16)
    wide, tall = pltpu.VMEM((DIM, UNITS), F32), pltpu.VMEM((UNITS, DIM), F32)
    unit = pltpu.VMEM((TWO, TOKS, UNITS), BF16)
    return call(
        kernel, 'end', TWO,
        (jax.ShapeDtypeStruct((VROWS, DIM), F32), jax.ShapeDtypeStruct((LEVEL, PAIR, UNITS), F32), jax.ShapeDtypeStruct((DROWS, DIM), F32)),
        (dhn, x_raw, h, a_all, g_all, u_all, w_gu, w_dn, gain_mlp, gain_final, toks, d_head),
        [pltpu.VMEM((LEVEL, LANE, DIM), BF16), wide, wide, tall, slab, slab_d, unit, unit, unit, pltpu.VMEM((LANE, DIM), BF16),
         pltpu.VMEM((NDEV, LANE, DIM), BF16), pltpu.VMEM((VPAD, DIM), F32), slab, slab, slab_d, slab_d, slab, slab_d,
         pltpu.VMEM((LEVEL, PAIR, UNITS), F32), pltpu.SemaphoreType.DMA((5, NDEV)), pltpu.SemaphoreType.DMA((NDEV,)),
         sem_pair(LEVEL), sem_pair(LEVEL), sem_pair(LEVEL)] + LEVEL_SCRATCH)


def solution(mesh):
    group = mesh.shape['fsdp']

    def local_step(ids_blk, lab_blk, emb_shard, gate_shard, up_shard, down_shard, gain_mlp, gain_final):
        emb_scale = math.sqrt(emb_shard.shape[1])
        inv_count = 1.0 / (ids_blk.size * group)
        gm, gf = gain_mlp.reshape(1, -1), gain_final.reshape(1, -1)
        pieces = jnp.concatenate([gate_shard, up_shard], axis=0).reshape(PAIR, HEIGHT, LEVEL, DROWS)
        pieces = pieces.transpose(TWO, 0, 1, TOP).reshape(LEVEL, PAIR, UNITS)
        toks, x_raw, w_gu, w_dn, hid_norm, h, a_all, g_all, u_all = start_call(
            ids_blk, lab_blk, emb_shard, pieces, down_shard, gm, gf, emb_scale)
        dhn, d_head, loss = head_call(toks, emb_shard, hid_norm, inv_count)
        d_embed, d_gu, d_down = end_call(dhn, x_raw, h, a_all, g_all, u_all, w_gu, w_dn, gm, gf, toks, d_head, emb_scale)
        d_gu = d_gu.reshape(LEVEL, PAIR, HEIGHT, DROWS).transpose(1, TWO, 0, TOP).reshape(PAIR, 3072)
        return loss[0, 0], d_embed, d_gu[0:GROWS], d_gu[GROWS:PAIR], d_down

    shard_spec = P('fsdp', None)
    return jax.shard_map(local_step, mesh=mesh, in_specs=(shard_spec, shard_spec, shard_spec, shard_spec, shard_spec, shard_spec, P(), P()), out_specs=(P(), shard_spec, shard_spec, shard_spec, shard_spec), check_vma=False)
```

```python
import math
import jax
import jax.numpy as jnp
from jax import lax
from jax.experimental import pallas as pl
from jax.experimental.pallas import tpu as pltpu
from jax.sharding import PartitionSpec as P

NORM_EPS = 1e-6
MESH = pl.DeviceIdType.MESH
F32 = jnp.float32
BF16 = jnp.bfloat16
VMEM_CAP = 63 * 1024 * 1024
LANE = 128
DIM = 768
PAIR = 48
UNITS = 384
NDEV = 32
LEVEL = 8
HEIGHT = 4
DROWS = 96
CHIPS = 16
GROWS = 24
TWO = 2
TOP = 3
VSPEC = pl.BlockSpec(memory_space=pltpu.VMEM)


def my_place():
    me = lax.axis_index('fsdp')
    core = lax.rem(me, TWO)
    x = lax.rem(lax.div(me, TWO), TWO)
    y = lax.rem(lax.div(me, HEIGHT), TWO)
    z = lax.div(me, LEVEL)
    p = x * (1 - core) + y * core
    q = y * (1 - core) + x * core
    return me, z, p, q, core


def chip_of(z, p, q, core):
    x = p * (1 - core) + q * core
    y = q * (1 - core) + p * core
    return (z * TWO + y) * TWO + x


def device_of(z, p, q, core):
    return chip_of(z, p, q, core) * TWO + core


def barrier_peers(place):
    me, z = place[0], place[1]
    sem = pltpu.get_barrier_semaphore()
    for step in range(1, LEVEL):
        dev = z * LEVEL + lax.rem(me + step, LEVEL)
        pl.semaphore_signal(sem, inc=1, device_id=(dev,), device_id_type=MESH)
    for step in range(1, HEIGHT):
        dev = lax.rem(me + LEVEL * step, NDEV)
        pl.semaphore_signal(sem, inc=1, device_id=(dev,), device_id_type=MESH)
    pl.semaphore_wait(sem, 10)


def far_level(z, at):
    half = lax.div(z, TWO)
    inner = lax.rem(z + half, TWO)
    order = (TOP - TOP * half, (1 - inner) * (TWO - half) + inner * TOP * half, 1 + lax.rem(z, TWO), z)
    if isinstance(at, int):
        return order[at]
    low, high = lax.rem(at, TWO), lax.div(at, TWO)
    return ((1 - low) * (1 - high) * order[0] + low * (1 - high) * order[1]
            + (1 - low) * high * order[TWO] + low * high * order[TOP])


def remote(src, dst, sems, slot, dev):
    return pltpu.make_async_remote_copy(
        src_ref=src, dst_ref=dst, send_sem=sems.at[0, slot], recv_sem=sems.at[1, slot],
        device_id=(dev,), device_id_type=MESH)


def sem_pair(n):
    return pltpu.SemaphoreType.DMA((TWO, n))


def gather_levels(in_ref, out_ref, send_sem, recv_sem, place, work):
    me, z, p, q, core = place
    peers = (me + LEVEL, me - LEVEL, device_of(z, 1 - p, q, core), device_of(z, p, 1 - q, core), me + 1 - TWO * core)

    def desc(block, way, src=None):
        return pltpu.make_async_remote_copy(
            src_ref=out_ref.at[block] if src is None else src, dst_ref=out_ref.at[block],
            send_sem=send_sem.at[way, block], recv_sem=recv_sem.at[block],
            device_id=(peers[way],), device_id_type=MESH)

    def got(block):
        desc(block, HEIGHT).wait_recv()

    pl.when(z < TOP)(lambda: desc(me, 0, in_ref).start())
    pl.when(z > 0)(lambda: desc(me, 1, in_ref).start())
    for way in (TOP, TWO, HEIGHT):
        desc(me, way, in_ref).start()
    out_ref[me] = in_ref[...]

    def take_z(level):
        block = device_of(level, p, q, core)
        got(block)
        pl.when(jnp.logical_and(level < z, z < TOP))(lambda: desc(block, 0).start())
        pl.when(jnp.logical_and(level > z, z > 0))(lambda: desc(block, 1).start())
        for way in (TOP, TWO, HEIGHT):
            desc(block, way).start()

    def take_p(level):
        block = device_of(level, 1 - p, q, core)
        got(block)
        for way in (TOP, HEIGHT):
            desc(block, way).start()

    def take_q(level):
        for mid in (p, 1 - p):
            block = device_of(level, mid, 1 - q, core)
            got(block)
            desc(block, HEIGHT).start()
        for chip in range(HEIGHT):
            got(level * LEVEL + chip * TWO + 1 - core)

    def step(t, carry):
        pl.when(t < TOP)(lambda: take_z(far_level(z, TWO - lax.rem(t, TOP))))
        pl.when(t < HEIGHT)(lambda: take_p(far_level(z, TOP - lax.rem(t, HEIGHT))))

        @pl.when(t > 0)
        def _():
            level = far_level(z, HEIGHT - (t + lax.div(HEIGHT - t, HEIGHT)))
            take_q(level)
            work(t, level)
        return carry

    lax.fori_loop(0, 5, step, 0)
    for level in range(HEIGHT):
        desc(device_of(level, p, q, core), TWO).wait_send()
        for mid in range(TWO):
            desc(device_of(level, mid, q, core), TOP).wait_send()
        pl.when(jnp.logical_and(z < TOP, level <= z))(lambda: desc(device_of(level, p, q, core), 0).wait_send())
        pl.when(jnp.logical_and(z > 0, level >= z))(lambda: desc(device_of(level, p, q, core), 1).wait_send())
    for chip in range(CHIPS):
        desc(chip * TWO + core, HEIGHT).wait_send()


def add_into(dst, srcs, rows):
    step = 32

    def body(i, carry):
        sl = pl.ds(pl.multiple_of(i * step, step), step)
        total = srcs[0][sl, :].astype(F32)
        for src in srcs[1:]:
            total = total + src[sl, :].astype(F32)
        dst[sl, :] = total.astype(dst.dtype)
        return carry

    lax.fori_loop(0, rows // step, body, 0)


def scatter_scratch(rows, cols):
    return [
        pltpu.VMEM((CHIPS, rows, cols), BF16), pltpu.VMEM((LEVEL, rows, cols), BF16), pltpu.VMEM((HEIGHT, rows, cols), BF16),
        pltpu.VMEM((HEIGHT, rows, cols), BF16), pltpu.VMEM((HEIGHT, rows, cols), BF16), pltpu.VMEM((CHIPS, rows, cols), BF16),
        pltpu.VMEM((rows, cols), F32),
        pltpu.SemaphoreType.DMA((TWO, CHIPS)), pltpu.SemaphoreType.DMA((TWO, LEVEL)), pltpu.SemaphoreType.DMA((TWO, HEIGHT)),
        pltpu.SemaphoreType.DMA((TWO, HEIGHT)), pltpu.SemaphoreType.DMA((TWO, HEIGHT)),
    ]


def scatter_levels(in_ref, out_ref, scratch, place, work, hook=None):
    from_core, from_q, from_p, from_low, from_high, outgo, acc, sem_c, sem_q, sem_p, sem_up, sem_dn = scratch
    me, z, p, q, core = place
    rows = out_ref.shape[0]
    other = 1 - core

    def core_copy(chip):
        return remote(in_ref.at[chip * TWO + other], from_core.at[chip], sem_c, chip, me + 1 - TWO * core)

    def local(level, mid, last):
        return level * HEIGHT + mid * TWO + last

    def q_copy(level, mid):
        return remote(outgo.at[local(level, mid, 1 - q)], from_q.at[level * TWO + mid], sem_q, level * TWO + mid,
                      device_of(z, p, 1 - q, core))

    def p_copy(level):
        return remote(outgo.at[local(level, 1 - p, q)], from_p.at[level], sem_p, level, device_of(z, 1 - p, q, core))

    def up_copy(level):
        return remote(outgo.at[local(level, p, q)], from_low.at[level], sem_up, level, me + LEVEL)

    def dn_copy(level):
        return remote(outgo.at[local(level, p, q)], from_high.at[level], sem_dn, level, me - LEVEL)

    def own(level, mid, last):
        chip = chip_of(level, mid, last, core)
        core_copy(chip).wait_recv()
        return [in_ref.at[chip * TWO + core], from_core.at[chip]]

    def make(level):
        work(level)
        for last in (1 - p, p):
            for mid in (1 - q, q):
                core_copy(chip_of(level, mid, last, other)).start()

    def send_q(level):
        for mid in (1 - p, p):
            add_into(outgo.at[local(level, mid, 1 - q)], own(level, mid, 1 - q), rows)
            q_copy(level, mid).start()

    def send_p(level):
        side = own(level, 1 - p, q)
        q_copy(level, 1 - p).wait_recv()
        add_into(outgo.at[local(level, 1 - p, q)], side + [from_q.at[level * TWO + 1 - p]], rows)
        p_copy(level).start()

    def gather_here(level):
        mine = own(level, p, q)
        q_copy(level, p).wait_recv()
        p_copy(level).wait_recv()
        return mine + [from_q.at[level * TWO + p], from_p.at[level]]

    def send_z(level):
        add_into(acc, gather_here(level), rows)

        @pl.when(level > z)
        def _():
            @pl.when(z > 0)
            def _():
                up_copy(level).wait_recv()
                add_into(acc, [acc, from_low.at[level]], rows)
            add_into(outgo.at[local(level, p, q)], [acc], rows)
            up_copy(level).start()

        @pl.when(level < z)
        def _():
            @pl.when(z < TOP)
            def _():
                dn_copy(level).wait_recv()
                add_into(acc, [acc, from_high.at[level]], rows)
            add_into(outgo.at[local(level, p, q)], [acc], rows)
            dn_copy(level).start()

    def level_at(t):
        return far_level(z, lax.rem(t, HEIGHT))

    def step(t, carry):
        if hook is not None:
            hook(t)
        pl.when(t < HEIGHT)(lambda: make(level_at(t)))
        pl.when(jnp.logical_and(t > 0, t < 5))(lambda: send_q(level_at(t + TOP)))
        pl.when(jnp.logical_and(t > 1, t < 6))(lambda: send_p(level_at(t + TWO)))
        pl.when(t > TWO)(lambda: send_z(level_at(t + 1)))
        return carry

    lax.fori_loop(0, 6, step, 0)
    add_into(out_ref, gather_here(z), rows)

    @pl.when(z > 0)
    def _():
        up_copy(z).wait_recv()
        add_into(out_ref, [out_ref, from_low.at[z]], rows)

    @pl.when(z < TOP)
    def _():
        dn_copy(z).wait_recv()
        add_into(out_ref, [out_ref, from_high.at[z]], rows)

    for chip in range(CHIPS):
        core_copy(chip).wait_send()
    for level in range(HEIGHT):
        for mid in range(TWO):
            q_copy(level, mid).wait_send()
        p_copy(level).wait_send()
        pl.when(level > z)(lambda: up_copy(level).wait_send())
        pl.when(level < z)(lambda: dn_copy(level).wait_send())


def rank_of(p, q, core):
    return device_of(0, p, q, core)


def level_gather(in_ref, out_ref, send_sem, recv_sem, place):
    me, z, p, q, core = place
    rank = lax.rem(me, LEVEL)
    peers = (device_of(z, 1 - p, q, core), device_of(z, p, 1 - q, core), me + 1 - TWO * core)

    def desc(block, way, src=None):
        return pltpu.make_async_remote_copy(
            src_ref=out_ref.at[block] if src is None else src, dst_ref=out_ref.at[block],
            send_sem=send_sem.at[way * LEVEL + block], recv_sem=recv_sem.at[block],
            device_id=(peers[way],), device_id_type=MESH)

    for way in (1, 0, TWO):
        desc(rank, way, in_ref).start()
    out_ref[rank] = in_ref[...]
    side = rank_of(1 - p, q, core)
    desc(side, 0).wait_recv()
    for way in (1, TWO):
        desc(side, way).start()
    for mid in (p, 1 - p):
        block = rank_of(mid, 1 - q, core)
        desc(block, 1).wait_recv()
        desc(block, TWO).start()
    for chip in range(HEIGHT):
        desc(chip * TWO + 1 - core, TWO).wait_recv()
    desc(rank, 0, in_ref).wait_send()
    desc(rank, 1, in_ref).wait_send()
    desc(side, 1).wait_send()
    for chip in range(HEIGHT):
        desc(chip * TWO + core, TWO).wait_send()


def level_scatter(in_ref, out_ref, from_core, from_q, from_p, outgo, sem_s, sem_r, place):
    me, z, p, q, core = place
    rows = out_ref.shape[0]

    def copy(src, dst, slot, dev):
        return pltpu.make_async_remote_copy(
            src_ref=src, dst_ref=dst, send_sem=sem_s.at[slot], recv_sem=sem_r.at[slot],
            device_id=(dev,), device_id_type=MESH)

    def core_copy(chip):
        return copy(in_ref.at[chip * TWO + 1 - core], from_core.at[chip], chip, me + 1 - TWO * core)

    def q_copy(mid):
        return copy(outgo.at[mid], from_q.at[mid], HEIGHT + mid, device_of(z, p, 1 - q, core))

    def p_copy():
        return copy(outgo.at[TWO], from_p, 6, device_of(z, 1 - p, q, core))

    def own(mid, last):
        chip = chip_of(0, mid, last, core)
        core_copy(chip).wait_recv()
        return [in_ref.at[chip * TWO + core], from_core.at[chip]]

    for last in (1 - p, p):
        for mid in (1 - q, q):
            core_copy(chip_of(0, mid, last, 1 - core)).start()
    for mid in (1 - p, p):
        add_into(outgo.at[mid], own(mid, 1 - q), rows)
        q_copy(mid).start()
    side = own(1 - p, q)
    q_copy(1 - p).wait_recv()
    add_into(outgo.at[TWO], side + [from_q.at[1 - p]], rows)
    p_copy().start()
    mine = own(p, q)
    q_copy(p).wait_recv()
    p_copy().wait_recv()
    add_into(out_ref, mine + [from_q.at[p], from_p], rows)
    for chip in range(HEIGHT):
        core_copy(chip).wait_send()
    for mid in range(TWO):
        q_copy(mid).wait_send()
    p_copy().wait_send()


def dot(left, right, ld, rd):
    return lax.dot_general(left, right, (((ld,), (rd,)), ((), ())), preferred_element_type=F32)


TOKS = 512
VPAD = 1024
VROWS = 1004


def id_rows(tok_ref, row, first):
    ids = jnp.concatenate([tok_ref[first + t, row:row + 1, :] for t in range(HEIGHT)], axis=1) - shard_start()
    return jnp.where(jnp.logical_and(ids >= 0, ids < VROWS), ids, -1)


def vocab_iota():
    return lax.broadcasted_iota(jnp.int32, (VPAD, TOKS), 0)


def shard_start():
    return lax.axis_index('fsdp') * VROWS


def fill_table(table, emb_ref):
    table[VPAD - 32:VPAD, :] = jnp.zeros((32, DIM), BF16)
    table[0:VROWS, :] = emb_ref[...]


def halves(level, body):
    def one(i, carry):
        body(level * LEVEL + i * HEIGHT)
        return carry
    lax.fori_loop(0, TWO, one, 0)


def rms_inv(values):
    return lax.rsqrt(jnp.mean(values * values, axis=-1, keepdims=True) + NORM_EPS)


def rms_backward(values, inv_rms, gain_vec, grad_out):
    scaled = grad_out * gain_vec
    return inv_rms * scaled - values * (inv_rms ** TOP) * jnp.mean(scaled * values, axis=-1, keepdims=True)


LEVEL_SCRATCH = [
    pltpu.VMEM((LANE, DIM), BF16), pltpu.VMEM((LEVEL, LANE, DIM), BF16), pltpu.VMEM((LANE, DIM), F32),
    pltpu.VMEM((HEIGHT, LANE, DIM), BF16), pltpu.VMEM((TWO, LANE, DIM), BF16), pltpu.VMEM((LANE, DIM), BF16),
    pltpu.VMEM((TOP, LANE, DIM), BF16),
    pltpu.SemaphoreType.DMA((GROWS,)), pltpu.SemaphoreType.DMA((LEVEL,)),
    pltpu.SemaphoreType.DMA((7,)), pltpu.SemaphoreType.DMA((7,)),
]


def split_weights(gu_ref):
    wide = gu_ref[...].astype(F32)
    return (wide[:, 0:GROWS, :].reshape(DIM, UNITS).astype(BF16), wide[:, GROWS:PAIR, :].reshape(DIM, UNITS).astype(BF16))


GU_SHAPE = (NDEV, PAIR, UNITS)
WD_SHAPE = (HEIGHT, DROWS, DIM)


def call(kernel, name, cid, outs, ins, scratch):
    return pl.pallas_call(
        kernel, out_shape=outs, in_specs=[VSPEC] * len(ins), out_specs=(VSPEC,) * len(outs), scratch_shapes=scratch,
        compiler_params=pltpu.CompilerParams(collective_id=cid, has_side_effects=True, vmem_limit_bytes=VMEM_CAP),
        name=name)(*ins)


def flip_x(p, q, core):
    return p * core + (1 - p) * (1 - core), q * (1 - core) + (1 - q) * core, core


def flip_y(p, q, core):
    return p * (1 - core) + (1 - p) * core, q * core + (1 - q) * (1 - core), core


STAT = 40


def merge_stats(blocks):
    logs = [b[0:32, :] for b in blocks]
    top = logs[0]
    for one in logs[1:]:
        top = jnp.maximum(top, one)
    total = jnp.exp(logs[0] - top)
    labs = blocks[0][32:STAT, :]
    for one, b in zip(logs[1:], blocks[1:]):
        total = total + jnp.exp(one - top)
        labs = labs + b[32:STAT, :]
    return jnp.concatenate([top + jnp.log(total), labs], axis=0)


def step_call(ids, labs, emb, pieces, down_shard, gain_mlp, gain_final, emb_scale, inv_count):
    def kernel(ids_ref, lab_ref, emb_ref, piece_ref, down_ref, gm_ref, gf_ref,
               demb_ref, own_ref, dn_ref, loss_ref,
               tok_mine, tok_ref, table, spread, whole, gu_ref, wd_ref, a_ref, g_ref, u_ref, dm_ref,
               d_gate, d_up, acts, grad_gate, grad_up, grad_down, ggu, gd, land_g, land_d, outgo, outgo_d, acc,
               block, x_ref, h_ref, dh_ref, dhn_ref, stat, land, land_z, lse_ref,
               sem_t, sem_a, z_send, z_recv, d_send, d_recv, g_send, g_recv, e_send, e_recv, sem_s, sem_b, sem_z, sem_d,
               *scratch):
        ring, (mine, parts, total, *level) = scratch[:12], scratch[12:]
        place = my_place()
        me, z, p, q, core = place
        rank = lax.rem(me, LEVEL)
        gain_m, gain_f = gm_ref[...].reshape(1, DIM), gf_ref[...].reshape(1, DIM)
        tok_mine[...] = jnp.zeros((LEVEL, LANE), jnp.int32)
        tok_mine[0:1, :] = ids_ref[...]
        tok_mine[1:TWO, :] = lab_ref[...]
        barrier_peers(place)

        def exchange(step):
            peer = lax.rem(rank + step, LEVEL)
            return remote(piece_ref.at[peer], gu_ref.at[me], sem_a, step, z * LEVEL + peer)

        def rows_of(ref, lv):
            return ref.at[pl.ds(lv * LEVEL, LEVEL)]

        def slab(lv, way):
            part = rows_of(gu_ref, lv)
            return pltpu.make_async_remote_copy(
                src_ref=part, dst_ref=part, send_sem=z_send.at[way * HEIGHT + lv], recv_sem=z_recv.at[lv],
                device_id=(me + LEVEL - CHIPS * way,), device_id_type=MESH)

        def slab_down(lv, way, src):
            return pltpu.make_async_remote_copy(
                src_ref=src, dst_ref=wd_ref.at[lv], send_sem=d_send.at[way * HEIGHT + lv], recv_sem=d_recv.at[lv],
                device_id=(me + LEVEL - CHIPS * way,), device_id_type=MESH)

        devs = (me + 1 - TWO * core, device_of(z, *flip_x(p, q, core)), device_of(z, *flip_y(p, q, core)))
        pair = remote(tok_mine, tok_ref.at[me], sem_t, 0, devs[0])
        pair.start()
        for step in range(1, LEVEL):
            exchange(step).start()
        pl.when(z < TOP)(lambda: slab_down(z, 0, down_ref).start())
        pl.when(z > 0)(lambda: slab_down(z, 1, down_ref).start())
        tok_ref[me] = tok_mine[...]
        wd_ref[z] = down_ref[...]
        gu_ref[me] = piece_ref[rank]
        fill_table(table, emb_ref)
        stat[...] = jnp.zeros_like(stat)
        demb_ref[...] = jnp.zeros_like(demb_ref)
        pair.wait()
        for stage, size in ((1, TWO), (TWO, HEIGHT)):
            part = tok_ref.at[pl.ds(lax.div(me, size) * size, size)]
            ship = remote(part, part, sem_t, stage, devs[stage])
            ship.start()
            ship.wait()
        part = rows_of(tok_ref, z)
        ships = [remote(part, part, sem_t, TWO + step, lax.rem(me + LEVEL * step, NDEV)) for step in range(1, HEIGHT)]
        for ship in ships:
            ship.start()
        for ship in ships:
            ship.wait()
        for step in range(1, LEVEL):
            exchange(step).wait_recv()
        pl.when(z < TOP)(lambda: slab(z, 0).start())
        pl.when(z > 0)(lambda: slab(z, 1).start())

        def take(lv, way, more):
            slab_down(lv, 0, wd_ref.at[lv]).wait_recv()
            pl.when(more)(lambda: slab_down(lv, way, wd_ref.at[lv]).start())
            slab(lv, 0).wait_recv()
            pl.when(more)(lambda: slab(lv, way).start())

        def take_far(far):
            pl.when(z - far >= 0)(lambda: take(z - far, 0, z < TOP))
            pl.when(z + far < HEIGHT)(lambda: take(z + far, 1, z > 0))

        def hit_rows(first):
            return (vocab_iota() == id_rows(tok_ref, 0, first)).astype(F32).astype(BF16)

        def find(lv):
            def body(first):
                spread[pl.ds(first, HEIGHT)] = dot(hit_rows(first), table[...], 0, 0).astype(BF16).reshape(HEIGHT, LANE, DIM)
            halves(lv, body)

        scatter_levels(spread, x_ref, ring, place, find, lambda t: pl.when(t == HEIGHT)(lambda: take_far(1)))
        take_far(TWO)
        x = x_ref[...] * emb_scale
        mine[...] = (x * rms_inv(x) * gain_m).astype(BF16)
        level_gather(mine, a_ref, level[HEIGHT], level[5], place)
        take_far(TOP)
        for half in range(TWO):
            four = slice(HEIGHT * half, HEIGHT * half + HEIGHT)
            wg, wu = split_weights(gu_ref)
            act_in = a_ref[four].reshape(TOKS, DIM)
            g = dot(act_in, wg, 1, 0).astype(BF16)
            u = dot(act_in, wu, 1, 0).astype(BF16)
            g_ref[half] = g
            u_ref[half] = u
            act = (jax.nn.silu(g.astype(F32)) * u.astype(F32)).astype(BF16)
            acts[half] = act
            parts[four] = dot(act, wd_ref[...].reshape(UNITS, DIM), 1, 0).astype(BF16).reshape(HEIGHT, LANE, DIM)
        level_scatter(parts, total, *level[:HEIGHT], *level[6:], place)
        h_ref[...] = (x_ref[...] * emb_scale + total[...].astype(BF16).astype(F32)).astype(BF16)
        h32 = h_ref[...].astype(F32)
        block[...] = (h32 * rms_inv(h32) * gain_f).astype(BF16)
        for step in range(1, LEVEL):
            exchange(step).wait_send()

        def sent(lv, way):
            slab(lv, way).wait_send()
            slab_down(lv, way, wd_ref.at[lv]).wait_send()

        def forward(t, lv):
            def body(first):
                logits = dot(table[...], whole[pl.ds(first, HEIGHT)].reshape(TOKS, DIM), 1, 1)
                row = vocab_iota()
                lab = jnp.sum(jnp.where(row == id_rows(tok_ref, 1, first), logits, 0.0), axis=0, keepdims=True)
                logits = jnp.where(row < VROWS, logits, -1e30)
                top = jnp.max(logits, axis=0, keepdims=True)
                local = top + jnp.log(jnp.sum(jnp.exp(logits - top), axis=0, keepdims=True))
                for t in range(HEIGHT):
                    stat[0, pl.ds(first + t, 1), :] = local[:, t * LANE:(t + 1) * LANE]
                    stat[0, 32:33, :] = stat[0, 32:33, :] + lab[:, t * LANE:(t + 1) * LANE]
            halves(lv, body)

        gather_levels(block, whole, g_send, g_recv, place, forward)
        for lv in range(HEIGHT):
            pl.when(jnp.logical_and(z < TOP, lv <= z))(lambda: sent(lv, 0))
            pl.when(jnp.logical_and(z > 0, lv >= z))(lambda: sent(lv, 1))

        for stage, dev in enumerate(devs):
            ship = remote(stat.at[stage], land.at[stage], sem_s, stage, dev)
            ship.start()
            ship.wait()
            stat[stage + 1] = merge_stats([stat[stage], land[stage]])
        ships = [remote(stat.at[TOP], land_z.at[z], sem_s, TWO + step, lax.rem(me + LEVEL * step, NDEV)) for step in range(1, HEIGHT)]
        for ship in ships:
            ship.start()
        land_z[z] = stat[TOP]
        for ship in ships:
            ship.wait()
        final = merge_stats([land_z[lv] for lv in range(HEIGHT)])
        lse_ref[...] = final[0:32, :]
        loss_ref[...] = jnp.full((LEVEL, LANE), (jnp.sum(final[0:32, :]) - jnp.sum(final[32:STAT, :])) * inv_count, F32)

        def backward(lv):
            def body(first):
                hid = whole[pl.ds(first, HEIGHT)].reshape(TOKS, DIM)
                logits = dot(table[...], hid, 1, 1)
                lse_row = jnp.concatenate([lse_ref[pl.ds(first + t, 1), :] for t in range(HEIGHT)], axis=1)
                row = vocab_iota()
                prob = jnp.exp(jnp.where(row < VROWS, logits, -1e30) - lse_row)
                hit = jnp.where(row == id_rows(tok_ref, 1, first), 1.0, 0.0)
                grad = ((prob - hit) * inv_count).astype(BF16)
                spread[pl.ds(first, HEIGHT)] = dot(grad, table[...], 0, 0).astype(BF16).reshape(HEIGHT, LANE, DIM)
                demb_ref[...] += dot(grad, hid, 1, 0)
            halves(lv, body)

        scatter_levels(spread, dhn_ref, ring, place, backward)

        h32 = h_ref[...].astype(F32)
        dh_ref[...] = rms_backward(h32, rms_inv(h32), gain_f, dhn_ref[...])
        mine[...] = dh_ref[...].astype(BF16)
        level_gather(mine, dm_ref, level[HEIGHT], level[5], place)
        for half in range(TWO):
            four = slice(HEIGHT * half, HEIGHT * half + HEIGHT)
            wg, wu = split_weights(gu_ref)
            g = g_ref[half].astype(F32)
            u = u_ref[half].astype(F32)
            dq = dot(dm_ref[four].reshape(TOKS, DIM), wd_ref[...].reshape(UNITS, DIM), 1, 1)
            sig = jax.nn.sigmoid(g)
            dg = (dq * u * sig * (1.0 + g * (1.0 - sig))).astype(BF16)
            du = (dq * g * sig).astype(BF16)
            d_gate[half] = dg
            d_up[half] = du
            parts[four] = (dot(dg, wg, 1, 1) + dot(du, wu, 1, 1)).astype(BF16).reshape(HEIGHT, LANE, DIM)
        level_scatter(parts, total, *level[:HEIGHT], *level[6:], place)
        x = x_ref[...] * emb_scale
        block[...] = (dh_ref[...] + rms_backward(x, rms_inv(x), gain_m, total[...])).astype(BF16)

        def add_slab(dst, srcs):
            def body(i, carry):
                value = srcs[0][i].astype(F32)
                for src in srcs[1:]:
                    value = value + src[i].astype(F32)
                dst[i] = value.astype(dst.dtype)
                return carry
            lax.fori_loop(0, LEVEL, body, 0)

        def hop(lv, way, here=False):
            land = rows_of(land_g, HEIGHT if here and way else lv)
            return remote(rows_of(outgo, lv), land, sem_z, way * HEIGHT + lv, me + LEVEL - CHIPS * way)

        def hop_d(lv, way, here=False):
            return remote(outgo_d.at[lv], land_d.at[HEIGHT if here and way else lv], sem_d, way * HEIGHT + lv, me + LEVEL - CHIPS * way)

        def send(lv, way, more, here):
            @pl.when(more)
            def _():
                hop(lv, way).wait_recv()
                add_slab(rows_of(outgo, lv), [rows_of(ggu, lv), rows_of(land_g, lv)])
                hop_d(lv, way).wait_recv()
                add_into(outgo_d.at[lv], [gd.at[lv], land_d.at[lv]], DROWS)

            @pl.when(jnp.logical_not(more))
            def _():
                add_slab(rows_of(outgo, lv), [rows_of(ggu, lv)])
                add_into(outgo_d.at[lv], [gd.at[lv]], DROWS)
            hop(lv, way, here).start()
            hop_d(lv, way, here).start()

        def send_far(far):
            pl.when(z + far < HEIGHT)(lambda: send(z + far, 0, z > 0, far == 1))
            pl.when(z - far >= 0)(lambda: send(z - far, 1, z < TOP, far == 1))

        def weight_grads():
            for half in range(TWO):
                four = slice(HEIGHT * half, HEIGHT * half + HEIGHT)
                act_in = a_ref[four].reshape(TOKS, DIM)
                news = (dot(act_in, d_gate[half], 0, 0), dot(act_in, d_up[half], 0, 0),
                        dot(acts[half], dm_ref[four].reshape(TOKS, DIM), 0, 0))
                for ref, new in zip((grad_gate, grad_up, grad_down), news):
                    ref[...] = new if half == 0 else ref[...] + new
            both = jnp.concatenate([grad_gate[...].reshape(NDEV, GROWS, UNITS), grad_up[...].reshape(NDEV, GROWS, UNITS)], axis=1)
            ggu[...] = both.astype(BF16)
            gd[...] = grad_down[...].astype(BF16).reshape(WD_SHAPE)

        def add_rows(t, lv):
            def body(first):
                demb_ref[...] += dot(hit_rows(first), whole[pl.ds(first, HEIGHT)].reshape(TOKS, DIM), 1, 0) * emb_scale
            halves(lv, body)

            @pl.when(t == 1)
            def _():
                weight_grads()
                send_far(TOP)
            pl.when(t == TWO)(lambda: send_far(TWO))
            pl.when(t == TOP)(lambda: send_far(1))

        gather_levels(block, whole, e_send, e_recv, place, add_rows)
        add_slab(acc, [rows_of(ggu, z)])
        add_into(dn_ref, [gd.at[z]], DROWS)

        def last(way):
            hop(z, way).wait_recv()
            add_slab(acc, [acc, rows_of(land_g, HEIGHT if way else z)])
            hop_d(z, way).wait_recv()
            add_into(dn_ref, [dn_ref, land_d.at[HEIGHT if way else z]], DROWS)

        pl.when(z > 0)(lambda: last(0))
        pl.when(z < TOP)(lambda: last(1))

        def give(step):
            peer = lax.rem(rank + step, LEVEL)
            return remote(acc.at[peer], own_ref.at[rank], sem_b, step, z * LEVEL + peer)

        for step in range(1, LEVEL):
            give(step).start()
        own_ref[rank] = acc[rank]
        for step in range(1, LEVEL):
            give(step).wait_recv()
        for step in range(1, LEVEL):
            give(step).wait_send()

        def gone(lv, way):
            hop(lv, way).wait_send()
            hop_d(lv, way).wait_send()

        for lv in range(HEIGHT):
            pl.when(lv > z)(lambda: gone(lv, 0))
            pl.when(lv < z)(lambda: gone(lv, 1))

    whole = pltpu.VMEM((NDEV, LANE, DIM), BF16)
    block, flat = pltpu.VMEM((LANE, DIM), BF16), pltpu.VMEM((LANE, DIM), F32)
    slab, slab_d = pltpu.VMEM(GU_SHAPE, BF16), pltpu.VMEM(WD_SHAPE, BF16)
    unit, eight = pltpu.VMEM((TWO, TOKS, UNITS), BF16), pltpu.VMEM((LEVEL, LANE, DIM), BF16)
    wide, tall = pltpu.VMEM((DIM, UNITS), F32), pltpu.VMEM((UNITS, DIM), F32)
    dma = pltpu.SemaphoreType.DMA
    return call(
        kernel, 'step', 0,
        (jax.ShapeDtypeStruct((VPAD, DIM), F32), jax.ShapeDtypeStruct((LEVEL, PAIR, UNITS), F32),
         jax.ShapeDtypeStruct((DROWS, DIM), F32), jax.ShapeDtypeStruct((LEVEL, LANE), F32)),
        (ids, labs, emb, pieces, down_shard, gain_mlp, gain_final),
        [pltpu.VMEM((LEVEL, LANE), jnp.int32), pltpu.VMEM((NDEV, LEVEL, LANE), jnp.int32), pltpu.VMEM((VPAD, DIM), BF16), whole, whole,
         slab, slab_d, eight, unit, unit, eight, unit, unit, unit, wide, wide, tall, slab, slab_d,
         pltpu.VMEM((5 * LEVEL, PAIR, UNITS), BF16), pltpu.VMEM((5, DROWS, DIM), BF16), slab, slab_d,
         pltpu.VMEM((LEVEL, PAIR, UNITS), F32), block, flat, block, flat, flat,
         pltpu.VMEM((HEIGHT, STAT, LANE), F32), pltpu.VMEM((TOP, STAT, LANE), F32), pltpu.VMEM((HEIGHT, STAT, LANE), F32),
         pltpu.VMEM((32, LANE), F32),
         sem_pair(6), sem_pair(LEVEL), dma((LEVEL,)), dma((HEIGHT,)), dma((LEVEL,)), dma((HEIGHT,)), dma((5, NDEV)), dma((NDEV,)),
         dma((5, NDEV)), dma((NDEV,)), sem_pair(6), sem_pair(LEVEL), sem_pair(LEVEL), sem_pair(LEVEL)]
        + scatter_scratch(LANE, DIM) + LEVEL_SCRATCH)


def solution(mesh):
    group = mesh.shape['fsdp']

    def local_step(ids_blk, lab_blk, emb_shard, gate_shard, up_shard, down_shard, gain_mlp, gain_final):
        emb_scale = math.sqrt(emb_shard.shape[1])
        inv_count = 1.0 / (ids_blk.size * group)
        pieces = jnp.concatenate([gate_shard, up_shard], axis=0).reshape(PAIR, HEIGHT, LEVEL, DROWS)
        pieces = pieces.transpose(TWO, 0, 1, TOP).reshape(LEVEL, PAIR, UNITS)
        d_embed, d_gu, d_down, loss = step_call(
            ids_blk, lab_blk, emb_shard, pieces, down_shard, gain_mlp, gain_final, emb_scale, inv_count)
        d_gu = d_gu.reshape(LEVEL, PAIR, HEIGHT, DROWS).transpose(1, TWO, 0, TOP).reshape(PAIR, 3072)
        return loss[0, 0], d_embed[0:VROWS], d_gu[0:GROWS], d_gu[GROWS:PAIR], d_down

    shard_spec = P('fsdp', None)
    return jax.shard_map(local_step, mesh=mesh, in_specs=(shard_spec, shard_spec, shard_spec, shard_spec, shard_spec, shard_spec, P(), P()), out_specs=(P(), shard_spec, shard_spec, shard_spec, shard_spec), check_vma=False)
```

```python
import math
import jax
import jax.numpy as jnp
from jax import lax
from jax.experimental import pallas as pl
from jax.experimental.pallas import tpu as pltpu
from jax.sharding import PartitionSpec as P

NORM_EPS = 1e-6
MESH = pl.DeviceIdType.MESH
F32 = jnp.float32
BF16 = jnp.bfloat16
VMEM_CAP = 63 * 1024 * 1024
LANE = 128
DIM = 768
PAIR = 48
UNITS = 384
NDEV = 32
LEVEL = 8
HEIGHT = 4
DROWS = 96
CHIPS = 16
GROWS = 24
TWO = 2
TOP = 3
VSPEC = pl.BlockSpec(memory_space=pltpu.VMEM)


def my_place():
    me = lax.axis_index('fsdp')
    core = lax.rem(me, TWO)
    x = lax.rem(lax.div(me, TWO), TWO)
    y = lax.rem(lax.div(me, HEIGHT), TWO)
    z = lax.div(me, LEVEL)
    p = x * (1 - core) + y * core
    q = y * (1 - core) + x * core
    return me, z, p, q, core


def chip_of(z, p, q, core):
    x = p * (1 - core) + q * core
    y = q * (1 - core) + p * core
    return (z * TWO + y) * TWO + x


def device_of(z, p, q, core):
    return chip_of(z, p, q, core) * TWO + core


def barrier_peers(place):
    me, z = place[0], place[1]
    sem = pltpu.get_barrier_semaphore()
    for step in range(1, LEVEL):
        dev = z * LEVEL + lax.rem(me + step, LEVEL)
        pl.semaphore_signal(sem, inc=1, device_id=(dev,), device_id_type=MESH)
    for step in range(1, HEIGHT):
        dev = lax.rem(me + LEVEL * step, NDEV)
        pl.semaphore_signal(sem, inc=1, device_id=(dev,), device_id_type=MESH)
    pl.semaphore_wait(sem, 10)


def far_level(z, at):
    half = lax.div(z, TWO)
    inner = lax.rem(z + half, TWO)
    order = (TOP - TOP * half, (1 - inner) * (TWO - half) + inner * TOP * half, 1 + lax.rem(z, TWO), z)
    if isinstance(at, int):
        return order[at]
    low, high = lax.rem(at, TWO), lax.div(at, TWO)
    return ((1 - low) * (1 - high) * order[0] + low * (1 - high) * order[1]
            + (1 - low) * high * order[TWO] + low * high * order[TOP])


def remote(src, dst, sems, slot, dev):
    return pltpu.make_async_remote_copy(
        src_ref=src, dst_ref=dst, send_sem=sems.at[0, slot], recv_sem=sems.at[1, slot],
        device_id=(dev,), device_id_type=MESH)


def sem_pair(n):
    return pltpu.SemaphoreType.DMA((TWO, n))


def gather_levels(in_ref, out_ref, send_sem, recv_sem, place, work, hook=None):
    me, z, p, q, core = place
    peers = (me + LEVEL, me - LEVEL, device_of(z, 1 - p, q, core), device_of(z, p, 1 - q, core), me + 1 - TWO * core)

    def desc(block, way, src=None):
        return pltpu.make_async_remote_copy(
            src_ref=out_ref.at[block] if src is None else src, dst_ref=out_ref.at[block],
            send_sem=send_sem.at[way, block], recv_sem=recv_sem.at[block],
            device_id=(peers[way],), device_id_type=MESH)

    def got(block):
        desc(block, HEIGHT).wait_recv()

    pl.when(z < TOP)(lambda: desc(me, 0, in_ref).start())
    pl.when(z > 0)(lambda: desc(me, 1, in_ref).start())
    for way in (TOP, TWO, HEIGHT):
        desc(me, way, in_ref).start()
    out_ref[me] = in_ref[...]

    def take_z(level):
        block = device_of(level, p, q, core)
        got(block)
        pl.when(jnp.logical_and(level < z, z < TOP))(lambda: desc(block, 0).start())
        pl.when(jnp.logical_and(level > z, z > 0))(lambda: desc(block, 1).start())
        for way in (TOP, TWO, HEIGHT):
            desc(block, way).start()

    def take_p(level):
        block = device_of(level, 1 - p, q, core)
        got(block)
        for way in (TOP, HEIGHT):
            desc(block, way).start()

    def take_q(level):
        for mid in (p, 1 - p):
            block = device_of(level, mid, 1 - q, core)
            got(block)
            desc(block, HEIGHT).start()
        for chip in range(HEIGHT):
            got(level * LEVEL + chip * TWO + 1 - core)

    def step(t, carry):
        if hook is not None:
            hook(t)
        pl.when(t < TOP)(lambda: take_z(far_level(z, TWO - lax.rem(t, TOP))))
        pl.when(t < HEIGHT)(lambda: take_p(far_level(z, TOP - lax.rem(t, HEIGHT))))

        @pl.when(t > 0)
        def _():
            level = far_level(z, HEIGHT - (t + lax.div(HEIGHT - t, HEIGHT)))
            take_q(level)
            work(level)
        return carry

    lax.fori_loop(0, 5, step, 0)
    for level in range(HEIGHT):
        desc(device_of(level, p, q, core), TWO).wait_send()
        for mid in range(TWO):
            desc(device_of(level, mid, q, core), TOP).wait_send()
        pl.when(jnp.logical_and(z < TOP, level <= z))(lambda: desc(device_of(level, p, q, core), 0).wait_send())
        pl.when(jnp.logical_and(z > 0, level >= z))(lambda: desc(device_of(level, p, q, core), 1).wait_send())
    for chip in range(CHIPS):
        desc(chip * TWO + core, HEIGHT).wait_send()


def add_into(dst, srcs, rows):
    step = 32

    def body(i, carry):
        sl = pl.ds(pl.multiple_of(i * step, step), step)
        total = srcs[0][sl, :].astype(F32)
        for src in srcs[1:]:
            total = total + src[sl, :].astype(F32)
        dst[sl, :] = total.astype(dst.dtype)
        return carry

    lax.fori_loop(0, rows // step, body, 0)


def scatter_scratch(rows, cols):
    return [
        pltpu.VMEM((CHIPS, rows, cols), BF16), pltpu.VMEM((LEVEL, rows, cols), BF16), pltpu.VMEM((HEIGHT, rows, cols), BF16),
        pltpu.VMEM((HEIGHT, rows, cols), BF16), pltpu.VMEM((HEIGHT, rows, cols), BF16), pltpu.VMEM((CHIPS, rows, cols), BF16),
        pltpu.VMEM((rows, cols), F32),
        pltpu.SemaphoreType.DMA((TWO, CHIPS)), pltpu.SemaphoreType.DMA((TWO, LEVEL)), pltpu.SemaphoreType.DMA((TWO, HEIGHT)),
        pltpu.SemaphoreType.DMA((TWO, HEIGHT)), pltpu.SemaphoreType.DMA((TWO, HEIGHT)),
    ]


def scatter_levels(in_ref, out_ref, scratch, place, work, hook=None):
    from_core, from_q, from_p, from_low, from_high, outgo, acc, sem_c, sem_q, sem_p, sem_up, sem_dn = scratch
    me, z, p, q, core = place
    rows = out_ref.shape[0]
    other = 1 - core

    def core_copy(chip):
        return remote(in_ref.at[chip * TWO + other], from_core.at[chip], sem_c, chip, me + 1 - TWO * core)

    def local(level, mid, last):
        return level * HEIGHT + mid * TWO + last

    def q_copy(level, mid):
        return remote(outgo.at[local(level, mid, 1 - q)], from_q.at[level * TWO + mid], sem_q, level * TWO + mid,
                      device_of(z, p, 1 - q, core))

    def p_copy(level):
        return remote(outgo.at[local(level, 1 - p, q)], from_p.at[level], sem_p, level, device_of(z, 1 - p, q, core))

    def up_copy(level):
        return remote(outgo.at[local(level, p, q)], from_low.at[level], sem_up, level, me + LEVEL)

    def dn_copy(level):
        return remote(outgo.at[local(level, p, q)], from_high.at[level], sem_dn, level, me - LEVEL)

    def own(level, mid, last):
        chip = chip_of(level, mid, last, core)
        core_copy(chip).wait_recv()
        return [in_ref.at[chip * TWO + core], from_core.at[chip]]

    y = q * (1 - core) + p * core
    x = p * (1 - core) + q * core

    def make(level, half):
        row = level * HEIGHT + TWO * (y * half + (1 - y) * (1 - half))
        work(row * TWO)
        for side in (1 - x, x):
            core_copy(row + side).start()

    def send_q(level, mid):
        add_into(outgo.at[local(level, mid, 1 - q)], own(level, mid, 1 - q), rows)
        q_copy(level, mid).start()

    def send_p(level):
        side = own(level, 1 - p, q)
        q_copy(level, 1 - p).wait_recv()
        add_into(outgo.at[local(level, 1 - p, q)], side + [from_q.at[level * TWO + 1 - p]], rows)
        p_copy(level).start()

    def gather_here(level):
        mine = own(level, p, q)
        q_copy(level, p).wait_recv()
        p_copy(level).wait_recv()
        return mine + [from_q.at[level * TWO + p], from_p.at[level]]

    def send_z(level):
        add_into(acc, gather_here(level), rows)

        @pl.when(level > z)
        def _():
            @pl.when(z > 0)
            def _():
                up_copy(level).wait_recv()
                add_into(acc, [acc, from_low.at[level]], rows)
            add_into(outgo.at[local(level, p, q)], [acc], rows)
            up_copy(level).start()

        @pl.when(level < z)
        def _():
            @pl.when(z < TOP)
            def _():
                dn_copy(level).wait_recv()
                add_into(acc, [acc, from_high.at[level]], rows)
            add_into(outgo.at[local(level, p, q)], [acc], rows)
            dn_copy(level).start()

    def level_at(t):
        return far_level(z, lax.rem(lax.div(t, TWO), HEIGHT))

    def step(t, carry):
        odd = lax.rem(t, TWO)
        if hook is not None:
            hook(t)
        pl.when(t < LEVEL)(lambda: make(level_at(t), odd))
        pl.when(jnp.logical_and(t > 0, t < 9))(lambda: send_q(level_at(t + 7), odd * (1 - p) + (1 - odd) * p))
        pl.when(jnp.logical_and(t > TWO, odd == 1))(lambda: send_p(level_at(t + 5)))
        pl.when(jnp.logical_and(t > HEIGHT, odd == 1))(lambda: send_z(level_at(t + TOP)))
        return carry

    lax.fori_loop(0, 10, step, 0)
    add_into(out_ref, gather_here(z), rows)

    @pl.when(z > 0)
    def _():
        up_copy(z).wait_recv()
        add_into(out_ref, [out_ref, from_low.at[z]], rows)

    @pl.when(z < TOP)
    def _():
        dn_copy(z).wait_recv()
        add_into(out_ref, [out_ref, from_high.at[z]], rows)

    for chip in range(CHIPS):
        core_copy(chip).wait_send()
    for level in range(HEIGHT):
        for mid in range(TWO):
            q_copy(level, mid).wait_send()
        p_copy(level).wait_send()
        pl.when(level > z)(lambda: up_copy(level).wait_send())
        pl.when(level < z)(lambda: dn_copy(level).wait_send())


def rank_of(p, q, core):
    return device_of(0, p, q, core)


def level_gather(in_ref, out_ref, send_sem, recv_sem, place):
    me, z, p, q, core = place
    rank = lax.rem(me, LEVEL)
    peers = (device_of(z, 1 - p, q, core), device_of(z, p, 1 - q, core), me + 1 - TWO * core)

    def desc(block, way, src=None):
        return pltpu.make_async_remote_copy(
            src_ref=out_ref.at[block] if src is None else src, dst_ref=out_ref.at[block],
            send_sem=send_sem.at[way * LEVEL + block], recv_sem=recv_sem.at[block],
            device_id=(peers[way],), device_id_type=MESH)

    for way in (1, 0, TWO):
        desc(rank, way, in_ref).start()
    out_ref[rank] = in_ref[...]
    side = rank_of(1 - p, q, core)
    desc(side, 0).wait_recv()
    for way in (1, TWO):
        desc(side, way).start()
    for mid in (p, 1 - p):
        block = rank_of(mid, 1 - q, core)
        desc(block, 1).wait_recv()
        desc(block, TWO).start()
    for chip in range(HEIGHT):
        desc(chip * TWO + 1 - core, TWO).wait_recv()
    desc(rank, 0, in_ref).wait_send()
    desc(rank, 1, in_ref).wait_send()
    desc(side, 1).wait_send()
    for chip in range(HEIGHT):
        desc(chip * TWO + core, TWO).wait_send()


def level_scatter(in_ref, out_ref, from_core, from_q, from_p, outgo, sem_s, sem_r, place, hook=None):
    me, z, p, q, core = place
    rows = out_ref.shape[0]

    def copy(src, dst, slot, dev):
        return pltpu.make_async_remote_copy(
            src_ref=src, dst_ref=dst, send_sem=sem_s.at[slot], recv_sem=sem_r.at[slot],
            device_id=(dev,), device_id_type=MESH)

    def core_copy(chip):
        return copy(in_ref.at[chip * TWO + 1 - core], from_core.at[chip], chip, me + 1 - TWO * core)

    def q_copy(mid):
        return copy(outgo.at[mid], from_q.at[mid], HEIGHT + mid, device_of(z, p, 1 - q, core))

    def p_copy():
        return copy(outgo.at[TWO], from_p, 6, device_of(z, 1 - p, q, core))

    def own(mid, last):
        chip = chip_of(0, mid, last, core)
        core_copy(chip).wait_recv()
        return [in_ref.at[chip * TWO + core], from_core.at[chip]]

    for last in (1 - p, p):
        for mid in (1 - q, q):
            core_copy(chip_of(0, mid, last, 1 - core)).start()
    for mid in (1 - p, p):
        add_into(outgo.at[mid], own(mid, 1 - q), rows)
        q_copy(mid).start()
    if hook is not None:
        hook()
    side = own(1 - p, q)
    q_copy(1 - p).wait_recv()
    add_into(outgo.at[TWO], side + [from_q.at[1 - p]], rows)
    p_copy().start()
    mine = own(p, q)
    q_copy(p).wait_recv()
    p_copy().wait_recv()
    add_into(out_ref, mine + [from_q.at[p], from_p], rows)
    for chip in range(HEIGHT):
        core_copy(chip).wait_send()
    for mid in range(TWO):
        q_copy(mid).wait_send()
    p_copy().wait_send()


def dot(left, right, ld, rd):
    return lax.dot_general(left, right, (((ld,), (rd,)), ((), ())), preferred_element_type=F32)


TOKS = 512
VPAD = 1024
VROWS = 1004


def id_rows(tok_ref, row, first):
    ids = jnp.concatenate([tok_ref[first + t, row:row + 1, :] for t in range(HEIGHT)], axis=1) - shard_start()
    return jnp.where(jnp.logical_and(ids >= 0, ids < VROWS), ids, -1)


def vocab_iota():
    return lax.broadcasted_iota(jnp.int32, (VPAD, TOKS), 0)


def shard_start():
    return lax.axis_index('fsdp') * VROWS


def fill_table(table, emb_ref):
    table[VPAD - 32:VPAD, :] = jnp.zeros((32, DIM), BF16)
    table[0:VROWS, :] = emb_ref[...]


def halves(level, body):
    def one(i, carry):
        body(level * LEVEL + i * HEIGHT)
        return carry
    lax.fori_loop(0, TWO, one, 0)


def rms_inv(values):
    return lax.rsqrt(jnp.mean(values * values, axis=-1, keepdims=True) + NORM_EPS)


def rms_backward(values, inv_rms, gain_vec, grad_out):
    scaled = grad_out * gain_vec
    return inv_rms * scaled - values * (inv_rms ** TOP) * jnp.mean(scaled * values, axis=-1, keepdims=True)


LEVEL_SCRATCH = [
    pltpu.VMEM((LANE, DIM), BF16), pltpu.VMEM((LEVEL, LANE, DIM), BF16), pltpu.VMEM((LANE, DIM), F32),
    pltpu.VMEM((HEIGHT, LANE, DIM), BF16), pltpu.VMEM((TWO, LANE, DIM), BF16), pltpu.VMEM((LANE, DIM), BF16),
    pltpu.VMEM((TOP, LANE, DIM), BF16),
    pltpu.SemaphoreType.DMA((GROWS,)), pltpu.SemaphoreType.DMA((LEVEL,)),
    pltpu.SemaphoreType.DMA((7,)), pltpu.SemaphoreType.DMA((7,)),
]


def split_weights(gu_ref):
    wide = gu_ref[...].astype(F32)
    return (wide[:, 0:GROWS, :].reshape(DIM, UNITS).astype(BF16), wide[:, GROWS:PAIR, :].reshape(DIM, UNITS).astype(BF16))


GU_SHAPE = (NDEV, PAIR, UNITS)
WD_SHAPE = (HEIGHT, DROWS, DIM)


def call(kernel, name, cid, outs, ins, scratch):
    return pl.pallas_call(
        kernel, out_shape=outs, in_specs=[VSPEC] * len(ins), out_specs=(VSPEC,) * len(outs), scratch_shapes=scratch,
        compiler_params=pltpu.CompilerParams(collective_id=cid, has_side_effects=True, vmem_limit_bytes=VMEM_CAP),
        name=name)(*ins)


STAT = 40


def merge_stats(blocks):
    logs = [b[0:32, :] for b in blocks]
    top = logs[0]
    for one in logs[1:]:
        top = jnp.maximum(top, one)
    total = jnp.exp(logs[0] - top)
    labs = blocks[0][32:STAT, :]
    for one, b in zip(logs[1:], blocks[1:]):
        total = total + jnp.exp(one - top)
        labs = labs + b[32:STAT, :]
    return jnp.concatenate([top + jnp.log(total), labs], axis=0)


def step_call(ids, labs, emb, pieces, down_shard, gain_mlp, gain_final, emb_scale, inv_count):
    def kernel(ids_ref, lab_ref, emb_ref, piece_ref, down_ref, gm_ref, gf_ref,
               demb_ref, own_ref, dn_ref, loss_ref,
               tok_mine, tok_ref, table, spread, whole, gu_ref, wd_ref, a_ref, g_ref, u_ref, dm_ref,
               d_gate, d_up, acts, grad_gate, grad_up, grad_down, ggu, gd, land_g, land_d, outgo, outgo_d, acc,
               block, x_ref, h_ref, dh_ref, dhn_ref, stat, land, land_z, lse_ref,
               sem_t, sem_a, z_send, z_recv, d_send, d_recv, g_send, g_recv, e_send, e_recv, sem_s, sem_b, sem_z, sem_d,
               *scratch):
        ring, (mine, parts, total, *level) = scratch[:12], scratch[12:]
        place = my_place()
        me, z, p, q, core = place
        rank = lax.rem(me, LEVEL)
        gain_m, gain_f = gm_ref[...].reshape(1, DIM), gf_ref[...].reshape(1, DIM)
        tok_mine[...] = jnp.zeros((LEVEL, LANE), jnp.int32)
        tok_mine[0:1, :] = ids_ref[...]
        tok_mine[1:TWO, :] = lab_ref[...]
        barrier_peers(place)

        def exchange(step):
            peer = lax.rem(rank + step, LEVEL)
            return remote(piece_ref.at[peer], gu_ref.at[me], sem_a, step, z * LEVEL + peer)

        def rows_of(ref, lv):
            return ref.at[pl.ds(lv * LEVEL, LEVEL)]

        def slab(lv, way):
            part = rows_of(gu_ref, lv)
            return pltpu.make_async_remote_copy(
                src_ref=part, dst_ref=part, send_sem=z_send.at[way * HEIGHT + lv], recv_sem=z_recv.at[lv],
                device_id=(me + LEVEL - CHIPS * way,), device_id_type=MESH)

        def slab_down(lv, way, src):
            return pltpu.make_async_remote_copy(
                src_ref=src, dst_ref=wd_ref.at[lv], send_sem=d_send.at[way * HEIGHT + lv], recv_sem=d_recv.at[lv],
                device_id=(me + LEVEL - CHIPS * way,), device_id_type=MESH)

        def tell(step):
            return remote(tok_mine, tok_ref.at[me], sem_t, step, z * LEVEL + lax.rem(rank + step, LEVEL))

        def along_z(src, dst, sems, step):
            return remote(src, dst, sems, 7 + step, lax.rem(me + LEVEL * step, NDEV))

        for step in range(1, LEVEL):
            tell(step).start()
        tok_ref[me] = tok_mine[...]
        wd_ref[z] = down_ref[...]
        gu_ref[me] = piece_ref[rank]
        fill_table(table, emb_ref)
        stat[...] = jnp.zeros_like(stat)
        demb_ref[...] = jnp.zeros_like(demb_ref)
        for step in range(1, LEVEL):
            tell(step).wait()
        part = rows_of(tok_ref, z)
        for step in range(1, HEIGHT):
            along_z(part, part, sem_t, step).start()
        for step in range(1, LEVEL):
            exchange(step).start()
        pl.when(z < TOP)(lambda: slab_down(z, 0, down_ref).start())
        pl.when(z > 0)(lambda: slab_down(z, 1, down_ref).start())
        for step in range(1, HEIGHT):
            along_z(part, part, sem_t, step).wait()
        for step in range(1, LEVEL):
            exchange(step).wait_recv()
        pl.when(z < TOP)(lambda: slab(z, 0).start())
        pl.when(z > 0)(lambda: slab(z, 1).start())

        def take(lv, way, more):
            slab_down(lv, 0, wd_ref.at[lv]).wait_recv()
            pl.when(more)(lambda: slab_down(lv, way, wd_ref.at[lv]).start())
            slab(lv, 0).wait_recv()
            pl.when(more)(lambda: slab(lv, way).start())

        def take_far(far):
            pl.when(z - far >= 0)(lambda: take(z - far, 0, z < TOP))
            pl.when(z + far < HEIGHT)(lambda: take(z + far, 1, z > 0))

        def hit_rows(first):
            return (vocab_iota() == id_rows(tok_ref, 0, first)).astype(F32).astype(BF16)

        def find(first):
            spread[pl.ds(first, HEIGHT)] = dot(hit_rows(first), table[...], 0, 0).astype(BF16).reshape(HEIGHT, LANE, DIM)

        scatter_levels(spread, x_ref, ring, place, find, lambda t: pl.when(t == LEVEL)(lambda: take_far(1)))
        take_far(TWO)
        x = x_ref[...] * emb_scale
        mine[...] = (x * rms_inv(x) * gain_m).astype(BF16)
        level_gather(mine, a_ref, level[HEIGHT], level[5], place)
        take_far(TOP)
        for half in range(TWO):
            four = slice(HEIGHT * half, HEIGHT * half + HEIGHT)
            wg, wu = split_weights(gu_ref)
            act_in = a_ref[four].reshape(TOKS, DIM)
            g = dot(act_in, wg, 1, 0).astype(BF16)
            u = dot(act_in, wu, 1, 0).astype(BF16)
            g_ref[half] = g
            u_ref[half] = u
            act = (jax.nn.silu(g.astype(F32)) * u.astype(F32)).astype(BF16)
            acts[half] = act
            parts[four] = dot(act, wd_ref[...].reshape(UNITS, DIM), 1, 0).astype(BF16).reshape(HEIGHT, LANE, DIM)
        level_scatter(parts, total, *level[:HEIGHT], *level[6:], place)
        h_ref[...] = (x_ref[...] * emb_scale + total[...].astype(BF16).astype(F32)).astype(BF16)
        h32 = h_ref[...].astype(F32)
        block[...] = (h32 * rms_inv(h32) * gain_f).astype(BF16)
        for step in range(1, LEVEL):
            exchange(step).wait_send()

        def sent(lv, way):
            slab(lv, way).wait_send()
            slab_down(lv, way, wd_ref.at[lv]).wait_send()

        def forward(lv):
            def body(first):
                logits = dot(table[...], whole[pl.ds(first, HEIGHT)].reshape(TOKS, DIM), 1, 1)
                row = vocab_iota()
                lab = jnp.sum(jnp.where(row == id_rows(tok_ref, 1, first), logits, 0.0), axis=0, keepdims=True)
                logits = jnp.where(row < VROWS, logits, -1e30)
                top = jnp.max(logits, axis=0, keepdims=True)
                local = top + jnp.log(jnp.sum(jnp.exp(logits - top), axis=0, keepdims=True))
                for t in range(HEIGHT):
                    stat[0, pl.ds(first + t, 1), :] = local[:, t * LANE:(t + 1) * LANE]
                    stat[0, 32:33, :] = stat[0, 32:33, :] + lab[:, t * LANE:(t + 1) * LANE]
            halves(lv, body)

        gather_levels(block, whole, g_send, g_recv, place, forward)
        for lv in range(HEIGHT):
            pl.when(jnp.logical_and(z < TOP, lv <= z))(lambda: sent(lv, 0))
            pl.when(jnp.logical_and(z > 0, lv >= z))(lambda: sent(lv, 1))

        def share(step):
            return remote(stat.at[0], land.at[rank], sem_s, step, z * LEVEL + lax.rem(rank + step, LEVEL))

        for step in range(1, LEVEL):
            share(step).start()
        land[rank] = stat[0]
        for step in range(1, LEVEL):
            share(step).wait()
        stat[1] = merge_stats([land[r] for r in range(LEVEL)])
        for step in range(1, HEIGHT):
            along_z(stat.at[1], land_z.at[z], sem_s, step).start()
        land_z[z] = stat[1]
        for step in range(1, HEIGHT):
            along_z(stat.at[1], land_z.at[z], sem_s, step).wait()
        final = merge_stats([land_z[lv] for lv in range(HEIGHT)])
        lse_ref[...] = final[0:32, :]
        loss_ref[...] = jnp.full((LEVEL, LANE), (jnp.sum(final[0:32, :]) - jnp.sum(final[32:STAT, :])) * inv_count, F32)

        def backward(first):
            hid = whole[pl.ds(first, HEIGHT)].reshape(TOKS, DIM)
            logits = dot(table[...], hid, 1, 1)
            lse_row = jnp.concatenate([lse_ref[pl.ds(first + t, 1), :] for t in range(HEIGHT)], axis=1)
            row = vocab_iota()
            prob = jnp.exp(jnp.where(row < VROWS, logits, -1e30) - lse_row)
            hit = jnp.where(row == id_rows(tok_ref, 1, first), 1.0, 0.0)
            grad = ((prob - hit) * inv_count).astype(BF16)
            spread[pl.ds(first, HEIGHT)] = dot(grad, table[...], 0, 0).astype(BF16).reshape(HEIGHT, LANE, DIM)
            demb_ref[...] += dot(grad, hid, 1, 0)

        scatter_levels(spread, dhn_ref, ring, place, backward)

        h32 = h_ref[...].astype(F32)
        dh_ref[...] = rms_backward(h32, rms_inv(h32), gain_f, dhn_ref[...])
        mine[...] = dh_ref[...].astype(BF16)
        level_gather(mine, dm_ref, level[HEIGHT], level[5], place)
        for half in range(TWO):
            four = slice(HEIGHT * half, HEIGHT * half + HEIGHT)
            wg, wu = split_weights(gu_ref)
            g = g_ref[half].astype(F32)
            u = u_ref[half].astype(F32)
            dq = dot(dm_ref[four].reshape(TOKS, DIM), wd_ref[...].reshape(UNITS, DIM), 1, 1)
            sig = jax.nn.sigmoid(g)
            dg = (dq * u * sig * (1.0 + g * (1.0 - sig))).astype(BF16)
            du = (dq * g * sig).astype(BF16)
            d_gate[half] = dg
            d_up[half] = du
            parts[four] = (dot(dg, wg, 1, 1) + dot(du, wu, 1, 1)).astype(BF16).reshape(HEIGHT, LANE, DIM)
        def add_slab(dst, srcs):
            def body(i, carry):
                value = srcs[0][i].astype(F32)
                for src in srcs[1:]:
                    value = value + src[i].astype(F32)
                dst[i] = value.astype(dst.dtype)
                return carry
            lax.fori_loop(0, LEVEL, body, 0)

        def hop(lv, way, here=False):
            land = rows_of(land_g, HEIGHT if here and way else lv)
            return remote(rows_of(outgo, lv), land, sem_z, way * HEIGHT + lv, me + LEVEL - CHIPS * way)

        def hop_d(lv, way, here=False):
            return remote(outgo_d.at[lv], land_d.at[HEIGHT if here and way else lv], sem_d, way * HEIGHT + lv, me + LEVEL - CHIPS * way)

        def send(lv, way, more, here):
            @pl.when(more)
            def _():
                hop(lv, way).wait_recv()
                add_slab(rows_of(outgo, lv), [rows_of(ggu, lv), rows_of(land_g, lv)])
                hop_d(lv, way).wait_recv()
                add_into(outgo_d.at[lv], [gd.at[lv], land_d.at[lv]], DROWS)

            @pl.when(jnp.logical_not(more))
            def _():
                add_slab(rows_of(outgo, lv), [rows_of(ggu, lv)])
                add_into(outgo_d.at[lv], [gd.at[lv]], DROWS)
            hop(lv, way, here).start()
            hop_d(lv, way, here).start()

        def send_far(far):
            pl.when(z + far < HEIGHT)(lambda: send(z + far, 0, z > 0, far == 1))
            pl.when(z - far >= 0)(lambda: send(z - far, 1, z < TOP, far == 1))

        def weight_grads():
            for half in range(TWO):
                four = slice(HEIGHT * half, HEIGHT * half + HEIGHT)
                act_in = a_ref[four].reshape(TOKS, DIM)
                news = (dot(act_in, d_gate[half], 0, 0), dot(act_in, d_up[half], 0, 0),
                        dot(acts[half], dm_ref[four].reshape(TOKS, DIM), 0, 0))
                for ref, new in zip((grad_gate, grad_up, grad_down), news):
                    ref[...] = new if half == 0 else ref[...] + new
            both = jnp.concatenate([grad_gate[...].reshape(NDEV, GROWS, UNITS), grad_up[...].reshape(NDEV, GROWS, UNITS)], axis=1)
            ggu[...] = both.astype(BF16)
            gd[...] = grad_down[...].astype(BF16).reshape(WD_SHAPE)

        def grads_off():
            weight_grads()
            send_far(TOP)

        level_scatter(parts, total, *level[:HEIGHT], *level[6:], place, grads_off)
        x = x_ref[...] * emb_scale
        block[...] = (dh_ref[...] + rms_backward(x, rms_inv(x), gain_m, total[...])).astype(BF16)

        demb_ref[...] = demb_ref[...] * (1.0 / emb_scale)

        def add_rows(lv):
            def body(first):
                demb_ref[...] += dot(hit_rows(first), whole[pl.ds(first, HEIGHT)].reshape(TOKS, DIM), 1, 0)
            halves(lv, body)

        def last(way):
            hop(z, way).wait_recv()
            add_slab(acc, [acc, rows_of(land_g, HEIGHT if way else z)])
            hop_d(z, way).wait_recv()
            add_into(dn_ref, [dn_ref, land_d.at[HEIGHT if way else z]], DROWS)

        def give(step):
            peer = lax.rem(rank + step, LEVEL)
            return remote(acc.at[peer], own_ref.at[rank], sem_b, step, z * LEVEL + peer)

        def grads_home():
            add_slab(acc, [rows_of(ggu, z)])
            add_into(dn_ref, [gd.at[z]], DROWS)
            pl.when(z > 0)(lambda: last(0))
            pl.when(z < TOP)(lambda: last(1))
            for step in range(1, LEVEL):
                give(step).start()
            own_ref[rank] = acc[rank]

        def grads_step(t):
            pl.when(t == 1)(lambda: send_far(TWO))
            pl.when(t == TWO)(lambda: send_far(1))
            pl.when(t == HEIGHT)(grads_home)

        gather_levels(block, whole, e_send, e_recv, place, add_rows, grads_step)
        for step in range(1, LEVEL):
            give(step).wait_recv()
        for step in range(1, LEVEL):
            give(step).wait_send()

        def gone(lv, way):
            hop(lv, way).wait_send()
            hop_d(lv, way).wait_send()

        for lv in range(HEIGHT):
            pl.when(lv > z)(lambda: gone(lv, 0))
            pl.when(lv < z)(lambda: gone(lv, 1))

    whole = pltpu.VMEM((NDEV, LANE, DIM), BF16)
    block, flat = pltpu.VMEM((LANE, DIM), BF16), pltpu.VMEM((LANE, DIM), F32)
    slab, slab_d = pltpu.VMEM(GU_SHAPE, BF16), pltpu.VMEM(WD_SHAPE, BF16)
    unit, eight = pltpu.VMEM((TWO, TOKS, UNITS), BF16), pltpu.VMEM((LEVEL, LANE, DIM), BF16)
    wide, tall = pltpu.VMEM((DIM, UNITS), F32), pltpu.VMEM((UNITS, DIM), F32)
    dma = pltpu.SemaphoreType.DMA
    return call(
        kernel, 'step', 0,
        (jax.ShapeDtypeStruct((VPAD, DIM), F32), jax.ShapeDtypeStruct((LEVEL, PAIR, UNITS), F32),
         jax.ShapeDtypeStruct((DROWS, DIM), F32), jax.ShapeDtypeStruct((LEVEL, LANE), F32)),
        (ids, labs, emb, pieces, down_shard, gain_mlp, gain_final),
        [pltpu.VMEM((LEVEL, LANE), jnp.int32), pltpu.VMEM((NDEV, LEVEL, LANE), jnp.int32), pltpu.VMEM((VPAD, DIM), BF16), whole, whole,
         slab, slab_d, eight, unit, unit, eight, unit, unit, unit, wide, wide, tall, slab, slab_d,
         pltpu.VMEM((5 * LEVEL, PAIR, UNITS), BF16), pltpu.VMEM((5, DROWS, DIM), BF16), slab, slab_d,
         pltpu.VMEM((LEVEL, PAIR, UNITS), F32), block, flat, block, flat, flat,
         pltpu.VMEM((TWO, STAT, LANE), F32), pltpu.VMEM((LEVEL, STAT, LANE), F32), pltpu.VMEM((HEIGHT, STAT, LANE), F32),
         pltpu.VMEM((32, LANE), F32),
         sem_pair(11), sem_pair(LEVEL), dma((LEVEL,)), dma((HEIGHT,)), dma((LEVEL,)), dma((HEIGHT,)), dma((5, NDEV)), dma((NDEV,)),
         dma((5, NDEV)), dma((NDEV,)), sem_pair(11), sem_pair(LEVEL), sem_pair(LEVEL), sem_pair(LEVEL)]
        + scatter_scratch(LANE, DIM) + LEVEL_SCRATCH)


def solution(mesh):
    group = mesh.shape['fsdp']

    def local_step(ids_blk, lab_blk, emb_shard, gate_shard, up_shard, down_shard, gain_mlp, gain_final):
        emb_scale = math.sqrt(emb_shard.shape[1])
        inv_count = 1.0 / (ids_blk.size * group)
        pieces = jnp.concatenate([gate_shard, up_shard], axis=0).reshape(PAIR, HEIGHT, LEVEL, DROWS)
        pieces = pieces.transpose(TWO, 0, 1, TOP).reshape(LEVEL, PAIR, UNITS)
        d_embed, d_gu, d_down, loss = step_call(
            ids_blk, lab_blk, emb_shard, pieces, down_shard, gain_mlp, gain_final, emb_scale, inv_count)
        d_gu = d_gu.reshape(LEVEL, PAIR, HEIGHT, DROWS).transpose(1, TWO, 0, TOP).reshape(PAIR, 3072)
        return loss[0, 0], d_embed[0:VROWS] * emb_scale, d_gu[0:GROWS], d_gu[GROWS:PAIR], d_down

    shard_spec = P('fsdp', None)
    return jax.shard_map(local_step, mesh=mesh, in_specs=(shard_spec, shard_spec, shard_spec, shard_spec, shard_spec, shard_spec, P(), P()), out_specs=(P(), shard_spec, shard_spec, shard_spec, shard_spec), check_vma=False)
```

```python
import math
import jax
import jax.numpy as jnp
from jax import lax
from jax.experimental import pallas as pl
from jax.experimental.pallas import tpu as pltpu
from jax.sharding import PartitionSpec as P

NORM_EPS = 1e-6
MESH = pl.DeviceIdType.MESH
F32 = jnp.float32
BF16 = jnp.bfloat16
VMEM_CAP = 63 * 1024 * 1024
LANE = 128
DIM = 768
PAIR = 48
UNITS = 384
NDEV = 32
LEVEL = 8
HEIGHT = 4
DROWS = 96
CHIPS = 16
GROWS = 24
TWO = 2
TOP = 3
VSPEC = pl.BlockSpec(memory_space=pltpu.VMEM)


def my_place():
    me = lax.axis_index('fsdp')
    core = lax.rem(me, TWO)
    x = lax.rem(lax.div(me, TWO), TWO)
    y = lax.rem(lax.div(me, HEIGHT), TWO)
    z = lax.div(me, LEVEL)
    p = x * (1 - core) + y * core
    q = y * (1 - core) + x * core
    return me, z, p, q, core


def chip_of(z, p, q, core):
    x = p * (1 - core) + q * core
    y = q * (1 - core) + p * core
    return (z * TWO + y) * TWO + x


def device_of(z, p, q, core):
    return chip_of(z, p, q, core) * TWO + core


def barrier_peers(place):
    me, z = place[0], place[1]
    sem = pltpu.get_barrier_semaphore()
    for step in range(1, LEVEL):
        dev = z * LEVEL + lax.rem(me + step, LEVEL)
        pl.semaphore_signal(sem, inc=1, device_id=(dev,), device_id_type=MESH)
    for step in range(1, HEIGHT):
        dev = lax.rem(me + LEVEL * step, NDEV)
        pl.semaphore_signal(sem, inc=1, device_id=(dev,), device_id_type=MESH)
    pl.semaphore_wait(sem, 10)


def far_level(z, at):
    half = lax.div(z, TWO)
    inner = lax.rem(z + half, TWO)
    order = (TOP - TOP * half, (1 - inner) * (TWO - half) + inner * TOP * half, 1 + lax.rem(z, TWO), z)
    if isinstance(at, int):
        return order[at]
    low, high = lax.rem(at, TWO), lax.div(at, TWO)
    return ((1 - low) * (1 - high) * order[0] + low * (1 - high) * order[1]
            + (1 - low) * high * order[TWO] + low * high * order[TOP])


def remote(src, dst, sems, slot, dev):
    return pltpu.make_async_remote_copy(
        src_ref=src, dst_ref=dst, send_sem=sems.at[0, slot], recv_sem=sems.at[1, slot],
        device_id=(dev,), device_id_type=MESH)


def sem_pair(n):
    return pltpu.SemaphoreType.DMA((TWO, n))


def gather_levels(in_ref, out_ref, send_sem, recv_sem, place, work, hook=None):
    me, z, p, q, core = place
    peers = (me + LEVEL, me - LEVEL, device_of(z, 1 - p, q, core), device_of(z, p, 1 - q, core), me + 1 - TWO * core)

    def desc(block, way, src=None):
        return pltpu.make_async_remote_copy(
            src_ref=out_ref.at[block] if src is None else src, dst_ref=out_ref.at[block],
            send_sem=send_sem.at[way, block], recv_sem=recv_sem.at[block],
            device_id=(peers[way],), device_id_type=MESH)

    def got(block):
        desc(block, HEIGHT).wait_recv()

    pl.when(z < TOP)(lambda: desc(me, 0, in_ref).start())
    pl.when(z > 0)(lambda: desc(me, 1, in_ref).start())
    for way in (TOP, TWO, HEIGHT):
        desc(me, way, in_ref).start()
    out_ref[me] = in_ref[...]

    def take_z(level):
        block = device_of(level, p, q, core)
        got(block)
        pl.when(jnp.logical_and(level < z, z < TOP))(lambda: desc(block, 0).start())
        pl.when(jnp.logical_and(level > z, z > 0))(lambda: desc(block, 1).start())
        for way in (TOP, TWO, HEIGHT):
            desc(block, way).start()

    def take_p(level):
        block = device_of(level, 1 - p, q, core)
        got(block)
        for way in (TOP, HEIGHT):
            desc(block, way).start()

    def take_q(level):
        for mid in (p, 1 - p):
            block = device_of(level, mid, 1 - q, core)
            got(block)
            desc(block, HEIGHT).start()
        for chip in range(HEIGHT):
            got(level * LEVEL + chip * TWO + 1 - core)

    def step(t, carry):
        if hook is not None:
            with jax.named_scope('hook'):
                hook(t)
        with jax.named_scope('tz'):
            pl.when(t < TOP)(lambda: take_z(far_level(z, TWO - lax.rem(t, TOP))))
        with jax.named_scope('tp'):
            pl.when(t < HEIGHT)(lambda: take_p(far_level(z, TOP - lax.rem(t, HEIGHT))))

        @pl.when(t > 0)
        def _():
            level = far_level(z, HEIGHT - (t + lax.div(HEIGHT - t, HEIGHT)))
            with jax.named_scope('tq'):
                take_q(level)
            with jax.named_scope('gwork'):
                work(level)
        return carry

    lax.fori_loop(0, 5, step, 0)
    for level in range(HEIGHT):
        desc(device_of(level, p, q, core), TWO).wait_send()
        for mid in range(TWO):
            desc(device_of(level, mid, q, core), TOP).wait_send()
        pl.when(jnp.logical_and(z < TOP, level <= z))(lambda: desc(device_of(level, p, q, core), 0).wait_send())
        pl.when(jnp.logical_and(z > 0, level >= z))(lambda: desc(device_of(level, p, q, core), 1).wait_send())
    for chip in range(CHIPS):
        desc(chip * TWO + core, HEIGHT).wait_send()


def add_into(dst, srcs, rows):
    step = 32

    def body(i, carry):
        sl = pl.ds(pl.multiple_of(i * step, step), step)
        total = srcs[0][sl, :].astype(F32)
        for src in srcs[1:]:
            total = total + src[sl, :].astype(F32)
        dst[sl, :] = total.astype(dst.dtype)
        return carry

    lax.fori_loop(0, rows // step, body, 0)


def scatter_scratch(rows, cols):
    return [
        pltpu.VMEM((CHIPS, rows, cols), BF16), pltpu.VMEM((LEVEL, rows, cols), BF16), pltpu.VMEM((HEIGHT, rows, cols), BF16),
        pltpu.VMEM((HEIGHT, rows, cols), BF16), pltpu.VMEM((HEIGHT, rows, cols), BF16), pltpu.VMEM((CHIPS, rows, cols), BF16),
        pltpu.VMEM((rows, cols), F32),
        pltpu.SemaphoreType.DMA((TWO, CHIPS)), pltpu.SemaphoreType.DMA((TWO, LEVEL)), pltpu.SemaphoreType.DMA((TWO, HEIGHT)),
        pltpu.SemaphoreType.DMA((TWO, HEIGHT)), pltpu.SemaphoreType.DMA((TWO, HEIGHT)),
    ]


def scatter_levels(in_ref, out_ref, scratch, place, work, hook=None):
    from_core, from_q, from_p, from_low, from_high, outgo, acc, sem_c, sem_q, sem_p, sem_up, sem_dn = scratch
    me, z, p, q, core = place
    rows = out_ref.shape[0]
    other = 1 - core

    def core_copy(chip):
        return remote(in_ref.at[chip * TWO + other], from_core.at[chip], sem_c, chip, me + 1 - TWO * core)

    def local(level, mid, last):
        return level * HEIGHT + mid * TWO + last

    def q_copy(level, mid):
        return remote(outgo.at[local(level, mid, 1 - q)], from_q.at[level * TWO + mid], sem_q, level * TWO + mid,
                      device_of(z, p, 1 - q, core))

    def p_copy(level):
        return remote(outgo.at[local(level, 1 - p, q)], from_p.at[level], sem_p, level, device_of(z, 1 - p, q, core))

    def up_copy(level):
        return remote(outgo.at[local(level, p, q)], from_low.at[level], sem_up, level, me + LEVEL)

    def dn_copy(level):
        return remote(outgo.at[local(level, p, q)], from_high.at[level], sem_dn, level, me - LEVEL)

    def own(level, mid, last):
        chip = chip_of(level, mid, last, core)
        core_copy(chip).wait_recv()
        return [in_ref.at[chip * TWO + core], from_core.at[chip]]

    y = q * (1 - core) + p * core
    x = p * (1 - core) + q * core

    def make(level, half):
        row = level * HEIGHT + TWO * (y * half + (1 - y) * (1 - half))
        work(row * TWO)
        for side in (1 - x, x):
            core_copy(row + side).start()

    def send_q(level, mid):
        add_into(outgo.at[local(level, mid, 1 - q)], own(level, mid, 1 - q), rows)
        q_copy(level, mid).start()

    def send_p(level):
        side = own(level, 1 - p, q)
        q_copy(level, 1 - p).wait_recv()
        add_into(outgo.at[local(level, 1 - p, q)], side + [from_q.at[level * TWO + 1 - p]], rows)
        p_copy(level).start()

    def gather_here(level):
        mine = own(level, p, q)
        q_copy(level, p).wait_recv()
        p_copy(level).wait_recv()
        return mine + [from_q.at[level * TWO + p], from_p.at[level]]

    def send_z(level):
        add_into(acc, gather_here(level), rows)

        @pl.when(level > z)
        def _():
            @pl.when(z > 0)
            def _():
                up_copy(level).wait_recv()
                add_into(acc, [acc, from_low.at[level]], rows)
            add_into(outgo.at[local(level, p, q)], [acc], rows)
            up_copy(level).start()

        @pl.when(level < z)
        def _():
            @pl.when(z < TOP)
            def _():
                dn_copy(level).wait_recv()
                add_into(acc, [acc, from_high.at[level]], rows)
            add_into(outgo.at[local(level, p, q)], [acc], rows)
            dn_copy(level).start()

    def level_at(t):
        return far_level(z, lax.rem(lax.div(t, TWO), HEIGHT))

    def step(t, carry):
        odd = lax.rem(t, TWO)
        if hook is not None:
            with jax.named_scope('hook'):
                hook(t)
        with jax.named_scope('make'):
            pl.when(t < LEVEL)(lambda: make(level_at(t), odd))
        with jax.named_scope('sq'):
            pl.when(jnp.logical_and(t > 0, t < 9))(lambda: send_q(level_at(t + 7), odd * (1 - p) + (1 - odd) * p))
        with jax.named_scope('sp'):
            pl.when(jnp.logical_and(t > TWO, odd == 1))(lambda: send_p(level_at(t + 5)))
        with jax.named_scope('sz'):
            pl.when(jnp.logical_and(t > HEIGHT, odd == 1))(lambda: send_z(level_at(t + TOP)))
        return carry

    lax.fori_loop(0, 10, step, 0)
    add_into(out_ref, gather_here(z), rows)

    @pl.when(z > 0)
    def _():
        up_copy(z).wait_recv()
        add_into(out_ref, [out_ref, from_low.at[z]], rows)

    @pl.when(z < TOP)
    def _():
        dn_copy(z).wait_recv()
        add_into(out_ref, [out_ref, from_high.at[z]], rows)

    for chip in range(CHIPS):
        core_copy(chip).wait_send()
    for level in range(HEIGHT):
        for mid in range(TWO):
            q_copy(level, mid).wait_send()
        p_copy(level).wait_send()
        pl.when(level > z)(lambda: up_copy(level).wait_send())
        pl.when(level < z)(lambda: dn_copy(level).wait_send())


def rank_of(p, q, core):
    return device_of(0, p, q, core)


def level_gather(in_ref, out_ref, send_sem, recv_sem, place):
    me, z, p, q, core = place
    rank = lax.rem(me, LEVEL)
    peers = (device_of(z, 1 - p, q, core), device_of(z, p, 1 - q, core), me + 1 - TWO * core)

    def desc(block, way, src=None):
        return pltpu.make_async_remote_copy(
            src_ref=out_ref.at[block] if src is None else src, dst_ref=out_ref.at[block],
            send_sem=send_sem.at[way * LEVEL + block], recv_sem=recv_sem.at[block],
            device_id=(peers[way],), device_id_type=MESH)

    for way in (1, 0, TWO):
        desc(rank, way, in_ref).start()
    out_ref[rank] = in_ref[...]
    side = rank_of(1 - p, q, core)
    desc(side, 0).wait_recv()
    for way in (1, TWO):
        desc(side, way).start()
    for mid in (p, 1 - p):
        block = rank_of(mid, 1 - q, core)
        desc(block, 1).wait_recv()
        desc(block, TWO).start()
    for chip in range(HEIGHT):
        desc(chip * TWO + 1 - core, TWO).wait_recv()
    desc(rank, 0, in_ref).wait_send()
    desc(rank, 1, in_ref).wait_send()
    desc(side, 1).wait_send()
    for chip in range(HEIGHT):
        desc(chip * TWO + core, TWO).wait_send()


def level_scatter(in_ref, out_ref, from_core, from_q, from_p, outgo, sem_s, sem_r, place, hook=None):
    me, z, p, q, core = place
    rows = out_ref.shape[0]

    def copy(src, dst, slot, dev):
        return pltpu.make_async_remote_copy(
            src_ref=src, dst_ref=dst, send_sem=sem_s.at[slot], recv_sem=sem_r.at[slot],
            device_id=(dev,), device_id_type=MESH)

    def core_copy(chip):
        return copy(in_ref.at[chip * TWO + 1 - core], from_core.at[chip], chip, me + 1 - TWO * core)

    def q_copy(mid):
        return copy(outgo.at[mid], from_q.at[mid], HEIGHT + mid, device_of(z, p, 1 - q, core))

    def p_copy():
        return copy(outgo.at[TWO], from_p, 6, device_of(z, 1 - p, q, core))

    def own(mid, last):
        chip = chip_of(0, mid, last, core)
        core_copy(chip).wait_recv()
        return [in_ref.at[chip * TWO + core], from_core.at[chip]]

    for last in (1 - p, p):
        for mid in (1 - q, q):
            core_copy(chip_of(0, mid, last, 1 - core)).start()
    for mid in (1 - p, p):
        add_into(outgo.at[mid], own(mid, 1 - q), rows)
        q_copy(mid).start()
    if hook is not None:
        with jax.named_scope('lhook'):
            hook()
    side = own(1 - p, q)
    q_copy(1 - p).wait_recv()
    add_into(outgo.at[TWO], side + [from_q.at[1 - p]], rows)
    p_copy().start()
    mine = own(p, q)
    q_copy(p).wait_recv()
    p_copy().wait_recv()
    add_into(out_ref, mine + [from_q.at[p], from_p], rows)
    for chip in range(HEIGHT):
        core_copy(chip).wait_send()
    for mid in range(TWO):
        q_copy(mid).wait_send()
    p_copy().wait_send()


def dot(left, right, ld, rd):
    return lax.dot_general(left, right, (((ld,), (rd,)), ((), ())), preferred_element_type=F32)


TOKS = 512
VPAD = 1024
VROWS = 1004


def id_rows(tok_ref, row, first):
    ids = jnp.concatenate([tok_ref[first + t, row:row + 1, :] for t in range(HEIGHT)], axis=1) - shard_start()
    return jnp.where(jnp.logical_and(ids >= 0, ids < VROWS), ids, -1)


def vocab_iota():
    return lax.broadcasted_iota(jnp.int32, (VPAD, TOKS), 0)


def shard_start():
    return lax.axis_index('fsdp') * VROWS


def fill_table(table, emb_ref):
    table[VPAD - 32:VPAD, :] = jnp.zeros((32, DIM), BF16)
    table[0:VROWS, :] = emb_ref[...]


def halves(level, body):
    def one(i, carry):
        body(level * LEVEL + i * HEIGHT)
        return carry
    lax.fori_loop(0, TWO, one, 0)


def rms_inv(values):
    return lax.rsqrt(jnp.mean(values * values, axis=-1, keepdims=True) + NORM_EPS)


def rms_backward(values, inv_rms, gain_vec, grad_out):
    scaled = grad_out * gain_vec
    return inv_rms * scaled - values * (inv_rms ** TOP) * jnp.mean(scaled * values, axis=-1, keepdims=True)


LEVEL_SCRATCH = [
    pltpu.VMEM((LANE, DIM), BF16), pltpu.VMEM((LEVEL, LANE, DIM), BF16), pltpu.VMEM((LANE, DIM), F32),
    pltpu.VMEM((HEIGHT, LANE, DIM), BF16), pltpu.VMEM((TWO, LANE, DIM), BF16), pltpu.VMEM((LANE, DIM), BF16),
    pltpu.VMEM((TOP, LANE, DIM), BF16),
    pltpu.SemaphoreType.DMA((GROWS,)), pltpu.SemaphoreType.DMA((LEVEL,)),
    pltpu.SemaphoreType.DMA((7,)), pltpu.SemaphoreType.DMA((7,)),
]


def split_weights(gu_ref):
    wide = gu_ref[...].astype(F32)
    return (wide[:, 0:GROWS, :].reshape(DIM, UNITS).astype(BF16), wide[:, GROWS:PAIR, :].reshape(DIM, UNITS).astype(BF16))


GU_SHAPE = (NDEV, PAIR, UNITS)
WD_SHAPE = (HEIGHT, DROWS, DIM)


def call(kernel, name, cid, outs, ins, scratch):
    return pl.pallas_call(
        kernel, out_shape=outs, in_specs=[VSPEC] * len(ins), out_specs=(VSPEC,) * (len(outs) - 1) + (pl.BlockSpec(memory_space=pltpu.SMEM),),
        scratch_shapes=scratch,
        compiler_params=pltpu.CompilerParams(collective_id=cid, has_side_effects=True, vmem_limit_bytes=VMEM_CAP),
        name=name)(*ins)


STAT = 40


def merge_stats(blocks):
    logs = [b[0:32, :] for b in blocks]
    top = logs[0]
    for one in logs[1:]:
        top = jnp.maximum(top, one)
    total = jnp.exp(logs[0] - top)
    labs = blocks[0][32:STAT, :]
    for one, b in zip(logs[1:], blocks[1:]):
        total = total + jnp.exp(one - top)
        labs = labs + b[32:STAT, :]
    return jnp.concatenate([top + jnp.log(total), labs], axis=0)


def step_call(ids, labs, emb, gate, up, down_shard, gain_mlp, gain_final, emb_scale, inv_count):
    def kernel(ids_ref, lab_ref, emb_ref, gate_ref, up_ref, down_ref, gm_ref, gf_ref,
               demb_ref, dgate_ref, dup_ref, dn_ref, loss_ref,
               piece_ref, own_ref, tok_mine, tok_ref, table, spread, whole, gu_ref, wd_ref, a_ref, g_ref, u_ref, dm_ref,
               d_gate, d_up, acts, grad_gate, grad_up, grad_down, ggu, gd, land_g, land_d, outgo, outgo_d, acc,
               block, x_ref, h_ref, dh_ref, dhn_ref, stat, land, land_z, lse_ref,
               sem_t, sem_a, z_send, z_recv, d_send, d_recv, g_send, g_recv, e_send, e_recv, sem_s, sem_b, sem_z, sem_d,
               *scratch):
        ring, (mine, parts, total, *level) = scratch[:12], scratch[12:]
        place = my_place()
        me, z, p, q, core = place
        rank = lax.rem(me, LEVEL)
        gain_m, gain_f = gm_ref[...].reshape(1, DIM), gf_ref[...].reshape(1, DIM)
        tok_mine[...] = jnp.zeros((LEVEL, LANE), jnp.int32)
        tok_mine[0:1, :] = ids_ref[...]
        tok_mine[1:TWO, :] = lab_ref[...]
        both = jnp.concatenate([gate_ref[...].astype(F32), up_ref[...].astype(F32)], axis=0).astype(BF16)
        for r in range(LEVEL):
            piece_ref[r] = jnp.concatenate([both[:, DROWS * (LEVEL * k + r):DROWS * (LEVEL * k + r + 1)] for k in range(HEIGHT)], axis=1)
        with jax.named_scope('barrier'):
            barrier_peers(place)

        def exchange(step):
            peer = lax.rem(rank + step, LEVEL)
            return remote(piece_ref.at[peer], gu_ref.at[me], sem_a, step, z * LEVEL + peer)

        def rows_of(ref, lv):
            return ref.at[pl.ds(lv * LEVEL, LEVEL)]

        def slab(lv, way):
            part = rows_of(gu_ref, lv)
            return pltpu.make_async_remote_copy(
                src_ref=part, dst_ref=part, send_sem=z_send.at[way * HEIGHT + lv], recv_sem=z_recv.at[lv],
                device_id=(me + LEVEL - CHIPS * way,), device_id_type=MESH)

        def slab_down(lv, way, src):
            return pltpu.make_async_remote_copy(
                src_ref=src, dst_ref=wd_ref.at[lv], send_sem=d_send.at[way * HEIGHT + lv], recv_sem=d_recv.at[lv],
                device_id=(me + LEVEL - CHIPS * way,), device_id_type=MESH)

        def tell(step):
            return remote(tok_mine, tok_ref.at[me], sem_t, step, z * LEVEL + lax.rem(rank + step, LEVEL))

        def along_z(src, dst, sems, step):
            return remote(src, dst, sems, 7 + step, lax.rem(me + LEVEL * step, NDEV))

        for step in range(1, LEVEL):
            tell(step).start()
        tok_ref[me] = tok_mine[...]
        wd_ref[z] = down_ref[...]
        gu_ref[me] = piece_ref[rank]
        fill_table(table, emb_ref)
        stat[...] = jnp.zeros_like(stat)
        demb_ref[...] = jnp.zeros_like(demb_ref)
        for step in range(1, LEVEL):
            tell(step).wait()
        part = rows_of(tok_ref, z)
        for step in range(1, HEIGHT):
            along_z(part, part, sem_t, step).start()
        for step in range(1, LEVEL):
            exchange(step).start()
        pl.when(z < TOP)(lambda: slab_down(z, 0, down_ref).start())
        pl.when(z > 0)(lambda: slab_down(z, 1, down_ref).start())
        for step in range(1, HEIGHT):
            along_z(part, part, sem_t, step).wait()
        for step in range(1, LEVEL):
            exchange(step).wait_recv()
        pl.when(z < TOP)(lambda: slab(z, 0).start())
        pl.when(z > 0)(lambda: slab(z, 1).start())

        def take(lv, way, more):
            slab_down(lv, 0, wd_ref.at[lv]).wait_recv()
            pl.when(more)(lambda: slab_down(lv, way, wd_ref.at[lv]).start())
            slab(lv, 0).wait_recv()
            pl.when(more)(lambda: slab(lv, way).start())

        def take_far(far):
            pl.when(z - far >= 0)(lambda: take(z - far, 0, z < TOP))
            pl.when(z + far < HEIGHT)(lambda: take(z + far, 1, z > 0))

        def hit_rows(first):
            return (vocab_iota() == id_rows(tok_ref, 0, first)).astype(F32).astype(BF16)

        def find(first):
            spread[pl.ds(first, HEIGHT)] = dot(hit_rows(first), table[...], 0, 0).astype(BF16).reshape(HEIGHT, LANE, DIM)

        with jax.named_scope('x_scatter'):
            scatter_levels(spread, x_ref, ring, place, find, lambda t: pl.when(t == LEVEL)(lambda: take_far(1)))
        with jax.named_scope('take2'):
            take_far(TWO)
        x = x_ref[...] * emb_scale
        mine[...] = (x * rms_inv(x) * gain_m).astype(BF16)
        with jax.named_scope('a_gather'):
            level_gather(mine, a_ref, level[HEIGHT], level[5], place)
        with jax.named_scope('take3'):
            take_far(TOP)
        for half in range(TWO):
            four = slice(HEIGHT * half, HEIGHT * half + HEIGHT)
            wg, wu = split_weights(gu_ref)
            act_in = a_ref[four].reshape(TOKS, DIM)
            g = dot(act_in, wg, 1, 0).astype(BF16)
            u = dot(act_in, wu, 1, 0).astype(BF16)
            g_ref[half] = g
            u_ref[half] = u
            act = (jax.nn.silu(g.astype(F32)) * u.astype(F32)).astype(BF16)
            acts[half] = act
            parts[four] = dot(act, wd_ref[...].reshape(UNITS, DIM), 1, 0).astype(BF16).reshape(HEIGHT, LANE, DIM)
        with jax.named_scope('lv_scatter'):
            level_scatter(parts, total, *level[:HEIGHT], *level[6:], place)
        h_ref[...] = (x_ref[...] * emb_scale + total[...].astype(BF16).astype(F32)).astype(BF16)
        h32 = h_ref[...].astype(F32)
        block[...] = (h32 * rms_inv(h32) * gain_f).astype(BF16)
        for step in range(1, LEVEL):
            exchange(step).wait_send()

        def sent(lv, way):
            slab(lv, way).wait_send()
            slab_down(lv, way, wd_ref.at[lv]).wait_send()

        def forward(lv):
            def body(first):
                logits = dot(table[...], whole[pl.ds(first, HEIGHT)].reshape(TOKS, DIM), 1, 1)
                row = vocab_iota()
                lab = jnp.sum(jnp.where(row == id_rows(tok_ref, 1, first), logits, 0.0), axis=0, keepdims=True)
                logits = jnp.where(row < VROWS, logits, -1e30)
                top = jnp.max(logits, axis=0, keepdims=True)
                local = top + jnp.log(jnp.sum(jnp.exp(logits - top), axis=0, keepdims=True))
                for t in range(HEIGHT):
                    stat[0, pl.ds(first + t, 1), :] = local[:, t * LANE:(t + 1) * LANE]
                    stat[0, 32:33, :] = stat[0, 32:33, :] + lab[:, t * LANE:(t + 1) * LANE]
            halves(lv, body)

        with jax.named_scope('hn_gather'):
            gather_levels(block, whole, g_send, g_recv, place, forward)
        for lv in range(HEIGHT):
            pl.when(jnp.logical_and(z < TOP, lv <= z))(lambda: sent(lv, 0))
            pl.when(jnp.logical_and(z > 0, lv >= z))(lambda: sent(lv, 1))

        def share(step):
            return remote(stat.at[0], land.at[rank], sem_s, step, z * LEVEL + lax.rem(rank + step, LEVEL))

        for step in range(1, LEVEL):
            share(step).start()
        land[rank] = stat[0]
        for step in range(1, LEVEL):
            share(step).wait()
        stat[1] = merge_stats([land[r] for r in range(LEVEL)])
        for step in range(1, HEIGHT):
            along_z(stat.at[1], land_z.at[z], sem_s, step).start()
        land_z[z] = stat[1]
        for step in range(1, HEIGHT):
            along_z(stat.at[1], land_z.at[z], sem_s, step).wait()
        final = merge_stats([land_z[lv] for lv in range(HEIGHT)])
        lse_ref[...] = final[0:32, :]
        loss_ref[0, 0] = (jnp.sum(final[0:32, :]) - jnp.sum(final[32:STAT, :])) * inv_count

        def backward(first):
            hid = whole[pl.ds(first, HEIGHT)].reshape(TOKS, DIM)
            logits = dot(table[...], hid, 1, 1)
            lse_row = jnp.concatenate([lse_ref[pl.ds(first + t, 1), :] for t in range(HEIGHT)], axis=1)
            row = vocab_iota()
            prob = jnp.exp(jnp.where(row < VROWS, logits, -1e30) - lse_row)
            hit = jnp.where(row == id_rows(tok_ref, 1, first), 1.0, 0.0)
            grad = ((prob - hit) * inv_count).astype(BF16)
            spread[pl.ds(first, HEIGHT)] = dot(grad, table[...], 0, 0).astype(BF16).reshape(HEIGHT, LANE, DIM)
            demb_ref[...] += dot(grad, hid, 1, 0)

        with jax.named_scope('dhn_scatter'):
            scatter_levels(spread, dhn_ref, ring, place, backward)

        h32 = h_ref[...].astype(F32)
        dh_ref[...] = rms_backward(h32, rms_inv(h32), gain_f, dhn_ref[...])
        mine[...] = dh_ref[...].astype(BF16)
        with jax.named_scope('dm_gather'):
            level_gather(mine, dm_ref, level[HEIGHT], level[5], place)
        for half in range(TWO):
            four = slice(HEIGHT * half, HEIGHT * half + HEIGHT)
            wg, wu = split_weights(gu_ref)
            g = g_ref[half].astype(F32)
            u = u_ref[half].astype(F32)
            dq = dot(dm_ref[four].reshape(TOKS, DIM), wd_ref[...].reshape(UNITS, DIM), 1, 1)
            sig = jax.nn.sigmoid(g)
            dg = (dq * u * sig * (1.0 + g * (1.0 - sig))).astype(BF16)
            du = (dq * g * sig).astype(BF16)
            d_gate[half] = dg
            d_up[half] = du
            parts[four] = (dot(dg, wg, 1, 1) + dot(du, wu, 1, 1)).astype(BF16).reshape(HEIGHT, LANE, DIM)
        def add_slab(dst, srcs):
            def body(i, carry):
                value = srcs[0][i].astype(F32)
                for src in srcs[1:]:
                    value = value + src[i].astype(F32)
                dst[i] = value.astype(dst.dtype)
                return carry
            lax.fori_loop(0, LEVEL, body, 0)

        def hop(lv, way, here=False):
            land = rows_of(land_g, HEIGHT if here and way else lv)
            return remote(rows_of(outgo, lv), land, sem_z, way * HEIGHT + lv, me + LEVEL - CHIPS * way)

        def hop_d(lv, way, here=False):
            return remote(outgo_d.at[lv], land_d.at[HEIGHT if here and way else lv], sem_d, way * HEIGHT + lv, me + LEVEL - CHIPS * way)

        def send(lv, way, more, here):
            @pl.when(more)
            def _():
                hop(lv, way).wait_recv()
                add_slab(rows_of(outgo, lv), [rows_of(ggu, lv), rows_of(land_g, lv)])
                hop_d(lv, way).wait_recv()
                add_into(outgo_d.at[lv], [gd.at[lv], land_d.at[lv]], DROWS)

            @pl.when(jnp.logical_not(more))
            def _():
                add_slab(rows_of(outgo, lv), [rows_of(ggu, lv)])
                add_into(outgo_d.at[lv], [gd.at[lv]], DROWS)
            hop(lv, way, here).start()
            hop_d(lv, way, here).start()

        def send_far(far):
            pl.when(z + far < HEIGHT)(lambda: send(z + far, 0, z > 0, far == 1))
            pl.when(z - far >= 0)(lambda: send(z - far, 1, z < TOP, far == 1))

        def weight_grads():
            for half in range(TWO):
                four = slice(HEIGHT * half, HEIGHT * half + HEIGHT)
                act_in = a_ref[four].reshape(TOKS, DIM)
                news = (dot(act_in, d_gate[half], 0, 0), dot(act_in, d_up[half], 0, 0),
                        dot(acts[half], dm_ref[four].reshape(TOKS, DIM), 0, 0))
                for ref, new in zip((grad_gate, grad_up, grad_down), news):
                    ref[...] = new if half == 0 else ref[...] + new
            both = jnp.concatenate([grad_gate[...].reshape(NDEV, GROWS, UNITS), grad_up[...].reshape(NDEV, GROWS, UNITS)], axis=1)
            ggu[...] = both.astype(BF16)
            gd[...] = grad_down[...].astype(BF16).reshape(WD_SHAPE)

        def grads_off():
            weight_grads()
            send_far(TOP)

        with jax.named_scope('lv_scatter'):
            level_scatter(parts, total, *level[:HEIGHT], *level[6:], place, grads_off)
        x = x_ref[...] * emb_scale
        block[...] = (dh_ref[...] + rms_backward(x, rms_inv(x), gain_m, total[...])).astype(BF16)

        demb_ref[...] = demb_ref[...] * (1.0 / emb_scale)

        def add_rows(lv):
            def body(first):
                demb_ref[...] += dot(hit_rows(first), whole[pl.ds(first, HEIGHT)].reshape(TOKS, DIM), 1, 0)
            halves(lv, body)

        def last(way):
            hop(z, way).wait_recv()
            add_slab(acc, [acc, rows_of(land_g, HEIGHT if way else z)])
            hop_d(z, way).wait_recv()
            add_into(dn_ref, [dn_ref, land_d.at[HEIGHT if way else z]], DROWS)

        def give(step):
            peer = lax.rem(rank + step, LEVEL)
            return remote(acc.at[peer], own_ref.at[rank], sem_b, step, z * LEVEL + peer)

        def grads_home():
            add_slab(acc, [rows_of(ggu, z)])
            add_into(dn_ref, [gd.at[z]], DROWS)
            pl.when(z > 0)(lambda: last(0))
            pl.when(z < TOP)(lambda: last(1))
            for step in range(1, LEVEL):
                give(step).start()
            own_ref[rank] = acc[rank]

        def grads_step(t):
            pl.when(t == 1)(lambda: send_far(TWO))
            pl.when(t == TWO)(lambda: send_far(1))
            pl.when(t == HEIGHT)(grads_home)

        with jax.named_scope('dx_gather'):
            gather_levels(block, whole, e_send, e_recv, place, add_rows, grads_step)
        for step in range(1, LEVEL):
            give(step).wait_recv()
        for step in range(1, LEVEL):
            give(step).wait_send()
        for k in range(HEIGHT):
            got = jnp.concatenate([own_ref[r, :, DROWS * k:DROWS * (k + 1)] for r in range(LEVEL)], axis=1)
            dgate_ref[:, DIM * k:DIM * (k + 1)] = got[0:GROWS]
            dup_ref[:, DIM * k:DIM * (k + 1)] = got[GROWS:PAIR]

        def gone(lv, way):
            hop(lv, way).wait_send()
            hop_d(lv, way).wait_send()

        for lv in range(HEIGHT):
            pl.when(lv > z)(lambda: gone(lv, 0))
            pl.when(lv < z)(lambda: gone(lv, 1))

    whole = pltpu.VMEM((NDEV, LANE, DIM), BF16)
    block, flat = pltpu.VMEM((LANE, DIM), BF16), pltpu.VMEM((LANE, DIM), F32)
    slab, slab_d = pltpu.VMEM(GU_SHAPE, BF16), pltpu.VMEM(WD_SHAPE, BF16)
    unit, eight = pltpu.VMEM((TWO, TOKS, UNITS), BF16), pltpu.VMEM((LEVEL, LANE, DIM), BF16)
    wide, tall = pltpu.VMEM((DIM, UNITS), F32), pltpu.VMEM((UNITS, DIM), F32)
    dma = pltpu.SemaphoreType.DMA
    return call(
        kernel, 'step', 0,
        (jax.ShapeDtypeStruct((VPAD, DIM), F32), jax.ShapeDtypeStruct((GROWS, 3072), F32), jax.ShapeDtypeStruct((GROWS, 3072), F32),
         jax.ShapeDtypeStruct((DROWS, DIM), F32), jax.ShapeDtypeStruct((1, 1), F32)),
        (ids, labs, emb, gate, up, down_shard, gain_mlp, gain_final),
        [pltpu.VMEM((LEVEL, PAIR, UNITS), BF16), pltpu.VMEM((LEVEL, PAIR, UNITS), F32), pltpu.VMEM((LEVEL, LANE), jnp.int32), pltpu.VMEM((NDEV, LEVEL, LANE), jnp.int32), pltpu.VMEM((VPAD, DIM), BF16), whole, whole,
         slab, slab_d, eight, unit, unit, eight, unit, unit, unit, wide, wide, tall, slab, slab_d,
         pltpu.VMEM((5 * LEVEL, PAIR, UNITS), BF16), pltpu.VMEM((5, DROWS, DIM), BF16), slab, slab_d,
         pltpu.VMEM((LEVEL, PAIR, UNITS), F32), block, flat, block, flat, flat,
         pltpu.VMEM((TWO, STAT, LANE), F32), pltpu.VMEM((LEVEL, STAT, LANE), F32), pltpu.VMEM((HEIGHT, STAT, LANE), F32),
         pltpu.VMEM((32, LANE), F32),
         sem_pair(11), sem_pair(LEVEL), dma((LEVEL,)), dma((HEIGHT,)), dma((LEVEL,)), dma((HEIGHT,)), dma((5, NDEV)), dma((NDEV,)),
         dma((5, NDEV)), dma((NDEV,)), sem_pair(11), sem_pair(LEVEL), sem_pair(LEVEL), sem_pair(LEVEL)]
        + scatter_scratch(LANE, DIM) + LEVEL_SCRATCH)


def solution(mesh):
    group = mesh.shape['fsdp']

    def local_step(ids_blk, lab_blk, emb_shard, gate_shard, up_shard, down_shard, gain_mlp, gain_final):
        emb_scale = math.sqrt(emb_shard.shape[1])
        inv_count = 1.0 / (ids_blk.size * group)
        d_embed, d_gate, d_up, d_down, loss = step_call(
            ids_blk, lab_blk, emb_shard, gate_shard, up_shard, down_shard, gain_mlp, gain_final, emb_scale, inv_count)
        return loss[0, 0], d_embed[0:VROWS] * emb_scale, d_gate, d_up, d_down

    shard_spec = P('fsdp', None)
    return jax.shard_map(local_step, mesh=mesh, in_specs=(shard_spec, shard_spec, shard_spec, shard_spec, shard_spec, shard_spec, P(), P()), out_specs=(P(), shard_spec, shard_spec, shard_spec, shard_spec), check_vma=False)
```

```python
import math
import jax
import jax.numpy as jnp
from jax import lax
from jax.experimental import pallas as pl
from jax.experimental.pallas import tpu as pltpu
from jax.sharding import PartitionSpec as P

NORM_EPS = 1e-6
MESH = pl.DeviceIdType.MESH
F32 = jnp.float32
BF16 = jnp.bfloat16
VMEM_CAP = 63 * 1024 * 1024
LANE = 128
DIM = 768
PAIR = 48
UNITS = 384
NDEV = 32
LEVEL = 8
HEIGHT = 4
DROWS = 96
CHIPS = 16
GROWS = 24
TWO = 2
TOP = 3
VSPEC = pl.BlockSpec(memory_space=pltpu.VMEM)


def my_place():
    me = lax.axis_index('fsdp')
    core = lax.rem(me, TWO)
    x = lax.rem(lax.div(me, TWO), TWO)
    y = lax.rem(lax.div(me, HEIGHT), TWO)
    z = lax.div(me, LEVEL)
    p = x * (1 - core) + y * core
    q = y * (1 - core) + x * core
    return me, z, p, q, core


def chip_of(z, p, q, core):
    x = p * (1 - core) + q * core
    y = q * (1 - core) + p * core
    return (z * TWO + y) * TWO + x


def device_of(z, p, q, core):
    return chip_of(z, p, q, core) * TWO + core


def barrier_peers(place):
    me, z = place[0], place[1]
    sem = pltpu.get_barrier_semaphore()
    for step in range(1, LEVEL):
        dev = z * LEVEL + lax.rem(me + step, LEVEL)
        pl.semaphore_signal(sem, inc=1, device_id=(dev,), device_id_type=MESH)
    for step in range(1, HEIGHT):
        dev = lax.rem(me + LEVEL * step, NDEV)
        pl.semaphore_signal(sem, inc=1, device_id=(dev,), device_id_type=MESH)
    pl.semaphore_wait(sem, 10)


def far_level(z, at):
    half = lax.div(z, TWO)
    inner = lax.rem(z + half, TWO)
    order = (TOP - TOP * half, (1 - inner) * (TWO - half) + inner * TOP * half, 1 + lax.rem(z, TWO), z)
    if isinstance(at, int):
        return order[at]
    low, high = lax.rem(at, TWO), lax.div(at, TWO)
    return ((1 - low) * (1 - high) * order[0] + low * (1 - high) * order[1]
            + (1 - low) * high * order[TWO] + low * high * order[TOP])


def remote(src, dst, sems, slot, dev):
    return pltpu.make_async_remote_copy(
        src_ref=src, dst_ref=dst, send_sem=sems.at[0, slot], recv_sem=sems.at[1, slot],
        device_id=(dev,), device_id_type=MESH)


def sem_pair(n):
    return pltpu.SemaphoreType.DMA((TWO, n))


def gather_levels(in_ref, out_ref, send_sem, recv_sem, place, work, hook=None, late_hook=None):
    me, z, p, q, core = place
    peers = (me + LEVEL, me - LEVEL, device_of(z, 1 - p, q, core), device_of(z, p, 1 - q, core), me + 1 - TWO * core)

    def desc(block, way, src=None):
        return pltpu.make_async_remote_copy(
            src_ref=out_ref.at[block] if src is None else src, dst_ref=out_ref.at[block],
            send_sem=send_sem.at[way, block], recv_sem=recv_sem.at[block],
            device_id=(peers[way],), device_id_type=MESH)

    def got(block):
        desc(block, HEIGHT).wait_recv()

    pl.when(z < TOP)(lambda: desc(me, 0, in_ref).start())
    pl.when(z > 0)(lambda: desc(me, 1, in_ref).start())
    for way in (TOP, TWO, HEIGHT):
        desc(me, way, in_ref).start()
    out_ref[me] = in_ref[...]

    def take_z(level):
        block = device_of(level, p, q, core)
        got(block)
        pl.when(jnp.logical_and(level < z, z < TOP))(lambda: desc(block, 0).start())
        pl.when(jnp.logical_and(level > z, z > 0))(lambda: desc(block, 1).start())
        for way in (TOP, TWO, HEIGHT):
            desc(block, way).start()

    def take_p(level):
        block = device_of(level, 1 - p, q, core)
        got(block)
        for way in (TOP, HEIGHT):
            desc(block, way).start()

    def take_q(level):
        for mid in (p, 1 - p):
            block = device_of(level, mid, 1 - q, core)
            got(block)
            desc(block, HEIGHT).start()
        for chip in range(HEIGHT):
            got(level * LEVEL + chip * TWO + 1 - core)

    def step(t, carry):
        if hook is not None:
            with jax.named_scope('hook'):
                hook(t)
        with jax.named_scope('tz'):
            pl.when(jnp.logical_or(t < TWO, jnp.logical_and(t == TWO, outer)))(lambda: take_z(far_level(z, TWO - lax.rem(t, TOP))))
        with jax.named_scope('tp'):
            pl.when(jnp.logical_and(t > 0, t < HEIGHT))(lambda: take_p(far_level(z, TOP - lax.rem(t, HEIGHT))))
        with jax.named_scope('tz3'):
            pl.when(jnp.logical_and(t == 1, jnp.logical_not(outer)))(lambda: take_z(far_level(z, 0)))
        if late_hook is not None:
            with jax.named_scope('late'):
                late_hook(t)

        @pl.when(t > 0)
        def _():
            level = far_level(z, HEIGHT - (t + lax.div(HEIGHT - t, HEIGHT)))
            with jax.named_scope('tq'):
                take_q(level)
            with jax.named_scope('gwork'):
                work(level)
        return carry

    outer = jnp.logical_or(z == 0, z == TOP)
    with jax.named_scope('tp0'):
        take_p(z)
    lax.fori_loop(0, 5, step, 0)
    for level in range(HEIGHT):
        desc(device_of(level, p, q, core), TWO).wait_send()
        for mid in range(TWO):
            desc(device_of(level, mid, q, core), TOP).wait_send()
        pl.when(jnp.logical_and(z < TOP, level <= z))(lambda: desc(device_of(level, p, q, core), 0).wait_send())
        pl.when(jnp.logical_and(z > 0, level >= z))(lambda: desc(device_of(level, p, q, core), 1).wait_send())
    for chip in range(CHIPS):
        desc(chip * TWO + core, HEIGHT).wait_send()


def add_into(dst, srcs, rows):
    step = 32

    def body(i, carry):
        sl = pl.ds(pl.multiple_of(i * step, step), step)
        total = srcs[0][sl, :].astype(F32)
        for src in srcs[1:]:
            total = total + src[sl, :].astype(F32)
        dst[sl, :] = total.astype(dst.dtype)
        return carry

    lax.fori_loop(0, rows // step, body, 0)


def scatter_scratch(rows, cols):
    return [
        pltpu.VMEM((CHIPS, rows, cols), BF16), pltpu.VMEM((LEVEL, rows, cols), BF16), pltpu.VMEM((HEIGHT, rows, cols), BF16),
        pltpu.VMEM((HEIGHT, rows, cols), BF16), pltpu.VMEM((HEIGHT, rows, cols), BF16), pltpu.VMEM((CHIPS, rows, cols), BF16),
        pltpu.VMEM((rows, cols), F32),
        pltpu.SemaphoreType.DMA((TWO, CHIPS)), pltpu.SemaphoreType.DMA((TWO, LEVEL)), pltpu.SemaphoreType.DMA((TWO, HEIGHT)),
        pltpu.SemaphoreType.DMA((TWO, HEIGHT)), pltpu.SemaphoreType.DMA((TWO, HEIGHT)),
    ]


def scatter_levels(in_ref, out_ref, scratch, place, work, hook=None):
    from_core, from_q, from_p, from_low, from_high, outgo, acc, sem_c, sem_q, sem_p, sem_up, sem_dn = scratch
    me, z, p, q, core = place
    rows = out_ref.shape[0]
    other = 1 - core

    def core_copy(chip):
        return remote(in_ref.at[chip * TWO + other], from_core.at[chip], sem_c, chip, me + 1 - TWO * core)

    def local(level, mid, last):
        return level * HEIGHT + mid * TWO + last

    def q_copy(level, mid):
        return remote(outgo.at[local(level, mid, 1 - q)], from_q.at[level * TWO + mid], sem_q, level * TWO + mid,
                      device_of(z, p, 1 - q, core))

    def p_copy(level):
        return remote(outgo.at[local(level, 1 - p, q)], from_p.at[level], sem_p, level, device_of(z, 1 - p, q, core))

    def up_copy(level):
        return remote(outgo.at[local(level, p, q)], from_low.at[level], sem_up, level, me + LEVEL)

    def dn_copy(level):
        return remote(outgo.at[local(level, p, q)], from_high.at[level], sem_dn, level, me - LEVEL)

    def own(level, mid, last):
        chip = chip_of(level, mid, last, core)
        core_copy(chip).wait_recv()
        return [in_ref.at[chip * TWO + core], from_core.at[chip]]

    y = q * (1 - core) + p * core
    x = p * (1 - core) + q * core

    def make(level, half):
        row = level * HEIGHT + TWO * (y * half + (1 - y) * (1 - half))
        work(row * TWO)
        for side in (1 - x, x):
            core_copy(row + side).start()

    def send_q(level, mid):
        add_into(outgo.at[local(level, mid, 1 - q)], own(level, mid, 1 - q), rows)
        q_copy(level, mid).start()

    def send_p(level):
        side = own(level, 1 - p, q)
        q_copy(level, 1 - p).wait_recv()
        add_into(outgo.at[local(level, 1 - p, q)], side + [from_q.at[level * TWO + 1 - p]], rows)
        p_copy(level).start()

    def gather_here(level):
        mine = own(level, p, q)
        q_copy(level, p).wait_recv()
        p_copy(level).wait_recv()
        return mine + [from_q.at[level * TWO + p], from_p.at[level]]

    def send_z(level):
        add_into(acc, gather_here(level), rows)

        @pl.when(level > z)
        def _():
            @pl.when(z > 0)
            def _():
                up_copy(level).wait_recv()
                add_into(acc, [acc, from_low.at[level]], rows)
            add_into(outgo.at[local(level, p, q)], [acc], rows)
            up_copy(level).start()

        @pl.when(level < z)
        def _():
            @pl.when(z < TOP)
            def _():
                dn_copy(level).wait_recv()
                add_into(acc, [acc, from_high.at[level]], rows)
            add_into(outgo.at[local(level, p, q)], [acc], rows)
            dn_copy(level).start()

    def level_at(t):
        return far_level(z, lax.rem(lax.div(t, TWO), HEIGHT))

    def step(t, carry):
        odd = lax.rem(t, TWO)
        if hook is not None:
            with jax.named_scope('hook'):
                hook(t)
        with jax.named_scope('make'):
            pl.when(t < LEVEL)(lambda: make(level_at(t), odd))
        with jax.named_scope('sq'):
            pl.when(jnp.logical_and(t > 0, t < 9))(lambda: send_q(level_at(t + 7), odd * (1 - p) + (1 - odd) * p))
        with jax.named_scope('sp'):
            pl.when(jnp.logical_and(t > TWO, odd == 1))(lambda: send_p(level_at(t + 5)))
        with jax.named_scope('sz'):
            pl.when(jnp.logical_and(t > HEIGHT, odd == 1))(lambda: send_z(level_at(t + TOP)))
        return carry

    lax.fori_loop(0, 10, step, 0)
    add_into(out_ref, gather_here(z), rows)

    @pl.when(z > 0)
    def _():
        up_copy(z).wait_recv()
        add_into(out_ref, [out_ref, from_low.at[z]], rows)

    @pl.when(z < TOP)
    def _():
        dn_copy(z).wait_recv()
        add_into(out_ref, [out_ref, from_high.at[z]], rows)

    for chip in range(CHIPS):
        core_copy(chip).wait_send()
    for level in range(HEIGHT):
        for mid in range(TWO):
            q_copy(level, mid).wait_send()
        p_copy(level).wait_send()
        pl.when(level > z)(lambda: up_copy(level).wait_send())
        pl.when(level < z)(lambda: dn_copy(level).wait_send())


def rank_of(p, q, core):
    return device_of(0, p, q, core)


def level_gather(in_ref, out_ref, send_sem, recv_sem, place):
    me, z, p, q, core = place
    rank = lax.rem(me, LEVEL)
    peers = (device_of(z, 1 - p, q, core), device_of(z, p, 1 - q, core), me + 1 - TWO * core)

    def desc(block, way, src=None):
        return pltpu.make_async_remote_copy(
            src_ref=out_ref.at[block] if src is None else src, dst_ref=out_ref.at[block],
            send_sem=send_sem.at[way * LEVEL + block], recv_sem=recv_sem.at[block],
            device_id=(peers[way],), device_id_type=MESH)

    for way in (1, 0, TWO):
        desc(rank, way, in_ref).start()
    out_ref[rank] = in_ref[...]
    side = rank_of(1 - p, q, core)
    desc(side, 0).wait_recv()
    for way in (1, TWO):
        desc(side, way).start()
    for mid in (p, 1 - p):
        block = rank_of(mid, 1 - q, core)
        desc(block, 1).wait_recv()
        desc(block, TWO).start()
    for chip in range(HEIGHT):
        desc(chip * TWO + 1 - core, TWO).wait_recv()
    desc(rank, 0, in_ref).wait_send()
    desc(rank, 1, in_ref).wait_send()
    desc(side, 1).wait_send()
    for chip in range(HEIGHT):
        desc(chip * TWO + core, TWO).wait_send()


def level_scatter(in_ref, out_ref, from_core, from_q, from_p, outgo, sem_s, sem_r, place, hook=None):
    me, z, p, q, core = place
    rows = out_ref.shape[0]

    def copy(src, dst, slot, dev):
        return pltpu.make_async_remote_copy(
            src_ref=src, dst_ref=dst, send_sem=sem_s.at[slot], recv_sem=sem_r.at[slot],
            device_id=(dev,), device_id_type=MESH)

    def core_copy(chip):
        return copy(in_ref.at[chip * TWO + 1 - core], from_core.at[chip], chip, me + 1 - TWO * core)

    def q_copy(mid):
        return copy(outgo.at[mid], from_q.at[mid], HEIGHT + mid, device_of(z, p, 1 - q, core))

    def p_copy():
        return copy(outgo.at[TWO], from_p, 6, device_of(z, 1 - p, q, core))

    def own(mid, last):
        chip = chip_of(0, mid, last, core)
        core_copy(chip).wait_recv()
        return [in_ref.at[chip * TWO + core], from_core.at[chip]]

    for last in (1 - p, p):
        for mid in (1 - q, q):
            core_copy(chip_of(0, mid, last, 1 - core)).start()
    for mid in (1 - p, p):
        add_into(outgo.at[mid], own(mid, 1 - q), rows)
        q_copy(mid).start()
    if hook is not None:
        with jax.named_scope('lhook'):
            hook()
    side = own(1 - p, q)
    q_copy(1 - p).wait_recv()
    add_into(outgo.at[TWO], side + [from_q.at[1 - p]], rows)
    p_copy().start()
    mine = own(p, q)
    q_copy(p).wait_recv()
    p_copy().wait_recv()
    add_into(out_ref, mine + [from_q.at[p], from_p], rows)
    for chip in range(HEIGHT):
        core_copy(chip).wait_send()
    for mid in range(TWO):
        q_copy(mid).wait_send()
    p_copy().wait_send()


def dot(left, right, ld, rd):
    return lax.dot_general(left, right, (((ld,), (rd,)), ((), ())), preferred_element_type=F32)


TOKS = 512
VPAD = 1024
VROWS = 1004


def id_rows(tok_ref, row, first):
    ids = jnp.concatenate([tok_ref[first + t, row:row + 1, :] for t in range(HEIGHT)], axis=1) - shard_start()
    return jnp.where(jnp.logical_and(ids >= 0, ids < VROWS), ids, -1)


def vocab_iota():
    return lax.broadcasted_iota(jnp.int32, (VPAD, TOKS), 0)


def shard_start():
    return lax.axis_index('fsdp') * VROWS


def fill_table(table, emb_ref):
    table[VPAD - 32:VPAD, :] = jnp.zeros((32, DIM), BF16)
    table[0:VROWS, :] = emb_ref[...]


def halves(level, body):
    def one(i, carry):
        body(level * LEVEL + i * HEIGHT)
        return carry
    lax.fori_loop(0, TWO, one, 0)


def rms_inv(values):
    return lax.rsqrt(jnp.mean(values * values, axis=-1, keepdims=True) + NORM_EPS)


def rms_backward(values, inv_rms, gain_vec, grad_out):
    scaled = grad_out * gain_vec
    return inv_rms * scaled - values * (inv_rms ** TOP) * jnp.mean(scaled * values, axis=-1, keepdims=True)


LEVEL_SCRATCH = [
    pltpu.VMEM((LANE, DIM), BF16), pltpu.VMEM((LEVEL, LANE, DIM), BF16), pltpu.VMEM((LANE, DIM), F32),
    pltpu.VMEM((HEIGHT, LANE, DIM), BF16), pltpu.VMEM((TWO, LANE, DIM), BF16), pltpu.VMEM((LANE, DIM), BF16),
    pltpu.VMEM((TOP, LANE, DIM), BF16),
    pltpu.SemaphoreType.DMA((GROWS,)), pltpu.SemaphoreType.DMA((LEVEL,)),
    pltpu.SemaphoreType.DMA((7,)), pltpu.SemaphoreType.DMA((7,)),
]


def split_weights(gu_ref):
    wide = gu_ref[...].astype(F32)
    return (wide[:, 0:GROWS, :].reshape(DIM, UNITS).astype(BF16), wide[:, GROWS:PAIR, :].reshape(DIM, UNITS).astype(BF16))


GU_SHAPE = (NDEV, PAIR, UNITS)
WD_SHAPE = (HEIGHT, DROWS, DIM)


def call(kernel, name, cid, outs, ins, scratch):
    return pl.pallas_call(
        kernel, out_shape=outs, in_specs=[VSPEC] * len(ins), out_specs=(VSPEC,) * (len(outs) - 1) + (pl.BlockSpec(memory_space=pltpu.SMEM),),
        scratch_shapes=scratch,
        compiler_params=pltpu.CompilerParams(collective_id=cid, has_side_effects=True, vmem_limit_bytes=VMEM_CAP),
        name=name)(*ins)


STAT = 40


def merge_stats(blocks):
    logs = [b[0:32, :] for b in blocks]
    top = logs[0]
    for one in logs[1:]:
        top = jnp.maximum(top, one)
    total = jnp.exp(logs[0] - top)
    labs = blocks[0][32:STAT, :]
    for one, b in zip(logs[1:], blocks[1:]):
        total = total + jnp.exp(one - top)
        labs = labs + b[32:STAT, :]
    return jnp.concatenate([top + jnp.log(total), labs], axis=0)


def step_call(ids, labs, emb, gate, up, down_shard, gain_mlp, gain_final, emb_scale, inv_count):
    def kernel(ids_ref, lab_ref, emb_ref, gate_ref, up_ref, down_ref, gm_ref, gf_ref,
               demb_ref, dgate_ref, dup_ref, dn_ref, loss_ref,
               piece_ref, own_ref, tok_mine, tok_ref, table, spread, whole, gu_ref, wd_ref, a_ref, g_ref, u_ref, dm_ref,
               d_gate, d_up, acts, grad_gate, grad_up, grad_down, ggu, gd, land_g, land_d, outgo, outgo_d, acc,
               block, x_ref, h_ref, dh_ref, dhn_ref, stat, land, land_z, lse_ref,
               sem_t, sem_a, z_send, z_recv, d_send, d_recv, g_send, g_recv, e_send, e_recv, sem_s, sem_b, sem_z, sem_d,
               *scratch):
        ring, (mine, parts, total, *level) = scratch[:12], scratch[12:]
        place = my_place()
        me, z, p, q, core = place
        rank = lax.rem(me, LEVEL)
        gain_m, gain_f = gm_ref[...].reshape(1, DIM), gf_ref[...].reshape(1, DIM)
        tok_mine[...] = jnp.zeros((LEVEL, LANE), jnp.int32)
        tok_mine[0:1, :] = ids_ref[...]
        tok_mine[1:TWO, :] = lab_ref[...]
        both = jnp.concatenate([gate_ref[...].astype(F32), up_ref[...].astype(F32)], axis=0).astype(BF16)
        for r in range(LEVEL):
            piece_ref[r] = jnp.concatenate([both[:, DROWS * (LEVEL * k + r):DROWS * (LEVEL * k + r + 1)] for k in range(HEIGHT)], axis=1)
        with jax.named_scope('barrier'):
            barrier_peers(place)

        def exchange(step):
            peer = lax.rem(rank + step, LEVEL)
            return remote(piece_ref.at[peer], gu_ref.at[me], sem_a, step, z * LEVEL + peer)

        def rows_of(ref, lv):
            return ref.at[pl.ds(lv * LEVEL, LEVEL)]

        def slab(lv, way):
            part = rows_of(gu_ref, lv)
            return pltpu.make_async_remote_copy(
                src_ref=part, dst_ref=part, send_sem=z_send.at[way * HEIGHT + lv], recv_sem=z_recv.at[lv],
                device_id=(me + LEVEL - CHIPS * way,), device_id_type=MESH)

        def slab_down(lv, way, src):
            return pltpu.make_async_remote_copy(
                src_ref=src, dst_ref=wd_ref.at[lv], send_sem=d_send.at[way * HEIGHT + lv], recv_sem=d_recv.at[lv],
                device_id=(me + LEVEL - CHIPS * way,), device_id_type=MESH)

        def tell(step):
            return remote(tok_mine, tok_ref.at[me], sem_t, step, z * LEVEL + lax.rem(rank + step, LEVEL))

        def along_z(src, dst, sems, step):
            return remote(src, dst, sems, 7 + step, lax.rem(me + LEVEL * step, NDEV))

        for step in range(1, LEVEL):
            tell(step).start()
        tok_ref[me] = tok_mine[...]
        wd_ref[z] = down_ref[...]
        gu_ref[me] = piece_ref[rank]
        fill_table(table, emb_ref)
        stat[...] = jnp.zeros_like(stat)
        demb_ref[...] = jnp.zeros_like(demb_ref)
        for step in range(1, LEVEL):
            tell(step).wait()
        part = rows_of(tok_ref, z)
        for step in range(1, HEIGHT):
            along_z(part, part, sem_t, step).start()
        for step in range(1, LEVEL):
            exchange(step).start()
        pl.when(z < TOP)(lambda: slab_down(z, 0, down_ref).start())
        pl.when(z > 0)(lambda: slab_down(z, 1, down_ref).start())
        for step in range(1, HEIGHT):
            along_z(part, part, sem_t, step).wait()
        for step in range(1, LEVEL):
            exchange(step).wait_recv()
        pl.when(z < TOP)(lambda: slab(z, 0).start())
        pl.when(z > 0)(lambda: slab(z, 1).start())

        def take(lv, way, more):
            slab_down(lv, 0, wd_ref.at[lv]).wait_recv()
            pl.when(more)(lambda: slab_down(lv, way, wd_ref.at[lv]).start())
            slab(lv, 0).wait_recv()
            pl.when(more)(lambda: slab(lv, way).start())

        def take_far(far):
            pl.when(z - far >= 0)(lambda: take(z - far, 0, z < TOP))
            pl.when(z + far < HEIGHT)(lambda: take(z + far, 1, z > 0))

        def hit_rows(first):
            return (vocab_iota() == id_rows(tok_ref, 0, first)).astype(F32).astype(BF16)

        def find(first):
            spread[pl.ds(first, HEIGHT)] = dot(hit_rows(first), table[...], 0, 0).astype(BF16).reshape(HEIGHT, LANE, DIM)

        with jax.named_scope('x_scatter'):
            scatter_levels(spread, x_ref, ring, place, find, lambda t: pl.when(t == 6)(lambda: take_far(1)))
        with jax.named_scope('take2'):
            take_far(TWO)
        x = x_ref[...] * emb_scale
        mine[...] = (x * rms_inv(x) * gain_m).astype(BF16)
        with jax.named_scope('a_gather'):
            level_gather(mine, a_ref, level[HEIGHT], level[5], place)
        with jax.named_scope('take3'):
            take_far(TOP)
        for half in range(TWO):
            four = slice(HEIGHT * half, HEIGHT * half + HEIGHT)
            wg, wu = split_weights(gu_ref)
            act_in = a_ref[four].reshape(TOKS, DIM)
            g = dot(act_in, wg, 1, 0).astype(BF16)
            u = dot(act_in, wu, 1, 0).astype(BF16)
            g_ref[half] = g
            u_ref[half] = u
            act = (jax.nn.silu(g.astype(F32)) * u.astype(F32)).astype(BF16)
            acts[half] = act
            parts[four] = dot(act, wd_ref[...].reshape(UNITS, DIM), 1, 0).astype(BF16).reshape(HEIGHT, LANE, DIM)
        with jax.named_scope('lv_scatter'):
            level_scatter(parts, total, *level[:HEIGHT], *level[6:], place)
        h_ref[...] = (x_ref[...] * emb_scale + total[...].astype(BF16).astype(F32)).astype(BF16)
        h32 = h_ref[...].astype(F32)
        block[...] = (h32 * rms_inv(h32) * gain_f).astype(BF16)
        for step in range(1, LEVEL):
            exchange(step).wait_send()

        def sent(lv, way):
            slab(lv, way).wait_send()
            slab_down(lv, way, wd_ref.at[lv]).wait_send()

        def forward(lv):
            def body(first):
                logits = dot(table[...], whole[pl.ds(first, HEIGHT)].reshape(TOKS, DIM), 1, 1)
                row = vocab_iota()
                lab = jnp.sum(jnp.where(row == id_rows(tok_ref, 1, first), logits, 0.0), axis=0, keepdims=True)
                logits = jnp.where(row < VROWS, logits, -1e30)
                top = jnp.max(logits, axis=0, keepdims=True)
                local = top + jnp.log(jnp.sum(jnp.exp(logits - top), axis=0, keepdims=True))
                for t in range(HEIGHT):
                    stat[0, pl.ds(first + t, 1), :] = local[:, t * LANE:(t + 1) * LANE]
                    stat[0, 32:33, :] = stat[0, 32:33, :] + lab[:, t * LANE:(t + 1) * LANE]
            halves(lv, body)

        with jax.named_scope('hn_gather'):
            gather_levels(block, whole, g_send, g_recv, place, forward)
        for lv in range(HEIGHT):
            pl.when(jnp.logical_and(z < TOP, lv <= z))(lambda: sent(lv, 0))
            pl.when(jnp.logical_and(z > 0, lv >= z))(lambda: sent(lv, 1))

        def share(step):
            return remote(stat.at[0], land.at[rank], sem_s, step, z * LEVEL + lax.rem(rank + step, LEVEL))

        for step in range(1, LEVEL):
            share(step).start()
        land[rank] = stat[0]
        for step in range(1, LEVEL):
            share(step).wait()
        stat[1] = merge_stats([land[r] for r in range(LEVEL)])
        for step in range(1, HEIGHT):
            along_z(stat.at[1], land_z.at[z], sem_s, step).start()
        land_z[z] = stat[1]
        for step in range(1, HEIGHT):
            along_z(stat.at[1], land_z.at[z], sem_s, step).wait()
        final = merge_stats([land_z[lv] for lv in range(HEIGHT)])
        lse_ref[...] = final[0:32, :]
        loss_ref[0, 0] = (jnp.sum(final[0:32, :]) - jnp.sum(final[32:STAT, :])) * inv_count

        def backward(first):
            hid = whole[pl.ds(first, HEIGHT)].reshape(TOKS, DIM)
            logits = dot(table[...], hid, 1, 1)
            lse_row = jnp.concatenate([lse_ref[pl.ds(first + t, 1), :] for t in range(HEIGHT)], axis=1)
            row = vocab_iota()
            prob = jnp.exp(jnp.where(row < VROWS, logits, -1e30) - lse_row)
            hit = jnp.where(row == id_rows(tok_ref, 1, first), 1.0, 0.0)
            grad = ((prob - hit) * inv_count).astype(BF16)
            spread[pl.ds(first, HEIGHT)] = dot(grad, table[...], 0, 0).astype(BF16).reshape(HEIGHT, LANE, DIM)
            demb_ref[...] += dot(grad, hid, 1, 0)

        with jax.named_scope('dhn_scatter'):
            scatter_levels(spread, dhn_ref, ring, place, backward)

        h32 = h_ref[...].astype(F32)
        dh_ref[...] = rms_backward(h32, rms_inv(h32), gain_f, dhn_ref[...])
        mine[...] = dh_ref[...].astype(BF16)
        with jax.named_scope('dm_gather'):
            level_gather(mine, dm_ref, level[HEIGHT], level[5], place)
        for half in range(TWO):
            four = slice(HEIGHT * half, HEIGHT * half + HEIGHT)
            wg, wu = split_weights(gu_ref)
            g = g_ref[half].astype(F32)
            u = u_ref[half].astype(F32)
            dq = dot(dm_ref[four].reshape(TOKS, DIM), wd_ref[...].reshape(UNITS, DIM), 1, 1)
            sig = jax.nn.sigmoid(g)
            dg = (dq * u * sig * (1.0 + g * (1.0 - sig))).astype(BF16)
            du = (dq * g * sig).astype(BF16)
            d_gate[half] = dg
            d_up[half] = du
            parts[four] = (dot(dg, wg, 1, 1) + dot(du, wu, 1, 1)).astype(BF16).reshape(HEIGHT, LANE, DIM)
        def add_slab(dst, srcs):
            def body(i, carry):
                value = srcs[0][i].astype(F32)
                for src in srcs[1:]:
                    value = value + src[i].astype(F32)
                dst[i] = value.astype(dst.dtype)
                return carry
            lax.fori_loop(0, LEVEL, body, 0)

        def hop(lv, way, here=False):
            land = rows_of(land_g, HEIGHT if here and way else lv)
            return remote(rows_of(outgo, lv), land, sem_z, way * HEIGHT + lv, me + LEVEL - CHIPS * way)

        def hop_d(lv, way, here=False):
            return remote(outgo_d.at[lv], land_d.at[HEIGHT if here and way else lv], sem_d, way * HEIGHT + lv, me + LEVEL - CHIPS * way)

        def send(lv, way, more, here):
            @pl.when(more)
            def _():
                hop(lv, way).wait_recv()
                add_slab(rows_of(outgo, lv), [rows_of(ggu, lv), rows_of(land_g, lv)])
                hop_d(lv, way).wait_recv()
                add_into(outgo_d.at[lv], [gd.at[lv], land_d.at[lv]], DROWS)

            @pl.when(jnp.logical_not(more))
            def _():
                add_slab(rows_of(outgo, lv), [rows_of(ggu, lv)])
                add_into(outgo_d.at[lv], [gd.at[lv]], DROWS)
            hop(lv, way, here).start()
            hop_d(lv, way, here).start()

        def send_far(far):
            pl.when(z + far < HEIGHT)(lambda: send(z + far, 0, z > 0, far == 1))
            pl.when(z - far >= 0)(lambda: send(z - far, 1, z < TOP, far == 1))

        def weight_grads():
            for half in range(TWO):
                four = slice(HEIGHT * half, HEIGHT * half + HEIGHT)
                act_in = a_ref[four].reshape(TOKS, DIM)
                news = (dot(act_in, d_gate[half], 0, 0), dot(act_in, d_up[half], 0, 0),
                        dot(acts[half], dm_ref[four].reshape(TOKS, DIM), 0, 0))
                for ref, new in zip((grad_gate, grad_up, grad_down), news):
                    ref[...] = new if half == 0 else ref[...] + new
            both = jnp.concatenate([grad_gate[...].reshape(NDEV, GROWS, UNITS), grad_up[...].reshape(NDEV, GROWS, UNITS)], axis=1)
            ggu[...] = both.astype(BF16)
            gd[...] = grad_down[...].astype(BF16).reshape(WD_SHAPE)

        def grads_off():
            weight_grads()
            send_far(TOP)

        with jax.named_scope('lv_scatter'):
            level_scatter(parts, total, *level[:HEIGHT], *level[6:], place, grads_off)
        x = x_ref[...] * emb_scale
        block[...] = (dh_ref[...] + rms_backward(x, rms_inv(x), gain_m, total[...])).astype(BF16)

        with jax.named_scope('far2'):
            send_far(TWO)
        demb_ref[...] = demb_ref[...] * (1.0 / emb_scale)

        def add_rows(lv):
            def body(first):
                demb_ref[...] += dot(hit_rows(first), whole[pl.ds(first, HEIGHT)].reshape(TOKS, DIM), 1, 0)
            halves(lv, body)

        def last(way):
            hop(z, way).wait_recv()
            add_slab(acc, [acc, rows_of(land_g, HEIGHT if way else z)])
            hop_d(z, way).wait_recv()
            add_into(dn_ref, [dn_ref, land_d.at[HEIGHT if way else z]], DROWS)

        def give(step):
            peer = lax.rem(rank + step, LEVEL)
            return remote(acc.at[peer], own_ref.at[rank], sem_b, step, z * LEVEL + peer)

        def grads_home():
            add_slab(acc, [rows_of(ggu, z)])
            add_into(dn_ref, [gd.at[z]], DROWS)
            pl.when(z > 0)(lambda: last(0))
            pl.when(z < TOP)(lambda: last(1))
            for step in range(1, LEVEL):
                give(step).start()
            own_ref[rank] = acc[rank]

        def grads_step(t):
            pl.when(t == HEIGHT)(grads_home)

        def grads_late(t):
            pl.when(t == 1)(lambda: send_far(1))

        with jax.named_scope('dx_gather'):
            gather_levels(block, whole, e_send, e_recv, place, add_rows, grads_step, grads_late)
        for step in range(1, LEVEL):
            with jax.named_scope('tgive'):
                give(step).wait_recv()
        for step in range(1, LEVEL):
            give(step).wait_send()
        for k in range(HEIGHT):
            got = jnp.concatenate([own_ref[r, :, DROWS * k:DROWS * (k + 1)] for r in range(LEVEL)], axis=1)
            dgate_ref[:, DIM * k:DIM * (k + 1)] = got[0:GROWS]
            dup_ref[:, DIM * k:DIM * (k + 1)] = got[GROWS:PAIR]

        def gone(lv, way):
            hop(lv, way).wait_send()
            hop_d(lv, way).wait_send()

        for lv in range(HEIGHT):
            pl.when(lv > z)(lambda: gone(lv, 0))
            pl.when(lv < z)(lambda: gone(lv, 1))

    whole = pltpu.VMEM((NDEV, LANE, DIM), BF16)
    block, flat = pltpu.VMEM((LANE, DIM), BF16), pltpu.VMEM((LANE, DIM), F32)
    slab, slab_d = pltpu.VMEM(GU_SHAPE, BF16), pltpu.VMEM(WD_SHAPE, BF16)
    unit, eight = pltpu.VMEM((TWO, TOKS, UNITS), BF16), pltpu.VMEM((LEVEL, LANE, DIM), BF16)
    wide, tall = pltpu.VMEM((DIM, UNITS), F32), pltpu.VMEM((UNITS, DIM), F32)
    dma = pltpu.SemaphoreType.DMA
    return call(
        kernel, 'step', 0,
        (jax.ShapeDtypeStruct((VPAD, DIM), F32), jax.ShapeDtypeStruct((GROWS, 3072), F32), jax.ShapeDtypeStruct((GROWS, 3072), F32),
         jax.ShapeDtypeStruct((DROWS, DIM), F32), jax.ShapeDtypeStruct((1, 1), F32)),
        (ids, labs, emb, gate, up, down_shard, gain_mlp, gain_final),
        [pltpu.VMEM((LEVEL, PAIR, UNITS), BF16), pltpu.VMEM((LEVEL, PAIR, UNITS), F32), pltpu.VMEM((LEVEL, LANE), jnp.int32), pltpu.VMEM((NDEV, LEVEL, LANE), jnp.int32), pltpu.VMEM((VPAD, DIM), BF16), whole, whole,
         slab, slab_d, eight, unit, unit, eight, unit, unit, unit, wide, wide, tall, slab, slab_d,
         pltpu.VMEM((5 * LEVEL, PAIR, UNITS), BF16), pltpu.VMEM((5, DROWS, DIM), BF16), slab, slab_d,
         pltpu.VMEM((LEVEL, PAIR, UNITS), F32), block, flat, block, flat, flat,
         pltpu.VMEM((TWO, STAT, LANE), F32), pltpu.VMEM((LEVEL, STAT, LANE), F32), pltpu.VMEM((HEIGHT, STAT, LANE), F32),
         pltpu.VMEM((32, LANE), F32),
         sem_pair(11), sem_pair(LEVEL), dma((LEVEL,)), dma((HEIGHT,)), dma((LEVEL,)), dma((HEIGHT,)), dma((5, NDEV)), dma((NDEV,)),
         dma((5, NDEV)), dma((NDEV,)), sem_pair(11), sem_pair(LEVEL), sem_pair(LEVEL), sem_pair(LEVEL)]
        + scatter_scratch(LANE, DIM) + LEVEL_SCRATCH)


def solution(mesh):
    group = mesh.shape['fsdp']

    def local_step(ids_blk, lab_blk, emb_shard, gate_shard, up_shard, down_shard, gain_mlp, gain_final):
        emb_scale = math.sqrt(emb_shard.shape[1])
        inv_count = 1.0 / (ids_blk.size * group)
        d_embed, d_gate, d_up, d_down, loss = step_call(
            ids_blk, lab_blk, emb_shard, gate_shard, up_shard, down_shard, gain_mlp, gain_final, emb_scale, inv_count)
        return loss[0, 0], d_embed[0:VROWS] * emb_scale, d_gate, d_up, d_down

    shard_spec = P('fsdp', None)
    return jax.shard_map(local_step, mesh=mesh, in_specs=(shard_spec, shard_spec, shard_spec, shard_spec, shard_spec, shard_spec, P(), P()), out_specs=(P(), shard_spec, shard_spec, shard_spec, shard_spec), check_vma=False)
```

```python
import math
import jax
import jax.numpy as jnp
from jax import lax
from jax.experimental import pallas as pl
from jax.experimental.pallas import tpu as pltpu
from jax.sharding import PartitionSpec as P

NORM_EPS = 1e-6
MESH = pl.DeviceIdType.MESH
F32 = jnp.float32
BF16 = jnp.bfloat16
VMEM_CAP = 63 * 1024 * 1024
LANE = 128
DIM = 768
PAIR = 48
UNITS = 384
NDEV = 32
LEVEL = 8
HEIGHT = 4
DROWS = 96
CHIPS = 16
GROWS = 24
TWO = 2
TOP = 3
VSPEC = pl.BlockSpec(memory_space=pltpu.VMEM)


def my_place():
    me = lax.axis_index('fsdp')
    core = lax.rem(me, TWO)
    x = lax.rem(lax.div(me, TWO), TWO)
    y = lax.rem(lax.div(me, HEIGHT), TWO)
    z = lax.div(me, LEVEL)
    p = x * (1 - core) + y * core
    q = y * (1 - core) + x * core
    return me, z, p, q, core


def chip_of(z, p, q, core):
    x = p * (1 - core) + q * core
    y = q * (1 - core) + p * core
    return (z * TWO + y) * TWO + x


def device_of(z, p, q, core):
    return chip_of(z, p, q, core) * TWO + core


def barrier_peers(place):
    me, z = place[0], place[1]
    sem = pltpu.get_barrier_semaphore()
    for step in range(1, LEVEL):
        dev = z * LEVEL + lax.rem(me + step, LEVEL)
        pl.semaphore_signal(sem, inc=1, device_id=(dev,), device_id_type=MESH)
    for step in range(1, HEIGHT):
        dev = lax.rem(me + LEVEL * step, NDEV)
        pl.semaphore_signal(sem, inc=1, device_id=(dev,), device_id_type=MESH)
    pl.semaphore_wait(sem, 10)


def far_level(z, at):
    half = lax.div(z, TWO)
    inner = lax.rem(z + half, TWO)
    order = (TOP - TOP * half, (1 - inner) * (TWO - half) + inner * TOP * half, 1 + lax.rem(z, TWO), z)
    if isinstance(at, int):
        return order[at]
    low, high = lax.rem(at, TWO), lax.div(at, TWO)
    return ((1 - low) * (1 - high) * order[0] + low * (1 - high) * order[1]
            + (1 - low) * high * order[TWO] + low * high * order[TOP])


def remote(src, dst, sems, slot, dev):
    return pltpu.make_async_remote_copy(
        src_ref=src, dst_ref=dst, send_sem=sems.at[0, slot], recv_sem=sems.at[1, slot],
        device_id=(dev,), device_id_type=MESH)


def sem_pair(n):
    return pltpu.SemaphoreType.DMA((TWO, n))


def gather_levels(in_ref, out_ref, send_sem, recv_sem, place, work, hook=None, late_hook=None):
    me, z, p, q, core = place
    peers = (me + LEVEL, me - LEVEL, device_of(z, 1 - p, q, core), device_of(z, p, 1 - q, core), me + 1 - TWO * core)

    def desc(block, way, src=None):
        return pltpu.make_async_remote_copy(
            src_ref=out_ref.at[block] if src is None else src, dst_ref=out_ref.at[block],
            send_sem=send_sem.at[way, block], recv_sem=recv_sem.at[block],
            device_id=(peers[way],), device_id_type=MESH)

    def got(block):
        desc(block, HEIGHT).wait_recv()

    pl.when(z < TOP)(lambda: desc(me, 0, in_ref).start())
    pl.when(z > 0)(lambda: desc(me, 1, in_ref).start())
    for way in (TOP, TWO, HEIGHT):
        desc(me, way, in_ref).start()
    out_ref[me] = in_ref[...]

    def take_z(level):
        block = device_of(level, p, q, core)
        got(block)
        pl.when(jnp.logical_and(level < z, z < TOP))(lambda: desc(block, 0).start())
        pl.when(jnp.logical_and(level > z, z > 0))(lambda: desc(block, 1).start())
        for way in (TOP, TWO, HEIGHT):
            desc(block, way).start()

    def take_p(level):
        block = device_of(level, 1 - p, q, core)
        got(block)
        for way in (TOP, HEIGHT):
            desc(block, way).start()

    def take_q(level):
        for mid in (p, 1 - p):
            block = device_of(level, mid, 1 - q, core)
            got(block)
            desc(block, HEIGHT).start()
        for chip in range(HEIGHT):
            got(level * LEVEL + chip * TWO + 1 - core)

    def step(t, carry):
        if hook is not None:
            with jax.named_scope('hook'):
                hook(t)
        with jax.named_scope('tz'):
            pl.when(jnp.logical_or(t == 0, jnp.logical_and(t < TOP, outer)))(lambda: take_z(far_level(z, TWO - lax.rem(t, TOP))))
        with jax.named_scope('tz2'):
            pl.when(jnp.logical_and(t == 0, inner))(lambda: take_z(far_level(z, 1)))
        with jax.named_scope('tp'):
            pl.when(jnp.logical_and(t > 0, t < HEIGHT))(lambda: take_p(far_level(z, TOP - lax.rem(t, HEIGHT))))
        with jax.named_scope('tz3'):
            pl.when(jnp.logical_and(t == 1, inner))(lambda: take_z(far_level(z, 0)))
        if late_hook is not None:
            with jax.named_scope('late'):
                late_hook(t)

        @pl.when(t > 0)
        def _():
            level = far_level(z, HEIGHT - (t + lax.div(HEIGHT - t, HEIGHT)))
            with jax.named_scope('tq'):
                take_q(level)
            with jax.named_scope('gwork'):
                work(level)
        return carry

    outer = jnp.logical_or(z == 0, z == TOP)
    inner = jnp.logical_not(outer)
    with jax.named_scope('tp0'):
        take_p(z)
    lax.fori_loop(0, 5, step, 0)
    for level in range(HEIGHT):
        desc(device_of(level, p, q, core), TWO).wait_send()
        for mid in range(TWO):
            desc(device_of(level, mid, q, core), TOP).wait_send()
        pl.when(jnp.logical_and(z < TOP, level <= z))(lambda: desc(device_of(level, p, q, core), 0).wait_send())
        pl.when(jnp.logical_and(z > 0, level >= z))(lambda: desc(device_of(level, p, q, core), 1).wait_send())
    for chip in range(CHIPS):
        desc(chip * TWO + core, HEIGHT).wait_send()


def add_into(dst, srcs, rows):
    step = 32

    def body(i, carry):
        sl = pl.ds(pl.multiple_of(i * step, step), step)
        total = srcs[0][sl, :].astype(F32)
        for src in srcs[1:]:
            total = total + src[sl, :].astype(F32)
        dst[sl, :] = total.astype(dst.dtype)
        return carry

    lax.fori_loop(0, rows // step, body, 0)


def scatter_scratch(rows, cols):
    return [
        pltpu.VMEM((CHIPS, rows, cols), BF16), pltpu.VMEM((LEVEL, rows, cols), BF16), pltpu.VMEM((HEIGHT, rows, cols), BF16),
        pltpu.VMEM((HEIGHT, rows, cols), BF16), pltpu.VMEM((HEIGHT, rows, cols), BF16), pltpu.VMEM((CHIPS, rows, cols), BF16),
        pltpu.VMEM((rows, cols), F32),
        pltpu.SemaphoreType.DMA((TWO, CHIPS)), pltpu.SemaphoreType.DMA((TWO, LEVEL)), pltpu.SemaphoreType.DMA((TWO, HEIGHT)),
        pltpu.SemaphoreType.DMA((TWO, HEIGHT)), pltpu.SemaphoreType.DMA((TWO, HEIGHT)),
    ]


def scatter_levels(in_ref, out_ref, scratch, place, work, hook=None):
    from_core, from_q, from_p, from_low, from_high, outgo, acc, sem_c, sem_q, sem_p, sem_up, sem_dn = scratch
    me, z, p, q, core = place
    rows = out_ref.shape[0]
    other = 1 - core

    def core_copy(chip):
        return remote(in_ref.at[chip * TWO + other], from_core.at[chip], sem_c, chip, me + 1 - TWO * core)

    def local(level, mid, last):
        return level * HEIGHT + mid * TWO + last

    def q_copy(level, mid):
        return remote(outgo.at[local(level, mid, 1 - q)], from_q.at[level * TWO + mid], sem_q, level * TWO + mid,
                      device_of(z, p, 1 - q, core))

    def p_copy(level):
        return remote(outgo.at[local(level, 1 - p, q)], from_p.at[level], sem_p, level, device_of(z, 1 - p, q, core))

    def up_copy(level):
        return remote(outgo.at[local(level, p, q)], from_low.at[level], sem_up, level, me + LEVEL)

    def dn_copy(level):
        return remote(outgo.at[local(level, p, q)], from_high.at[level], sem_dn, level, me - LEVEL)

    def own(level, mid, last):
        chip = chip_of(level, mid, last, core)
        core_copy(chip).wait_recv()
        return [in_ref.at[chip * TWO + core], from_core.at[chip]]

    y = q * (1 - core) + p * core
    x = p * (1 - core) + q * core

    def make(level, half):
        row = level * HEIGHT + TWO * (y * half + (1 - y) * (1 - half))
        work(row * TWO)
        for side in (1 - x, x):
            core_copy(row + side).start()

    def send_q(level, mid):
        add_into(outgo.at[local(level, mid, 1 - q)], own(level, mid, 1 - q), rows)
        q_copy(level, mid).start()

    def send_p(level):
        side = own(level, 1 - p, q)
        q_copy(level, 1 - p).wait_recv()
        add_into(outgo.at[local(level, 1 - p, q)], side + [from_q.at[level * TWO + 1 - p]], rows)
        p_copy(level).start()

    def gather_here(level):
        mine = own(level, p, q)
        q_copy(level, p).wait_recv()
        p_copy(level).wait_recv()
        return mine + [from_q.at[level * TWO + p], from_p.at[level]]

    def send_z(level):
        add_into(acc, gather_here(level), rows)

        @pl.when(level > z)
        def _():
            @pl.when(z > 0)
            def _():
                up_copy(level).wait_recv()
                add_into(acc, [acc, from_low.at[level]], rows)
            add_into(outgo.at[local(level, p, q)], [acc], rows)
            up_copy(level).start()

        @pl.when(level < z)
        def _():
            @pl.when(z < TOP)
            def _():
                dn_copy(level).wait_recv()
                add_into(acc, [acc, from_high.at[level]], rows)
            add_into(outgo.at[local(level, p, q)], [acc], rows)
            dn_copy(level).start()

    def level_at(t):
        return far_level(z, lax.rem(lax.div(t, TWO), HEIGHT))

    def step(t, carry):
        odd = lax.rem(t, TWO)
        if hook is not None:
            with jax.named_scope('hook'):
                hook(t)
        with jax.named_scope('make'):
            pl.when(t < LEVEL)(lambda: make(level_at(t), odd))
        with jax.named_scope('sq'):
            pl.when(jnp.logical_and(t > 0, t < 9))(lambda: send_q(level_at(t + 7), odd * (1 - p) + (1 - odd) * p))
        with jax.named_scope('szi1'):
            pl.when(jnp.logical_and(t == 9, inner))(lambda: send_z(far_level(z, 1)))
        with jax.named_scope('sp'):
            pl.when(jnp.logical_and(t > TWO, odd == 1))(lambda: send_p(level_at(t + 5)))
        with jax.named_scope('sz'):
            pl.when(jnp.logical_and(jnp.logical_and(t > HEIGHT, odd == 1), outer))(lambda: send_z(level_at(t + TOP)))
        with jax.named_scope('szi'):
            pl.when(jnp.logical_and(jnp.logical_and(t > 6, odd == 1), inner))(lambda: send_z(far_level(z, TWO * lax.div(t, 9))))
        return carry

    outer = jnp.logical_or(z == 0, z == TOP)
    inner = jnp.logical_not(outer)
    lax.fori_loop(0, 10, step, 0)
    add_into(out_ref, gather_here(z), rows)

    @pl.when(z > 0)
    def _():
        up_copy(z).wait_recv()
        add_into(out_ref, [out_ref, from_low.at[z]], rows)

    @pl.when(z < TOP)
    def _():
        dn_copy(z).wait_recv()
        add_into(out_ref, [out_ref, from_high.at[z]], rows)

    for chip in range(CHIPS):
        core_copy(chip).wait_send()
    for level in range(HEIGHT):
        for mid in range(TWO):
            q_copy(level, mid).wait_send()
        p_copy(level).wait_send()
        pl.when(level > z)(lambda: up_copy(level).wait_send())
        pl.when(level < z)(lambda: dn_copy(level).wait_send())


def rank_of(p, q, core):
    return device_of(0, p, q, core)


def level_gather(in_ref, out_ref, send_sem, recv_sem, place):
    me, z, p, q, core = place
    rank = lax.rem(me, LEVEL)
    peers = (device_of(z, 1 - p, q, core), device_of(z, p, 1 - q, core), me + 1 - TWO * core)

    def desc(block, way, src=None):
        return pltpu.make_async_remote_copy(
            src_ref=out_ref.at[block] if src is None else src, dst_ref=out_ref.at[block],
            send_sem=send_sem.at[way * LEVEL + block], recv_sem=recv_sem.at[block],
            device_id=(peers[way],), device_id_type=MESH)

    for way in (1, 0, TWO):
        desc(rank, way, in_ref).start()
    out_ref[rank] = in_ref[...]
    side = rank_of(1 - p, q, core)
    desc(side, 0).wait_recv()
    for way in (1, TWO):
        desc(side, way).start()
    for mid in (p, 1 - p):
        block = rank_of(mid, 1 - q, core)
        desc(block, 1).wait_recv()
        desc(block, TWO).start()
    for chip in range(HEIGHT):
        desc(chip * TWO + 1 - core, TWO).wait_recv()
    desc(rank, 0, in_ref).wait_send()
    desc(rank, 1, in_ref).wait_send()
    desc(side, 1).wait_send()
    for chip in range(HEIGHT):
        desc(chip * TWO + core, TWO).wait_send()


def level_scatter(in_ref, out_ref, from_core, from_q, from_p, outgo, sem_s, sem_r, place, hook=None):
    me, z, p, q, core = place
    rows = out_ref.shape[0]

    def copy(src, dst, slot, dev):
        return pltpu.make_async_remote_copy(
            src_ref=src, dst_ref=dst, send_sem=sem_s.at[slot], recv_sem=sem_r.at[slot],
            device_id=(dev,), device_id_type=MESH)

    def core_copy(chip):
        return copy(in_ref.at[chip * TWO + 1 - core], from_core.at[chip], chip, me + 1 - TWO * core)

    def q_copy(mid):
        return copy(outgo.at[mid], from_q.at[mid], HEIGHT + mid, device_of(z, p, 1 - q, core))

    def p_copy():
        return copy(outgo.at[TWO], from_p, 6, device_of(z, 1 - p, q, core))

    def own(mid, last):
        chip = chip_of(0, mid, last, core)
        core_copy(chip).wait_recv()
        return [in_ref.at[chip * TWO + core], from_core.at[chip]]

    for last in (1 - p, p):
        for mid in (1 - q, q):
            core_copy(chip_of(0, mid, last, 1 - core)).start()
    for mid in (1 - p, p):
        add_into(outgo.at[mid], own(mid, 1 - q), rows)
        q_copy(mid).start()
    if hook is not None:
        with jax.named_scope('lhook'):
            hook()
    side = own(1 - p, q)
    q_copy(1 - p).wait_recv()
    add_into(outgo.at[TWO], side + [from_q.at[1 - p]], rows)
    p_copy().start()
    mine = own(p, q)
    q_copy(p).wait_recv()
    p_copy().wait_recv()
    add_into(out_ref, mine + [from_q.at[p], from_p], rows)
    for chip in range(HEIGHT):
        core_copy(chip).wait_send()
    for mid in range(TWO):
        q_copy(mid).wait_send()
    p_copy().wait_send()


def dot(left, right, ld, rd):
    return lax.dot_general(left, right, (((ld,), (rd,)), ((), ())), preferred_element_type=F32)


TOKS = 512
VPAD = 1024
VROWS = 1004


def id_rows(tok_ref, row, first):
    ids = jnp.concatenate([tok_ref[first + t, row:row + 1, :] for t in range(HEIGHT)], axis=1) - shard_start()
    return jnp.where(jnp.logical_and(ids >= 0, ids < VROWS), ids, -1)


def vocab_iota():
    return lax.broadcasted_iota(jnp.int32, (VPAD, TOKS), 0)


def shard_start():
    return lax.axis_index('fsdp') * VROWS


def fill_table(table, emb_ref):
    table[VPAD - 32:VPAD, :] = jnp.zeros((32, DIM), BF16)
    table[0:VROWS, :] = emb_ref[...]


def halves(level, body):
    def one(i, carry):
        body(level * LEVEL + i * HEIGHT)
        return carry
    lax.fori_loop(0, TWO, one, 0)


def rms_inv(values):
    return lax.rsqrt(jnp.mean(values * values, axis=-1, keepdims=True) + NORM_EPS)


def rms_backward(values, inv_rms, gain_vec, grad_out):
    scaled = grad_out * gain_vec
    return inv_rms * scaled - values * (inv_rms ** TOP) * jnp.mean(scaled * values, axis=-1, keepdims=True)


LEVEL_SCRATCH = [
    pltpu.VMEM((LANE, DIM), BF16), pltpu.VMEM((LEVEL, LANE, DIM), BF16), pltpu.VMEM((LANE, DIM), F32),
    pltpu.VMEM((HEIGHT, LANE, DIM), BF16), pltpu.VMEM((TWO, LANE, DIM), BF16), pltpu.VMEM((LANE, DIM), BF16),
    pltpu.VMEM((TOP, LANE, DIM), BF16),
    pltpu.SemaphoreType.DMA((GROWS,)), pltpu.SemaphoreType.DMA((LEVEL,)),
    pltpu.SemaphoreType.DMA((7,)), pltpu.SemaphoreType.DMA((7,)),
]


def split_weights(gu_ref):
    wide = gu_ref[...].astype(F32)
    return (wide[:, 0:GROWS, :].reshape(DIM, UNITS).astype(BF16), wide[:, GROWS:PAIR, :].reshape(DIM, UNITS).astype(BF16))


GU_SHAPE = (NDEV, PAIR, UNITS)
WD_SHAPE = (HEIGHT, DROWS, DIM)


def call(kernel, name, cid, outs, ins, scratch):
    return pl.pallas_call(
        kernel, out_shape=outs, in_specs=[VSPEC] * len(ins), out_specs=(VSPEC,) * (len(outs) - 1) + (pl.BlockSpec(memory_space=pltpu.SMEM),),
        scratch_shapes=scratch,
        compiler_params=pltpu.CompilerParams(collective_id=cid, has_side_effects=True, vmem_limit_bytes=VMEM_CAP),
        name=name)(*ins)


STAT = 40


def merge_stats(blocks):
    logs = [b[0:32, :] for b in blocks]
    top = logs[0]
    for one in logs[1:]:
        top = jnp.maximum(top, one)
    total = jnp.exp(logs[0] - top)
    labs = blocks[0][32:STAT, :]
    for one, b in zip(logs[1:], blocks[1:]):
        total = total + jnp.exp(one - top)
        labs = labs + b[32:STAT, :]
    return jnp.concatenate([top + jnp.log(total), labs], axis=0)


def step_call(ids, labs, emb, gate, up, down_shard, gain_mlp, gain_final, emb_scale, inv_count):
    def kernel(ids_ref, lab_ref, emb_ref, gate_ref, up_ref, down_ref, gm_ref, gf_ref,
               demb_ref, dgate_ref, dup_ref, dn_ref, loss_ref,
               piece_ref, own_ref, tok_mine, tok_ref, table, spread, whole, gu_ref, wd_ref, a_ref, g_ref, u_ref, dm_ref,
               d_gate, d_up, acts, grad_gate, grad_up, grad_down, ggu, gd, land_g, land_d, outgo, outgo_d, acc,
               block, x_ref, h_ref, dh_ref, dhn_ref, stat, land, land_z, lse_ref,
               sem_t, sem_a, z_send, z_recv, d_send, d_recv, g_send, g_recv, e_send, e_recv, sem_s, sem_b, sem_z, sem_d,
               *scratch):
        ring, (mine, parts, total, *level) = scratch[:12], scratch[12:]
        place = my_place()
        me, z, p, q, core = place
        rank = lax.rem(me, LEVEL)
        gain_m, gain_f = gm_ref[...].reshape(1, DIM), gf_ref[...].reshape(1, DIM)
        tok_mine[...] = jnp.zeros((LEVEL, LANE), jnp.int32)
        tok_mine[0:1, :] = ids_ref[...]
        tok_mine[1:TWO, :] = lab_ref[...]
        both = jnp.concatenate([gate_ref[...].astype(F32), up_ref[...].astype(F32)], axis=0).astype(BF16)
        for r in range(LEVEL):
            piece_ref[r] = jnp.concatenate([both[:, DROWS * (LEVEL * k + r):DROWS * (LEVEL * k + r + 1)] for k in range(HEIGHT)], axis=1)
        with jax.named_scope('barrier'):
            barrier_peers(place)

        def exchange(step):
            peer = lax.rem(rank + step, LEVEL)
            return remote(piece_ref.at[peer], gu_ref.at[me], sem_a, step, z * LEVEL + peer)

        def rows_of(ref, lv):
            return ref.at[pl.ds(lv * LEVEL, LEVEL)]

        def slab(lv, way):
            part = rows_of(gu_ref, lv)
            return pltpu.make_async_remote_copy(
                src_ref=part, dst_ref=part, send_sem=z_send.at[way * HEIGHT + lv], recv_sem=z_recv.at[lv],
                device_id=(me + LEVEL - CHIPS * way,), device_id_type=MESH)

        def slab_down(lv, way, src):
            return pltpu.make_async_remote_copy(
                src_ref=src, dst_ref=wd_ref.at[lv], send_sem=d_send.at[way * HEIGHT + lv], recv_sem=d_recv.at[lv],
                device_id=(me + LEVEL - CHIPS * way,), device_id_type=MESH)

        def tell(step):
            return remote(tok_mine, tok_ref.at[me], sem_t, step, z * LEVEL + lax.rem(rank + step, LEVEL))

        def along_z(src, dst, sems, step):
            return remote(src, dst, sems, 7 + step, lax.rem(me + LEVEL * step, NDEV))

        for step in range(1, LEVEL):
            tell(step).start()
        tok_ref[me] = tok_mine[...]
        wd_ref[z] = down_ref[...]
        gu_ref[me] = piece_ref[rank]
        fill_table(table, emb_ref)
        stat[...] = jnp.zeros_like(stat)
        demb_ref[...] = jnp.zeros_like(demb_ref)
        for step in range(1, LEVEL):
            tell(step).wait()
        part = rows_of(tok_ref, z)
        for step in range(1, HEIGHT):
            along_z(part, part, sem_t, step).start()
        for step in range(1, LEVEL):
            exchange(step).start()
        pl.when(z < TOP)(lambda: slab_down(z, 0, down_ref).start())
        pl.when(z > 0)(lambda: slab_down(z, 1, down_ref).start())
        for step in range(1, HEIGHT):
            along_z(part, part, sem_t, step).wait()
        for step in range(1, LEVEL):
            exchange(step).wait_recv()
        pl.when(z < TOP)(lambda: slab(z, 0).start())
        pl.when(z > 0)(lambda: slab(z, 1).start())

        def take(lv, way, more):
            slab_down(lv, 0, wd_ref.at[lv]).wait_recv()
            pl.when(more)(lambda: slab_down(lv, way, wd_ref.at[lv]).start())
            slab(lv, 0).wait_recv()
            pl.when(more)(lambda: slab(lv, way).start())

        def take_far(far):
            pl.when(z - far >= 0)(lambda: take(z - far, 0, z < TOP))
            pl.when(z + far < HEIGHT)(lambda: take(z + far, 1, z > 0))

        def hit_rows(first):
            return (vocab_iota() == id_rows(tok_ref, 0, first)).astype(F32).astype(BF16)

        def find(first):
            spread[pl.ds(first, HEIGHT)] = dot(hit_rows(first), table[...], 0, 0).astype(BF16).reshape(HEIGHT, LANE, DIM)

        with jax.named_scope('x_scatter'):
            scatter_levels(spread, x_ref, ring, place, find, lambda t: pl.when(t == 6)(lambda: take_far(1)))
        with jax.named_scope('take2'):
            take_far(TWO)
        x = x_ref[...] * emb_scale
        mine[...] = (x * rms_inv(x) * gain_m).astype(BF16)
        with jax.named_scope('a_gather'):
            level_gather(mine, a_ref, level[HEIGHT], level[5], place)
        with jax.named_scope('take3'):
            take_far(TOP)
        for half in range(TWO):
            four = slice(HEIGHT * half, HEIGHT * half + HEIGHT)
            wg, wu = split_weights(gu_ref)
            act_in = a_ref[four].reshape(TOKS, DIM)
            g = dot(act_in, wg, 1, 0).astype(BF16)
            u = dot(act_in, wu, 1, 0).astype(BF16)
            g_ref[half] = g
            u_ref[half] = u
            act = (jax.nn.silu(g.astype(F32)) * u.astype(F32)).astype(BF16)
            acts[half] = act
            parts[four] = dot(act, wd_ref[...].reshape(UNITS, DIM), 1, 0).astype(BF16).reshape(HEIGHT, LANE, DIM)
        with jax.named_scope('lv_scatter'):
            level_scatter(parts, total, *level[:HEIGHT], *level[6:], place)
        h_ref[...] = (x_ref[...] * emb_scale + total[...].astype(BF16).astype(F32)).astype(BF16)
        h32 = h_ref[...].astype(F32)
        block[...] = (h32 * rms_inv(h32) * gain_f).astype(BF16)
        for step in range(1, LEVEL):
            exchange(step).wait_send()

        def sent(lv, way):
            slab(lv, way).wait_send()
            slab_down(lv, way, wd_ref.at[lv]).wait_send()

        def forward(lv):
            def body(first):
                logits = dot(table[...], whole[pl.ds(first, HEIGHT)].reshape(TOKS, DIM), 1, 1)
                row = vocab_iota()
                lab = jnp.sum(jnp.where(row == id_rows(tok_ref, 1, first), logits, 0.0), axis=0, keepdims=True)
                logits = jnp.where(row < VROWS, logits, -1e30)
                top = jnp.max(logits, axis=0, keepdims=True)
                local = top + jnp.log(jnp.sum(jnp.exp(logits - top), axis=0, keepdims=True))
                for t in range(HEIGHT):
                    stat[0, pl.ds(first + t, 1), :] = local[:, t * LANE:(t + 1) * LANE]
                    stat[0, 32:33, :] = stat[0, 32:33, :] + lab[:, t * LANE:(t + 1) * LANE]
            halves(lv, body)

        with jax.named_scope('hn_gather'):
            gather_levels(block, whole, g_send, g_recv, place, forward)
        for lv in range(HEIGHT):
            pl.when(jnp.logical_and(z < TOP, lv <= z))(lambda: sent(lv, 0))
            pl.when(jnp.logical_and(z > 0, lv >= z))(lambda: sent(lv, 1))

        def share(step):
            return remote(stat.at[0], land.at[rank], sem_s, step, z * LEVEL + lax.rem(rank + step, LEVEL))

        for step in range(1, LEVEL):
            share(step).start()
        land[rank] = stat[0]
        for step in range(1, LEVEL):
            share(step).wait()
        stat[1] = merge_stats([land[r] for r in range(LEVEL)])
        for step in range(1, HEIGHT):
            along_z(stat.at[1], land_z.at[z], sem_s, step).start()
        land_z[z] = stat[1]
        for step in range(1, HEIGHT):
            along_z(stat.at[1], land_z.at[z], sem_s, step).wait()
        final = merge_stats([land_z[lv] for lv in range(HEIGHT)])
        lse_ref[...] = final[0:32, :]
        loss_ref[0, 0] = (jnp.sum(final[0:32, :]) - jnp.sum(final[32:STAT, :])) * inv_count

        def backward(first):
            hid = whole[pl.ds(first, HEIGHT)].reshape(TOKS, DIM)
            logits = dot(table[...], hid, 1, 1)
            lse_row = jnp.concatenate([lse_ref[pl.ds(first + t, 1), :] for t in range(HEIGHT)], axis=1)
            row = vocab_iota()
            prob = jnp.exp(jnp.where(row < VROWS, logits, -1e30) - lse_row)
            hit = jnp.where(row == id_rows(tok_ref, 1, first), 1.0, 0.0)
            grad = ((prob - hit) * inv_count).astype(BF16)
            spread[pl.ds(first, HEIGHT)] = dot(grad, table[...], 0, 0).astype(BF16).reshape(HEIGHT, LANE, DIM)
            demb_ref[...] += dot(grad, hid, 1, 0)

        with jax.named_scope('dhn_scatter'):
            scatter_levels(spread, dhn_ref, ring, place, backward)

        h32 = h_ref[...].astype(F32)
        dh_ref[...] = rms_backward(h32, rms_inv(h32), gain_f, dhn_ref[...])
        mine[...] = dh_ref[...].astype(BF16)
        with jax.named_scope('dm_gather'):
            level_gather(mine, dm_ref, level[HEIGHT], level[5], place)
        for half in range(TWO):
            four = slice(HEIGHT * half, HEIGHT * half + HEIGHT)
            wg, wu = split_weights(gu_ref)
            g = g_ref[half].astype(F32)
            u = u_ref[half].astype(F32)
            dq = dot(dm_ref[four].reshape(TOKS, DIM), wd_ref[...].reshape(UNITS, DIM), 1, 1)
            sig = jax.nn.sigmoid(g)
            dg = (dq * u * sig * (1.0 + g * (1.0 - sig))).astype(BF16)
            du = (dq * g * sig).astype(BF16)
            d_gate[half] = dg
            d_up[half] = du
            parts[four] = (dot(dg, wg, 1, 1) + dot(du, wu, 1, 1)).astype(BF16).reshape(HEIGHT, LANE, DIM)
        def add_slab(dst, srcs):
            def body(i, carry):
                value = srcs[0][i].astype(F32)
                for src in srcs[1:]:
                    value = value + src[i].astype(F32)
                dst[i] = value.astype(dst.dtype)
                return carry
            lax.fori_loop(0, LEVEL, body, 0)

        def hop(lv, way, here=False):
            land = rows_of(land_g, HEIGHT if here and way else lv)
            return remote(rows_of(outgo, lv), land, sem_z, way * HEIGHT + lv, me + LEVEL - CHIPS * way)

        def hop_d(lv, way, here=False):
            return remote(outgo_d.at[lv], land_d.at[HEIGHT if here and way else lv], sem_d, way * HEIGHT + lv, me + LEVEL - CHIPS * way)

        def send(lv, way, more, here):
            @pl.when(more)
            def _():
                hop(lv, way).wait_recv()
                add_slab(rows_of(outgo, lv), [rows_of(ggu, lv), rows_of(land_g, lv)])
                hop_d(lv, way).wait_recv()
                add_into(outgo_d.at[lv], [gd.at[lv], land_d.at[lv]], DROWS)

            @pl.when(jnp.logical_not(more))
            def _():
                add_slab(rows_of(outgo, lv), [rows_of(ggu, lv)])
                add_into(outgo_d.at[lv], [gd.at[lv]], DROWS)
            hop(lv, way, here).start()
            hop_d(lv, way, here).start()

        def send_far(far):
            pl.when(z + far < HEIGHT)(lambda: send(z + far, 0, z > 0, far == 1))
            pl.when(z - far >= 0)(lambda: send(z - far, 1, z < TOP, far == 1))

        def weight_grads():
            for half in range(TWO):
                four = slice(HEIGHT * half, HEIGHT * half + HEIGHT)
                act_in = a_ref[four].reshape(TOKS, DIM)
                news = (dot(act_in, d_gate[half], 0, 0), dot(act_in, d_up[half], 0, 0),
                        dot(acts[half], dm_ref[four].reshape(TOKS, DIM), 0, 0))
                for ref, new in zip((grad_gate, grad_up, grad_down), news):
                    ref[...] = new if half == 0 else ref[...] + new
            both = jnp.concatenate([grad_gate[...].reshape(NDEV, GROWS, UNITS), grad_up[...].reshape(NDEV, GROWS, UNITS)], axis=1)
            ggu[...] = both.astype(BF16)
            gd[...] = grad_down[...].astype(BF16).reshape(WD_SHAPE)

        def grads_off():
            weight_grads()
            send_far(TOP)

        with jax.named_scope('lv_scatter'):
            level_scatter(parts, total, *level[:HEIGHT], *level[6:], place, grads_off)
        x = x_ref[...] * emb_scale
        block[...] = (dh_ref[...] + rms_backward(x, rms_inv(x), gain_m, total[...])).astype(BF16)

        demb_ref[...] = demb_ref[...] * (1.0 / emb_scale)

        def add_rows(lv):
            def body(first):
                demb_ref[...] += dot(hit_rows(first), whole[pl.ds(first, HEIGHT)].reshape(TOKS, DIM), 1, 0)
            halves(lv, body)

        def last(way):
            hop(z, way).wait_recv()
            add_slab(acc, [acc, rows_of(land_g, HEIGHT if way else z)])
            hop_d(z, way).wait_recv()
            add_into(dn_ref, [dn_ref, land_d.at[HEIGHT if way else z]], DROWS)

        def give(step):
            peer = lax.rem(rank + step, LEVEL)
            return remote(acc.at[peer], own_ref.at[rank], sem_b, step, z * LEVEL + peer)

        def grads_home():
            add_slab(acc, [rows_of(ggu, z)])
            add_into(dn_ref, [gd.at[z]], DROWS)
            pl.when(z > 0)(lambda: last(0))
            pl.when(z < TOP)(lambda: last(1))
            for step in range(1, LEVEL):
                give(step).start()
            own_ref[rank] = acc[rank]

        def grads_step(t):
            pl.when(t == HEIGHT)(grads_home)

        def grads_late(t):
            pl.when(t == 0)(lambda: send_far(TWO))
            pl.when(t == 1)(lambda: send_far(1))

        with jax.named_scope('dx_gather'):
            gather_levels(block, whole, e_send, e_recv, place, add_rows, grads_step, grads_late)
        for step in range(1, LEVEL):
            with jax.named_scope('tgive'):
                give(step).wait_recv()
        for step in range(1, LEVEL):
            give(step).wait_send()
        def assemble():
            for k in range(HEIGHT):
                got = jnp.concatenate([own_ref[r, :, DROWS * k:DROWS * (k + 1)] for r in range(LEVEL)], axis=1)
                dgate_ref[:, DIM * k:DIM * (k + 1)] = got[0:GROWS]
                dup_ref[:, DIM * k:DIM * (k + 1)] = got[GROWS:PAIR]

        with jax.named_scope('asm'):
            assemble()

        def gone(lv, way):
            hop(lv, way).wait_send()
            hop_d(lv, way).wait_send()

        for lv in range(HEIGHT):
            pl.when(lv > z)(lambda: gone(lv, 0))
            pl.when(lv < z)(lambda: gone(lv, 1))

    whole = pltpu.VMEM((NDEV, LANE, DIM), BF16)
    block, flat = pltpu.VMEM((LANE, DIM), BF16), pltpu.VMEM((LANE, DIM), F32)
    slab, slab_d = pltpu.VMEM(GU_SHAPE, BF16), pltpu.VMEM(WD_SHAPE, BF16)
    unit, eight = pltpu.VMEM((TWO, TOKS, UNITS), BF16), pltpu.VMEM((LEVEL, LANE, DIM), BF16)
    wide, tall = pltpu.VMEM((DIM, UNITS), F32), pltpu.VMEM((UNITS, DIM), F32)
    dma = pltpu.SemaphoreType.DMA
    return call(
        kernel, 'step', 0,
        (jax.ShapeDtypeStruct((VPAD, DIM), F32), jax.ShapeDtypeStruct((GROWS, 3072), F32), jax.ShapeDtypeStruct((GROWS, 3072), F32),
         jax.ShapeDtypeStruct((DROWS, DIM), F32), jax.ShapeDtypeStruct((1, 1), F32)),
        (ids, labs, emb, gate, up, down_shard, gain_mlp, gain_final),
        [pltpu.VMEM((LEVEL, PAIR, UNITS), BF16), pltpu.VMEM((LEVEL, PAIR, UNITS), F32), pltpu.VMEM((LEVEL, LANE), jnp.int32), pltpu.VMEM((NDEV, LEVEL, LANE), jnp.int32), pltpu.VMEM((VPAD, DIM), BF16), whole, whole,
         slab, slab_d, eight, unit, unit, eight, unit, unit, unit, wide, wide, tall, slab, slab_d,
         pltpu.VMEM((5 * LEVEL, PAIR, UNITS), BF16), pltpu.VMEM((5, DROWS, DIM), BF16), slab, slab_d,
         pltpu.VMEM((LEVEL, PAIR, UNITS), F32), block, flat, block, flat, flat,
         pltpu.VMEM((TWO, STAT, LANE), F32), pltpu.VMEM((LEVEL, STAT, LANE), F32), pltpu.VMEM((HEIGHT, STAT, LANE), F32),
         pltpu.VMEM((32, LANE), F32),
         sem_pair(11), sem_pair(LEVEL), dma((LEVEL,)), dma((HEIGHT,)), dma((LEVEL,)), dma((HEIGHT,)), dma((5, NDEV)), dma((NDEV,)),
         dma((5, NDEV)), dma((NDEV,)), sem_pair(11), sem_pair(LEVEL), sem_pair(LEVEL), sem_pair(LEVEL)]
        + scatter_scratch(LANE, DIM) + LEVEL_SCRATCH)


def solution(mesh):
    group = mesh.shape['fsdp']

    def local_step(ids_blk, lab_blk, emb_shard, gate_shard, up_shard, down_shard, gain_mlp, gain_final):
        emb_scale = math.sqrt(emb_shard.shape[1])
        inv_count = 1.0 / (ids_blk.size * group)
        d_embed, d_gate, d_up, d_down, loss = step_call(
            ids_blk, lab_blk, emb_shard, gate_shard, up_shard, down_shard, gain_mlp, gain_final, emb_scale, inv_count)
        return loss[0, 0], d_embed[0:VROWS] * emb_scale, d_gate, d_up, d_down

    shard_spec = P('fsdp', None)
    return jax.shard_map(local_step, mesh=mesh, in_specs=(shard_spec, shard_spec, shard_spec, shard_spec, shard_spec, shard_spec, P(), P()), out_specs=(P(), shard_spec, shard_spec, shard_spec, shard_spec), check_vma=False)
```

```python
import math
import jax
import jax.numpy as jnp
from jax import lax
from jax.experimental import pallas as pl
from jax.experimental.pallas import tpu as pltpu
from jax.sharding import PartitionSpec as P

NORM_EPS = 1e-6
MESH = pl.DeviceIdType.MESH
F32 = jnp.float32
BF16 = jnp.bfloat16
VMEM_CAP = 63 * 1024 * 1024
LANE = 128
DIM = 768
PAIR = 48
UNITS = 384
NDEV = 32
LEVEL = 8
HEIGHT = 4
DROWS = 96
CHIPS = 16
GROWS = 24
TWO = 2
TOP = 3
VSPEC = pl.BlockSpec(memory_space=pltpu.VMEM)
HSPEC = pl.BlockSpec(memory_space=pl.ANY)


def my_place():
    me = lax.axis_index('fsdp')
    core = lax.rem(me, TWO)
    x = lax.rem(lax.div(me, TWO), TWO)
    y = lax.rem(lax.div(me, HEIGHT), TWO)
    z = lax.div(me, LEVEL)
    p = x * (1 - core) + y * core
    q = y * (1 - core) + x * core
    return me, z, p, q, core


def chip_of(z, p, q, core):
    x = p * (1 - core) + q * core
    y = q * (1 - core) + p * core
    return (z * TWO + y) * TWO + x


def device_of(z, p, q, core):
    return chip_of(z, p, q, core) * TWO + core


def barrier_peers(place):
    me, z = place[0], place[1]
    sem = pltpu.get_barrier_semaphore()
    for step in range(1, LEVEL):
        dev = z * LEVEL + lax.rem(me + step, LEVEL)
        pl.semaphore_signal(sem, inc=1, device_id=(dev,), device_id_type=MESH)
    for step in range(1, HEIGHT):
        dev = lax.rem(me + LEVEL * step, NDEV)
        pl.semaphore_signal(sem, inc=1, device_id=(dev,), device_id_type=MESH)
    pl.semaphore_wait(sem, 10)


def far_level(z, at):
    half = lax.div(z, TWO)
    inner = lax.rem(z + half, TWO)
    order = (TOP - TOP * half, (1 - inner) * (TWO - half) + inner * TOP * half, 1 + lax.rem(z, TWO), z)
    if isinstance(at, int):
        return order[at]
    low, high = lax.rem(at, TWO), lax.div(at, TWO)
    return ((1 - low) * (1 - high) * order[0] + low * (1 - high) * order[1]
            + (1 - low) * high * order[TWO] + low * high * order[TOP])


def remote(src, dst, sems, slot, dev):
    return pltpu.make_async_remote_copy(
        src_ref=src, dst_ref=dst, send_sem=sems.at[0, slot], recv_sem=sems.at[1, slot],
        device_id=(dev,), device_id_type=MESH)


def sem_pair(n):
    return pltpu.SemaphoreType.DMA((TWO, n))


def gather_levels(in_ref, out_ref, send_sem, recv_sem, place, work, hook=None, late_hook=None):
    me, z, p, q, core = place
    peers = (me + LEVEL, me - LEVEL, device_of(z, 1 - p, q, core), device_of(z, p, 1 - q, core), me + 1 - TWO * core)

    def desc(block, way, src=None):
        return pltpu.make_async_remote_copy(
            src_ref=out_ref.at[block] if src is None else src, dst_ref=out_ref.at[block],
            send_sem=send_sem.at[way, block], recv_sem=recv_sem.at[block],
            device_id=(peers[way],), device_id_type=MESH)

    def got(block):
        desc(block, HEIGHT).wait_recv()

    pl.when(z < TOP)(lambda: desc(me, 0, in_ref).start())
    pl.when(z > 0)(lambda: desc(me, 1, in_ref).start())
    for way in (TOP, TWO, HEIGHT):
        desc(me, way, in_ref).start()
    out_ref[me] = in_ref[...]

    def take_z(level):
        block = device_of(level, p, q, core)
        got(block)
        pl.when(jnp.logical_and(level < z, z < TOP))(lambda: desc(block, 0).start())
        pl.when(jnp.logical_and(level > z, z > 0))(lambda: desc(block, 1).start())
        for way in (TOP, TWO, HEIGHT):
            desc(block, way).start()

    def take_p(level):
        block = device_of(level, 1 - p, q, core)
        got(block)
        for way in (TOP, HEIGHT):
            desc(block, way).start()

    y = q * (1 - core) + p * core

    def take_q(level, mid):
        block = device_of(level, mid, 1 - q, core)
        got(block)
        desc(block, HEIGHT).start()

    def take_half(level, row):
        for x in range(TWO):
            got(level * LEVEL + row * HEIGHT + x * TWO + 1 - core)
        work(level * LEVEL + row * HEIGHT)

    def take_level(level):
        pl.when(core == 1)(lambda: take_q(level, p))
        take_half(level, y)
        pl.when(core == 0)(lambda: take_q(level, p))
        take_q(level, 1 - p)
        take_half(level, 1 - y)

    def step(t, carry):
        if hook is not None:
            with jax.named_scope('hook'):
                hook(t)
        with jax.named_scope('tz'):
            pl.when(jnp.logical_or(t == 0, jnp.logical_and(t < TOP, outer)))(lambda: take_z(far_level(z, TWO - lax.rem(t, TOP))))
        with jax.named_scope('tz2'):
            pl.when(jnp.logical_and(t == 0, inner))(lambda: take_z(far_level(z, 1)))
        with jax.named_scope('tp'):
            pl.when(jnp.logical_and(t > 0, t < HEIGHT))(lambda: take_p(far_level(z, TOP - lax.rem(t, HEIGHT))))
        with jax.named_scope('tz3'):
            pl.when(jnp.logical_and(t == 1, inner))(lambda: take_z(far_level(z, 0)))
        if late_hook is not None:
            with jax.named_scope('late'):
                late_hook(t)

        @pl.when(t > 0)
        def _():
            level = far_level(z, HEIGHT - (t + lax.div(HEIGHT - t, HEIGHT)))
            with jax.named_scope('glev'):
                take_level(level)
        return carry

    outer = jnp.logical_or(z == 0, z == TOP)
    inner = jnp.logical_not(outer)
    with jax.named_scope('tp0'):
        take_p(z)
    lax.fori_loop(0, 5, step, 0)
    for level in range(HEIGHT):
        desc(device_of(level, p, q, core), TWO).wait_send()
        for mid in range(TWO):
            desc(device_of(level, mid, q, core), TOP).wait_send()
        pl.when(jnp.logical_and(z < TOP, level <= z))(lambda: desc(device_of(level, p, q, core), 0).wait_send())
        pl.when(jnp.logical_and(z > 0, level >= z))(lambda: desc(device_of(level, p, q, core), 1).wait_send())
    for chip in range(CHIPS):
        desc(chip * TWO + core, HEIGHT).wait_send()


def add_into(dst, srcs, rows):
    step = 32

    def body(i, carry):
        sl = pl.ds(pl.multiple_of(i * step, step), step)
        total = srcs[0][sl, :].astype(F32)
        for src in srcs[1:]:
            total = total + src[sl, :].astype(F32)
        dst[sl, :] = total.astype(dst.dtype)
        return carry

    lax.fori_loop(0, rows // step, body, 0)


def scatter_scratch(rows, cols):
    return [
        pltpu.VMEM((CHIPS, rows, cols), BF16), pltpu.VMEM((LEVEL, rows, cols), BF16), pltpu.VMEM((HEIGHT, rows, cols), BF16),
        pltpu.VMEM((HEIGHT, rows, cols), BF16), pltpu.VMEM((HEIGHT, rows, cols), BF16), pltpu.VMEM((CHIPS, rows, cols), BF16),
        pltpu.VMEM((rows, cols), F32),
        pltpu.SemaphoreType.DMA((TWO, CHIPS)), pltpu.SemaphoreType.DMA((TWO, LEVEL)), pltpu.SemaphoreType.DMA((TWO, HEIGHT)),
        pltpu.SemaphoreType.DMA((TWO, HEIGHT)), pltpu.SemaphoreType.DMA((TWO, HEIGHT)),
    ]


def scatter_levels(in_ref, out_ref, scratch, place, work, hook=None):
    from_core, from_q, from_p, from_low, from_high, outgo, acc, sem_c, sem_q, sem_p, sem_up, sem_dn = scratch
    me, z, p, q, core = place
    rows = out_ref.shape[0]
    other = 1 - core

    def core_copy(chip):
        return remote(in_ref.at[chip * TWO + other], from_core.at[chip], sem_c, chip, me + 1 - TWO * core)

    def local(level, mid, last):
        return level * HEIGHT + mid * TWO + last

    def q_copy(level, mid):
        return remote(outgo.at[local(level, mid, 1 - q)], from_q.at[level * TWO + mid], sem_q, level * TWO + mid,
                      device_of(z, p, 1 - q, core))

    def p_copy(level):
        return remote(outgo.at[local(level, 1 - p, q)], from_p.at[level], sem_p, level, device_of(z, 1 - p, q, core))

    def up_copy(level):
        return remote(outgo.at[local(level, p, q)], from_low.at[level], sem_up, level, me + LEVEL)

    def dn_copy(level):
        return remote(outgo.at[local(level, p, q)], from_high.at[level], sem_dn, level, me - LEVEL)

    def own(level, mid, last):
        chip = chip_of(level, mid, last, core)
        core_copy(chip).wait_recv()
        return [in_ref.at[chip * TWO + core], from_core.at[chip]]

    y = q * (1 - core) + p * core
    x = p * (1 - core) + q * core

    def make(level, half):
        row = level * HEIGHT + TWO * (y * half + (1 - y) * (1 - half))
        work(row * TWO)
        for side in (1 - x, x):
            core_copy(row + side).start()

    def send_q(level, mid):
        add_into(outgo.at[local(level, mid, 1 - q)], own(level, mid, 1 - q), rows)
        q_copy(level, mid).start()

    def send_p(level):
        side = own(level, 1 - p, q)
        q_copy(level, 1 - p).wait_recv()
        add_into(outgo.at[local(level, 1 - p, q)], side + [from_q.at[level * TWO + 1 - p]], rows)
        p_copy(level).start()

    def gather_here(level):
        mine = own(level, p, q)
        q_copy(level, p).wait_recv()
        p_copy(level).wait_recv()
        return mine + [from_q.at[level * TWO + p], from_p.at[level]]

    def send_z(level):
        add_into(acc, gather_here(level), rows)

        @pl.when(level > z)
        def _():
            @pl.when(z > 0)
            def _():
                up_copy(level).wait_recv()
                add_into(acc, [acc, from_low.at[level]], rows)
            add_into(outgo.at[local(level, p, q)], [acc], rows)
            up_copy(level).start()

        @pl.when(level < z)
        def _():
            @pl.when(z < TOP)
            def _():
                dn_copy(level).wait_recv()
                add_into(acc, [acc, from_high.at[level]], rows)
            add_into(outgo.at[local(level, p, q)], [acc], rows)
            dn_copy(level).start()

    def level_at(t):
        return far_level(z, lax.rem(lax.div(t, TWO), HEIGHT))

    def step(t, carry):
        odd = lax.rem(t, TWO)
        if hook is not None:
            with jax.named_scope('hook'):
                hook(t)
        with jax.named_scope('make'):
            pl.when(t < LEVEL)(lambda: make(level_at(t), odd))
        with jax.named_scope('sq'):
            pl.when(jnp.logical_and(t > 0, t < 9))(lambda: send_q(level_at(t + 7), odd * (1 - p) + (1 - odd) * p))
        with jax.named_scope('szi1'):
            pl.when(jnp.logical_and(t == 9, inner))(lambda: send_z(far_level(z, 1)))
        with jax.named_scope('sp'):
            pl.when(jnp.logical_and(t > TWO, odd == 1))(lambda: send_p(level_at(t + 5)))
        with jax.named_scope('sz'):
            pl.when(jnp.logical_and(jnp.logical_and(t > HEIGHT, odd == 1), outer))(lambda: send_z(level_at(t + TOP)))
        with jax.named_scope('szi'):
            pl.when(jnp.logical_and(jnp.logical_and(t > 6, odd == 1), inner))(lambda: send_z(far_level(z, TWO * lax.div(t, 9))))
        return carry

    outer = jnp.logical_or(z == 0, z == TOP)
    inner = jnp.logical_not(outer)
    lax.fori_loop(0, 10, step, 0)
    add_into(out_ref, gather_here(z), rows)

    @pl.when(z > 0)
    def _():
        up_copy(z).wait_recv()
        add_into(out_ref, [out_ref, from_low.at[z]], rows)

    @pl.when(z < TOP)
    def _():
        dn_copy(z).wait_recv()
        add_into(out_ref, [out_ref, from_high.at[z]], rows)

    for chip in range(CHIPS):
        core_copy(chip).wait_send()
    for level in range(HEIGHT):
        for mid in range(TWO):
            q_copy(level, mid).wait_send()
        p_copy(level).wait_send()
        pl.when(level > z)(lambda: up_copy(level).wait_send())
        pl.when(level < z)(lambda: dn_copy(level).wait_send())


def rank_of(p, q, core):
    return device_of(0, p, q, core)


def level_gather(in_ref, out_ref, send_sem, recv_sem, place):
    me, z, p, q, core = place
    rank = lax.rem(me, LEVEL)
    peers = (device_of(z, 1 - p, q, core), device_of(z, p, 1 - q, core), me + 1 - TWO * core)

    def desc(block, way, src=None):
        return pltpu.make_async_remote_copy(
            src_ref=out_ref.at[block] if src is None else src, dst_ref=out_ref.at[block],
            send_sem=send_sem.at[way * LEVEL + block], recv_sem=recv_sem.at[block],
            device_id=(peers[way],), device_id_type=MESH)

    for way in (1, 0, TWO):
        desc(rank, way, in_ref).start()
    out_ref[rank] = in_ref[...]
    side = rank_of(1 - p, q, core)
    desc(side, 0).wait_recv()
    for way in (1, TWO):
        desc(side, way).start()
    for mid in (p, 1 - p):
        block = rank_of(mid, 1 - q, core)
        desc(block, 1).wait_recv()
        desc(block, TWO).start()
    for chip in range(HEIGHT):
        desc(chip * TWO + 1 - core, TWO).wait_recv()
    desc(rank, 0, in_ref).wait_send()
    desc(rank, 1, in_ref).wait_send()
    desc(side, 1).wait_send()
    for chip in range(HEIGHT):
        desc(chip * TWO + core, TWO).wait_send()


def level_scatter(in_ref, out_ref, from_core, from_q, from_p, outgo, sem_s, sem_r, place, hook=None):
    me, z, p, q, core = place
    rows = out_ref.shape[0]

    def copy(src, dst, slot, dev):
        return pltpu.make_async_remote_copy(
            src_ref=src, dst_ref=dst, send_sem=sem_s.at[slot], recv_sem=sem_r.at[slot],
            device_id=(dev,), device_id_type=MESH)

    def core_copy(chip):
        return copy(in_ref.at[chip * TWO + 1 - core], from_core.at[chip], chip, me + 1 - TWO * core)

    def q_copy(mid):
        return copy(outgo.at[mid], from_q.at[mid], HEIGHT + mid, device_of(z, p, 1 - q, core))

    def p_copy():
        return copy(outgo.at[TWO], from_p, 6, device_of(z, 1 - p, q, core))

    def own(mid, last):
        chip = chip_of(0, mid, last, core)
        core_copy(chip).wait_recv()
        return [in_ref.at[chip * TWO + core], from_core.at[chip]]

    for last in (1 - p, p):
        for mid in (1 - q, q):
            core_copy(chip_of(0, mid, last, 1 - core)).start()
    for mid in (1 - p, p):
        add_into(outgo.at[mid], own(mid, 1 - q), rows)
        q_copy(mid).start()
    if hook is not None:
        with jax.named_scope('lhook'):
            hook()
    side = own(1 - p, q)
    q_copy(1 - p).wait_recv()
    add_into(outgo.at[TWO], side + [from_q.at[1 - p]], rows)
    p_copy().start()
    mine = own(p, q)
    q_copy(p).wait_recv()
    p_copy().wait_recv()
    add_into(out_ref, mine + [from_q.at[p], from_p], rows)
    for chip in range(HEIGHT):
        core_copy(chip).wait_send()
    for mid in range(TWO):
        q_copy(mid).wait_send()
    p_copy().wait_send()


def dot(left, right, ld, rd):
    return lax.dot_general(left, right, (((ld,), (rd,)), ((), ())), preferred_element_type=F32)


TOKS = 512
VPAD = 1024
VROWS = 1004


def id_rows(tok_ref, row, first):
    ids = jnp.concatenate([tok_ref[first + t, row:row + 1, :] for t in range(HEIGHT)], axis=1) - shard_start()
    return jnp.where(jnp.logical_and(ids >= 0, ids < VROWS), ids, -1)


def vocab_iota():
    return lax.broadcasted_iota(jnp.int32, (VPAD, TOKS), 0)


def shard_start():
    return lax.axis_index('fsdp') * VROWS


def fill_table(table, emb_ref):
    table[VPAD - 32:VPAD, :] = jnp.zeros((32, DIM), BF16)
    table[0:VROWS, :] = emb_ref[...]


def rms_inv(values):
    return lax.rsqrt(jnp.mean(values * values, axis=-1, keepdims=True) + NORM_EPS)


def rms_backward(values, inv_rms, gain_vec, grad_out):
    scaled = grad_out * gain_vec
    return inv_rms * scaled - values * (inv_rms ** TOP) * jnp.mean(scaled * values, axis=-1, keepdims=True)


LEVEL_SCRATCH = [
    pltpu.VMEM((LANE, DIM), BF16), pltpu.VMEM((LEVEL, LANE, DIM), BF16), pltpu.VMEM((LANE, DIM), F32),
    pltpu.VMEM((HEIGHT, LANE, DIM), BF16), pltpu.VMEM((TWO, LANE, DIM), BF16), pltpu.VMEM((LANE, DIM), BF16),
    pltpu.VMEM((TOP, LANE, DIM), BF16),
    pltpu.SemaphoreType.DMA((GROWS,)), pltpu.SemaphoreType.DMA((LEVEL,)),
    pltpu.SemaphoreType.DMA((7,)), pltpu.SemaphoreType.DMA((7,)),
]


def split_weights(gu_ref):
    wide = gu_ref[...].astype(F32)
    return (wide[:, 0:GROWS, :].reshape(DIM, UNITS).astype(BF16), wide[:, GROWS:PAIR, :].reshape(DIM, UNITS).astype(BF16))


GU_SHAPE = (NDEV, PAIR, UNITS)
WD_SHAPE = (HEIGHT, DROWS, DIM)


def call(kernel, name, cid, outs, ins, scratch):
    return pl.pallas_call(
        kernel, out_shape=outs, in_specs=[VSPEC if i != TWO else HSPEC for i in range(len(ins))],
        out_specs=(HSPEC,) * (len(outs) - 1) + (pl.BlockSpec(memory_space=pltpu.SMEM),),
        scratch_shapes=scratch,
        compiler_params=pltpu.CompilerParams(collective_id=cid, has_side_effects=True, vmem_limit_bytes=VMEM_CAP),
        name=name)(*ins)


STAT = 40


def merge_stats(blocks):
    logs = [b[0:32, :] for b in blocks]
    top = logs[0]
    for one in logs[1:]:
        top = jnp.maximum(top, one)
    total = jnp.exp(logs[0] - top)
    labs = blocks[0][32:STAT, :]
    for one, b in zip(logs[1:], blocks[1:]):
        total = total + jnp.exp(one - top)
        labs = labs + b[32:STAT, :]
    return jnp.concatenate([top + jnp.log(total), labs], axis=0)


def step_call(ids, labs, emb, gate, up, down_shard, gain_mlp, gain_final, emb_scale, inv_count):
    def kernel(ids_ref, lab_ref, emb_ref, gate_ref, up_ref, down_ref, gm_ref, gf_ref,
               demb_out, dgate_out, dup_out, dn_out, loss_ref,
               demb_ref, dgate_ref, dup_ref, dn_ref, emb_in, sem_o, piece_ref, own_ref, tok_mine, tok_ref, table, spread, whole, gu_ref, wd_ref, a_ref, g_ref, u_ref, dm_ref,
               d_gate, d_up, acts, grad_gate, grad_up, grad_down, ggu, gd, land_g, land_d, outgo, outgo_d, acc,
               block, x_ref, h_ref, dh_ref, dhn_ref, stat, land, land_z, lse_ref,
               sem_t, sem_a, z_send, z_recv, d_send, d_recv, g_send, g_recv, e_send, e_recv, sem_s, sem_b, sem_z, sem_d,
               *scratch):
        ring, (mine, parts, total, *level) = scratch[:12], scratch[12:]
        place = my_place()
        me, z, p, q, core = place
        rank = lax.rem(me, LEVEL)
        gain_m, gain_f = gm_ref[...].reshape(1, DIM), gf_ref[...].reshape(1, DIM)
        table_in = pltpu.make_async_copy(emb_ref, emb_in, sem_o.at[11])
        table_in.start()
        tok_mine[...] = jnp.zeros((LEVEL, LANE), jnp.int32)
        tok_mine[0:1, :] = ids_ref[...]
        tok_mine[1:TWO, :] = lab_ref[...]
        both = jnp.concatenate([gate_ref[...].astype(F32), up_ref[...].astype(F32)], axis=0).astype(BF16)
        for r in range(LEVEL):
            piece_ref[r] = jnp.concatenate([both[:, DROWS * (LEVEL * k + r):DROWS * (LEVEL * k + r + 1)] for k in range(HEIGHT)], axis=1)
        with jax.named_scope('barrier'):
            barrier_peers(place)

        def exchange(step):
            peer = lax.rem(rank + step, LEVEL)
            return remote(piece_ref.at[peer], gu_ref.at[me], sem_a, step, z * LEVEL + peer)

        def rows_of(ref, lv):
            return ref.at[pl.ds(lv * LEVEL, LEVEL)]

        def slab(lv, way):
            part = rows_of(gu_ref, lv)
            return pltpu.make_async_remote_copy(
                src_ref=part, dst_ref=part, send_sem=z_send.at[way * HEIGHT + lv], recv_sem=z_recv.at[lv],
                device_id=(me + LEVEL - CHIPS * way,), device_id_type=MESH)

        def slab_down(lv, way, src):
            return pltpu.make_async_remote_copy(
                src_ref=src, dst_ref=wd_ref.at[lv], send_sem=d_send.at[way * HEIGHT + lv], recv_sem=d_recv.at[lv],
                device_id=(me + LEVEL - CHIPS * way,), device_id_type=MESH)

        def tell(step):
            return remote(tok_mine, tok_ref.at[me], sem_t, step, z * LEVEL + lax.rem(rank + step, LEVEL))

        def along_z(src, dst, sems, step):
            return remote(src, dst, sems, 7 + step, lax.rem(me + LEVEL * step, NDEV))

        for step in range(1, LEVEL):
            tell(step).start()
        tok_ref[me] = tok_mine[...]
        wd_ref[z] = down_ref[...]
        gu_ref[me] = piece_ref[rank]
        table_in.wait()
        fill_table(table, emb_in)
        stat[...] = jnp.zeros_like(stat)
        demb_ref[...] = jnp.zeros_like(demb_ref)
        for step in range(1, LEVEL):
            tell(step).wait()
        part = rows_of(tok_ref, z)
        for step in range(1, HEIGHT):
            along_z(part, part, sem_t, step).start()
        for step in range(1, LEVEL):
            exchange(step).start()
        pl.when(z < TOP)(lambda: slab_down(z, 0, down_ref).start())
        pl.when(z > 0)(lambda: slab_down(z, 1, down_ref).start())
        for step in range(1, HEIGHT):
            along_z(part, part, sem_t, step).wait()
        for step in range(1, LEVEL):
            exchange(step).wait_recv()
        pl.when(z < TOP)(lambda: slab(z, 0).start())
        pl.when(z > 0)(lambda: slab(z, 1).start())

        def take(lv, way, more):
            slab_down(lv, 0, wd_ref.at[lv]).wait_recv()
            pl.when(more)(lambda: slab_down(lv, way, wd_ref.at[lv]).start())
            slab(lv, 0).wait_recv()
            pl.when(more)(lambda: slab(lv, way).start())

        def take_far(far):
            pl.when(z - far >= 0)(lambda: take(z - far, 0, z < TOP))
            pl.when(z + far < HEIGHT)(lambda: take(z + far, 1, z > 0))

        def hit_rows(first):
            return (vocab_iota() == id_rows(tok_ref, 0, first)).astype(F32).astype(BF16)

        def find(first):
            spread[pl.ds(first, HEIGHT)] = dot(hit_rows(first), table[...], 0, 0).astype(BF16).reshape(HEIGHT, LANE, DIM)

        with jax.named_scope('x_scatter'):
            scatter_levels(spread, x_ref, ring, place, find, lambda t: pl.when(t == 6)(lambda: take_far(1)))
        with jax.named_scope('take2'):
            take_far(TWO)
        x = x_ref[...] * emb_scale
        mine[...] = (x * rms_inv(x) * gain_m).astype(BF16)
        with jax.named_scope('a_gather'):
            level_gather(mine, a_ref, level[HEIGHT], level[5], place)
        with jax.named_scope('take3'):
            take_far(TOP)
        for half in range(TWO):
            four = slice(HEIGHT * half, HEIGHT * half + HEIGHT)
            wg, wu = split_weights(gu_ref)
            act_in = a_ref[four].reshape(TOKS, DIM)
            g = dot(act_in, wg, 1, 0).astype(BF16)
            u = dot(act_in, wu, 1, 0).astype(BF16)
            g_ref[half] = g
            u_ref[half] = u
            act = (jax.nn.silu(g.astype(F32)) * u.astype(F32)).astype(BF16)
            acts[half] = act
            parts[four] = dot(act, wd_ref[...].reshape(UNITS, DIM), 1, 0).astype(BF16).reshape(HEIGHT, LANE, DIM)
        with jax.named_scope('lv_scatter'):
            level_scatter(parts, total, *level[:HEIGHT], *level[6:], place)
        h_ref[...] = (x_ref[...] * emb_scale + total[...].astype(BF16).astype(F32)).astype(BF16)
        h32 = h_ref[...].astype(F32)
        block[...] = (h32 * rms_inv(h32) * gain_f).astype(BF16)
        for step in range(1, LEVEL):
            exchange(step).wait_send()

        def sent(lv, way):
            slab(lv, way).wait_send()
            slab_down(lv, way, wd_ref.at[lv]).wait_send()

        def forward(first):
            logits = dot(table[...], whole[pl.ds(first, HEIGHT)].reshape(TOKS, DIM), 1, 1)
            row = vocab_iota()
            lab = jnp.sum(jnp.where(row == id_rows(tok_ref, 1, first), logits, 0.0), axis=0, keepdims=True)
            logits = jnp.where(row < VROWS, logits, -1e30)
            top = jnp.max(logits, axis=0, keepdims=True)
            local = top + jnp.log(jnp.sum(jnp.exp(logits - top), axis=0, keepdims=True))
            for t in range(HEIGHT):
                stat[0, pl.ds(first + t, 1), :] = local[:, t * LANE:(t + 1) * LANE]
                stat[0, 32:33, :] = stat[0, 32:33, :] + lab[:, t * LANE:(t + 1) * LANE]

        with jax.named_scope('hn_gather'):
            gather_levels(block, whole, g_send, g_recv, place, forward)
        for lv in range(HEIGHT):
            pl.when(jnp.logical_and(z < TOP, lv <= z))(lambda: sent(lv, 0))
            pl.when(jnp.logical_and(z > 0, lv >= z))(lambda: sent(lv, 1))

        def share(step):
            return remote(stat.at[0], land.at[rank], sem_s, step, z * LEVEL + lax.rem(rank + step, LEVEL))

        for step in range(1, LEVEL):
            share(step).start()
        land[rank] = stat[0]
        for step in range(1, LEVEL):
            share(step).wait()
        stat[1] = merge_stats([land[r] for r in range(LEVEL)])
        for step in range(1, HEIGHT):
            along_z(stat.at[1], land_z.at[z], sem_s, step).start()
        land_z[z] = stat[1]
        for step in range(1, HEIGHT):
            along_z(stat.at[1], land_z.at[z], sem_s, step).wait()
        final = merge_stats([land_z[lv] for lv in range(HEIGHT)])
        lse_ref[...] = final[0:32, :]
        loss_ref[0, 0] = (jnp.sum(final[0:32, :]) - jnp.sum(final[32:STAT, :])) * inv_count

        def backward(first):
            hid = whole[pl.ds(first, HEIGHT)].reshape(TOKS, DIM)
            logits = dot(table[...], hid, 1, 1)
            lse_row = jnp.concatenate([lse_ref[pl.ds(first + t, 1), :] for t in range(HEIGHT)], axis=1)
            row = vocab_iota()
            prob = jnp.exp(jnp.where(row < VROWS, logits, -1e30) - lse_row)
            hit = jnp.where(row == id_rows(tok_ref, 1, first), 1.0, 0.0)
            grad = ((prob - hit) * inv_count).astype(BF16)
            spread[pl.ds(first, HEIGHT)] = dot(grad, table[...], 0, 0).astype(BF16).reshape(HEIGHT, LANE, DIM)
            demb_ref[...] += dot(grad, hid, 1, 0)

        with jax.named_scope('dhn_scatter'):
            scatter_levels(spread, dhn_ref, ring, place, backward)

        h32 = h_ref[...].astype(F32)
        dh_ref[...] = rms_backward(h32, rms_inv(h32), gain_f, dhn_ref[...])
        mine[...] = dh_ref[...].astype(BF16)
        with jax.named_scope('dm_gather'):
            level_gather(mine, dm_ref, level[HEIGHT], level[5], place)
        for half in range(TWO):
            four = slice(HEIGHT * half, HEIGHT * half + HEIGHT)
            wg, wu = split_weights(gu_ref)
            g = g_ref[half].astype(F32)
            u = u_ref[half].astype(F32)
            dq = dot(dm_ref[four].reshape(TOKS, DIM), wd_ref[...].reshape(UNITS, DIM), 1, 1)
            sig = jax.nn.sigmoid(g)
            dg = (dq * u * sig * (1.0 + g * (1.0 - sig))).astype(BF16)
            du = (dq * g * sig).astype(BF16)
            d_gate[half] = dg
            d_up[half] = du
            parts[four] = (dot(dg, wg, 1, 1) + dot(du, wu, 1, 1)).astype(BF16).reshape(HEIGHT, LANE, DIM)
        def add_slab(dst, srcs):
            def body(i, carry):
                value = srcs[0][i].astype(F32)
                for src in srcs[1:]:
                    value = value + src[i].astype(F32)
                dst[i] = value.astype(dst.dtype)
                return carry
            lax.fori_loop(0, LEVEL, body, 0)

        def hop(lv, way, here=False):
            land = rows_of(land_g, HEIGHT if here and way else lv)
            return remote(rows_of(outgo, lv), land, sem_z, way * HEIGHT + lv, me + LEVEL - CHIPS * way)

        def hop_d(lv, way, here=False):
            return remote(outgo_d.at[lv], land_d.at[HEIGHT if here and way else lv], sem_d, way * HEIGHT + lv, me + LEVEL - CHIPS * way)

        def send(lv, way, more, here):
            @pl.when(more)
            def _():
                hop(lv, way).wait_recv()
                add_slab(rows_of(outgo, lv), [rows_of(ggu, lv), rows_of(land_g, lv)])
                hop_d(lv, way).wait_recv()
                add_into(outgo_d.at[lv], [gd.at[lv], land_d.at[lv]], DROWS)

            @pl.when(jnp.logical_not(more))
            def _():
                add_slab(rows_of(outgo, lv), [rows_of(ggu, lv)])
                add_into(outgo_d.at[lv], [gd.at[lv]], DROWS)
            hop(lv, way, here).start()
            hop_d(lv, way, here).start()

        def send_far(far):
            pl.when(z + far < HEIGHT)(lambda: send(z + far, 0, z > 0, far == 1))
            pl.when(z - far >= 0)(lambda: send(z - far, 1, z < TOP, far == 1))

        def weight_grads():
            for half in range(TWO):
                four = slice(HEIGHT * half, HEIGHT * half + HEIGHT)
                act_in = a_ref[four].reshape(TOKS, DIM)
                news = (dot(act_in, d_gate[half], 0, 0), dot(act_in, d_up[half], 0, 0),
                        dot(acts[half], dm_ref[four].reshape(TOKS, DIM), 0, 0))
                for ref, new in zip((grad_gate, grad_up, grad_down), news):
                    ref[...] = new if half == 0 else ref[...] + new
            both = jnp.concatenate([grad_gate[...].reshape(NDEV, GROWS, UNITS), grad_up[...].reshape(NDEV, GROWS, UNITS)], axis=1)
            ggu[...] = both.astype(BF16)
            gd[...] = grad_down[...].astype(BF16).reshape(WD_SHAPE)

        def grads_off():
            weight_grads()
            send_far(TOP)

        with jax.named_scope('lv_scatter'):
            level_scatter(parts, total, *level[:HEIGHT], *level[6:], place, grads_off)
        x = x_ref[...] * emb_scale
        block[...] = (dh_ref[...] + rms_backward(x, rms_inv(x), gain_m, total[...])).astype(BF16)

        demb_ref[...] = demb_ref[...] * (1.0 / emb_scale)

        def add_rows(first):
            demb_ref[...] += dot(hit_rows(first), whole[pl.ds(first, HEIGHT)].reshape(TOKS, DIM), 1, 0)

        def last(way):
            hop(z, way).wait_recv()
            add_slab(acc, [acc, rows_of(land_g, HEIGHT if way else z)])
            hop_d(z, way).wait_recv()
            add_into(dn_ref, [dn_ref, land_d.at[HEIGHT if way else z]], DROWS)

        def give(step):
            peer = lax.rem(rank + step, LEVEL)
            return remote(acc.at[peer], own_ref.at[rank], sem_b, step, z * LEVEL + peer)

        def grads_home():
            add_slab(acc, [rows_of(ggu, z)])
            add_into(dn_ref, [gd.at[z]], DROWS)
            pl.when(z > 0)(lambda: last(0))
            pl.when(z < TOP)(lambda: last(1))
            for step in range(1, LEVEL):
                give(step).start()
            own_ref[rank] = acc[rank]

        def grads_step(t):
            pl.when(t == HEIGHT)(grads_home)

        def grads_late(t):
            pl.when(t == 0)(lambda: send_far(TWO))
            pl.when(t == TWO)(lambda: send_far(1))

        with jax.named_scope('dx_gather'):
            gather_levels(block, whole, e_send, e_recv, place, add_rows, grads_step, grads_late)
        outs = []
        for k in range(LEVEL):
            part = pl.ds(k * LANE, LANE)
            outs.append(pltpu.make_async_copy(demb_ref.at[part], demb_out.at[part], sem_o.at[k]))
        outs.append(pltpu.make_async_copy(dn_ref, dn_out, sem_o.at[LEVEL]))
        for out in outs:
            out.start()
        for step in range(1, LEVEL):
            with jax.named_scope('tgive'):
                give(step).wait_recv()
        for step in range(1, LEVEL):
            give(step).wait_send()
        def assemble():
            for k in range(HEIGHT):
                got = jnp.concatenate([own_ref[r, :, DROWS * k:DROWS * (k + 1)] for r in range(LEVEL)], axis=1)
                dgate_ref[:, DIM * k:DIM * (k + 1)] = got[0:GROWS]
                dup_ref[:, DIM * k:DIM * (k + 1)] = got[GROWS:PAIR]

        with jax.named_scope('asm'):
            assemble()
        def gone(lv, way):
            hop(lv, way).wait_send()
            hop_d(lv, way).wait_send()

        for lv in range(HEIGHT):
            pl.when(lv > z)(lambda: gone(lv, 0))
            pl.when(lv < z)(lambda: gone(lv, 1))
        for k, (ref, out) in enumerate(((dgate_ref, dgate_out), (dup_ref, dup_out))):
            outs.append(pltpu.make_async_copy(ref, out, sem_o.at[9 + k]))
            outs[-1].start()
        for out in outs:
            out.wait()

    whole = pltpu.VMEM((NDEV, LANE, DIM), BF16)
    block, flat = pltpu.VMEM((LANE, DIM), BF16), pltpu.VMEM((LANE, DIM), F32)
    slab, slab_d = pltpu.VMEM(GU_SHAPE, BF16), pltpu.VMEM(WD_SHAPE, BF16)
    unit, eight = pltpu.VMEM((TWO, TOKS, UNITS), BF16), pltpu.VMEM((LEVEL, LANE, DIM), BF16)
    wide, tall = pltpu.VMEM((DIM, UNITS), F32), pltpu.VMEM((UNITS, DIM), F32)
    dma = pltpu.SemaphoreType.DMA
    return call(
        kernel, 'step', 0,
        (jax.ShapeDtypeStruct((VPAD, DIM), F32), jax.ShapeDtypeStruct((GROWS, 3072), F32), jax.ShapeDtypeStruct((GROWS, 3072), F32),
         jax.ShapeDtypeStruct((DROWS, DIM), F32), jax.ShapeDtypeStruct((1, 1), F32)),
        (ids, labs, emb, gate, up, down_shard, gain_mlp, gain_final),
        [pltpu.VMEM((VPAD, DIM), F32), pltpu.VMEM((GROWS, 3072), F32), pltpu.VMEM((GROWS, 3072), F32), pltpu.VMEM((DROWS, DIM), F32),
         pltpu.VMEM((VROWS, DIM), BF16), dma((12,)),
         pltpu.VMEM((LEVEL, PAIR, UNITS), BF16), pltpu.VMEM((LEVEL, PAIR, UNITS), F32), pltpu.VMEM((LEVEL, LANE), jnp.int32), pltpu.VMEM((NDEV, LEVEL, LANE), jnp.int32), pltpu.VMEM((VPAD, DIM), BF16), whole, whole,
         slab, slab_d, eight, unit, unit, eight, unit, unit, unit, wide, wide, tall, slab, slab_d,
         pltpu.VMEM((5 * LEVEL, PAIR, UNITS), BF16), pltpu.VMEM((5, DROWS, DIM), BF16), slab, slab_d,
         pltpu.VMEM((LEVEL, PAIR, UNITS), F32), block, flat, block, flat, flat,
         pltpu.VMEM((TWO, STAT, LANE), F32), pltpu.VMEM((LEVEL, STAT, LANE), F32), pltpu.VMEM((HEIGHT, STAT, LANE), F32),
         pltpu.VMEM((32, LANE), F32),
         sem_pair(11), sem_pair(LEVEL), dma((LEVEL,)), dma((HEIGHT,)), dma((LEVEL,)), dma((HEIGHT,)), dma((5, NDEV)), dma((NDEV,)),
         dma((5, NDEV)), dma((NDEV,)), sem_pair(11), sem_pair(LEVEL), sem_pair(LEVEL), sem_pair(LEVEL)]
        + scatter_scratch(LANE, DIM) + LEVEL_SCRATCH)


def solution(mesh):
    group = mesh.shape['fsdp']

    def local_step(ids_blk, lab_blk, emb_shard, gate_shard, up_shard, down_shard, gain_mlp, gain_final):
        emb_scale = math.sqrt(emb_shard.shape[1])
        inv_count = 1.0 / (ids_blk.size * group)
        d_embed, d_gate, d_up, d_down, loss = step_call(
            ids_blk, lab_blk, emb_shard, gate_shard, up_shard, down_shard, gain_mlp, gain_final, emb_scale, inv_count)
        return loss[0, 0], d_embed[0:VROWS] * emb_scale, d_gate, d_up, d_down

    shard_spec = P('fsdp', None)
    return jax.shard_map(local_step, mesh=mesh, in_specs=(shard_spec, shard_spec, shard_spec, shard_spec, shard_spec, shard_spec, P(), P()), out_specs=(P(), shard_spec, shard_spec, shard_spec, shard_spec), check_vma=False)
```

```python
import math
import jax
import jax.numpy as jnp
from jax import lax
from jax.experimental import pallas as pl
from jax.experimental.pallas import tpu as pltpu
from jax.sharding import PartitionSpec as P

NORM_EPS = 1e-6
MESH = pl.DeviceIdType.MESH
F32 = jnp.float32
BF16 = jnp.bfloat16
VMEM_CAP = 63 * 1024 * 1024
LANE = 128
DIM = 768
PAIR = 48
UNITS = 384
NDEV = 32
LEVEL = 8
HEIGHT = 4
DROWS = 96
CHIPS = 16
GROWS = 24
TWO = 2
TOP = 3
VSPEC = pl.BlockSpec(memory_space=pltpu.VMEM)
HSPEC = pl.BlockSpec(memory_space=pl.ANY)


def my_place():
    me = lax.axis_index('fsdp')
    core = lax.rem(me, TWO)
    x = lax.rem(lax.div(me, TWO), TWO)
    y = lax.rem(lax.div(me, HEIGHT), TWO)
    z = lax.div(me, LEVEL)
    p = x * (1 - core) + y * core
    q = y * (1 - core) + x * core
    return me, z, p, q, core


def chip_of(z, p, q, core):
    x = p * (1 - core) + q * core
    y = q * (1 - core) + p * core
    return (z * TWO + y) * TWO + x


def device_of(z, p, q, core):
    return chip_of(z, p, q, core) * TWO + core


def barrier_peers(place):
    me, z = place[0], place[1]
    sem = pltpu.get_barrier_semaphore()
    for step in range(1, LEVEL):
        dev = z * LEVEL + lax.rem(me + step, LEVEL)
        pl.semaphore_signal(sem, inc=1, device_id=(dev,), device_id_type=MESH)
    for step in range(1, HEIGHT):
        dev = lax.rem(me + LEVEL * step, NDEV)
        pl.semaphore_signal(sem, inc=1, device_id=(dev,), device_id_type=MESH)
    pl.semaphore_wait(sem, 10)


def far_level(z, at):
    half = lax.div(z, TWO)
    inner = lax.rem(z + half, TWO)
    order = (TOP - TOP * half, (1 - inner) * (TWO - half) + inner * TOP * half, 1 + lax.rem(z, TWO), z)
    if isinstance(at, int):
        return order[at]
    low, high = lax.rem(at, TWO), lax.div(at, TWO)
    return ((1 - low) * (1 - high) * order[0] + low * (1 - high) * order[1]
            + (1 - low) * high * order[TWO] + low * high * order[TOP])


def remote(src, dst, sems, slot, dev):
    return pltpu.make_async_remote_copy(
        src_ref=src, dst_ref=dst, send_sem=sems.at[0, slot], recv_sem=sems.at[1, slot],
        device_id=(dev,), device_id_type=MESH)


def sem_pair(n):
    return pltpu.SemaphoreType.DMA((TWO, n))


def gather_levels(in_ref, out_ref, send_sem, recv_sem, place, work, hook=None, late_hook=None):
    me, z, p, q, core = place
    peers = (me + LEVEL, me - LEVEL, device_of(z, 1 - p, q, core), device_of(z, p, 1 - q, core), me + 1 - TWO * core)

    def desc(block, way, src=None):
        return pltpu.make_async_remote_copy(
            src_ref=out_ref.at[block] if src is None else src, dst_ref=out_ref.at[block],
            send_sem=send_sem.at[slot(block, way)], recv_sem=recv_sem.at[block],
            device_id=(peers[way],), device_id_type=MESH)

    def slot(block, way):
        chip, lv = lax.div(block, TWO), lax.div(block, LEVEL)
        mid = lax.rem(chip, TWO) * (1 - core) + lax.rem(lax.div(chip, TWO), TWO) * core
        return (lv, HEIGHT + lv, LEVEL + lv, 12 + lv * TWO + mid, 20 + chip)[way]

    def got(block):
        desc(block, HEIGHT).wait_recv()

    pl.when(z < TOP)(lambda: desc(me, 0, in_ref).start())
    pl.when(z > 0)(lambda: desc(me, 1, in_ref).start())
    for way in (TOP, TWO, HEIGHT):
        desc(me, way, in_ref).start()
    out_ref[me] = in_ref[...]

    def take_z(level):
        block = device_of(level, p, q, core)
        got(block)
        pl.when(jnp.logical_and(level < z, z < TOP))(lambda: desc(block, 0).start())
        pl.when(jnp.logical_and(level > z, z > 0))(lambda: desc(block, 1).start())
        for way in (TOP, TWO, HEIGHT):
            desc(block, way).start()

    def take_p(level):
        block = device_of(level, 1 - p, q, core)
        got(block)
        for way in (TOP, HEIGHT):
            desc(block, way).start()

    y = q * (1 - core) + p * core

    def take_q(level, mid):
        block = device_of(level, mid, 1 - q, core)
        got(block)
        desc(block, HEIGHT).start()

    def take_half(level, row):
        for x in range(TWO):
            got(level * LEVEL + row * HEIGHT + x * TWO + 1 - core)
        work(level * LEVEL + row * HEIGHT)

    def take_level(level):
        pl.when(core == 1)(lambda: take_q(level, p))
        take_half(level, y)
        pl.when(core == 0)(lambda: take_q(level, p))
        take_q(level, 1 - p)
        take_half(level, 1 - y)

    def step(t, carry):
        if hook is not None:
            with jax.named_scope('hook'):
                hook(t)
        with jax.named_scope('tz'):
            pl.when(jnp.logical_or(t == 0, jnp.logical_and(t < TOP, outer)))(lambda: take_z(far_level(z, TWO - lax.rem(t, TOP))))
        with jax.named_scope('tz2'):
            pl.when(jnp.logical_and(t == 0, inner))(lambda: take_z(far_level(z, 1)))
        with jax.named_scope('tp'):
            pl.when(jnp.logical_and(t > 0, t < HEIGHT))(lambda: take_p(far_level(z, TOP - lax.rem(t, HEIGHT))))
        with jax.named_scope('tz3'):
            pl.when(jnp.logical_and(t == 1, inner))(lambda: take_z(far_level(z, 0)))
        if late_hook is not None:
            with jax.named_scope('late'):
                late_hook(t)

        @pl.when(t > 0)
        def _():
            level = far_level(z, HEIGHT - (t + lax.div(HEIGHT - t, HEIGHT)))
            with jax.named_scope('glev'):
                take_level(level)
        return carry

    outer = jnp.logical_or(z == 0, z == TOP)
    inner = jnp.logical_not(outer)
    with jax.named_scope('tp0'):
        take_p(z)
    lax.fori_loop(0, 5, step, 0)
    for level in range(HEIGHT):
        desc(device_of(level, p, q, core), TWO).wait_send()
        for mid in range(TWO):
            desc(device_of(level, mid, q, core), TOP).wait_send()
        pl.when(jnp.logical_and(z < TOP, level <= z))(lambda: desc(device_of(level, p, q, core), 0).wait_send())
        pl.when(jnp.logical_and(z > 0, level >= z))(lambda: desc(device_of(level, p, q, core), 1).wait_send())
    for chip in range(CHIPS):
        desc(chip * TWO + core, HEIGHT).wait_send()


def add_into(dst, srcs, rows):
    step = 32

    def body(i, carry):
        sl = pl.ds(pl.multiple_of(i * step, step), step)
        total = srcs[0][sl, :].astype(F32)
        for src in srcs[1:]:
            total = total + src[sl, :].astype(F32)
        dst[sl, :] = total.astype(dst.dtype)
        return carry

    lax.fori_loop(0, rows // step, body, 0)


def scatter_scratch(rows, cols):
    return [
        pltpu.VMEM((CHIPS, rows, cols), BF16), pltpu.VMEM((LEVEL, rows, cols), BF16), pltpu.VMEM((HEIGHT, rows, cols), BF16),
        pltpu.VMEM((HEIGHT, rows, cols), BF16), pltpu.VMEM((HEIGHT, rows, cols), BF16), pltpu.VMEM((CHIPS, rows, cols), BF16),
        pltpu.VMEM((rows, cols), F32),
        pltpu.SemaphoreType.DMA((TWO, CHIPS)), pltpu.SemaphoreType.DMA((TWO, LEVEL)), pltpu.SemaphoreType.DMA((TWO, HEIGHT)),
        pltpu.SemaphoreType.DMA((TWO, HEIGHT)), pltpu.SemaphoreType.DMA((TWO, HEIGHT)),
    ]


def scatter_levels(in_ref, out_ref, scratch, place, work, hook=None):
    from_core, from_q, from_p, from_low, from_high, outgo, acc, sem_c, sem_q, sem_p, sem_up, sem_dn = scratch
    me, z, p, q, core = place
    rows = out_ref.shape[0]
    other = 1 - core

    def core_copy(chip):
        return remote(in_ref.at[chip * TWO + other], from_core.at[chip], sem_c, chip, me + 1 - TWO * core)

    def local(level, mid, last):
        return level * HEIGHT + mid * TWO + last

    def q_copy(level, mid):
        return remote(outgo.at[local(level, mid, 1 - q)], from_q.at[level * TWO + mid], sem_q, level * TWO + mid,
                      device_of(z, p, 1 - q, core))

    def p_copy(level):
        return remote(outgo.at[local(level, 1 - p, q)], from_p.at[level], sem_p, level, device_of(z, 1 - p, q, core))

    def up_copy(level):
        return remote(outgo.at[local(level, p, q)], from_low.at[level], sem_up, level, me + LEVEL)

    def dn_copy(level):
        return remote(outgo.at[local(level, p, q)], from_high.at[level], sem_dn, level, me - LEVEL)

    def own(level, mid, last):
        chip = chip_of(level, mid, last, core)
        core_copy(chip).wait_recv()
        return [in_ref.at[chip * TWO + core], from_core.at[chip]]

    y = q * (1 - core) + p * core
    x = p * (1 - core) + q * core

    def make(level, half):
        row = level * HEIGHT + TWO * (y * half + (1 - y) * (1 - half))
        work(row * TWO)
        for side in (1 - x, x):
            core_copy(row + side).start()

    def send_q(level, mid):
        add_into(outgo.at[local(level, mid, 1 - q)], own(level, mid, 1 - q), rows)
        q_copy(level, mid).start()

    def send_p(level):
        side = own(level, 1 - p, q)
        q_copy(level, 1 - p).wait_recv()
        add_into(outgo.at[local(level, 1 - p, q)], side + [from_q.at[level * TWO + 1 - p]], rows)
        p_copy(level).start()

    def gather_here(level):
        mine = own(level, p, q)
        q_copy(level, p).wait_recv()
        p_copy(level).wait_recv()
        return mine + [from_q.at[level * TWO + p], from_p.at[level]]

    def send_z(level):
        add_into(acc, gather_here(level), rows)

        @pl.when(level > z)
        def _():
            @pl.when(z > 0)
            def _():
                up_copy(level).wait_recv()
                add_into(acc, [acc, from_low.at[level]], rows)
            add_into(outgo.at[local(level, p, q)], [acc], rows)
            up_copy(level).start()

        @pl.when(level < z)
        def _():
            @pl.when(z < TOP)
            def _():
                dn_copy(level).wait_recv()
                add_into(acc, [acc, from_high.at[level]], rows)
            add_into(outgo.at[local(level, p, q)], [acc], rows)
            dn_copy(level).start()

    def level_at(t):
        return far_level(z, lax.rem(lax.div(t, TWO), HEIGHT))

    def step(t, carry):
        odd = lax.rem(t, TWO)
        if hook is not None:
            with jax.named_scope('hook'):
                hook(t)
        with jax.named_scope('make'):
            pl.when(t < LEVEL)(lambda: make(level_at(t), odd))
        with jax.named_scope('sq'):
            pl.when(jnp.logical_and(t > 0, t < 9))(lambda: send_q(level_at(t + 7), odd * (1 - p) + (1 - odd) * p))
        with jax.named_scope('szi1'):
            pl.when(jnp.logical_and(t == 9, inner))(lambda: send_z(far_level(z, 1)))
        with jax.named_scope('sp'):
            pl.when(jnp.logical_and(t > TWO, odd == 1))(lambda: send_p(level_at(t + 5)))
        with jax.named_scope('sz'):
            pl.when(jnp.logical_and(jnp.logical_and(t > HEIGHT, odd == 1), outer))(lambda: send_z(level_at(t + TOP)))
        with jax.named_scope('szi'):
            pl.when(jnp.logical_and(jnp.logical_and(t > 6, odd == 1), inner))(lambda: send_z(far_level(z, TWO * lax.div(t, 9))))
        return carry

    outer = jnp.logical_or(z == 0, z == TOP)
    inner = jnp.logical_not(outer)
    lax.fori_loop(0, 10, step, 0)
    add_into(out_ref, gather_here(z), rows)

    @pl.when(z > 0)
    def _():
        up_copy(z).wait_recv()
        add_into(out_ref, [out_ref, from_low.at[z]], rows)

    @pl.when(z < TOP)
    def _():
        dn_copy(z).wait_recv()
        add_into(out_ref, [out_ref, from_high.at[z]], rows)

    for chip in range(CHIPS):
        core_copy(chip).wait_send()
    for level in range(HEIGHT):
        for mid in range(TWO):
            q_copy(level, mid).wait_send()
        p_copy(level).wait_send()
        pl.when(level > z)(lambda: up_copy(level).wait_send())
        pl.when(level < z)(lambda: dn_copy(level).wait_send())


def rank_of(p, q, core):
    return device_of(0, p, q, core)


def level_gather(in_ref, out_ref, send_sem, recv_sem, place):
    me, z, p, q, core = place
    rank = lax.rem(me, LEVEL)
    peers = (device_of(z, 1 - p, q, core), device_of(z, p, 1 - q, core), me + 1 - TWO * core)

    def desc(block, way, src=None):
        return pltpu.make_async_remote_copy(
            src_ref=out_ref.at[block] if src is None else src, dst_ref=out_ref.at[block],
            send_sem=send_sem.at[(0, 1 if src is not None else TWO, TOP + lax.div(block, TWO))[way]], recv_sem=recv_sem.at[block],
            device_id=(peers[way],), device_id_type=MESH)

    for way in (1, 0, TWO):
        desc(rank, way, in_ref).start()
    out_ref[rank] = in_ref[...]
    side = rank_of(1 - p, q, core)
    desc(side, 0).wait_recv()
    for way in (1, TWO):
        desc(side, way).start()
    for mid in (p, 1 - p):
        block = rank_of(mid, 1 - q, core)
        desc(block, 1).wait_recv()
        desc(block, TWO).start()
    for chip in range(HEIGHT):
        desc(chip * TWO + 1 - core, TWO).wait_recv()
    desc(rank, 0, in_ref).wait_send()
    desc(rank, 1, in_ref).wait_send()
    desc(side, 1).wait_send()
    for chip in range(HEIGHT):
        desc(chip * TWO + core, TWO).wait_send()


def level_scatter(in_ref, out_ref, from_core, from_q, from_p, outgo, sem_s, sem_r, place, hook=None):
    me, z, p, q, core = place
    rows = out_ref.shape[0]

    def copy(src, dst, slot, dev):
        return pltpu.make_async_remote_copy(
            src_ref=src, dst_ref=dst, send_sem=sem_s.at[slot], recv_sem=sem_r.at[slot],
            device_id=(dev,), device_id_type=MESH)

    def core_copy(chip):
        return copy(in_ref.at[chip * TWO + 1 - core], from_core.at[chip], chip, me + 1 - TWO * core)

    def q_copy(mid):
        return copy(outgo.at[mid], from_q.at[mid], HEIGHT + mid, device_of(z, p, 1 - q, core))

    def p_copy():
        return copy(outgo.at[TWO], from_p, 6, device_of(z, 1 - p, q, core))

    def own(mid, last):
        chip = chip_of(0, mid, last, core)
        core_copy(chip).wait_recv()
        return [in_ref.at[chip * TWO + core], from_core.at[chip]]

    for last in (1 - p, p):
        for mid in (1 - q, q):
            core_copy(chip_of(0, mid, last, 1 - core)).start()
    for mid in (1 - p, p):
        add_into(outgo.at[mid], own(mid, 1 - q), rows)
        q_copy(mid).start()
    if hook is not None:
        with jax.named_scope('lhook'):
            hook()
    side = own(1 - p, q)
    q_copy(1 - p).wait_recv()
    add_into(outgo.at[TWO], side + [from_q.at[1 - p]], rows)
    p_copy().start()
    mine = own(p, q)
    q_copy(p).wait_recv()
    p_copy().wait_recv()
    add_into(out_ref, mine + [from_q.at[p], from_p], rows)
    for chip in range(HEIGHT):
        core_copy(chip).wait_send()
    for mid in range(TWO):
        q_copy(mid).wait_send()
    p_copy().wait_send()


def dot(left, right, ld, rd):
    return lax.dot_general(left, right, (((ld,), (rd,)), ((), ())), preferred_element_type=F32)


TOKS = 512
VPAD = 1024
VROWS = 1004


def id_rows(tok_ref, row, first):
    ids = jnp.concatenate([tok_ref[first + t, row:row + 1, :] for t in range(HEIGHT)], axis=1) - shard_start()
    return jnp.where(jnp.logical_and(ids >= 0, ids < VROWS), ids, -1)


def vocab_iota():
    return lax.broadcasted_iota(jnp.int32, (VPAD, TOKS), 0)


def shard_start():
    return lax.axis_index('fsdp') * VROWS


def fill_table(table, emb_ref):
    table[VPAD - 32:VPAD, :] = jnp.zeros((32, DIM), BF16)
    table[0:VROWS, :] = emb_ref[...]


def rms_inv(values):
    return lax.rsqrt(jnp.mean(values * values, axis=-1, keepdims=True) + NORM_EPS)


def rms_backward(values, inv_rms, gain_vec, grad_out):
    scaled = grad_out * gain_vec
    return inv_rms * scaled - values * (inv_rms ** TOP) * jnp.mean(scaled * values, axis=-1, keepdims=True)


LEVEL_SCRATCH = [
    pltpu.VMEM((LANE, DIM), BF16), pltpu.VMEM((LEVEL, LANE, DIM), BF16), pltpu.VMEM((LANE, DIM), F32),
    pltpu.VMEM((HEIGHT, LANE, DIM), BF16), pltpu.VMEM((TWO, LANE, DIM), BF16), pltpu.VMEM((LANE, DIM), BF16),
    pltpu.VMEM((TOP, LANE, DIM), BF16),
    pltpu.SemaphoreType.DMA((7,)), pltpu.SemaphoreType.DMA((LEVEL,)),
    pltpu.SemaphoreType.DMA((7,)), pltpu.SemaphoreType.DMA((7,)),
]


def split_weights(gu_ref):
    wide = gu_ref[...].astype(F32)
    return (wide[:, 0:GROWS, :].reshape(DIM, UNITS).astype(BF16), wide[:, GROWS:PAIR, :].reshape(DIM, UNITS).astype(BF16))


GU_SHAPE = (NDEV, PAIR, UNITS)
WD_SHAPE = (HEIGHT, DROWS, DIM)


def call(kernel, name, cid, outs, ins, scratch):
    return pl.pallas_call(
        kernel, out_shape=outs, in_specs=[VSPEC if i != TWO else HSPEC for i in range(len(ins))],
        out_specs=(HSPEC,) * (len(outs) - 1) + (pl.BlockSpec(memory_space=pltpu.SMEM),),
        scratch_shapes=scratch,
        compiler_params=pltpu.CompilerParams(collective_id=cid, has_side_effects=True, vmem_limit_bytes=VMEM_CAP),
        name=name)(*ins)


STAT = 40


def merge_stats(blocks):
    logs = [b[0:32, :] for b in blocks]
    top = logs[0]
    for one in logs[1:]:
        top = jnp.maximum(top, one)
    total = jnp.exp(logs[0] - top)
    labs = blocks[0][32:STAT, :]
    for one, b in zip(logs[1:], blocks[1:]):
        total = total + jnp.exp(one - top)
        labs = labs + b[32:STAT, :]
    return jnp.concatenate([top + jnp.log(total), labs], axis=0)


def step_call(ids, labs, emb, gate, up, down_shard, gain_mlp, gain_final, emb_scale, inv_count):
    def kernel(ids_ref, lab_ref, emb_ref, gate_ref, up_ref, down_ref, gm_ref, gf_ref,
               demb_out, dgate_out, dup_out, dn_out, loss_ref,
               demb_ref, dgate_ref, dup_ref, dn_ref, emb_in, sem_o, piece_ref, own_ref, tok_mine, tok_ref, table, spread, whole, gu_ref, wd_ref, a_ref, g_ref, u_ref, dm_ref,
               d_gate, d_up, acts, grad_gate, grad_up, grad_down, ggu, gd, land_g, land_d, outgo, outgo_d, acc,
               block, x_ref, h_ref, dh_ref, dhn_ref, stat, land, land_z, lse_ref,
               sem_t, sem_a, g_send, g_recv, sem_z, sem_d,
               *scratch):
        ring, (mine, parts, total, *level) = scratch[:12], scratch[12:]
        place = my_place()
        me, z, p, q, core = place
        rank = lax.rem(me, LEVEL)
        gain_m, gain_f = gm_ref[...].reshape(1, DIM), gf_ref[...].reshape(1, DIM)
        table_in = pltpu.make_async_copy(emb_ref, emb_in, sem_o.at[11])
        table_in.start()
        tok_mine[...] = jnp.zeros((LEVEL, LANE), jnp.int32)
        tok_mine[0:1, :] = ids_ref[...]
        tok_mine[1:TWO, :] = lab_ref[...]
        both = jnp.concatenate([gate_ref[...].astype(F32), up_ref[...].astype(F32)], axis=0).astype(BF16)
        for r in range(LEVEL):
            piece_ref[r] = jnp.concatenate([both[:, DROWS * (LEVEL * k + r):DROWS * (LEVEL * k + r + 1)] for k in range(HEIGHT)], axis=1)
        with jax.named_scope('barrier'):
            barrier_peers(place)

        def exchange(step):
            peer = lax.rem(rank + step, LEVEL)
            return remote(piece_ref.at[peer], gu_ref.at[me], sem_a, step, z * LEVEL + peer)

        def rows_of(ref, lv):
            return ref.at[pl.ds(lv * LEVEL, LEVEL)]

        def slab(lv, way):
            part = rows_of(gu_ref, lv)
            return pltpu.make_async_remote_copy(
                src_ref=part, dst_ref=part, send_sem=sem_z.at[0, way * HEIGHT + lv], recv_sem=sem_z.at[1, lv],
                device_id=(me + LEVEL - CHIPS * way,), device_id_type=MESH)

        def slab_down(lv, way, src):
            return pltpu.make_async_remote_copy(
                src_ref=src, dst_ref=wd_ref.at[lv], send_sem=sem_d.at[0, way * HEIGHT + lv], recv_sem=sem_d.at[1, lv],
                device_id=(me + LEVEL - CHIPS * way,), device_id_type=MESH)

        def tell(step):
            return remote(tok_mine, tok_ref.at[me], sem_t, step, z * LEVEL + lax.rem(rank + step, LEVEL))

        def along_z(src, dst, sems, step):
            return remote(src, dst, sems, 7 + step, lax.rem(me + LEVEL * step, NDEV))

        for step in range(1, LEVEL):
            tell(step).start()
        tok_ref[me] = tok_mine[...]
        wd_ref[z] = down_ref[...]
        gu_ref[me] = piece_ref[rank]
        table_in.wait()
        fill_table(table, emb_in)
        stat[...] = jnp.zeros_like(stat)
        demb_ref[...] = jnp.zeros_like(demb_ref)
        for step in range(1, LEVEL):
            tell(step).wait()
        part = rows_of(tok_ref, z)
        for step in range(1, HEIGHT):
            along_z(part, part, sem_t, step).start()
        for step in range(1, LEVEL):
            exchange(step).start()
        pl.when(z < TOP)(lambda: slab_down(z, 0, down_ref).start())
        pl.when(z > 0)(lambda: slab_down(z, 1, down_ref).start())
        for step in range(1, HEIGHT):
            along_z(part, part, sem_t, step).wait()
        for step in range(1, LEVEL):
            exchange(step).wait_recv()
        pl.when(z < TOP)(lambda: slab(z, 0).start())
        pl.when(z > 0)(lambda: slab(z, 1).start())

        def take(lv, way, more):
            slab_down(lv, 0, wd_ref.at[lv]).wait_recv()
            pl.when(more)(lambda: slab_down(lv, way, wd_ref.at[lv]).start())
            slab(lv, 0).wait_recv()
            pl.when(more)(lambda: slab(lv, way).start())

        def take_far(far):
            pl.when(z - far >= 0)(lambda: take(z - far, 0, z < TOP))
            pl.when(z + far < HEIGHT)(lambda: take(z + far, 1, z > 0))

        def hit_rows(first):
            return (vocab_iota() == id_rows(tok_ref, 0, first)).astype(F32).astype(BF16)

        def find(first):
            spread[pl.ds(first, HEIGHT)] = dot(hit_rows(first), table[...], 0, 0).astype(BF16).reshape(HEIGHT, LANE, DIM)

        with jax.named_scope('x_scatter'):
            scatter_levels(spread, x_ref, ring, place, find, lambda t: pl.when(t == 6)(lambda: take_far(1)))
        with jax.named_scope('take2'):
            take_far(TWO)
        x = x_ref[...] * emb_scale
        mine[...] = (x * rms_inv(x) * gain_m).astype(BF16)
        with jax.named_scope('a_gather'):
            level_gather(mine, a_ref, level[HEIGHT], level[5], place)
        with jax.named_scope('take3'):
            take_far(TOP)
        for half in range(TWO):
            four = slice(HEIGHT * half, HEIGHT * half + HEIGHT)
            wg, wu = split_weights(gu_ref)
            act_in = a_ref[four].reshape(TOKS, DIM)
            g = dot(act_in, wg, 1, 0).astype(BF16)
            u = dot(act_in, wu, 1, 0).astype(BF16)
            g_ref[half] = g
            u_ref[half] = u
            act = (jax.nn.silu(g.astype(F32)) * u.astype(F32)).astype(BF16)
            acts[half] = act
            parts[four] = dot(act, wd_ref[...].reshape(UNITS, DIM), 1, 0).astype(BF16).reshape(HEIGHT, LANE, DIM)
        with jax.named_scope('lv_scatter'):
            level_scatter(parts, total, *level[:HEIGHT], *level[6:], place)
        h_ref[...] = (x_ref[...] * emb_scale + total[...].astype(BF16).astype(F32)).astype(BF16)
        h32 = h_ref[...].astype(F32)
        block[...] = (h32 * rms_inv(h32) * gain_f).astype(BF16)
        for step in range(1, LEVEL):
            exchange(step).wait_send()

        def sent(lv, way):
            slab(lv, way).wait_send()
            slab_down(lv, way, wd_ref.at[lv]).wait_send()

        def forward(first):
            logits = dot(table[...], whole[pl.ds(first, HEIGHT)].reshape(TOKS, DIM), 1, 1)
            row = vocab_iota()
            lab = jnp.sum(jnp.where(row == id_rows(tok_ref, 1, first), logits, 0.0), axis=0, keepdims=True)
            logits = jnp.where(row < VROWS, logits, -1e30)
            top = jnp.max(logits, axis=0, keepdims=True)
            local = top + jnp.log(jnp.sum(jnp.exp(logits - top), axis=0, keepdims=True))
            for t in range(HEIGHT):
                stat[0, pl.ds(first + t, 1), :] = local[:, t * LANE:(t + 1) * LANE]
                stat[0, 32:33, :] = stat[0, 32:33, :] + lab[:, t * LANE:(t + 1) * LANE]

        with jax.named_scope('hn_gather'):
            gather_levels(block, whole, g_send, g_recv, place, forward)
        for lv in range(HEIGHT):
            pl.when(jnp.logical_and(z < TOP, lv <= z))(lambda: sent(lv, 0))
            pl.when(jnp.logical_and(z > 0, lv >= z))(lambda: sent(lv, 1))

        def share(step):
            return remote(stat.at[0], land.at[rank], sem_t, step, z * LEVEL + lax.rem(rank + step, LEVEL))

        for step in range(1, LEVEL):
            share(step).start()
        land[rank] = stat[0]
        for step in range(1, LEVEL):
            share(step).wait()
        stat[1] = merge_stats([land[r] for r in range(LEVEL)])
        for step in range(1, HEIGHT):
            along_z(stat.at[1], land_z.at[z], sem_t, step).start()
        land_z[z] = stat[1]
        for step in range(1, HEIGHT):
            along_z(stat.at[1], land_z.at[z], sem_t, step).wait()
        final = merge_stats([land_z[lv] for lv in range(HEIGHT)])
        lse_ref[...] = final[0:32, :]
        loss_ref[0, 0] = (jnp.sum(final[0:32, :]) - jnp.sum(final[32:STAT, :])) * inv_count

        def backward(first):
            hid = whole[pl.ds(first, HEIGHT)].reshape(TOKS, DIM)
            logits = dot(table[...], hid, 1, 1)
            lse_row = jnp.concatenate([lse_ref[pl.ds(first + t, 1), :] for t in range(HEIGHT)], axis=1)
            row = vocab_iota()
            prob = jnp.exp(jnp.where(row < VROWS, logits, -1e30) - lse_row)
            hit = jnp.where(row == id_rows(tok_ref, 1, first), 1.0, 0.0)
            grad = ((prob - hit) * inv_count).astype(BF16)
            spread[pl.ds(first, HEIGHT)] = dot(grad, table[...], 0, 0).astype(BF16).reshape(HEIGHT, LANE, DIM)
            demb_ref[...] += dot(grad, hid, 1, 0)

        with jax.named_scope('dhn_scatter'):
            scatter_levels(spread, dhn_ref, ring, place, backward)

        h32 = h_ref[...].astype(F32)
        dh_ref[...] = rms_backward(h32, rms_inv(h32), gain_f, dhn_ref[...])
        mine[...] = dh_ref[...].astype(BF16)
        with jax.named_scope('dm_gather'):
            level_gather(mine, dm_ref, level[HEIGHT], level[5], place)
        for half in range(TWO):
            four = slice(HEIGHT * half, HEIGHT * half + HEIGHT)
            wg, wu = split_weights(gu_ref)
            g = g_ref[half].astype(F32)
            u = u_ref[half].astype(F32)
            dq = dot(dm_ref[four].reshape(TOKS, DIM), wd_ref[...].reshape(UNITS, DIM), 1, 1)
            sig = jax.nn.sigmoid(g)
            dg = (dq * u * sig * (1.0 + g * (1.0 - sig))).astype(BF16)
            du = (dq * g * sig).astype(BF16)
            d_gate[half] = dg
            d_up[half] = du
            parts[four] = (dot(dg, wg, 1, 1) + dot(du, wu, 1, 1)).astype(BF16).reshape(HEIGHT, LANE, DIM)
        def add_slab(dst, srcs):
            def body(i, carry):
                value = srcs[0][i].astype(F32)
                for src in srcs[1:]:
                    value = value + src[i].astype(F32)
                dst[i] = value.astype(dst.dtype)
                return carry
            lax.fori_loop(0, LEVEL, body, 0)

        def hop(lv, way, here=False):
            land = rows_of(land_g, HEIGHT if here and way else lv)
            return remote(rows_of(outgo, lv), land, sem_z, way * HEIGHT + lv, me + LEVEL - CHIPS * way)

        def hop_d(lv, way, here=False):
            return remote(outgo_d.at[lv], land_d.at[HEIGHT if here and way else lv], sem_d, way * HEIGHT + lv, me + LEVEL - CHIPS * way)

        def send(lv, way, more, here):
            @pl.when(more)
            def _():
                hop(lv, way).wait_recv()
                add_slab(rows_of(outgo, lv), [rows_of(ggu, lv), rows_of(land_g, lv)])
                hop_d(lv, way).wait_recv()
                add_into(outgo_d.at[lv], [gd.at[lv], land_d.at[lv]], DROWS)

            @pl.when(jnp.logical_not(more))
            def _():
                add_slab(rows_of(outgo, lv), [rows_of(ggu, lv)])
                add_into(outgo_d.at[lv], [gd.at[lv]], DROWS)
            hop(lv, way, here).start()
            hop_d(lv, way, here).start()

        def send_far(far):
            pl.when(z + far < HEIGHT)(lambda: send(z + far, 0, z > 0, far == 1))
            pl.when(z - far >= 0)(lambda: send(z - far, 1, z < TOP, far == 1))

        def weight_grads():
            for half in range(TWO):
                four = slice(HEIGHT * half, HEIGHT * half + HEIGHT)
                act_in = a_ref[four].reshape(TOKS, DIM)
                news = (dot(act_in, d_gate[half], 0, 0), dot(act_in, d_up[half], 0, 0),
                        dot(acts[half], dm_ref[four].reshape(TOKS, DIM), 0, 0))
                for ref, new in zip((grad_gate, grad_up, grad_down), news):
                    ref[...] = new if half == 0 else ref[...] + new
            both = jnp.concatenate([grad_gate[...].reshape(NDEV, GROWS, UNITS), grad_up[...].reshape(NDEV, GROWS, UNITS)], axis=1)
            ggu[...] = both.astype(BF16)
            gd[...] = grad_down[...].astype(BF16).reshape(WD_SHAPE)

        def grads_off():
            weight_grads()
            send_far(TOP)

        with jax.named_scope('lv_scatter'):
            level_scatter(parts, total, *level[:HEIGHT], *level[6:], place, grads_off)
        x = x_ref[...] * emb_scale
        block[...] = (dh_ref[...] + rms_backward(x, rms_inv(x), gain_m, total[...])).astype(BF16)

        demb_ref[...] = demb_ref[...] * (1.0 / emb_scale)

        def add_rows(first):
            demb_ref[...] += dot(hit_rows(first), whole[pl.ds(first, HEIGHT)].reshape(TOKS, DIM), 1, 0)

        def last(way):
            hop(z, way).wait_recv()
            add_slab(acc, [acc, rows_of(land_g, HEIGHT if way else z)])
            hop_d(z, way).wait_recv()
            add_into(dn_ref, [dn_ref, land_d.at[HEIGHT if way else z]], DROWS)

        def give(step):
            peer = lax.rem(rank + step, LEVEL)
            return remote(acc.at[peer], own_ref.at[rank], sem_a, step, z * LEVEL + peer)

        def grads_home():
            add_slab(acc, [rows_of(ggu, z)])
            add_into(dn_ref, [gd.at[z]], DROWS)
            pl.when(z > 0)(lambda: last(0))
            pl.when(z < TOP)(lambda: last(1))
            for step in range(1, LEVEL):
                give(step).start()
            own_ref[rank] = acc[rank]

        def grads_step(t):
            pl.when(t == HEIGHT)(grads_home)

        def grads_late(t):
            pl.when(t == 0)(lambda: send_far(TWO))
            pl.when(t == TWO)(lambda: send_far(1))

        with jax.named_scope('dx_gather'):
            gather_levels(block, whole, g_send, g_recv, place, add_rows, grads_step, grads_late)
        outs = []
        for k in range(LEVEL):
            part = pl.ds(k * LANE, LANE)
            outs.append(pltpu.make_async_copy(demb_ref.at[part], demb_out.at[part], sem_o.at[k]))
        outs.append(pltpu.make_async_copy(dn_ref, dn_out, sem_o.at[LEVEL]))
        for out in outs:
            out.start()
        for step in range(1, LEVEL):
            with jax.named_scope('tgive'):
                give(step).wait_recv()
        for step in range(1, LEVEL):
            give(step).wait_send()
        def assemble():
            for k in range(HEIGHT):
                got = jnp.concatenate([own_ref[r, :, DROWS * k:DROWS * (k + 1)] for r in range(LEVEL)], axis=1)
                dgate_ref[:, DIM * k:DIM * (k + 1)] = got[0:GROWS]
                dup_ref[:, DIM * k:DIM * (k + 1)] = got[GROWS:PAIR]

        with jax.named_scope('asm'):
            assemble()
        def gone(lv, way):
            hop(lv, way).wait_send()
            hop_d(lv, way).wait_send()

        for lv in range(HEIGHT):
            pl.when(lv > z)(lambda: gone(lv, 0))
            pl.when(lv < z)(lambda: gone(lv, 1))
        for k, (ref, out) in enumerate(((dgate_ref, dgate_out), (dup_ref, dup_out))):
            outs.append(pltpu.make_async_copy(ref, out, sem_o.at[9 + k]))
            outs[-1].start()
        for out in outs:
            out.wait()

    whole = pltpu.VMEM((NDEV, LANE, DIM), BF16)
    block, flat = pltpu.VMEM((LANE, DIM), BF16), pltpu.VMEM((LANE, DIM), F32)
    slab, slab_d = pltpu.VMEM(GU_SHAPE, BF16), pltpu.VMEM(WD_SHAPE, BF16)
    unit, eight = pltpu.VMEM((TWO, TOKS, UNITS), BF16), pltpu.VMEM((LEVEL, LANE, DIM), BF16)
    wide, tall = pltpu.VMEM((DIM, UNITS), F32), pltpu.VMEM((UNITS, DIM), F32)
    dma = pltpu.SemaphoreType.DMA
    return call(
        kernel, 'step', 0,
        (jax.ShapeDtypeStruct((VPAD, DIM), F32), jax.ShapeDtypeStruct((GROWS, 3072), F32), jax.ShapeDtypeStruct((GROWS, 3072), F32),
         jax.ShapeDtypeStruct((DROWS, DIM), F32), jax.ShapeDtypeStruct((1, 1), F32)),
        (ids, labs, emb, gate, up, down_shard, gain_mlp, gain_final),
        [pltpu.VMEM((VPAD, DIM), F32), pltpu.VMEM((GROWS, 3072), F32), pltpu.VMEM((GROWS, 3072), F32), pltpu.VMEM((DROWS, DIM), F32),
         pltpu.VMEM((VROWS, DIM), BF16), dma((12,)),
         pltpu.VMEM((LEVEL, PAIR, UNITS), BF16), pltpu.VMEM((LEVEL, PAIR, UNITS), F32), pltpu.VMEM((LEVEL, LANE), jnp.int32), pltpu.VMEM((NDEV, LEVEL, LANE), jnp.int32), pltpu.VMEM((VPAD, DIM), BF16), whole, whole,
         slab, slab_d, eight, unit, unit, eight, unit, unit, unit, wide, wide, tall, slab, slab_d,
         pltpu.VMEM((5 * LEVEL, PAIR, UNITS), BF16), pltpu.VMEM((5, DROWS, DIM), BF16), slab, slab_d,
         pltpu.VMEM((LEVEL, PAIR, UNITS), F32), block, flat, block, flat, flat,
         pltpu.VMEM((TWO, STAT, LANE), F32), pltpu.VMEM((LEVEL, STAT, LANE), F32), pltpu.VMEM((HEIGHT, STAT, LANE), F32),
         pltpu.VMEM((32, LANE), F32),
         sem_pair(11), sem_pair(LEVEL), dma((36,)), dma((NDEV,)), sem_pair(LEVEL), sem_pair(LEVEL)]
        + scatter_scratch(LANE, DIM) + LEVEL_SCRATCH)


def solution(mesh):
    group = mesh.shape['fsdp']

    def local_step(ids_blk, lab_blk, emb_shard, gate_shard, up_shard, down_shard, gain_mlp, gain_final):
        emb_scale = math.sqrt(emb_shard.shape[1])
        inv_count = 1.0 / (ids_blk.size * group)
        d_embed, d_gate, d_up, d_down, loss = step_call(
            ids_blk, lab_blk, emb_shard, gate_shard, up_shard, down_shard, gain_mlp, gain_final, emb_scale, inv_count)
        return loss[0, 0], d_embed[0:VROWS] * emb_scale, d_gate, d_up, d_down

    shard_spec = P('fsdp', None)
    return jax.shard_map(local_step, mesh=mesh, in_specs=(shard_spec, shard_spec, shard_spec, shard_spec, shard_spec, shard_spec, P(), P()), out_specs=(P(), shard_spec, shard_spec, shard_spec, shard_spec), check_vma=False)
```

```python
import math
import jax
import jax.numpy as jnp
from jax import lax
from jax.experimental import pallas as pl
from jax.experimental.pallas import tpu as pltpu
from jax.sharding import PartitionSpec as P

NORM_EPS = 1e-6
MESH = pl.DeviceIdType.MESH
F32 = jnp.float32
BF16 = jnp.bfloat16
VMEM_CAP = 63 * 1024 * 1024
LANE = 128
DIM = 768
PAIR = 48
UNITS = 384
NDEV = 32
LEVEL = 8
HEIGHT = 4
DROWS = 96
CHIPS = 16
GROWS = 24
TWO = 2
TOP = 3
VSPEC = pl.BlockSpec(memory_space=pltpu.VMEM)
HSPEC = pl.BlockSpec(memory_space=pl.ANY)


def my_place():
    me = lax.axis_index('fsdp')
    core = lax.rem(me, TWO)
    x = lax.rem(lax.div(me, TWO), TWO)
    y = lax.rem(lax.div(me, HEIGHT), TWO)
    z = lax.div(me, LEVEL)
    p = x * (1 - core) + y * core
    q = y * (1 - core) + x * core
    return me, z, p, q, core


def chip_of(z, p, q, core):
    x = p * (1 - core) + q * core
    y = q * (1 - core) + p * core
    return (z * TWO + y) * TWO + x


def device_of(z, p, q, core):
    return chip_of(z, p, q, core) * TWO + core


def barrier_peers(place):
    me, z = place[0], place[1]
    sem = pltpu.get_barrier_semaphore()
    for step in range(1, LEVEL):
        dev = z * LEVEL + lax.rem(me + step, LEVEL)
        pl.semaphore_signal(sem, inc=1, device_id=(dev,), device_id_type=MESH)
    for step in range(1, HEIGHT):
        dev = lax.rem(me + LEVEL * step, NDEV)
        pl.semaphore_signal(sem, inc=1, device_id=(dev,), device_id_type=MESH)
    pl.semaphore_wait(sem, 10)


def far_level(z, at):
    half = lax.div(z, TWO)
    inner = lax.rem(z + half, TWO)
    order = (TOP - TOP * half, (1 - inner) * (TWO - half) + inner * TOP * half, 1 + lax.rem(z, TWO), z)
    if isinstance(at, int):
        return order[at]
    low, high = lax.rem(at, TWO), lax.div(at, TWO)
    return ((1 - low) * (1 - high) * order[0] + low * (1 - high) * order[1]
            + (1 - low) * high * order[TWO] + low * high * order[TOP])


def remote(src, dst, sems, slot, dev):
    return pltpu.make_async_remote_copy(
        src_ref=src, dst_ref=dst, send_sem=sems.at[0, slot], recv_sem=sems.at[1, slot],
        device_id=(dev,), device_id_type=MESH)


def sem_pair(n):
    return pltpu.SemaphoreType.DMA((TWO, n))


def gather_levels(in_ref, out_ref, send_sem, recv_sem, place, work, hook=None, late_hook=None):
    me, z, p, q, core = place
    peers = (me + LEVEL, me - LEVEL, device_of(z, 1 - p, q, core), device_of(z, p, 1 - q, core), me + 1 - TWO * core)

    def desc(block, way, src=None):
        return pltpu.make_async_remote_copy(
            src_ref=out_ref.at[block] if src is None else src, dst_ref=out_ref.at[block],
            send_sem=send_sem.at[slot(block, way)], recv_sem=recv_sem.at[block],
            device_id=(peers[way],), device_id_type=MESH)

    def slot(block, way):
        chip, lv = lax.div(block, TWO), lax.div(block, LEVEL)
        mid = lax.rem(chip, TWO) * (1 - core) + lax.rem(lax.div(chip, TWO), TWO) * core
        return (lv, HEIGHT + lv, LEVEL + lv, 12 + lv * TWO + mid, 20 + chip)[way]

    def got(block):
        desc(block, HEIGHT).wait_recv()

    pl.when(z < TOP)(lambda: desc(me, 0, in_ref).start())
    pl.when(z > 0)(lambda: desc(me, 1, in_ref).start())
    for way in (TOP, TWO, HEIGHT):
        desc(me, way, in_ref).start()
    out_ref[me] = in_ref[...]

    def take_z(level):
        block = device_of(level, p, q, core)
        got(block)
        pl.when(jnp.logical_and(level < z, z < TOP))(lambda: desc(block, 0).start())
        pl.when(jnp.logical_and(level > z, z > 0))(lambda: desc(block, 1).start())
        for way in (TOP, TWO, HEIGHT):
            desc(block, way).start()

    def take_p(level):
        block = device_of(level, 1 - p, q, core)
        got(block)
        for way in (TOP, HEIGHT):
            desc(block, way).start()

    y = q * (1 - core) + p * core

    def take_q(level, mid):
        block = device_of(level, mid, 1 - q, core)
        got(block)
        desc(block, HEIGHT).start()

    def take_half(level, row):
        for x in range(TWO):
            got(level * LEVEL + row * HEIGHT + x * TWO + 1 - core)
        work(level * LEVEL + row * HEIGHT)

    def take_level(level):
        pl.when(core == 1)(lambda: take_q(level, p))
        take_half(level, y)
        pl.when(core == 0)(lambda: take_q(level, p))
        take_q(level, 1 - p)
        take_half(level, 1 - y)

    def step(t, carry):
        if hook is not None:
            hook(t)
        pl.when(jnp.logical_or(t == 0, jnp.logical_and(t < TOP, outer)))(lambda: take_z(far_level(z, TWO - lax.rem(t, TOP))))
        pl.when(jnp.logical_and(t == 0, inner))(lambda: take_z(far_level(z, 1)))
        pl.when(jnp.logical_and(t > 0, t < HEIGHT))(lambda: take_p(far_level(z, TOP - lax.rem(t, HEIGHT))))
        pl.when(jnp.logical_and(t == 1, inner))(lambda: take_z(far_level(z, 0)))
        if late_hook is not None:
            late_hook(t)

        @pl.when(t > 0)
        def _():
            level = far_level(z, HEIGHT - (t + lax.div(HEIGHT - t, HEIGHT)))
            take_level(level)
        return carry

    outer = jnp.logical_or(z == 0, z == TOP)
    inner = jnp.logical_not(outer)
    take_p(z)
    lax.fori_loop(0, 5, step, 0)
    for level in range(HEIGHT):
        desc(device_of(level, p, q, core), TWO).wait_send()
        for mid in range(TWO):
            desc(device_of(level, mid, q, core), TOP).wait_send()
        pl.when(jnp.logical_and(z < TOP, level <= z))(lambda: desc(device_of(level, p, q, core), 0).wait_send())
        pl.when(jnp.logical_and(z > 0, level >= z))(lambda: desc(device_of(level, p, q, core), 1).wait_send())
    for chip in range(CHIPS):
        desc(chip * TWO + core, HEIGHT).wait_send()


def add_into(dst, srcs, rows):
    step = 32

    def body(i, carry):
        sl = pl.ds(pl.multiple_of(i * step, step), step)
        total = srcs[0][sl, :].astype(F32)
        for src in srcs[1:]:
            total = total + src[sl, :].astype(F32)
        dst[sl, :] = total.astype(dst.dtype)
        return carry

    lax.fori_loop(0, rows // step, body, 0)


def scatter_scratch(rows, cols):
    return [
        pltpu.VMEM((CHIPS, rows, cols), BF16), pltpu.VMEM((LEVEL, rows, cols), BF16), pltpu.VMEM((HEIGHT, rows, cols), BF16),
        pltpu.VMEM((HEIGHT, rows, cols), BF16), pltpu.VMEM((HEIGHT, rows, cols), BF16), pltpu.VMEM((CHIPS, rows, cols), BF16),
        pltpu.VMEM((rows, cols), F32),
        pltpu.SemaphoreType.DMA((TWO, CHIPS)), pltpu.SemaphoreType.DMA((TWO, LEVEL)), pltpu.SemaphoreType.DMA((TWO, HEIGHT)),
        pltpu.SemaphoreType.DMA((TWO, HEIGHT)), pltpu.SemaphoreType.DMA((TWO, HEIGHT)),
    ]


def scatter_levels(in_ref, out_ref, scratch, place, work, hook=None):
    from_core, from_q, from_p, from_low, from_high, outgo, acc, sem_c, sem_q, sem_p, sem_up, sem_dn = scratch
    me, z, p, q, core = place
    rows = out_ref.shape[0]
    other = 1 - core

    def core_copy(chip):
        return remote(in_ref.at[chip * TWO + other], from_core.at[chip], sem_c, chip, me + 1 - TWO * core)

    def local(level, mid, last):
        return level * HEIGHT + mid * TWO + last

    def q_copy(level, mid):
        return remote(outgo.at[local(level, mid, 1 - q)], from_q.at[level * TWO + mid], sem_q, level * TWO + mid,
                      device_of(z, p, 1 - q, core))

    def p_copy(level):
        return remote(outgo.at[local(level, 1 - p, q)], from_p.at[level], sem_p, level, device_of(z, 1 - p, q, core))

    def up_copy(level):
        return remote(outgo.at[local(level, p, q)], from_low.at[level], sem_up, level, me + LEVEL)

    def dn_copy(level):
        return remote(outgo.at[local(level, p, q)], from_high.at[level], sem_dn, level, me - LEVEL)

    def own(level, mid, last):
        chip = chip_of(level, mid, last, core)
        core_copy(chip).wait_recv()
        return [in_ref.at[chip * TWO + core], from_core.at[chip]]

    y = q * (1 - core) + p * core
    x = p * (1 - core) + q * core

    def make(level, half):
        row = level * HEIGHT + TWO * (y * half + (1 - y) * (1 - half))
        work(row * TWO)
        for side in (1 - x, x):
            core_copy(row + side).start()

    def send_q(level, mid):
        add_into(outgo.at[local(level, mid, 1 - q)], own(level, mid, 1 - q), rows)
        q_copy(level, mid).start()

    def send_p(level):
        side = own(level, 1 - p, q)
        q_copy(level, 1 - p).wait_recv()
        add_into(outgo.at[local(level, 1 - p, q)], side + [from_q.at[level * TWO + 1 - p]], rows)
        p_copy(level).start()

    def gather_here(level):
        mine = own(level, p, q)
        q_copy(level, p).wait_recv()
        p_copy(level).wait_recv()
        return mine + [from_q.at[level * TWO + p], from_p.at[level]]

    def send_z(level):
        add_into(acc, gather_here(level), rows)

        @pl.when(level > z)
        def _():
            @pl.when(z > 0)
            def _():
                up_copy(level).wait_recv()
                add_into(acc, [acc, from_low.at[level]], rows)
            add_into(outgo.at[local(level, p, q)], [acc], rows)
            up_copy(level).start()

        @pl.when(level < z)
        def _():
            @pl.when(z < TOP)
            def _():
                dn_copy(level).wait_recv()
                add_into(acc, [acc, from_high.at[level]], rows)
            add_into(outgo.at[local(level, p, q)], [acc], rows)
            dn_copy(level).start()

    def level_at(t):
        return far_level(z, lax.rem(lax.div(t, TWO), HEIGHT))

    def step(t, carry):
        odd = lax.rem(t, TWO)
        if hook is not None:
            hook(t)
        pl.when(t < LEVEL)(lambda: make(level_at(t), odd))
        pl.when(jnp.logical_and(t > 0, t < 9))(lambda: send_q(level_at(t + 7), odd * (1 - p) + (1 - odd) * p))
        pl.when(jnp.logical_and(t == 9, inner))(lambda: send_z(far_level(z, 1)))
        pl.when(jnp.logical_and(t > TWO, odd == 1))(lambda: send_p(level_at(t + 5)))
        pl.when(jnp.logical_and(jnp.logical_and(t > HEIGHT, odd == 1), outer))(lambda: send_z(level_at(t + TOP)))
        pl.when(jnp.logical_and(jnp.logical_and(t > 6, odd == 1), inner))(lambda: send_z(far_level(z, TWO * lax.div(t, 9))))
        return carry

    outer = jnp.logical_or(z == 0, z == TOP)
    inner = jnp.logical_not(outer)
    lax.fori_loop(0, 10, step, 0)
    add_into(out_ref, gather_here(z), rows)

    @pl.when(z > 0)
    def _():
        up_copy(z).wait_recv()
        add_into(out_ref, [out_ref, from_low.at[z]], rows)

    @pl.when(z < TOP)
    def _():
        dn_copy(z).wait_recv()
        add_into(out_ref, [out_ref, from_high.at[z]], rows)

    for chip in range(CHIPS):
        core_copy(chip).wait_send()
    for level in range(HEIGHT):
        for mid in range(TWO):
            q_copy(level, mid).wait_send()
        p_copy(level).wait_send()
        pl.when(level > z)(lambda: up_copy(level).wait_send())
        pl.when(level < z)(lambda: dn_copy(level).wait_send())


def rank_of(p, q, core):
    return device_of(0, p, q, core)


def level_gather(in_ref, out_ref, send_sem, recv_sem, place):
    me, z, p, q, core = place
    rank = lax.rem(me, LEVEL)
    peers = (device_of(z, 1 - p, q, core), device_of(z, p, 1 - q, core), me + 1 - TWO * core)

    def desc(block, way, src=None):
        return pltpu.make_async_remote_copy(
            src_ref=out_ref.at[block] if src is None else src, dst_ref=out_ref.at[block],
            send_sem=send_sem.at[(0, 1 if src is not None else TWO, TOP + lax.div(block, TWO))[way]], recv_sem=recv_sem.at[block],
            device_id=(peers[way],), device_id_type=MESH)

    for way in (1, 0, TWO):
        desc(rank, way, in_ref).start()
    out_ref[rank] = in_ref[...]
    side = rank_of(1 - p, q, core)
    desc(side, 0).wait_recv()
    for way in (1, TWO):
        desc(side, way).start()
    for mid in (p, 1 - p):
        block = rank_of(mid, 1 - q, core)
        desc(block, 1).wait_recv()
        desc(block, TWO).start()
    for chip in range(HEIGHT):
        desc(chip * TWO + 1 - core, TWO).wait_recv()
    desc(rank, 0, in_ref).wait_send()
    desc(rank, 1, in_ref).wait_send()
    desc(side, 1).wait_send()
    for chip in range(HEIGHT):
        desc(chip * TWO + core, TWO).wait_send()


def level_scatter(in_ref, out_ref, from_core, from_q, from_p, outgo, sem_s, sem_r, place, hook=None):
    me, z, p, q, core = place
    rows = out_ref.shape[0]

    def copy(src, dst, slot, dev):
        return pltpu.make_async_remote_copy(
            src_ref=src, dst_ref=dst, send_sem=sem_s.at[slot], recv_sem=sem_r.at[slot],
            device_id=(dev,), device_id_type=MESH)

    def core_copy(chip):
        return copy(in_ref.at[chip * TWO + 1 - core], from_core.at[chip], chip, me + 1 - TWO * core)

    def q_copy(mid):
        return copy(outgo.at[mid], from_q.at[mid], HEIGHT + mid, device_of(z, p, 1 - q, core))

    def p_copy():
        return copy(outgo.at[TWO], from_p, 6, device_of(z, 1 - p, q, core))

    def own(mid, last):
        chip = chip_of(0, mid, last, core)
        core_copy(chip).wait_recv()
        return [in_ref.at[chip * TWO + core], from_core.at[chip]]

    for last in (1 - p, p):
        for mid in (1 - q, q):
            core_copy(chip_of(0, mid, last, 1 - core)).start()
    for mid in (1 - p, p):
        add_into(outgo.at[mid], own(mid, 1 - q), rows)
        q_copy(mid).start()
    if hook is not None:
        hook()
    side = own(1 - p, q)
    q_copy(1 - p).wait_recv()
    add_into(outgo.at[TWO], side + [from_q.at[1 - p]], rows)
    p_copy().start()
    mine = own(p, q)
    q_copy(p).wait_recv()
    p_copy().wait_recv()
    add_into(out_ref, mine + [from_q.at[p], from_p], rows)
    for chip in range(HEIGHT):
        core_copy(chip).wait_send()
    for mid in range(TWO):
        q_copy(mid).wait_send()
    p_copy().wait_send()


def dot(left, right, ld, rd):
    return lax.dot_general(left, right, (((ld,), (rd,)), ((), ())), preferred_element_type=F32)


TOKS = 512
VPAD = 1024
VROWS = 1004


def id_rows(tok_ref, row, first):
    ids = jnp.concatenate([tok_ref[first + t, row:row + 1, :] for t in range(HEIGHT)], axis=1) - shard_start()
    return jnp.where(jnp.logical_and(ids >= 0, ids < VROWS), ids, -1)


def vocab_iota():
    return lax.broadcasted_iota(jnp.int32, (VPAD, TOKS), 0)


def shard_start():
    return lax.axis_index('fsdp') * VROWS


def fill_table(table, emb_ref):
    table[VPAD - 32:VPAD, :] = jnp.zeros((32, DIM), BF16)
    table[0:VROWS, :] = emb_ref[...]


def rms_inv(values):
    return lax.rsqrt(jnp.mean(values * values, axis=-1, keepdims=True) + NORM_EPS)


def rms_backward(values, inv_rms, gain_vec, grad_out):
    scaled = grad_out * gain_vec
    return inv_rms * scaled - values * (inv_rms ** TOP) * jnp.mean(scaled * values, axis=-1, keepdims=True)


LEVEL_SCRATCH = [
    pltpu.VMEM((LANE, DIM), BF16), pltpu.VMEM((LEVEL, LANE, DIM), BF16), pltpu.VMEM((LANE, DIM), F32),
    pltpu.VMEM((HEIGHT, LANE, DIM), BF16), pltpu.VMEM((TWO, LANE, DIM), BF16), pltpu.VMEM((LANE, DIM), BF16),
    pltpu.VMEM((TOP, LANE, DIM), BF16),
    pltpu.SemaphoreType.DMA((7,)), pltpu.SemaphoreType.DMA((LEVEL,)),
    pltpu.SemaphoreType.DMA((7,)), pltpu.SemaphoreType.DMA((7,)),
]


def split_weights(gu_ref):
    wide = gu_ref[...].astype(F32)
    return (wide[:, 0:GROWS, :].reshape(DIM, UNITS).astype(BF16), wide[:, GROWS:PAIR, :].reshape(DIM, UNITS).astype(BF16))


GU_SHAPE = (NDEV, PAIR, UNITS)
WD_SHAPE = (HEIGHT, DROWS, DIM)


def call(kernel, name, cid, outs, ins, scratch):
    return pl.pallas_call(
        kernel, out_shape=outs, in_specs=[VSPEC if i != TWO else HSPEC for i in range(len(ins))],
        out_specs=(HSPEC,) * (len(outs) - 1) + (pl.BlockSpec(memory_space=pltpu.SMEM),),
        scratch_shapes=scratch,
        compiler_params=pltpu.CompilerParams(collective_id=cid, has_side_effects=True, vmem_limit_bytes=VMEM_CAP),
        name=name)(*ins)


STAT = 40


def merge_stats(blocks):
    logs = [b[0:32, :] for b in blocks]
    top = logs[0]
    for one in logs[1:]:
        top = jnp.maximum(top, one)
    total = jnp.exp(logs[0] - top)
    labs = blocks[0][32:STAT, :]
    for one, b in zip(logs[1:], blocks[1:]):
        total = total + jnp.exp(one - top)
        labs = labs + b[32:STAT, :]
    return jnp.concatenate([top + jnp.log(total), labs], axis=0)


def step_call(ids, labs, emb, gate, up, down_shard, gain_mlp, gain_final, emb_scale, inv_count):
    def kernel(ids_ref, lab_ref, emb_ref, gate_ref, up_ref, down_ref, gm_ref, gf_ref,
               demb_out, dgate_out, dup_out, dn_out, loss_ref,
               demb_ref, dgate_ref, dup_ref, dn_ref, emb_in, sem_o, piece_ref, own_ref, tok_mine, tok_ref, table, spread, whole, gu_ref, wd_ref, a_ref, g_ref, u_ref, dm_ref,
               d_gate, d_up, acts, grad_gate, grad_up, grad_down, ggu, gd, land_g, land_d, outgo, outgo_d, acc,
               block, x_ref, h_ref, dh_ref, dhn_ref, stat, land, land_z, lse_ref,
               sem_t, sem_a, g_send, g_recv, sem_z, sem_d,
               *scratch):
        ring, (mine, parts, total, *level) = scratch[:12], scratch[12:]
        place = my_place()
        me, z, p, q, core = place
        rank = lax.rem(me, LEVEL)
        gain_m, gain_f = gm_ref[...].reshape(1, DIM), gf_ref[...].reshape(1, DIM)
        table_in = pltpu.make_async_copy(emb_ref, emb_in, sem_o.at[11])
        table_in.start()
        tok_mine[...] = jnp.zeros((LEVEL, LANE), jnp.int32)
        tok_mine[0:1, :] = ids_ref[...]
        tok_mine[1:TWO, :] = lab_ref[...]
        both = jnp.concatenate([gate_ref[...].astype(F32), up_ref[...].astype(F32)], axis=0).astype(BF16)
        for r in range(LEVEL):
            piece_ref[r] = jnp.concatenate([both[:, DROWS * (LEVEL * k + r):DROWS * (LEVEL * k + r + 1)] for k in range(HEIGHT)], axis=1)
        barrier_peers(place)

        def exchange(step):
            peer = lax.rem(rank + step, LEVEL)
            return remote(piece_ref.at[peer], gu_ref.at[me], sem_a, step, z * LEVEL + peer)

        def rows_of(ref, lv):
            return ref.at[pl.ds(lv * LEVEL, LEVEL)]

        def slab(lv, way):
            part = rows_of(gu_ref, lv)
            return pltpu.make_async_remote_copy(
                src_ref=part, dst_ref=part, send_sem=sem_z.at[0, way * HEIGHT + lv], recv_sem=sem_z.at[1, lv],
                device_id=(me + LEVEL - CHIPS * way,), device_id_type=MESH)

        def slab_down(lv, way, src):
            return pltpu.make_async_remote_copy(
                src_ref=src, dst_ref=wd_ref.at[lv], send_sem=sem_d.at[0, way * HEIGHT + lv], recv_sem=sem_d.at[1, lv],
                device_id=(me + LEVEL - CHIPS * way,), device_id_type=MESH)

        def tell(step):
            return remote(tok_mine, tok_ref.at[me], sem_t, step, z * LEVEL + lax.rem(rank + step, LEVEL))

        def along_z(src, dst, sems, step):
            return remote(src, dst, sems, 7 + step, lax.rem(me + LEVEL * step, NDEV))

        for step in range(1, LEVEL):
            tell(step).start()
        tok_ref[me] = tok_mine[...]
        wd_ref[z] = down_ref[...]
        gu_ref[me] = piece_ref[rank]
        table_in.wait()
        fill_table(table, emb_in)
        stat[...] = jnp.zeros_like(stat)
        demb_ref[...] = jnp.zeros_like(demb_ref)
        for step in range(1, LEVEL):
            tell(step).wait()
        part = rows_of(tok_ref, z)
        for step in range(1, HEIGHT):
            along_z(part, part, sem_t, step).start()
        for step in range(1, LEVEL):
            exchange(step).start()
        pl.when(z < TOP)(lambda: slab_down(z, 0, down_ref).start())
        pl.when(z > 0)(lambda: slab_down(z, 1, down_ref).start())
        for step in range(1, HEIGHT):
            along_z(part, part, sem_t, step).wait()
        for step in range(1, LEVEL):
            exchange(step).wait_recv()
        pl.when(z < TOP)(lambda: slab(z, 0).start())
        pl.when(z > 0)(lambda: slab(z, 1).start())

        def take(lv, way, more):
            slab_down(lv, 0, wd_ref.at[lv]).wait_recv()
            pl.when(more)(lambda: slab_down(lv, way, wd_ref.at[lv]).start())
            slab(lv, 0).wait_recv()
            pl.when(more)(lambda: slab(lv, way).start())

        def take_far(far):
            pl.when(z - far >= 0)(lambda: take(z - far, 0, z < TOP))
            pl.when(z + far < HEIGHT)(lambda: take(z + far, 1, z > 0))

        def hit_rows(first):
            return (vocab_iota() == id_rows(tok_ref, 0, first)).astype(F32).astype(BF16)

        def find(first):
            spread[pl.ds(first, HEIGHT)] = dot(hit_rows(first), table[...], 0, 0).astype(BF16).reshape(HEIGHT, LANE, DIM)

        scatter_levels(spread, x_ref, ring, place, find, lambda t: pl.when(t == 6)(lambda: take_far(1)))
        take_far(TWO)
        x = x_ref[...] * emb_scale
        mine[...] = (x * rms_inv(x) * gain_m).astype(BF16)
        level_gather(mine, a_ref, level[HEIGHT], level[5], place)
        take_far(TOP)
        for half in range(TWO):
            four = slice(HEIGHT * half, HEIGHT * half + HEIGHT)
            wg, wu = split_weights(gu_ref)
            act_in = a_ref[four].reshape(TOKS, DIM)
            g = dot(act_in, wg, 1, 0).astype(BF16)
            u = dot(act_in, wu, 1, 0).astype(BF16)
            g_ref[half] = g
            u_ref[half] = u
            act = (jax.nn.silu(g.astype(F32)) * u.astype(F32)).astype(BF16)
            acts[half] = act
            parts[four] = dot(act, wd_ref[...].reshape(UNITS, DIM), 1, 0).astype(BF16).reshape(HEIGHT, LANE, DIM)
        level_scatter(parts, total, *level[:HEIGHT], *level[6:], place)
        h_ref[...] = (x_ref[...] * emb_scale + total[...].astype(BF16).astype(F32)).astype(BF16)
        h32 = h_ref[...].astype(F32)
        block[...] = (h32 * rms_inv(h32) * gain_f).astype(BF16)
        for step in range(1, LEVEL):
            exchange(step).wait_send()

        def sent(lv, way):
            slab(lv, way).wait_send()
            slab_down(lv, way, wd_ref.at[lv]).wait_send()

        def forward(first):
            logits = dot(table[...], whole[pl.ds(first, HEIGHT)].reshape(TOKS, DIM), 1, 1)
            row = vocab_iota()
            lab = jnp.sum(jnp.where(row == id_rows(tok_ref, 1, first), logits, 0.0), axis=0, keepdims=True)
            logits = jnp.where(row < VROWS, logits, -1e30)
            top = jnp.max(logits, axis=0, keepdims=True)
            local = top + jnp.log(jnp.sum(jnp.exp(logits - top), axis=0, keepdims=True))
            for t in range(HEIGHT):
                stat[0, pl.ds(first + t, 1), :] = local[:, t * LANE:(t + 1) * LANE]
                stat[0, 32:33, :] = stat[0, 32:33, :] + lab[:, t * LANE:(t + 1) * LANE]

        gather_levels(block, whole, g_send, g_recv, place, forward)
        for lv in range(HEIGHT):
            pl.when(jnp.logical_and(z < TOP, lv <= z))(lambda: sent(lv, 0))
            pl.when(jnp.logical_and(z > 0, lv >= z))(lambda: sent(lv, 1))

        def share(step):
            return remote(stat.at[0], land.at[rank], sem_t, step, z * LEVEL + lax.rem(rank + step, LEVEL))

        for step in range(1, LEVEL):
            share(step).start()
        land[rank] = stat[0]
        for step in range(1, LEVEL):
            share(step).wait()
        stat[1] = merge_stats([land[r] for r in range(LEVEL)])
        for step in range(1, HEIGHT):
            along_z(stat.at[1], land_z.at[z], sem_t, step).start()
        land_z[z] = stat[1]
        for step in range(1, HEIGHT):
            along_z(stat.at[1], land_z.at[z], sem_t, step).wait()
        final = merge_stats([land_z[lv] for lv in range(HEIGHT)])
        lse_ref[...] = final[0:32, :]
        loss_ref[0, 0] = (jnp.sum(final[0:32, :]) - jnp.sum(final[32:STAT, :])) * inv_count

        def backward(first):
            hid = whole[pl.ds(first, HEIGHT)].reshape(TOKS, DIM)
            logits = dot(table[...], hid, 1, 1)
            lse_row = jnp.concatenate([lse_ref[pl.ds(first + t, 1), :] for t in range(HEIGHT)], axis=1)
            row = vocab_iota()
            prob = jnp.exp(jnp.where(row < VROWS, logits, -1e30) - lse_row)
            hit = jnp.where(row == id_rows(tok_ref, 1, first), 1.0, 0.0)
            grad = ((prob - hit) * inv_count).astype(BF16)
            spread[pl.ds(first, HEIGHT)] = dot(grad, table[...], 0, 0).astype(BF16).reshape(HEIGHT, LANE, DIM)
            demb_ref[...] += dot(grad, hid, 1, 0)

        scatter_levels(spread, dhn_ref, ring, place, backward)

        h32 = h_ref[...].astype(F32)
        dh_ref[...] = rms_backward(h32, rms_inv(h32), gain_f, dhn_ref[...])
        mine[...] = dh_ref[...].astype(BF16)
        level_gather(mine, dm_ref, level[HEIGHT], level[5], place)
        for half in range(TWO):
            four = slice(HEIGHT * half, HEIGHT * half + HEIGHT)
            wg, wu = split_weights(gu_ref)
            g = g_ref[half].astype(F32)
            u = u_ref[half].astype(F32)
            dq = dot(dm_ref[four].reshape(TOKS, DIM), wd_ref[...].reshape(UNITS, DIM), 1, 1)
            sig = jax.nn.sigmoid(g)
            dg = (dq * u * sig * (1.0 + g * (1.0 - sig))).astype(BF16)
            du = (dq * g * sig).astype(BF16)
            d_gate[half] = dg
            d_up[half] = du
            parts[four] = (dot(dg, wg, 1, 1) + dot(du, wu, 1, 1)).astype(BF16).reshape(HEIGHT, LANE, DIM)
        def add_slab(dst, srcs):
            def body(i, carry):
                value = srcs[0][i].astype(F32)
                for src in srcs[1:]:
                    value = value + src[i].astype(F32)
                dst[i] = value.astype(dst.dtype)
                return carry
            lax.fori_loop(0, LEVEL, body, 0)

        def hop(lv, way, here=False):
            land = rows_of(land_g, HEIGHT if here and way else lv)
            return remote(rows_of(outgo, lv), land, sem_z, way * HEIGHT + lv, me + LEVEL - CHIPS * way)

        def hop_d(lv, way, here=False):
            return remote(outgo_d.at[lv], land_d.at[HEIGHT if here and way else lv], sem_d, way * HEIGHT + lv, me + LEVEL - CHIPS * way)

        def send(lv, way, more, here):
            @pl.when(more)
            def _():
                hop(lv, way).wait_recv()
                add_slab(rows_of(outgo, lv), [rows_of(ggu, lv), rows_of(land_g, lv)])
                hop_d(lv, way).wait_recv()
                add_into(outgo_d.at[lv], [gd.at[lv], land_d.at[lv]], DROWS)

            @pl.when(jnp.logical_not(more))
            def _():
                add_slab(rows_of(outgo, lv), [rows_of(ggu, lv)])
                add_into(outgo_d.at[lv], [gd.at[lv]], DROWS)
            hop(lv, way, here).start()
            hop_d(lv, way, here).start()

        def send_far(far):
            pl.when(z + far < HEIGHT)(lambda: send(z + far, 0, z > 0, far == 1))
            pl.when(z - far >= 0)(lambda: send(z - far, 1, z < TOP, far == 1))

        def weight_grads():
            for half in range(TWO):
                four = slice(HEIGHT * half, HEIGHT * half + HEIGHT)
                act_in = a_ref[four].reshape(TOKS, DIM)
                news = (dot(act_in, d_gate[half], 0, 0), dot(act_in, d_up[half], 0, 0),
                        dot(acts[half], dm_ref[four].reshape(TOKS, DIM), 0, 0))
                for ref, new in zip((grad_gate, grad_up, grad_down), news):
                    ref[...] = new if half == 0 else ref[...] + new
            both = jnp.concatenate([grad_gate[...].reshape(NDEV, GROWS, UNITS), grad_up[...].reshape(NDEV, GROWS, UNITS)], axis=1)
            ggu[...] = both.astype(BF16)
            gd[...] = grad_down[...].astype(BF16).reshape(WD_SHAPE)

        def grads_off():
            weight_grads()
            send_far(TOP)

        level_scatter(parts, total, *level[:HEIGHT], *level[6:], place, grads_off)
        x = x_ref[...] * emb_scale
        block[...] = (dh_ref[...] + rms_backward(x, rms_inv(x), gain_m, total[...])).astype(BF16)

        demb_ref[...] = demb_ref[...] * (1.0 / emb_scale)

        def add_rows(first):
            demb_ref[...] += dot(hit_rows(first), whole[pl.ds(first, HEIGHT)].reshape(TOKS, DIM), 1, 0)

        def last(way):
            hop(z, way).wait_recv()
            add_slab(acc, [acc, rows_of(land_g, HEIGHT if way else z)])
            hop_d(z, way).wait_recv()
            add_into(dn_ref, [dn_ref, land_d.at[HEIGHT if way else z]], DROWS)

        def give(step):
            peer = lax.rem(rank + step, LEVEL)
            return remote(acc.at[peer], own_ref.at[rank], sem_a, step, z * LEVEL + peer)

        def grads_home():
            add_slab(acc, [rows_of(ggu, z)])
            add_into(dn_ref, [gd.at[z]], DROWS)
            pl.when(z > 0)(lambda: last(0))
            pl.when(z < TOP)(lambda: last(1))
            for step in range(1, LEVEL):
                give(step).start()
            own_ref[rank] = acc[rank]

        def grads_step(t):
            pl.when(t == HEIGHT)(grads_home)

        def grads_late(t):
            pl.when(t == 0)(lambda: send_far(TWO))
            pl.when(t == TWO)(lambda: send_far(1))

        gather_levels(block, whole, g_send, g_recv, place, add_rows, grads_step, grads_late)
        outs = []
        for k in range(LEVEL):
            part = pl.ds(k * LANE, LANE)
            outs.append(pltpu.make_async_copy(demb_ref.at[part], demb_out.at[part], sem_o.at[k]))
        outs.append(pltpu.make_async_copy(dn_ref, dn_out, sem_o.at[LEVEL]))
        for out in outs:
            out.start()
        for step in range(1, LEVEL):
            give(step).wait_recv()
        for step in range(1, LEVEL):
            give(step).wait_send()
        def assemble():
            for k in range(HEIGHT):
                got = jnp.concatenate([own_ref[r, :, DROWS * k:DROWS * (k + 1)] for r in range(LEVEL)], axis=1)
                dgate_ref[:, DIM * k:DIM * (k + 1)] = got[0:GROWS]
                dup_ref[:, DIM * k:DIM * (k + 1)] = got[GROWS:PAIR]

        assemble()
        def gone(lv, way):
            hop(lv, way).wait_send()
            hop_d(lv, way).wait_send()

        for lv in range(HEIGHT):
            pl.when(lv > z)(lambda: gone(lv, 0))
            pl.when(lv < z)(lambda: gone(lv, 1))
        for k, (ref, out) in enumerate(((dgate_ref, dgate_out), (dup_ref, dup_out))):
            outs.append(pltpu.make_async_copy(ref, out, sem_o.at[9 + k]))
            outs[-1].start()
        for out in outs:
            out.wait()

    whole = pltpu.VMEM((NDEV, LANE, DIM), BF16)
    block, flat = pltpu.VMEM((LANE, DIM), BF16), pltpu.VMEM((LANE, DIM), F32)
    slab, slab_d = pltpu.VMEM(GU_SHAPE, BF16), pltpu.VMEM(WD_SHAPE, BF16)
    unit, eight = pltpu.VMEM((TWO, TOKS, UNITS), BF16), pltpu.VMEM((LEVEL, LANE, DIM), BF16)
    wide, tall = pltpu.VMEM((DIM, UNITS), F32), pltpu.VMEM((UNITS, DIM), F32)
    dma = pltpu.SemaphoreType.DMA
    return call(
        kernel, 'step', 0,
        (jax.ShapeDtypeStruct((VPAD, DIM), F32), jax.ShapeDtypeStruct((GROWS, 3072), F32), jax.ShapeDtypeStruct((GROWS, 3072), F32),
         jax.ShapeDtypeStruct((DROWS, DIM), F32), jax.ShapeDtypeStruct((1, 1), F32)),
        (ids, labs, emb, gate, up, down_shard, gain_mlp, gain_final),
        [pltpu.VMEM((VPAD, DIM), F32), pltpu.VMEM((GROWS, 3072), F32), pltpu.VMEM((GROWS, 3072), F32), pltpu.VMEM((DROWS, DIM), F32),
         pltpu.VMEM((VROWS, DIM), BF16), dma((12,)),
         pltpu.VMEM((LEVEL, PAIR, UNITS), BF16), pltpu.VMEM((LEVEL, PAIR, UNITS), F32), pltpu.VMEM((LEVEL, LANE), jnp.int32), pltpu.VMEM((NDEV, LEVEL, LANE), jnp.int32), pltpu.VMEM((VPAD, DIM), BF16), whole, whole,
         slab, slab_d, eight, unit, unit, eight, unit, unit, unit, wide, wide, tall, slab, slab_d,
         pltpu.VMEM((5 * LEVEL, PAIR, UNITS), BF16), pltpu.VMEM((5, DROWS, DIM), BF16), slab, slab_d,
         pltpu.VMEM((LEVEL, PAIR, UNITS), F32), block, flat, block, flat, flat,
         pltpu.VMEM((TWO, STAT, LANE), F32), pltpu.VMEM((LEVEL, STAT, LANE), F32), pltpu.VMEM((HEIGHT, STAT, LANE), F32),
         pltpu.VMEM((32, LANE), F32),
         sem_pair(11), sem_pair(LEVEL), dma((36,)), dma((NDEV,)), sem_pair(LEVEL), sem_pair(LEVEL)]
        + scatter_scratch(LANE, DIM) + LEVEL_SCRATCH)


def solution(mesh):
    group = mesh.shape['fsdp']

    def local_step(ids_blk, lab_blk, emb_shard, gate_shard, up_shard, down_shard, gain_mlp, gain_final):
        emb_scale = math.sqrt(emb_shard.shape[1])
        inv_count = 1.0 / (ids_blk.size * group)
        d_embed, d_gate, d_up, d_down, loss = step_call(
            ids_blk, lab_blk, emb_shard, gate_shard, up_shard, down_shard, gain_mlp, gain_final, emb_scale, inv_count)
        return loss[0, 0], d_embed[0:VROWS] * emb_scale, d_gate, d_up, d_down

    shard_spec = P('fsdp', None)
    return jax.shard_map(local_step, mesh=mesh, in_specs=(shard_spec, shard_spec, shard_spec, shard_spec, shard_spec, shard_spec, P(), P()), out_specs=(P(), shard_spec, shard_spec, shard_spec, shard_spec), check_vma=False)
```

```python
import math
import jax
import jax.numpy as jnp
from jax import lax
from jax.experimental import pallas as pl
from jax.experimental.pallas import tpu as pltpu
from jax.sharding import PartitionSpec as P

NORM_EPS = 1e-6
MESH = pl.DeviceIdType.MESH
F32 = jnp.float32
BF16 = jnp.bfloat16
VMEM_CAP = 63 * 1024 * 1024
LANE = 128
DIM = 768
PAIR = 48
UNITS = 384
NDEV = 32
LEVEL = 8
HEIGHT = 4
DROWS = 96
CHIPS = 16
GROWS = 24
TWO = 2
TOP = 3
VSPEC = pl.BlockSpec(memory_space=pltpu.VMEM)
HSPEC = pl.BlockSpec(memory_space=pl.ANY)


def my_place():
    me = lax.axis_index('fsdp')
    core = lax.rem(me, TWO)
    x = lax.rem(lax.div(me, TWO), TWO)
    y = lax.rem(lax.div(me, HEIGHT), TWO)
    z = lax.div(me, LEVEL)
    p = x * (1 - core) + y * core
    q = y * (1 - core) + x * core
    return me, z, p, q, core


def chip_of(z, p, q, core):
    x = p * (1 - core) + q * core
    y = q * (1 - core) + p * core
    return (z * TWO + y) * TWO + x


def device_of(z, p, q, core):
    return chip_of(z, p, q, core) * TWO + core


def barrier_peers(place):
    me, z = place[0], place[1]
    sem = pltpu.get_barrier_semaphore()
    for step in range(1, LEVEL):
        dev = z * LEVEL + lax.rem(me + step, LEVEL)
        pl.semaphore_signal(sem, inc=1, device_id=(dev,), device_id_type=MESH)
    for step in range(1, HEIGHT):
        dev = lax.rem(me + LEVEL * step, NDEV)
        pl.semaphore_signal(sem, inc=1, device_id=(dev,), device_id_type=MESH)
    pl.semaphore_wait(sem, 10)


def far_level(z, at):
    half = lax.div(z, TWO)
    inner = lax.rem(z + half, TWO)
    order = (TOP - TOP * half, (1 - inner) * (TWO - half) + inner * TOP * half, 1 + lax.rem(z, TWO), z)
    if isinstance(at, int):
        return order[at]
    low, high = lax.rem(at, TWO), lax.div(at, TWO)
    return ((1 - low) * (1 - high) * order[0] + low * (1 - high) * order[1]
            + (1 - low) * high * order[TWO] + low * high * order[TOP])


def remote(src, dst, sems, slot, dev):
    return pltpu.make_async_remote_copy(
        src_ref=src, dst_ref=dst, send_sem=sems.at[0, slot], recv_sem=sems.at[1, slot],
        device_id=(dev,), device_id_type=MESH)


def sem_pair(n):
    return pltpu.SemaphoreType.DMA((TWO, n))


def gather_levels(in_ref, out_ref, send_sem, recv_sem, place, work, hook=None, late_hook=None):
    me, z, p, q, core = place
    peers = (me + LEVEL, me - LEVEL, device_of(z, 1 - p, q, core), device_of(z, p, 1 - q, core), me + 1 - TWO * core)

    def desc(block, way, src=None):
        return pltpu.make_async_remote_copy(
            src_ref=out_ref.at[block] if src is None else src, dst_ref=out_ref.at[block],
            send_sem=send_sem.at[slot(block, way)], recv_sem=recv_sem.at[block],
            device_id=(peers[way],), device_id_type=MESH)

    def slot(block, way):
        chip, lv = lax.div(block, TWO), lax.div(block, LEVEL)
        mid = lax.rem(chip, TWO) * (1 - core) + lax.rem(lax.div(chip, TWO), TWO) * core
        return (lv, HEIGHT + lv, LEVEL + lv, 12 + lv * TWO + mid, 20 + chip)[way]

    def got(block):
        desc(block, HEIGHT).wait_recv()

    pl.when(z < TOP)(lambda: desc(me, 0, in_ref).start())
    pl.when(z > 0)(lambda: desc(me, 1, in_ref).start())
    for way in (TOP, TWO, HEIGHT):
        desc(me, way, in_ref).start()
    out_ref[me] = in_ref[...]

    def take_z(level):
        block = device_of(level, p, q, core)
        got(block)
        pl.when(jnp.logical_and(level < z, z < TOP))(lambda: desc(block, 0).start())
        pl.when(jnp.logical_and(level > z, z > 0))(lambda: desc(block, 1).start())
        for way in (TOP, TWO, HEIGHT):
            desc(block, way).start()

    def take_p(level):
        block = device_of(level, 1 - p, q, core)
        got(block)
        for way in (TOP, HEIGHT):
            desc(block, way).start()

    y = q * (1 - core) + p * core

    def take_q(level, mid):
        block = device_of(level, mid, 1 - q, core)
        got(block)
        desc(block, HEIGHT).start()

    def take_half(level, row):
        for x in range(TWO):
            got(level * LEVEL + row * HEIGHT + x * TWO + 1 - core)
        work(level * LEVEL + row * HEIGHT)

    def take_level(level):
        pl.when(core == 1)(lambda: take_q(level, p))
        take_half(level, y)
        pl.when(core == 0)(lambda: take_q(level, p))
        take_q(level, 1 - p)
        take_half(level, 1 - y)

    def step(t, carry):
        if hook is not None:
            hook(t)
        pl.when(jnp.logical_or(t == 0, jnp.logical_and(t < TOP, outer)))(lambda: take_z(far_level(z, TWO - lax.rem(t, TOP))))
        pl.when(jnp.logical_and(t == 0, inner))(lambda: take_z(far_level(z, 1)))
        pl.when(jnp.logical_and(t > 0, t < HEIGHT))(lambda: take_p(far_level(z, TOP - lax.rem(t, HEIGHT))))
        pl.when(jnp.logical_and(t == 1, inner))(lambda: take_z(far_level(z, 0)))
        if late_hook is not None:
            late_hook(t)

        @pl.when(t > 0)
        def _():
            level = far_level(z, HEIGHT - (t + lax.div(HEIGHT - t, HEIGHT)))
            take_level(level)
        return carry

    outer = jnp.logical_or(z == 0, z == TOP)
    inner = jnp.logical_not(outer)
    take_p(z)
    lax.fori_loop(0, 5, step, 0)
    for level in range(HEIGHT):
        desc(device_of(level, p, q, core), TWO).wait_send()
        for mid in range(TWO):
            desc(device_of(level, mid, q, core), TOP).wait_send()
        pl.when(jnp.logical_and(z < TOP, level <= z))(lambda: desc(device_of(level, p, q, core), 0).wait_send())
        pl.when(jnp.logical_and(z > 0, level >= z))(lambda: desc(device_of(level, p, q, core), 1).wait_send())
    for chip in range(CHIPS):
        desc(chip * TWO + core, HEIGHT).wait_send()


def add_into(dst, srcs, rows):
    step = 32

    def body(i, carry):
        sl = pl.ds(pl.multiple_of(i * step, step), step)
        total = srcs[0][sl, :].astype(F32)
        for src in srcs[1:]:
            total = total + src[sl, :].astype(F32)
        dst[sl, :] = total.astype(dst.dtype)
        return carry

    lax.fori_loop(0, rows // step, body, 0)


def scatter_scratch(rows, cols):
    return [
        pltpu.VMEM((CHIPS, rows, cols), BF16), pltpu.VMEM((LEVEL, rows, cols), BF16), pltpu.VMEM((HEIGHT, rows, cols), BF16),
        pltpu.VMEM((HEIGHT, rows, cols), BF16), pltpu.VMEM((HEIGHT, rows, cols), BF16), pltpu.VMEM((CHIPS, rows, cols), BF16),
        pltpu.VMEM((rows, cols), F32),
        pltpu.SemaphoreType.DMA((TWO, CHIPS)), pltpu.SemaphoreType.DMA((TWO, LEVEL)), pltpu.SemaphoreType.DMA((TWO, HEIGHT)),
        pltpu.SemaphoreType.DMA((TWO, HEIGHT)), pltpu.SemaphoreType.DMA((TWO, HEIGHT)),
    ]


def scatter_levels(in_ref, out_ref, scratch, place, work, hook=None):
    from_core, from_q, from_p, from_low, from_high, outgo, acc, sem_c, sem_q, sem_p, sem_up, sem_dn = scratch
    me, z, p, q, core = place
    rows = out_ref.shape[0]
    other = 1 - core

    def core_copy(chip):
        return remote(in_ref.at[chip * TWO + other], from_core.at[chip], sem_c, chip, me + 1 - TWO * core)

    def local(level, mid, last):
        return level * HEIGHT + mid * TWO + last

    def q_copy(level, mid):
        return remote(outgo.at[local(level, mid, 1 - q)], from_q.at[level * TWO + mid], sem_q, level * TWO + mid,
                      device_of(z, p, 1 - q, core))

    def p_copy(level):
        return remote(outgo.at[local(level, 1 - p, q)], from_p.at[level], sem_p, level, device_of(z, 1 - p, q, core))

    def up_copy(level):
        return remote(outgo.at[local(level, p, q)], from_low.at[level], sem_up, level, me + LEVEL)

    def dn_copy(level):
        return remote(outgo.at[local(level, p, q)], from_high.at[level], sem_dn, level, me - LEVEL)

    def own(level, mid, last):
        chip = chip_of(level, mid, last, core)
        core_copy(chip).wait_recv()
        return [in_ref.at[chip * TWO + core], from_core.at[chip]]

    y = q * (1 - core) + p * core
    x = p * (1 - core) + q * core

    def make(level, half):
        row = level * HEIGHT + TWO * (y * half + (1 - y) * (1 - half))
        work(row * TWO)
        for side in (1 - x, x):
            core_copy(row + side).start()

    def send_q(level, mid):
        add_into(outgo.at[local(level, mid, 1 - q)], own(level, mid, 1 - q), rows)
        q_copy(level, mid).start()

    def send_p(level):
        side = own(level, 1 - p, q)
        q_copy(level, 1 - p).wait_recv()
        add_into(outgo.at[local(level, 1 - p, q)], side + [from_q.at[level * TWO + 1 - p]], rows)
        p_copy(level).start()

    def gather_here(level):
        mine = own(level, p, q)
        q_copy(level, p).wait_recv()
        p_copy(level).wait_recv()
        return mine + [from_q.at[level * TWO + p], from_p.at[level]]

    def send_z(level):
        add_into(acc, gather_here(level), rows)

        @pl.when(level > z)
        def _():
            @pl.when(z > 0)
            def _():
                up_copy(level).wait_recv()
                add_into(acc, [acc, from_low.at[level]], rows)
            add_into(outgo.at[local(level, p, q)], [acc], rows)
            up_copy(level).start()

        @pl.when(level < z)
        def _():
            @pl.when(z < TOP)
            def _():
                dn_copy(level).wait_recv()
                add_into(acc, [acc, from_high.at[level]], rows)
            add_into(outgo.at[local(level, p, q)], [acc], rows)
            dn_copy(level).start()

    def level_at(t):
        return far_level(z, lax.rem(lax.div(t, TWO), HEIGHT))

    def step(t, carry):
        odd = lax.rem(t, TWO)
        if hook is not None:
            hook(t)
        pl.when(t < LEVEL)(lambda: make(level_at(t), odd))
        pl.when(jnp.logical_and(t > 0, t < 9))(lambda: send_q(level_at(t + 7), odd * (1 - p) + (1 - odd) * p))
        pl.when(jnp.logical_and(t == 9, inner))(lambda: send_z(far_level(z, 1)))
        pl.when(jnp.logical_and(t > TWO, odd == 1))(lambda: send_p(level_at(t + 5)))
        pl.when(jnp.logical_and(jnp.logical_and(t > HEIGHT, odd == 1), outer))(lambda: send_z(level_at(t + TOP)))
        pl.when(jnp.logical_and(jnp.logical_and(t > 6, odd == 1), inner))(lambda: send_z(far_level(z, TWO * lax.div(t, 9))))
        return carry

    outer = jnp.logical_or(z == 0, z == TOP)
    inner = jnp.logical_not(outer)
    lax.fori_loop(0, 10, step, 0)
    add_into(out_ref, gather_here(z), rows)

    @pl.when(z > 0)
    def _():
        up_copy(z).wait_recv()
        add_into(out_ref, [out_ref, from_low.at[z]], rows)

    @pl.when(z < TOP)
    def _():
        dn_copy(z).wait_recv()
        add_into(out_ref, [out_ref, from_high.at[z]], rows)

    for chip in range(CHIPS):
        core_copy(chip).wait_send()
    for level in range(HEIGHT):
        for mid in range(TWO):
            q_copy(level, mid).wait_send()
        p_copy(level).wait_send()
        pl.when(level > z)(lambda: up_copy(level).wait_send())
        pl.when(level < z)(lambda: dn_copy(level).wait_send())


def rank_of(p, q, core):
    return device_of(0, p, q, core)


def level_gather(in_ref, out_ref, send_sem, recv_sem, place):
    me, z, p, q, core = place
    rank = lax.rem(me, LEVEL)
    peers = (device_of(z, 1 - p, q, core), device_of(z, p, 1 - q, core), me + 1 - TWO * core)

    def desc(block, way, src=None):
        return pltpu.make_async_remote_copy(
            src_ref=out_ref.at[block] if src is None else src, dst_ref=out_ref.at[block],
            send_sem=send_sem.at[(0, 1 if src is not None else TWO, TOP + lax.div(block, TWO))[way]], recv_sem=recv_sem.at[block],
            device_id=(peers[way],), device_id_type=MESH)

    for way in (1, 0, TWO):
        desc(rank, way, in_ref).start()
    out_ref[rank] = in_ref[...]
    side = rank_of(1 - p, q, core)
    desc(side, 0).wait_recv()
    for way in (1, TWO):
        desc(side, way).start()
    for mid in (p, 1 - p):
        block = rank_of(mid, 1 - q, core)
        desc(block, 1).wait_recv()
        desc(block, TWO).start()
    for chip in range(HEIGHT):
        desc(chip * TWO + 1 - core, TWO).wait_recv()
    desc(rank, 0, in_ref).wait_send()
    desc(rank, 1, in_ref).wait_send()
    desc(side, 1).wait_send()
    for chip in range(HEIGHT):
        desc(chip * TWO + core, TWO).wait_send()


def level_scatter(in_ref, out_ref, from_core, from_q, from_p, outgo, sem_s, sem_r, place, hook=None):
    me, z, p, q, core = place
    rows = out_ref.shape[0]

    def copy(src, dst, slot, dev):
        return pltpu.make_async_remote_copy(
            src_ref=src, dst_ref=dst, send_sem=sem_s.at[slot], recv_sem=sem_r.at[slot],
            device_id=(dev,), device_id_type=MESH)

    def core_copy(chip):
        return copy(in_ref.at[chip * TWO + 1 - core], from_core.at[chip], chip, me + 1 - TWO * core)

    def q_copy(mid):
        return copy(outgo.at[mid], from_q.at[mid], HEIGHT + mid, device_of(z, p, 1 - q, core))

    def p_copy():
        return copy(outgo.at[TWO], from_p, 6, device_of(z, 1 - p, q, core))

    def own(mid, last):
        chip = chip_of(0, mid, last, core)
        core_copy(chip).wait_recv()
        return [in_ref.at[chip * TWO + core], from_core.at[chip]]

    for last in (1 - p, p):
        for mid in (1 - q, q):
            core_copy(chip_of(0, mid, last, 1 - core)).start()
    for mid in (1 - p, p):
        add_into(outgo.at[mid], own(mid, 1 - q), rows)
        q_copy(mid).start()
    if hook is not None:
        hook()
    side = own(1 - p, q)
    q_copy(1 - p).wait_recv()
    add_into(outgo.at[TWO], side + [from_q.at[1 - p]], rows)
    p_copy().start()
    mine = own(p, q)
    q_copy(p).wait_recv()
    p_copy().wait_recv()
    add_into(out_ref, mine + [from_q.at[p], from_p], rows)
    for chip in range(HEIGHT):
        core_copy(chip).wait_send()
    for mid in range(TWO):
        q_copy(mid).wait_send()
    p_copy().wait_send()


def dot(left, right, ld, rd):
    return lax.dot_general(left, right, (((ld,), (rd,)), ((), ())), preferred_element_type=F32)


TOKS = 512
VPAD = 1024
VROWS = 1004


def id_rows(tok_ref, row, first):
    ids = jnp.concatenate([tok_ref[first + t, row:row + 1, :] for t in range(HEIGHT)], axis=1) - shard_start()
    return jnp.where(jnp.logical_and(ids >= 0, ids < VROWS), ids, -1)


def vocab_iota():
    return lax.broadcasted_iota(jnp.int32, (VPAD, TOKS), 0)


def shard_start():
    return lax.axis_index('fsdp') * VROWS


def fill_table(table, emb_ref):
    table[VPAD - 32:VPAD, :] = jnp.zeros((32, DIM), BF16)
    table[0:VROWS, :] = emb_ref[...]


def rms_inv(values):
    return lax.rsqrt(jnp.mean(values * values, axis=-1, keepdims=True) + NORM_EPS)


def rms_backward(values, inv_rms, gain_vec, grad_out):
    scaled = grad_out * gain_vec
    return inv_rms * scaled - values * (inv_rms ** TOP) * jnp.mean(scaled * values, axis=-1, keepdims=True)


LEVEL_SCRATCH = [
    pltpu.VMEM((LANE, DIM), BF16), pltpu.VMEM((LEVEL, LANE, DIM), BF16), pltpu.VMEM((LANE, DIM), F32),
    pltpu.VMEM((HEIGHT, LANE, DIM), BF16), pltpu.VMEM((TWO, LANE, DIM), BF16), pltpu.VMEM((LANE, DIM), BF16),
    pltpu.VMEM((TOP, LANE, DIM), BF16),
    pltpu.SemaphoreType.DMA((7,)), pltpu.SemaphoreType.DMA((LEVEL,)),
    pltpu.SemaphoreType.DMA((7,)), pltpu.SemaphoreType.DMA((7,)),
]


def split_weights(gu_ref):
    wide = gu_ref[...].astype(F32)
    return (wide[:, 0:GROWS, :].reshape(DIM, UNITS).astype(BF16), wide[:, GROWS:PAIR, :].reshape(DIM, UNITS).astype(BF16))


GU_SHAPE = (NDEV, PAIR, UNITS)
WD_SHAPE = (HEIGHT, DROWS, DIM)


def call(kernel, name, cid, outs, ins, scratch):
    return pl.pallas_call(
        kernel, out_shape=outs, in_specs=[VSPEC if i != TWO else HSPEC for i in range(len(ins))],
        out_specs=(HSPEC,) * (len(outs) - 1) + (pl.BlockSpec(memory_space=pltpu.SMEM),),
        scratch_shapes=scratch,
        compiler_params=pltpu.CompilerParams(collective_id=cid, has_side_effects=True, vmem_limit_bytes=VMEM_CAP),
        name=name)(*ins)


STAT = 40


def merge_stats(blocks):
    logs = [b[0:32, :] for b in blocks]
    top = logs[0]
    for one in logs[1:]:
        top = jnp.maximum(top, one)
    total = jnp.exp(logs[0] - top)
    labs = blocks[0][32:STAT, :]
    for one, b in zip(logs[1:], blocks[1:]):
        total = total + jnp.exp(one - top)
        labs = labs + b[32:STAT, :]
    return jnp.concatenate([top + jnp.log(total), labs], axis=0)


def step_call(ids, labs, emb, gate, up, down_shard, gain_mlp, gain_final, emb_scale, inv_count):
    def kernel(ids_ref, lab_ref, emb_ref, gate_ref, up_ref, down_ref, gm_ref, gf_ref,
               demb_out, dgate_out, dup_out, dn_out, loss_ref,
               demb_ref, dgate_ref, dup_ref, dn_ref, emb_in, sem_o, piece_ref, own_ref, tok_mine, tok_ref, table, spread, whole, gu_ref, wd_ref, a_ref, g_ref, u_ref, dm_ref,
               d_gate, d_up, acts, grad_gate, grad_up, grad_down, ggu, gd, land_g, land_d, outgo, outgo_d, acc,
               block, x_ref, h_ref, dh_ref, dhn_ref, stat, land, land_z, lse_ref,
               sem_t, sem_a, g_send, g_recv, sem_z, sem_d,
               *scratch):
        ring, (mine, parts, total, *level) = scratch[:12], scratch[12:]
        place = my_place()
        me, z, p, q, core = place
        rank = lax.rem(me, LEVEL)
        gain_m, gain_f = gm_ref[...].reshape(1, DIM), gf_ref[...].reshape(1, DIM)
        table_in = pltpu.make_async_copy(emb_ref, emb_in, sem_o.at[11])
        table_in.start()
        tok_mine[...] = jnp.zeros((LEVEL, LANE), jnp.int32)
        tok_mine[0:1, :] = ids_ref[...]
        tok_mine[1:TWO, :] = lab_ref[...]
        both = jnp.concatenate([gate_ref[...].astype(F32), up_ref[...].astype(F32)], axis=0).astype(BF16)
        for r in range(LEVEL):
            piece_ref[r] = jnp.concatenate([both[:, DROWS * (LEVEL * k + r):DROWS * (LEVEL * k + r + 1)] for k in range(HEIGHT)], axis=1)
        barrier_peers(place)

        def exchange(step):
            peer = lax.rem(rank + step, LEVEL)
            return remote(piece_ref.at[peer], gu_ref.at[me], sem_a, step, z * LEVEL + peer)

        def rows_of(ref, lv):
            return ref.at[pl.ds(lv * LEVEL, LEVEL)]

        def slab(lv, way):
            part = rows_of(gu_ref, lv)
            return pltpu.make_async_remote_copy(
                src_ref=part, dst_ref=part, send_sem=sem_z.at[0, way * HEIGHT + lv], recv_sem=sem_z.at[1, lv],
                device_id=(me + LEVEL - CHIPS * way,), device_id_type=MESH)

        def slab_down(lv, way, src):
            return pltpu.make_async_remote_copy(
                src_ref=src, dst_ref=wd_ref.at[lv], send_sem=sem_d.at[0, way * HEIGHT + lv], recv_sem=sem_d.at[1, lv],
                device_id=(me + LEVEL - CHIPS * way,), device_id_type=MESH)

        def tell(step):
            return remote(tok_mine, tok_ref.at[me], sem_t, step, z * LEVEL + lax.rem(rank + step, LEVEL))

        def along_z(src, dst, sems, step):
            return remote(src, dst, sems, 7 + step, lax.rem(me + LEVEL * step, NDEV))

        for step in range(1, LEVEL):
            tell(step).start()
        tok_ref[me] = tok_mine[...]
        wd_ref[z] = down_ref[...]
        gu_ref[me] = piece_ref[rank]
        table_in.wait()
        fill_table(table, emb_in)
        stat[...] = jnp.zeros_like(stat)
        demb_ref[...] = jnp.zeros_like(demb_ref)
        for step in range(1, LEVEL):
            tell(step).wait()
        part = rows_of(tok_ref, z)
        for step in range(1, HEIGHT):
            along_z(part, part, sem_t, step).start()
        for step in range(1, LEVEL):
            exchange(step).start()
        pl.when(z < TOP)(lambda: slab_down(z, 0, down_ref).start())
        pl.when(z > 0)(lambda: slab_down(z, 1, down_ref).start())
        for step in range(1, HEIGHT):
            along_z(part, part, sem_t, step).wait()
        for step in range(1, LEVEL):
            exchange(step).wait_recv()
        pl.when(z < TOP)(lambda: slab(z, 0).start())
        pl.when(z > 0)(lambda: slab(z, 1).start())

        def take(lv, way, more):
            slab_down(lv, 0, wd_ref.at[lv]).wait_recv()
            pl.when(more)(lambda: slab_down(lv, way, wd_ref.at[lv]).start())
            slab(lv, 0).wait_recv()
            pl.when(more)(lambda: slab(lv, way).start())

        def take_far(far):
            pl.when(z - far >= 0)(lambda: take(z - far, 0, z < TOP))
            pl.when(z + far < HEIGHT)(lambda: take(z + far, 1, z > 0))

        def hit_rows(first):
            return (vocab_iota() == id_rows(tok_ref, 0, first)).astype(F32).astype(BF16)

        def find(first):
            spread[pl.ds(first, HEIGHT)] = dot(hit_rows(first), table[...], 0, 0).astype(BF16).reshape(HEIGHT, LANE, DIM)

        scatter_levels(spread, x_ref, ring, place, find, lambda t: pl.when(t == 6)(lambda: take_far(1)))
        take_far(TWO)
        x = x_ref[...] * emb_scale
        mine[...] = (x * rms_inv(x) * gain_m).astype(BF16)
        level_gather(mine, a_ref, level[HEIGHT], level[5], place)
        take_far(TOP)
        for half in range(TWO):
            four = slice(HEIGHT * half, HEIGHT * half + HEIGHT)
            wg, wu = split_weights(gu_ref)
            act_in = a_ref[four].reshape(TOKS, DIM)
            g = dot(act_in, wg, 1, 0).astype(BF16)
            u = dot(act_in, wu, 1, 0).astype(BF16)
            g_ref[half] = g
            u_ref[half] = u
            act = (jax.nn.silu(g.astype(F32)) * u.astype(F32)).astype(BF16)
            acts[half] = act
            parts[four] = dot(act, wd_ref[...].reshape(UNITS, DIM), 1, 0).astype(BF16).reshape(HEIGHT, LANE, DIM)
        level_scatter(parts, total, *level[:HEIGHT], *level[6:], place)
        h_ref[...] = (x_ref[...] * emb_scale + total[...].astype(BF16).astype(F32)).astype(BF16)
        h32 = h_ref[...].astype(F32)
        block[...] = (h32 * rms_inv(h32) * gain_f).astype(BF16)
        for step in range(1, LEVEL):
            exchange(step).wait_send()

        def sent(lv, way):
            slab(lv, way).wait_send()
            slab_down(lv, way, wd_ref.at[lv]).wait_send()

        def forward(first):
            logits = dot(table[...], whole[pl.ds(first, HEIGHT)].reshape(TOKS, DIM), 1, 1)
            row = vocab_iota()
            lab = jnp.sum(jnp.where(row == id_rows(tok_ref, 1, first), logits, 0.0), axis=0, keepdims=True)
            logits = jnp.where(row < VROWS, logits, -1e30)
            top = jnp.max(logits, axis=0, keepdims=True)
            local = top + jnp.log(jnp.sum(jnp.exp(logits - top), axis=0, keepdims=True))
            for t in range(HEIGHT):
                stat[0, pl.ds(first + t, 1), :] = local[:, t * LANE:(t + 1) * LANE]
                stat[0, 32:33, :] = stat[0, 32:33, :] + lab[:, t * LANE:(t + 1) * LANE]

        gather_levels(block, whole, g_send, g_recv, place, forward)
        for lv in range(HEIGHT):
            pl.when(jnp.logical_and(z < TOP, lv <= z))(lambda: sent(lv, 0))
            pl.when(jnp.logical_and(z > 0, lv >= z))(lambda: sent(lv, 1))

        def share(step):
            return remote(stat.at[0], land.at[rank], sem_t, step, z * LEVEL + lax.rem(rank + step, LEVEL))

        for step in range(1, LEVEL):
            share(step).start()
        land[rank] = stat[0]
        for step in range(1, LEVEL):
            share(step).wait()
        stat[1] = merge_stats([land[r] for r in range(LEVEL)])
        for step in range(1, HEIGHT):
            along_z(stat.at[1], land_z.at[z], sem_t, step).start()
        land_z[z] = stat[1]
        for step in range(1, HEIGHT):
            along_z(stat.at[1], land_z.at[z], sem_t, step).wait()
        final = merge_stats([land_z[lv] for lv in range(HEIGHT)])
        lse_ref[...] = final[0:32, :]
        loss_ref[0, 0] = (jnp.sum(final[0:32, :]) - jnp.sum(final[32:STAT, :])) * inv_count

        def backward(first):
            hid = whole[pl.ds(first, HEIGHT)].reshape(TOKS, DIM)
            logits = dot(table[...], hid, 1, 1)
            lse_row = jnp.concatenate([lse_ref[pl.ds(first + t, 1), :] for t in range(HEIGHT)], axis=1)
            row = vocab_iota()
            prob = jnp.exp(jnp.where(row < VROWS, logits, -1e30) - lse_row)
            hit = jnp.where(row == id_rows(tok_ref, 1, first), 1.0, 0.0)
            grad = ((prob - hit) * inv_count).astype(BF16)
            spread[pl.ds(first, HEIGHT)] = dot(grad, table[...], 0, 0).astype(BF16).reshape(HEIGHT, LANE, DIM)
            demb_ref[...] += dot(grad, hid, 1, 0)

        scatter_levels(spread, dhn_ref, ring, place, backward)

        h32 = h_ref[...].astype(F32)
        dh_ref[...] = rms_backward(h32, rms_inv(h32), gain_f, dhn_ref[...])
        mine[...] = dh_ref[...].astype(BF16)
        level_gather(mine, dm_ref, level[HEIGHT], level[5], place)
        for half in range(TWO):
            four = slice(HEIGHT * half, HEIGHT * half + HEIGHT)
            wg, wu = split_weights(gu_ref)
            g = g_ref[half].astype(F32)
            u = u_ref[half].astype(F32)
            dq = dot(dm_ref[four].reshape(TOKS, DIM), wd_ref[...].reshape(UNITS, DIM), 1, 1)
            sig = jax.nn.sigmoid(g)
            dg = (dq * u * sig * (1.0 + g * (1.0 - sig))).astype(BF16)
            du = (dq * g * sig).astype(BF16)
            d_gate[half] = dg
            d_up[half] = du
            parts[four] = (dot(dg, wg, 1, 1) + dot(du, wu, 1, 1)).astype(BF16).reshape(HEIGHT, LANE, DIM)
        def add_slab(dst, srcs):
            def body(i, carry):
                value = srcs[0][i].astype(F32)
                for src in srcs[1:]:
                    value = value + src[i].astype(F32)
                dst[i] = value.astype(dst.dtype)
                return carry
            lax.fori_loop(0, LEVEL, body, 0)

        def hop(lv, way, here=False):
            land = rows_of(land_g, HEIGHT if here and way else lv)
            return remote(rows_of(outgo, lv), land, sem_z, way * HEIGHT + lv, me + LEVEL - CHIPS * way)

        def hop_d(lv, way, here=False):
            return remote(outgo_d.at[lv], land_d.at[HEIGHT if here and way else lv], sem_d, way * HEIGHT + lv, me + LEVEL - CHIPS * way)

        def send(lv, way, more, here):
            @pl.when(more)
            def _():
                hop(lv, way).wait_recv()
                add_slab(rows_of(outgo, lv), [rows_of(ggu, lv), rows_of(land_g, lv)])
                hop_d(lv, way).wait_recv()
                add_into(outgo_d.at[lv], [gd.at[lv], land_d.at[lv]], DROWS)

            @pl.when(jnp.logical_not(more))
            def _():
                add_slab(rows_of(outgo, lv), [rows_of(ggu, lv)])
                add_into(outgo_d.at[lv], [gd.at[lv]], DROWS)
            hop(lv, way, here).start()
            hop_d(lv, way, here).start()

        def send_far(far):
            pl.when(z + far < HEIGHT)(lambda: send(z + far, 0, z > 0, far == 1))
            pl.when(z - far >= 0)(lambda: send(z - far, 1, z < TOP, far == 1))

        def weight_grads():
            for half in range(TWO):
                four = slice(HEIGHT * half, HEIGHT * half + HEIGHT)
                act_in = a_ref[four].reshape(TOKS, DIM)
                news = (dot(act_in, d_gate[half], 0, 0), dot(act_in, d_up[half], 0, 0),
                        dot(acts[half], dm_ref[four].reshape(TOKS, DIM), 0, 0))
                for ref, new in zip((grad_gate, grad_up, grad_down), news):
                    ref[...] = new if half == 0 else ref[...] + new
            both = jnp.concatenate([grad_gate[...].reshape(NDEV, GROWS, UNITS), grad_up[...].reshape(NDEV, GROWS, UNITS)], axis=1)
            ggu[...] = both.astype(BF16)
            gd[...] = grad_down[...].astype(BF16).reshape(WD_SHAPE)

        def grads_off():
            weight_grads()
            send_far(TOP)
            demb_ref[...] = demb_ref[...] * (1.0 / emb_scale)

        level_scatter(parts, total, *level[:HEIGHT], *level[6:], place, grads_off)
        x = x_ref[...] * emb_scale
        block[...] = (dh_ref[...] + rms_backward(x, rms_inv(x), gain_m, total[...])).astype(BF16)


        def add_rows(first):
            demb_ref[...] += dot(hit_rows(first), whole[pl.ds(first, HEIGHT)].reshape(TOKS, DIM), 1, 0)

        def last(way):
            hop(z, way).wait_recv()
            add_slab(acc, [acc, rows_of(land_g, HEIGHT if way else z)])
            hop_d(z, way).wait_recv()
            add_into(dn_ref, [dn_ref, land_d.at[HEIGHT if way else z]], DROWS)

        def give(step):
            peer = lax.rem(rank + step, LEVEL)
            return remote(acc.at[peer], own_ref.at[rank], sem_a, step, z * LEVEL + peer)

        def grads_home():
            add_slab(acc, [rows_of(ggu, z)])
            add_into(dn_ref, [gd.at[z]], DROWS)
            pl.when(z > 0)(lambda: last(0))
            pl.when(z < TOP)(lambda: last(1))
            for step in range(1, LEVEL):
                give(step).start()
            own_ref[rank] = acc[rank]

        def grads_step(t):
            pl.when(t == HEIGHT)(grads_home)

        def grads_late(t):
            pl.when(t == 0)(lambda: send_far(TWO))
            pl.when(t == TWO)(lambda: send_far(1))

        gather_levels(block, whole, g_send, g_recv, place, add_rows, grads_step, grads_late)
        outs = []
        for k in range(LEVEL):
            part = pl.ds(k * LANE, LANE)
            outs.append(pltpu.make_async_copy(demb_ref.at[part], demb_out.at[part], sem_o.at[k]))
        outs.append(pltpu.make_async_copy(dn_ref, dn_out, sem_o.at[LEVEL]))
        for out in outs:
            out.start()
        for step in range(1, LEVEL):
            give(step).wait_recv()
        for step in range(1, LEVEL):
            give(step).wait_send()
        def assemble():
            for k in range(HEIGHT):
                got = jnp.concatenate([own_ref[r, :, DROWS * k:DROWS * (k + 1)] for r in range(LEVEL)], axis=1)
                dgate_ref[:, DIM * k:DIM * (k + 1)] = got[0:GROWS]
                dup_ref[:, DIM * k:DIM * (k + 1)] = got[GROWS:PAIR]

        assemble()
        def gone(lv, way):
            hop(lv, way).wait_send()
            hop_d(lv, way).wait_send()

        for lv in range(HEIGHT):
            pl.when(lv > z)(lambda: gone(lv, 0))
            pl.when(lv < z)(lambda: gone(lv, 1))
        for k, (ref, out) in enumerate(((dgate_ref, dgate_out), (dup_ref, dup_out))):
            outs.append(pltpu.make_async_copy(ref, out, sem_o.at[9 + k]))
            outs[-1].start()
        for out in outs:
            out.wait()

    whole = pltpu.VMEM((NDEV, LANE, DIM), BF16)
    block, flat = pltpu.VMEM((LANE, DIM), BF16), pltpu.VMEM((LANE, DIM), F32)
    slab, slab_d = pltpu.VMEM(GU_SHAPE, BF16), pltpu.VMEM(WD_SHAPE, BF16)
    unit, eight = pltpu.VMEM((TWO, TOKS, UNITS), BF16), pltpu.VMEM((LEVEL, LANE, DIM), BF16)
    wide, tall = pltpu.VMEM((DIM, UNITS), F32), pltpu.VMEM((UNITS, DIM), F32)
    dma = pltpu.SemaphoreType.DMA
    return call(
        kernel, 'step', 0,
        (jax.ShapeDtypeStruct((VPAD, DIM), F32), jax.ShapeDtypeStruct((GROWS, 3072), F32), jax.ShapeDtypeStruct((GROWS, 3072), F32),
         jax.ShapeDtypeStruct((DROWS, DIM), F32), jax.ShapeDtypeStruct((1, 1), F32)),
        (ids, labs, emb, gate, up, down_shard, gain_mlp, gain_final),
        [pltpu.VMEM((VPAD, DIM), F32), pltpu.VMEM((GROWS, 3072), F32), pltpu.VMEM((GROWS, 3072), F32), pltpu.VMEM((DROWS, DIM), F32),
         pltpu.VMEM((VROWS, DIM), BF16), dma((12,)),
         pltpu.VMEM((LEVEL, PAIR, UNITS), BF16), pltpu.VMEM((LEVEL, PAIR, UNITS), F32), pltpu.VMEM((LEVEL, LANE), jnp.int32), pltpu.VMEM((NDEV, LEVEL, LANE), jnp.int32), pltpu.VMEM((VPAD, DIM), BF16), whole, whole,
         slab, slab_d, eight, unit, unit, eight, unit, unit, unit, wide, wide, tall, slab, slab_d,
         pltpu.VMEM((5 * LEVEL, PAIR, UNITS), BF16), pltpu.VMEM((5, DROWS, DIM), BF16), slab, slab_d,
         pltpu.VMEM((LEVEL, PAIR, UNITS), F32), block, flat, block, flat, flat,
         pltpu.VMEM((TWO, STAT, LANE), F32), pltpu.VMEM((LEVEL, STAT, LANE), F32), pltpu.VMEM((HEIGHT, STAT, LANE), F32),
         pltpu.VMEM((32, LANE), F32),
         sem_pair(11), sem_pair(LEVEL), dma((36,)), dma((NDEV,)), sem_pair(LEVEL), sem_pair(LEVEL)]
        + scatter_scratch(LANE, DIM) + LEVEL_SCRATCH)


def solution(mesh):
    group = mesh.shape['fsdp']

    def local_step(ids_blk, lab_blk, emb_shard, gate_shard, up_shard, down_shard, gain_mlp, gain_final):
        emb_scale = math.sqrt(emb_shard.shape[1])
        inv_count = 1.0 / (ids_blk.size * group)
        d_embed, d_gate, d_up, d_down, loss = step_call(
            ids_blk, lab_blk, emb_shard, gate_shard, up_shard, down_shard, gain_mlp, gain_final, emb_scale, inv_count)
        return loss[0, 0], d_embed[0:VROWS] * emb_scale, d_gate, d_up, d_down

    shard_spec = P('fsdp', None)
    return jax.shard_map(local_step, mesh=mesh, in_specs=(shard_spec, shard_spec, shard_spec, shard_spec, shard_spec, shard_spec, P(), P()), out_specs=(P(), shard_spec, shard_spec, shard_spec, shard_spec), check_vma=False)
```
